32 devices in a mesh: rep: 2 (over y), grp: 16 (over z, x, core).
Axes of the slice: x: 2, y: 2, z: 4, core: 2. Of those that a mesh axis runs over, the one named last changes fastest.
Arguments:
- hidden: bfloat16 [2, 3072, 2048], P('rep', 'grp'), may hold values from -6 to 6
- grad_out: bfloat16 [2, 3072, 2048], P('rep', 'grp'), may hold values from -6 to 6
- expert_ids: int32 [2, 3072, 6], P('rep', 'grp'), may hold values from 0 to 15, all different within a row; in each aligned block of 192 rows (0 to 191, 192 to 383, ..., all dimensions but the last counted through in order) at most 90 rows name the same one
- prefix_len: int32 [2], P('rep'), may hold values from 1 to 1536
- adapter_id: int32 [2], P('rep'), may hold values from 0 to 7
- attn_gain: float32 [2048], replicated, may hold values from 0.1 to 1.9
- kv_gain: float32 [512], replicated, may hold values from 0.1 to 1.9
- ffn_gain: float32 [2048], replicated, may hold values from 0.1 to 1.9
- w_q: bfloat16 [2048, 3072], P('grp'), may hold values from -0.125 to 0.125
- w_kva: bfloat16 [2048, 576], P('grp'), may hold values from -0.125 to 0.125
- w_kvb: bfloat16 [512, 4096], P('grp'), may hold values from -0.25 to 0.25
- w_o: bfloat16 [2048, 2048], P('grp'), may hold values from -1 to 1
- w_router: bfloat16 [2048, 16], P('grp'), may hold values from -0.125 to 0.125
- shared_gate: bfloat16 [2048, 2816], P('grp'), may hold values from -0.125 to 0.125
- shared_up: bfloat16 [2048, 2816], P('grp'), may hold values from -0.125 to 0.125
- shared_down: bfloat16 [2816, 2048], P('grp'), may hold values from -0.109375 to 0.109375
- expert_gate: bfloat16 [16, 2048, 1408], P('grp'), may hold values from -0.125 to 0.125
- expert_up_weight: bfloat16 [16, 2048, 1408], P('grp'), may hold values from -0.125 to 0.125
- expert_down: bfloat16 [16, 1408, 2048], P('grp'), may hold values from -0.625 to 0.625
- q_down: bfloat16 [8, 2048, 16], replicated, may hold values from -0.125 to 0.125
- q_up: bfloat16 [8, 16, 3072], replicated, may hold values from -0.59765625 to 0.59765625
- o_down: bfloat16 [8, 2048, 16], replicated, may hold values from -1 to 1
- o_up: bfloat16 [8, 16, 2048], replicated, may hold values from -0.59765625 to 0.59765625
Outputs:
- output: bfloat16 [2, 3072, 2048], P('rep', 'grp')
- grad_hidden: bfloat16 [2, 3072, 2048], P('rep', 'grp')
- grad_q_down: float32 [8, 2048, 16], P(None, 'grp')
- grad_q_up: float32 [8, 16, 3072], P(None, None, 'grp')
- grad_o_down: float32 [8, 2048, 16], P(None, 'grp')
- grad_o_up: float32 [8, 16, 2048], P(None, None, 'grp')
The draws below stay inside these ranges and needn't reach their ends.
Inputs may be any that keep to these rules, and one draw needn't show every extreme that they name: `expert_ids`: each row names 6 different experts; among the rows of one device no expert is named more than 90 times, and that count is reached.
All inputs are finite; a program needn't handle non-finite values.
Results may differ from the reference program's by a relative error of at most 0.024.
Values may be sent and summed in bfloat16 or wider, within the bound.
A program may use at most 384 MiB of HBM per device.

```python
import math
import jax
import jax.numpy as jnp
import numpy as np
from jax import lax

D = 2048
H = 16
NOPE = 128
ROPE = 64
VD = 128
KVR = 512
FE = 1408
TOP = 6
FS = 2816
RANK = 16
ADAPTERS = 8
TOK_DEV = 192
EXPERTS = 16
CAP = 90
LENGTH = 3072
SEQS = 2
N_GRP = 16


def shard_levels(stream_key, extent, split, least, largest):
    gain = 1.0
    for position, blocks in split:
        steps = jax.random.uniform(jax.random.fold_in(jax.random.fold_in(stream_key, 6), position), (blocks,), jnp.float32, least / len(split), largest / len(split))
        gain = gain * jnp.repeat(jnp.exp(steps), extent[position] // blocks).reshape((-1,) + (1,) * (len(extent) - 1 - position))
    return gain


def routed_block(rng, own, number, rows, amount, top, reach, slope):
    order = jax.random.permutation(rng, amount)
    crowded, usual = portions_of(amount, rows * top, reach, slope, True), portions_of(amount, rows * top, reach, slope, False)
    places = jnp.arange(amount)

    def named(lengths, turn):
        used = int((lengths > 0).sum())
        fixed = max(1, used // 4)
        passed = fixed + (places - fixed + turn * (used - fixed)) % max(1, amount - fixed)
        return jnp.zeros((amount,), jnp.int32).at[order[jnp.where(places < fixed, places, passed)]].set(jnp.asarray(lengths, jnp.int32))

    lengths = jnp.where(number % 4 == 0, named(crowded, number // 4), named(usual, number - number // 4 - 1))
    mixed = jax.random.permutation(jax.random.fold_in(own, 3), amount)
    giver, taker = mixed[0:amount // 2 * 2:2], mixed[1:amount // 2 * 2:2]
    room = jnp.minimum(lengths[giver] - 1, reach - lengths[taker]) // 2
    room = jnp.where((giver == order[0]) | (taker == order[0]) | (lengths[taker] == 0), 0, jnp.maximum(room, 0))
    passed = jax.random.randint(jax.random.fold_in(own, 4), (amount // 2,), 0, 1 << 20) % (room + 1)
    lengths = lengths.at[giver].add(-passed).at[taker].add(passed)
    members = jnp.searchsorted(jnp.cumsum(lengths), jnp.arange(rows * top), side="right").astype(jnp.int32)
    listing = members.reshape(top, rows).T
    listing = listing[jax.random.permutation(jax.random.fold_in(own, 1), rows)]
    turn = jax.random.randint(jax.random.fold_in(own, 2), (rows, 1), 0, top)
    return jnp.take_along_axis(listing, (jnp.arange(top)[None, :] + turn) % top, axis=1)


def portions_of(number_of, total, limit, slope, full):
    weights = [(1 << 20) // math.isqrt(grade ** slope) + 1 for grade in range(1, number_of + 1)]
    largest = limit if full else min(limit, max(-(-total // number_of), total * weights[0] // sum(weights)))
    least = 1 if total - largest >= number_of - 1 else 0
    holding, surplus = [largest] + [least] * (number_of - 1), total - largest - least * (number_of - 1)
    while surplus > 0:
        free = [i for i in range(1, number_of) if holding[i] < largest] or [i for i in range(1, number_of) if holding[i] < limit]
        mass, budget = sum([weights[i] for i in free]), surplus
        for i in free:
            more = min(limit - holding[i], max(1, budget * weights[i] // mass), surplus)
            holding[i] = holding[i] + more
            surplus = surplus - more
    return np.array(holding)


def gaussian(own_key, shape, spread, bound, cuts=(), kind=jnp.bfloat16):
    entries = jax.random.normal(own_key, shape, jnp.float32) * spread
    if len(cuts) > 0:
        entries = shard_levels(own_key, shape, cuts, -0.22, 0.18) * entries
    return jnp.clip(entries, min=-bound, max=bound).astype(kind)


def setup_inputs(seed: int = 0) -> dict:
    key_list = jax.random.split(jax.random.key(seed), 24)
    hidden = gaussian(key_list[0], (SEQS, LENGTH, D), 1.0, 6.0, ((0, 2), (1, 16)))
    grad_out = gaussian(key_list[1], (SEQS, LENGTH, D), 1.0, 6.0, ((0, 2), (1, 16)))
    expert_ids_keys = jax.random.split(jax.random.fold_in(key_list[2], 1), SEQS * LENGTH // TOK_DEV)
    expert_ids_turns = jax.random.permutation(jax.random.fold_in(key_list[2], 3), SEQS * LENGTH // TOK_DEV)
    expert_ids = jax.vmap(lambda own, number: routed_block(jax.random.fold_in(key_list[2], 2), own, number, TOK_DEV, EXPERTS, TOP, CAP, 2))(expert_ids_keys, expert_ids_turns).reshape((SEQS, LENGTH, TOP))
    prefix_len = jax.random.randint(key_list[3], (SEQS,), 1, LENGTH // 2 + 1).astype(jnp.int32)
    adapter_id = jax.random.randint(key_list[4], (SEQS,), 0, ADAPTERS).astype(jnp.int32)
    attn_gain = jnp.clip(1.0 + 0.18 * jax.random.normal(key_list[5], (D,), jnp.float32), 0.1, 1.9)
    kv_gain = jnp.clip(1.0 + 0.18 * jax.random.normal(key_list[6], (KVR,), jnp.float32), 0.1, 1.9)
    ffn_gain = jnp.clip(1.0 + 0.18 * jax.random.normal(key_list[7], (D,), jnp.float32), 0.1, 1.9)
    w_q = gaussian(key_list[8], (D, H * (NOPE + ROPE)), D ** -0.5, 0.125, ((0, 16),))
    w_kva = gaussian(key_list[9], (D, KVR + ROPE), D ** -0.5, 0.125, ((0, 16),))
    w_kvb = gaussian(key_list[10], (KVR, H * (NOPE + VD)), KVR ** -0.5, 0.25, ((0, 16),))
    w_o = gaussian(key_list[11], (H * VD, D), (max(D // 64, 1)) ** -0.5, 1.0, ((0, 16),))
    w_router = gaussian(key_list[12], (D, EXPERTS), D ** -0.5, 0.125, ((0, 16),))
    shared_gate = gaussian(key_list[13], (D, FS), D ** -0.5, 0.125, ((0, 16),))
    shared_up = gaussian(key_list[14], (D, FS), D ** -0.5, 0.125, ((0, 16),))
    shared_down = gaussian(key_list[15], (FS, D), FS ** -0.5, 0.109375, ((0, 16),))
    expert_gate = gaussian(key_list[16], (EXPERTS, D, FE), D ** -0.5, 0.125, ((0, 16),))
    expert_up_weight = gaussian(key_list[17], (EXPERTS, D, FE), D ** -0.5, 0.125, ((0, 16),))
    expert_down = gaussian(key_list[18], (EXPERTS, FE, D), (max(FE // 16, 1)) ** -0.5, 0.625, ((0, 16),))
    q_down = gaussian(key_list[19], (ADAPTERS, D, RANK), D ** -0.5, 0.125)
    q_up = gaussian(key_list[20], (ADAPTERS, RANK, H * (NOPE + ROPE)), 0.1, 0.59765625)
    o_down = gaussian(key_list[21], (ADAPTERS, H * VD, RANK), (max(H * VD // 64, 1)) ** -0.5, 1.0)
    o_up = gaussian(key_list[22], (ADAPTERS, RANK, D), 0.1, 0.59765625)
    return {"hidden": hidden, "grad_out": grad_out, "expert_ids": expert_ids, "prefix_len": prefix_len, "adapter_id": adapter_id, "attn_gain": attn_gain, "kv_gain": kv_gain, "ffn_gain": ffn_gain, "w_q": w_q, "w_kva": w_kva, "w_kvb": w_kvb, "w_o": w_o, "w_router": w_router, "shared_gate": shared_gate, "shared_up": shared_up, "shared_down": shared_down, "expert_gate": expert_gate, "expert_up_weight": expert_up_weight, "expert_down": expert_down, "q_down": q_down, "q_up": q_up, "o_down": o_down, "o_up": o_up}


@jax.custom_vjp
def low(v):
    return lax.optimization_barrier(v.astype(jnp.bfloat16)).astype(jnp.float32)

@jax.custom_vjp
def low_back(v):
    return v

def low_keep(v):
    return (low(v), None)

def low_pass(kept, grad):
    return (grad,)

def back_keep(v):
    return (v, None)

def back_low(kept, grad):
    return (low(grad),)
low.defvjp(low_keep, low_pass)
low_back.defvjp(back_keep, back_low)
EPS = 1e-06
HIGHEST = lax.Precision.HIGHEST

def round_both(array_value):
    return low(low_back(array_value))

def matmul(former, latter):
    return jnp.dot(former, latter, precision=HIGHEST)

def root_norm(array_value, gains):
    factor = lax.rsqrt(lax.optimization_barrier(jnp.mean(array_value * array_value, axis=-1, keepdims=True)) + EPS)
    return array_value * factor * gains

def angles(positions, width):
    frequency = 10000.0 ** (-jnp.arange(0, width, 2, dtype=jnp.float32) / width)
    phases = positions.astype(jnp.float32)[:, None] * frequency[None, :]
    return (jnp.cos(phases), jnp.sin(phases))

def rotate(array_value, cosine, sine_part):
    midway = array_value.shape[-1] // 2
    leading = array_value[..., :midway]
    trailing = array_value[..., midway:]
    return jnp.concatenate([leading * cosine - trailing * sine_part, trailing * cosine + leading * sine_part], axis=-1)

def attend_head(q_head, r_head, k_head, v_head, k_rope, allowed):
    factor = (NOPE + ROPE) ** (-0.5)
    scores = (matmul(q_head, k_head.T) + matmul(r_head, k_rope.T)) * factor
    scores = jnp.where(allowed, low_back(scores), -1e+30)
    chances = jax.nn.softmax(scores, axis=-1)
    return matmul(low(chances), v_head)

def expert_rows(items):
    rows, gate_w, up_w, down_w = items
    expert_gate_rows = low_back(matmul(rows, gate_w))
    e_up = low_back(matmul(rows, up_w))
    e_hidden = round_both(jax.nn.silu(expert_gate_rows) * e_up)
    return round_both(matmul(e_hidden, down_w))

def slot_tables(routes):
    blocks = routes.reshape(N_GRP, TOK_DEV * TOP)
    onehot = (blocks[:, :, None] == jnp.arange(EXPERTS, dtype=jnp.int32)[None, None, :]).astype(jnp.int32)
    ranks = lax.optimization_barrier(jnp.sum((jnp.cumsum(onehot, axis=1, dtype=jnp.int32) - 1) * onehot, axis=2, dtype=jnp.int32))
    block_index = jnp.arange(N_GRP, dtype=jnp.int32)[:, None]
    target = blocks * (N_GRP * CAP) + block_index * CAP + ranks
    target = target.reshape(LENGTH, TOP).astype(jnp.int32)
    token_index = jnp.broadcast_to(jnp.arange(LENGTH, dtype=jnp.int32)[:, None], (LENGTH, TOP))
    source = jnp.full((EXPERTS * N_GRP * CAP,), LENGTH, jnp.int32).at[target.reshape(-1)].set(token_index.reshape(-1))
    return (target, source)

def layer(inputs, q_down, q_up, o_down, o_up, frozen, routes, prefix, adapter):
    attn_gain, kv_gain, ffn_gain, w_q, w_kva, w_kvb, w_o, w_router, shared_gate, shared_up, shared_down, expert_gate, expert_up_weight, expert_down = frozen
    qa_down = lax.dynamic_index_in_dim(q_down, adapter, 0, keepdims=False)
    qa_up = lax.dynamic_index_in_dim(q_up, adapter, 0, keepdims=False)
    oa_down = lax.dynamic_index_in_dim(o_down, adapter, 0, keepdims=False)
    oa_up = lax.dynamic_index_in_dim(o_up, adapter, 0, keepdims=False)
    cosine, sine_part = angles(jnp.arange(LENGTH, dtype=jnp.int32), ROPE)
    normed = low(root_norm(inputs, attn_gain))
    q_small = round_both(matmul(normed, qa_down))
    query = low_back(matmul(normed, w_q) + matmul(q_small, qa_up)).reshape(LENGTH, H, NOPE + ROPE)
    q_nope = low(query[:, :, :NOPE])
    q_rope = low(rotate(query[:, :, NOPE:], cosine[:, None, :], sine_part[:, None, :]))
    latent = low_back(matmul(normed, w_kva))
    compressed = low(root_norm(latent[:, :KVR], kv_gain))
    k_rope = low(rotate(latent[:, KVR:], cosine, sine_part))
    expanded = matmul(compressed, w_kvb).reshape(LENGTH, H, NOPE + VD)
    k_nope = low(expanded[:, :, :NOPE])
    values = low(expanded[:, :, NOPE:])
    index_rows = jnp.arange(LENGTH, dtype=jnp.int32)
    allowed = (index_rows[None, :] <= index_rows[:, None]) | (index_rows[:, None] < prefix) & (index_rows[None, :] < prefix)
    per_head = lax.map(jax.checkpoint(lambda items: attend_head(items[0], items[1], items[2], items[3], k_rope, allowed)), (q_nope.transpose(1, 0, 2), q_rope.transpose(1, 0, 2), k_nope.transpose(1, 0, 2), values.transpose(1, 0, 2)))
    mixed = round_both(per_head.transpose(1, 0, 2).reshape(LENGTH, H * VD))
    o_small = round_both(matmul(mixed, oa_down))
    middle = inputs + low_back(matmul(mixed, w_o) + matmul(o_small, oa_up))
    ffn_in = low(root_norm(middle, ffn_gain))
    logits = low_back(matmul(ffn_in, w_router))
    route = jax.nn.softmax(logits, axis=-1)
    gate_weight = jnp.take_along_axis(route, routes, axis=1)
    s_gate = low_back(matmul(ffn_in, shared_gate))
    s_up = low_back(matmul(ffn_in, shared_up))
    shared_out = matmul(round_both(jax.nn.silu(s_gate) * s_up), shared_down)
    target, source = slot_tables(routes)
    padded = jnp.concatenate([ffn_in, jnp.zeros((1, D), jnp.float32)], axis=0)
    buffers = low_back(padded[source]).reshape(EXPERTS, N_GRP * CAP, D)
    results = lax.map(jax.checkpoint(expert_rows), (buffers, expert_gate, expert_up_weight, expert_down))
    picked = results.reshape(EXPERTS * N_GRP * CAP, D)[target]
    routed = lax.optimization_barrier(jnp.sum(gate_weight[:, :, None] * picked, axis=1))
    return middle + shared_out + routed

def reference(hidden, grad_out, expert_ids, prefix_len, adapter_id, attn_gain, kv_gain, ffn_gain, w_q, w_kva, w_kvb, w_o, w_router, shared_gate, shared_up, shared_down, expert_gate, expert_up_weight, expert_down, q_down, q_up, o_down, o_up):
    frozen = tuple((array_value.astype(jnp.float32) for array_value in (attn_gain, kv_gain, ffn_gain, w_q, w_kva, w_kvb, w_o, w_router, shared_gate, shared_up, shared_down, expert_gate, expert_up_weight, expert_down)))
    adapters = tuple((array_value.astype(jnp.float32) for array_value in (q_down, q_up, o_down, o_up)))

    def one_sequence(carry, items):
        inputs, cotangent, routes, prefix, adapter = items

        def forward(x_value, qd_value, qu_value, od_value, ou_value):
            return layer(x_value, qd_value, qu_value, od_value, ou_value, frozen, routes, prefix, adapter)
        result, pullback = jax.vjp(forward, inputs.astype(jnp.float32), *adapters)
        gradients = pullback(cotangent.astype(jnp.float32))
        carry = tuple((total + piece for total, piece in zip(carry, gradients[1:])))
        return (carry, (result.astype(jnp.bfloat16), gradients[0].astype(jnp.bfloat16)))
    start = tuple((jnp.zeros(array_value.shape, jnp.float32) for array_value in adapters))
    totals, (output, grad_hidden) = lax.scan(one_sequence, start, (hidden, grad_out, expert_ids, prefix_len, adapter_id))
    return (output, grad_hidden, totals[0], totals[1], totals[2], totals[3])
```

```python
import functools

import jax
import jax.numpy as jnp
from jax import lax
from jax.experimental import pallas as pl
from jax.experimental.pallas import tpu as pltpu
from jax.sharding import PartitionSpec as P

H = 16
NOPE = 128
ROPE = 64
VD = 128
KVR = 512
TOP = 6
QK = NOPE + ROPE
EPS = 1e-06
F32 = jnp.float32
BF16 = jnp.bfloat16


def dot(former, latter):
    return jnp.dot(former, latter, preferred_element_type=F32)


def dot_t(former, latter):
    return lax.dot_general(
        former, latter, (((1,), (1,)), ((), ())), preferred_element_type=F32
    )


def t_dot(former, latter):
    return lax.dot_general(
        former, latter, (((0,), (0,)), ((), ())), preferred_element_type=F32
    )


def root_norm(v, gains):
    factor = lax.rsqrt(jnp.mean(v * v, axis=-1, keepdims=True) + EPS)
    return v * factor * gains


def norm_back(v, gains, gradient):
    factor = lax.rsqrt(jnp.mean(v * v, axis=-1, keepdims=True) + EPS)
    weighted = gradient * gains
    return factor * weighted - v * (factor * factor * factor) * jnp.mean(
        weighted * v, axis=-1, keepdims=True
    )


def gated_slope(v):
    logistic = jax.nn.sigmoid(v)
    return logistic * (1.0 + v * (1.0 - logistic))


def angles(positions, width):
    frequency = 10000.0 ** (-jnp.arange(0, width, 2, dtype=F32) / width)
    phases = positions.astype(F32)[:, None] * frequency[None, :]
    return (jnp.cos(phases), jnp.sin(phases))


def rotate(v, cosine, sine):
    half = v.shape[-1] // 2
    a, b = v[..., :half], v[..., half:]
    return jnp.concatenate([a * cosine - b * sine, b * cosine + a * sine], axis=-1)


def unrotate(v, cosine, sine):
    half = v.shape[-1] // 2
    a, b = v[..., :half], v[..., half:]
    return jnp.concatenate([a * cosine + b * sine, b * cosine - a * sine], axis=-1)


def gather(v, axis=0):
    return lax.all_gather(v, "grp", axis=axis, tiled=True)


def exchange(v):
    return lax.all_to_all(v, "grp", split_axis=0, concat_axis=0, tiled=True)


def scatter_sum(v):
    return lax.psum_scatter(v, "grp", scatter_dimension=0, tiled=True)


def block_of(length):
    return next(b for b in (512, 384, 256, 128) if length % b == 0)


def attend_kernel(prefix_ref, q_ref, k_ref, v_ref, o_ref, lse_ref, *, block, factor):
    i = pl.program_id(0)
    prefix = prefix_ref[0]
    start = i * block
    q = q_ref[...]
    seen = jnp.where(start < prefix, (prefix + block - 1) // block, 0)
    stop = jnp.maximum(i + 1, seen)
    rows = start + lax.broadcasted_iota(jnp.int32, (block, block), 0)

    def step(j, carry):
        top, total, acc = carry
        at = pl.multiple_of(j * block, block)
        k = k_ref[pl.ds(at, block), :]
        v = v_ref[pl.ds(at, block), :]
        s = dot_t(q, k) * factor
        cols = at + lax.broadcasted_iota(jnp.int32, (block, block), 1)
        limit = jnp.where(rows < prefix, jnp.maximum(rows, prefix - 1), rows)
        s = jnp.where(cols <= limit, s, -1e30)
        fresh = jnp.maximum(top, jnp.max(s, axis=1, keepdims=True))
        p = jnp.exp(s - fresh)
        scale = jnp.exp(top - fresh)
        total = total * scale + jnp.sum(p, axis=1, keepdims=True)
        acc = acc * scale + dot(p.astype(BF16), v)
        return fresh, total, acc

    top, total, acc = lax.fori_loop(
        0,
        stop,
        step,
        (
            jnp.full((block, 1), -1e30, F32),
            jnp.zeros((block, 1), F32),
            jnp.zeros((block, VD), F32),
        ),
    )
    o_ref[...] = acc / total
    lse_ref[...] = top + jnp.log(total)


def attend(prefix, q, k, v):
    length = q.shape[0]
    block = block_of(length)
    return pl.pallas_call(
        functools.partial(attend_kernel, block=block, factor=QK**-0.5),
        grid=(length // block,),
        in_specs=[
            pl.BlockSpec(memory_space=pltpu.SMEM),
            pl.BlockSpec((block, QK), lambda i: (i, 0)),
            pl.BlockSpec((length, QK), lambda i: (0, 0)),
            pl.BlockSpec((length, VD), lambda i: (0, 0)),
        ],
        out_specs=[
            pl.BlockSpec((block, VD), lambda i: (i, 0)),
            pl.BlockSpec((block, 1), lambda i: (i, 0)),
        ],
        out_shape=[
            jax.ShapeDtypeStruct((length, VD), F32),
            jax.ShapeDtypeStruct((length, 1), F32),
        ],
        cost_estimate=pl.CostEstimate(
            flops=length * length * (QK + VD), bytes_accessed=length * 1000, transcendentals=length * length // 2
        ),
        name="attend",
    )(prefix, q, k, v)


def attend_back_kernel(
    prefix_ref, q_ref, k_ref, v_ref, d_ref, lse_ref, delta_ref, dq_ref, dk_ref, dv_ref, *, block, factor
):
    i = pl.program_id(0)
    prefix = prefix_ref[0]
    start = i * block

    @pl.when(i == 0)
    def _():
        dk_ref[...] = jnp.zeros_like(dk_ref)
        dv_ref[...] = jnp.zeros_like(dv_ref)

    q = q_ref[...]
    d = d_ref[...]
    lse = lse_ref[...]
    delta = delta_ref[...]
    seen = jnp.where(start < prefix, (prefix + block - 1) // block, 0)
    stop = jnp.maximum(i + 1, seen)
    rows = start + lax.broadcasted_iota(jnp.int32, (block, block), 1)

    def step(j, dq):
        at = pl.multiple_of(j * block, block)
        k = k_ref[pl.ds(at, block), :]
        v = v_ref[pl.ds(at, block), :]
        s = dot_t(k, q) * factor
        cols = at + lax.broadcasted_iota(jnp.int32, (block, block), 0)
        limit = jnp.where(rows < prefix, jnp.maximum(rows, prefix - 1), rows)
        p = jnp.where(cols <= limit, jnp.exp(s - lse), 0.0)
        dp = dot_t(v, d)
        ds = (p * (dp - delta)).astype(BF16)
        dv_ref[pl.ds(at, block), :] += dot(p.astype(BF16), d)
        dk_ref[pl.ds(at, block), :] += dot(ds, q) * factor
        return dq + t_dot(ds, k)

    dq = lax.fori_loop(0, stop, step, jnp.zeros((block, QK), F32))
    dq_ref[...] = dq * factor


def attend_back(prefix, q, k, v, d, lse, delta):
    length = q.shape[0]
    block = block_of(length)
    whole = lambda i: (0, 0)
    return pl.pallas_call(
        functools.partial(attend_back_kernel, block=block, factor=QK**-0.5),
        grid=(length // block,),
        in_specs=[
            pl.BlockSpec(memory_space=pltpu.SMEM),
            pl.BlockSpec((block, QK), lambda i: (i, 0)),
            pl.BlockSpec((length, QK), whole),
            pl.BlockSpec((length, VD), whole),
            pl.BlockSpec((block, VD), lambda i: (i, 0)),
            pl.BlockSpec((1, block), lambda i: (0, i)),
            pl.BlockSpec((1, block), lambda i: (0, i)),
        ],
        out_specs=[
            pl.BlockSpec((block, QK), lambda i: (i, 0)),
            pl.BlockSpec((length, QK), whole),
            pl.BlockSpec((length, VD), whole),
        ],
        out_shape=[
            jax.ShapeDtypeStruct((length, QK), F32),
            jax.ShapeDtypeStruct((length, QK), F32),
            jax.ShapeDtypeStruct((length, VD), F32),
        ],
        cost_estimate=pl.CostEstimate(
            flops=length * length * (3 * QK + 2 * VD), bytes_accessed=length * 2000, transcendentals=length * length // 2
        ),
        name="attend_back",
    )(prefix, q, k, v, d, lse, delta)


def split_two(v):
    high = v.astype(BF16)
    low = (v - high.astype(F32)).astype(BF16)
    return high, low


def per_device(
    hidden,
    grad_out,
    expert_ids,
    prefix_len,
    adapter_id,
    attn_gain,
    kv_gain,
    ffn_gain,
    w_q,
    w_kva,
    w_kvb,
    w_o,
    w_router,
    shared_gate,
    shared_up,
    shared_down,
    expert_gate,
    expert_up_weight,
    expert_down,
    q_down,
    q_up,
    o_down,
    o_up,
):
    tokens = hidden.shape[1]
    width = hidden.shape[2]
    members = lax.axis_size("grp")
    length = tokens * members
    experts = expert_gate.shape[0] * members
    capacity = tokens * TOP * 5 // (4 * experts)
    slots = -(-capacity // 16) * 16
    me = lax.axis_index("grp")

    inputs = hidden[0].astype(F32)
    cotangent = grad_out[0]
    c32 = cotangent.astype(F32)
    routes = expert_ids[0]
    adapter = adapter_id[0]
    pick = lambda table: lax.dynamic_index_in_dim(table, adapter, 0, keepdims=False)
    qa_down, qa_up, oa_down, oa_up = pick(q_down), pick(q_up), pick(o_down), pick(o_up)

    full_kva = gather(w_kva)
    full_q = gather(w_q)
    hidden_slice = shared_down.shape[0]
    kvb_cols = w_kvb.shape[1] // members
    own_kvb = exchange(
        w_kvb.reshape(w_kvb.shape[0], members, kvb_cols).transpose(1, 0, 2)
    ).reshape(KVR, kvb_cols)
    shared = jnp.stack([shared_gate, shared_up], axis=1)
    shared = shared.reshape(shared.shape[0], 2, members, hidden_slice).transpose(2, 0, 1, 3)
    own_shared = exchange(shared.reshape(members, -1, 2 * hidden_slice)).reshape(width, 2 * hidden_slice)
    full_o = gather(w_o)
    full_router = gather(w_router)

    positions = me * tokens + jnp.arange(tokens, dtype=jnp.int32)
    cosine, sine = angles(positions, ROPE)
    normed = root_norm(inputs, attn_gain).astype(BF16)
    latent = dot(normed, full_kva)
    compressed = root_norm(latent[:, :KVR], kv_gain).astype(BF16)
    k_rope = rotate(latent[:, KVR:], cosine, sine).astype(BF16)
    all_latent = gather(jnp.concatenate([compressed, k_rope], axis=-1))
    q_small = dot(normed, qa_down).astype(BF16)
    query = (dot(normed, full_q) + dot(q_small, qa_up)).reshape(tokens, H, QK)
    query = jnp.concatenate(
        [query[:, :, :NOPE], rotate(query[:, :, NOPE:], cosine[:, None], sine[:, None])], axis=-1
    ).astype(BF16)
    q_head = exchange(query.transpose(1, 0, 2)).reshape(length, QK)
    expanded = dot(all_latent[:, :KVR], own_kvb).astype(BF16)
    k_head = jnp.concatenate([expanded[:, :NOPE], all_latent[:, KVR:]], axis=-1)
    v_head = expanded[:, NOPE:]
    mixture, lse = attend(prefix_len, q_head, k_head, v_head)
    mixed = (
        exchange(mixture.astype(BF16).reshape(members, tokens, VD))
        .transpose(1, 0, 2)
        .reshape(tokens, H * VD)
    )
    o_small = dot(mixed, oa_down).astype(BF16)
    middle = inputs + dot(mixed, full_o) + dot(o_small, oa_up)
    ffn_in = root_norm(middle, ffn_gain).astype(BF16)
    route_probs = jax.nn.softmax(dot(ffn_in, full_router), axis=-1)

    lanes = 128
    high, low = split_two(route_probs)
    extra = jnp.concatenate(
        [high, low, jnp.zeros((tokens, lanes - 2 * experts), BF16)], axis=-1
    )
    all_in = gather(jnp.concatenate([ffn_in, extra], axis=-1))
    all_ids = gather(routes)
    all_c = gather(cotangent)
    ffn_all = all_in[:, :width]
    mine = jnp.arange(experts, dtype=jnp.int32)[None, :] == me
    probs = jnp.sum(
        jnp.where(
            mine,
            all_in[:, width : width + experts].astype(F32)
            + all_in[:, width + experts : width + 2 * experts].astype(F32),
            0.0,
        ),
        axis=-1,
    ).reshape(members, tokens)
    chosen = jnp.any(all_ids == me, axis=-1).reshape(members, tokens)
    order = jnp.arange(tokens, dtype=jnp.int32)
    before = (order[:, None] < order[None, :]).astype(BF16)
    rank = dot(chosen.astype(BF16), before).astype(jnp.int32)
    place = (rank[:, None, :] == jnp.arange(slots, dtype=jnp.int32)[None, :, None]) & chosen[:, None, :]
    select = place.astype(BF16)
    weight_rows = jnp.sum(jnp.where(place, probs[:, None, :], 0.0), axis=-1)

    def compact(rows):
        return lax.dot_general(
            select,
            rows.reshape(members, tokens, width),
            (((2,), (1,)), ((0,), (0,))),
            preferred_element_type=F32,
        ).astype(BF16).reshape(members * slots, width)

    def spread(rows):
        return lax.dot_general(
            select,
            rows.reshape(members, slots, width),
            (((1,), (1,)), ((0,), (0,))),
            preferred_element_type=F32,
        ).reshape(length, width)

    rows_in = compact(ffn_all)
    e_gate = dot(rows_in, expert_gate[0])
    e_up = dot(rows_in, expert_up_weight[0])
    e_hidden = (jax.nn.silu(e_gate) * e_up).astype(BF16)
    e_out = dot(e_hidden, expert_down[0]).astype(BF16)
    gates = weight_rows.reshape(members * slots, 1)
    s_gate = dot(ffn_all, own_shared[:, :hidden_slice])
    s_up = dot(ffn_all, own_shared[:, hidden_slice:])
    s_hidden = (jax.nn.silu(s_gate) * s_up).astype(BF16)
    partial = spread((gates * e_out.astype(F32)).astype(BF16)) + dot(s_hidden, shared_down)
    ffn_out = scatter_sum(partial.astype(BF16))
    output = (middle + ffn_out.astype(F32)).astype(BF16)

    rows_c = compact(all_c)
    rows_c32 = rows_c.astype(F32)
    d_gate = jnp.sum(rows_c32 * e_out.astype(F32), axis=-1).reshape(members, slots)
    d_eout = (gates * rows_c32).astype(BF16)
    d_eh = dot_t(d_eout, expert_down[0])
    d_egate = (d_eh * e_up * gated_slope(e_gate)).astype(BF16)
    d_eup = (d_eh * jax.nn.silu(e_gate)).astype(BF16)
    d_rows = (dot_t(d_egate, expert_gate[0]) + dot_t(d_eup, expert_up_weight[0])).astype(BF16)
    d_sh = dot_t(all_c, shared_down)
    d_sgate = (d_sh * s_up * gated_slope(s_gate)).astype(BF16)
    d_sup = (d_sh * jax.nn.silu(s_gate)).astype(BF16)
    d_shared = jnp.concatenate([d_sgate, d_sup], axis=-1)
    d_partial = spread(d_rows) + dot_t(d_shared, own_shared)
    d_gate_all = jnp.sum(jnp.where(place, d_gate[:, :, None], 0.0), axis=1).reshape(length, 1)
    g_high, g_low = split_two(d_gate_all)
    d_extra = jnp.concatenate(
        [
            jnp.where(mine, g_high, 0).astype(BF16),
            jnp.where(mine, g_low, 0).astype(BF16),
            jnp.zeros((length, lanes - 2 * experts), BF16),
        ],
        axis=-1,
    )
    d_own = scatter_sum(jnp.concatenate([d_partial.astype(BF16), d_extra], axis=-1))
    d_route = d_own[:, width : width + experts].astype(F32) + d_own[
        :, width + experts : width + 2 * experts
    ].astype(F32)
    d_logits = (
        route_probs * (d_route - jnp.sum(route_probs * d_route, axis=-1, keepdims=True))
    ).astype(BF16)
    d_ffn = d_own[:, :width].astype(F32) + dot_t(d_logits, full_router)
    d_middle = c32 + norm_back(middle, ffn_gain, d_ffn)
    d_attn = d_middle.astype(BF16)
    grad_oup = t_dot(o_small, d_attn)
    d_osmall = dot_t(d_attn, oa_up).astype(BF16)
    grad_odown = t_dot(d_osmall, mixed)
    d_mixed = (dot_t(d_attn, full_o) + dot_t(d_osmall, oa_down)).astype(BF16)
    d_head = exchange(d_mixed.reshape(tokens, H, VD).transpose(1, 0, 2)).reshape(length, VD)
    delta = jnp.sum(d_head.astype(F32) * mixture, axis=-1)
    dq, dk, dv = attend_back(
        prefix_len, q_head, k_head, v_head, d_head, lse.reshape(1, length), delta.reshape(1, length)
    )
    d_query = exchange(dq.astype(BF16).reshape(members, tokens, QK)).transpose(1, 0, 2).astype(F32)
    d_expanded = jnp.concatenate([dk[:, :NOPE], dv], axis=-1).astype(BF16)
    d_latents = scatter_sum(
        jnp.concatenate([dot_t(d_expanded, own_kvb), dk[:, NOPE:]], axis=-1).astype(BF16)
    ).astype(F32)
    d_latent = jnp.concatenate(
        [
            norm_back(latent[:, :KVR], kv_gain, d_latents[:, :KVR]),
            unrotate(d_latents[:, KVR:], cosine, sine),
        ],
        axis=-1,
    ).astype(BF16)
    d_query = (
        jnp.concatenate(
            [d_query[:, :, :NOPE], unrotate(d_query[:, :, NOPE:], cosine[:, None], sine[:, None])],
            axis=-1,
        )
        .reshape(tokens, H * QK)
        .astype(BF16)
    )
    grad_qup = t_dot(q_small, d_query)
    d_qsmall = dot_t(d_query, qa_up).astype(BF16)
    grad_qdown = t_dot(d_qsmall, normed)
    d_normed = dot_t(d_query, full_q) + dot_t(d_qsmall, qa_down) + dot_t(d_latent, full_kva)
    grad_inputs = (d_middle + norm_back(inputs, attn_gain, d_normed)).astype(BF16)

    rank_of = qa_up.shape[0]
    parts = [
        g.astype(BF16).reshape(rank_of, members, -1).transpose(1, 0, 2)
        for g in (grad_qdown, grad_qup, grad_odown, grad_oup)
    ]
    sizes = [g.shape[2] for g in parts]
    share = jnp.sum(exchange(jnp.concatenate(parts, axis=-1)).astype(F32), axis=0)
    selector = (jnp.arange(q_down.shape[0], dtype=jnp.int32) == adapter).astype(F32)[:, None, None]
    summed = lax.psum((selector * share[None]).astype(BF16), "rep").astype(F32)
    ends = [sum(sizes[: n + 1]) for n in range(4)]
    outs = [summed[:, :, e - s : e] for e, s in zip(ends, sizes)]
    return (
        output[None],
        grad_inputs[None],
        outs[0].transpose(0, 2, 1),
        outs[1],
        outs[2].transpose(0, 2, 1),
        outs[3],
    )


def solution(mesh):
    seq = P("rep", "grp", None)
    rows = P("grp", None)
    in_specs = (
        (seq, seq, seq, P("rep"), P("rep"), P(), P(), P())
        + (rows,) * 8
        + (P("grp", None, None),) * 3
        + (P(),) * 4
    )
    out_specs = (
        seq,
        seq,
        P(None, "grp", None),
        P(None, None, "grp"),
        P(None, "grp", None),
        P(None, None, "grp"),
    )
    return jax.shard_map(
        per_device, mesh=mesh, in_specs=in_specs, out_specs=out_specs, check_vma=False
    )
```

```python
import functools

import jax
import jax.numpy as jnp
from jax import lax
from jax.experimental import pallas as pl
from jax.experimental.pallas import tpu as pltpu
from jax.sharding import PartitionSpec as P

H = 16
NOPE = 128
ROPE = 64
VD = 128
KVR = 512
TOP = 6
QK = NOPE + ROPE
EPS = 1e-06
F32 = jnp.float32
BF16 = jnp.bfloat16


def dot(former, latter):
    return jnp.dot(former, latter, preferred_element_type=F32)


def dot_t(former, latter):
    return lax.dot_general(
        former, latter, (((1,), (1,)), ((), ())), preferred_element_type=F32
    )


def t_dot(former, latter):
    return lax.dot_general(
        former, latter, (((0,), (0,)), ((), ())), preferred_element_type=F32
    )


def root_norm(v, gains):
    factor = lax.rsqrt(jnp.mean(v * v, axis=-1, keepdims=True) + EPS)
    return v * factor * gains


def norm_back(v, gains, gradient):
    factor = lax.rsqrt(jnp.mean(v * v, axis=-1, keepdims=True) + EPS)
    weighted = gradient * gains
    return factor * weighted - v * (factor * factor * factor) * jnp.mean(
        weighted * v, axis=-1, keepdims=True
    )


def gated_slope(v):
    logistic = jax.nn.sigmoid(v)
    return logistic * (1.0 + v * (1.0 - logistic))


def angles(positions, width):
    frequency = 10000.0 ** (-jnp.arange(0, width, 2, dtype=F32) / width)
    phases = positions.astype(F32)[:, None] * frequency[None, :]
    return (jnp.cos(phases), jnp.sin(phases))


def rotate(v, cosine, sine):
    half = v.shape[-1] // 2
    a, b = v[..., :half], v[..., half:]
    return jnp.concatenate([a * cosine - b * sine, b * cosine + a * sine], axis=-1)


def unrotate(v, cosine, sine):
    half = v.shape[-1] // 2
    a, b = v[..., :half], v[..., half:]
    return jnp.concatenate([a * cosine + b * sine, b * cosine - a * sine], axis=-1)


SIDE = 2
CORES = 2


def place_of(members):
    me = lax.axis_index("grp")
    return me // (SIDE * CORES), (me // CORES) % SIDE, me % CORES


def index_of(z, x, c):
    return (z * SIDE + x) * CORES + c


def send(src, dst, sent, got, to):
    return pltpu.make_async_remote_copy(
        src_ref=src,
        dst_ref=dst,
        send_sem=sent,
        recv_sem=got,
        device_id={"grp": to},
        device_id_type=pl.DeviceIdType.MESH,
    )


def meet(members):
    barrier = pltpu.get_barrier_semaphore()
    me = lax.axis_index("grp")

    @pl.loop(1, members)
    def _(d):
        pl.semaphore_signal(
            barrier, 1, device_id={"grp": lax.rem(me + d, members)}, device_id_type=pl.DeviceIdType.MESH
        )

    pl.semaphore_wait(barrier, members - 1)


def gather_steps(src, out, sent, got, members):
    levels = members // (SIDE * CORES)
    z, x, c = place_of(members)
    me = lax.axis_index("grp")
    up, down = index_of(z + 1, x, c), index_of(z - 1, x, c)
    side, twin = index_of(z, 1 - x, c), index_of(z, x, 1 - c)

    def copy(slot, kind, to, own=False):
        return send(src if own else out.at[slot], out.at[slot], sent.at[kind, slot], got.at[slot], to)

    def arrive(slot):
        copy(slot, 0, twin).wait_recv()

    def first():
        @pl.when(z < levels - 1)
        def _():
            copy(me, 0, up, True).start()

        @pl.when(z > 0)
        def _():
            copy(me, 1, down, True).start()

        copy(me, 2, side, True).start()
        copy(me, 3, twin, True).start()

    def step(s):
        @pl.when(z >= s)
        def _():
            slot = index_of(z - s, x, c)
            arrive(slot)

            @pl.when(z < levels - 1)
            def _():
                copy(slot, 0, up).start()

            copy(slot, 2, side).start()
            copy(slot, 3, twin).start()

        @pl.when(z + s < levels)
        def _():
            slot = index_of(z + s, x, c)
            arrive(slot)

            @pl.when(z > 0)
            def _():
                copy(slot, 1, down).start()

            copy(slot, 2, side).start()
            copy(slot, 3, twin).start()

    def pass_on(s):
        @pl.when(z >= s)
        def _():
            slot = index_of(z - s, 1 - x, c)
            arrive(slot)
            copy(slot, 3, twin).start()

        if s > 0:

            @pl.when(z + s < levels)
            def _():
                slot = index_of(z + s, 1 - x, c)
                arrive(slot)
                copy(slot, 3, twin).start()

    def finish():
        @pl.loop(0, members // CORES)
        def _(i):
            arrive(i * CORES + 1 - c)

        @pl.loop(0, levels)
        def _(k):
            slot = index_of(k, x, c)
            copy(slot, 2, side).wait_send()

            @pl.when((k <= z) & (z < levels - 1))
            def _():
                copy(slot, 0, up).wait_send()

            @pl.when((k >= z) & (z > 0))
            def _():
                copy(slot, 1, down).wait_send()

        @pl.loop(0, members // CORES)
        def _(i):
            copy(i * CORES + c, 3, twin).wait_send()

    return first, step, pass_on, finish, levels


def comm_kernel(*refs, members, n_g, n_e):
    n = n_g + n_e
    ins, outs = refs[:n], refs[n : 2 * n]
    stage = refs[2 * n : 3 * n]
    local = refs[3 * n]
    g_sem = refs[3 * n + 1 : 3 * n + 1 + 2 * n_g]
    e_sem = refs[3 * n + 1 + 2 * n_g :]
    me = lax.axis_index("grp")
    own = [r if k < n_g else r.at[me] for k, r in enumerate(ins)]
    into = [pltpu.make_async_copy(own[k], stage[k], local.at[k]) for k in range(n)]
    out_of = [pltpu.make_async_copy(stage[k], outs[k].at[me], local.at[k]) for k in range(n)]
    for k in range(n):
        into[k].start()
    meet(members)

    plans = [
        gather_steps(ins[k], outs[k], g_sem[2 * k], g_sem[2 * k + 1], members) for k in range(n_g)
    ]

    def exchange_copy(k, d):
        to = lax.rem(me + d, members)
        return send(ins[n_g + k].at[to], outs[n_g + k].at[me], e_sem[2 * k].at[d], e_sem[2 * k + 1].at[d], to)

    for first, *_ in plans:
        first()
    for k in range(n_e):

        @pl.loop(1, members)
        def _(d):
            exchange_copy(k, d).start()

    for k in range(n):
        into[k].wait()
        out_of[k].start()
    levels = members // (SIDE * CORES)
    for s in range(1, levels):
        for _, step, *_ in plans:
            step(s)
    for s in range(levels):
        for _, _, pass_on, *_ in plans:
            pass_on(s)
    for *_, finish, _ in plans:
        finish()
    for k in range(n_e):

        @pl.loop(1, members)
        def _(d):
            exchange_copy(k, d).wait()

    for k in range(n):
        out_of[k].wait()


def communicate(gathers, exchanges, members, collective_id):
    gathers, exchanges = list(gathers), list(exchanges)
    n_g, n_e = len(gathers), len(exchanges)
    blocks = [g.shape for g in gathers] + [e.shape[1:] for e in exchanges]
    kinds = [a.dtype for a in gathers + exchanges]
    anywhere = pl.BlockSpec(memory_space=pl.ANY)
    sem = pltpu.SemaphoreType.DMA
    moved = sum(members * b[0] * b[1] * 2 for b in blocks)
    outs = pl.pallas_call(
        functools.partial(comm_kernel, members=members, n_g=n_g, n_e=n_e),
        in_specs=[anywhere] * (n_g + n_e),
        out_specs=[anywhere] * (n_g + n_e),
        out_shape=[jax.ShapeDtypeStruct((members, *b), k) for b, k in zip(blocks, kinds)],
        scratch_shapes=[pltpu.VMEM(b, k) for b, k in zip(blocks, kinds)]
        + [sem((n_g + n_e,))]
        + [sem((4, members)), sem((members,))] * n_g
        + [sem((members,)), sem((members,))] * n_e,
        compiler_params=pltpu.CompilerParams(collective_id=collective_id, has_side_effects=True),
        cost_estimate=pl.CostEstimate(flops=0, bytes_accessed=moved * 8, transcendentals=0),
        name=f"communicate_{collective_id}",
    )(*gathers, *exchanges)
    return outs[:n_g], outs[n_g:]


def reduce_kernel(*refs, members, n_e):
    p, extra, out, landed = refs[0], refs[1 : 1 + n_e], refs[1 + n_e], refs[2 + n_e : 2 + 2 * n_e]
    twin_in, side_in, up_in, down_in = refs[2 + 2 * n_e : 6 + 2 * n_e]
    sems = refs[6 + 2 * n_e :]
    twin_sent, twin_got, side_sent, side_got, up_sent, up_got, down_sent, down_got = sems[:8]
    stage, local, e_sem = sems[8 : 8 + n_e], sems[8 + n_e : 8 + 2 * n_e], sems[8 + 2 * n_e :]
    me = lax.axis_index("grp")
    levels = members // (SIDE * CORES)
    z, x, c = place_of(members)
    up, down = index_of(z + 1, x, c), index_of(z - 1, x, c)
    side, twin = index_of(z, 1 - x, c), index_of(z, x, 1 - c)

    def level(s):
        orders = []
        for k in range(levels):
            far = sorted((v for v in range(levels) if v != k), key=lambda v: (-abs(v - k), v))
            orders.append(far + [k])
        v = 0
        for k in range(levels):
            v = v + jnp.where(z == k, orders[k][s], 0)
        return v

    steps = [level(s) for s in range(levels)]
    into = [pltpu.make_async_copy(extra[k].at[me], stage[k], local[k]) for k in range(n_e)]
    out_of = [pltpu.make_async_copy(stage[k], landed[k].at[me], local[k]) for k in range(n_e)]
    for k in range(n_e):
        into[k].start()
    meet(members)

    def exchange_copy(k, d):
        to = lax.rem(me + d, members)
        return send(extra[k].at[to], landed[k].at[me], e_sem[2 * k].at[d], e_sem[2 * k + 1].at[d], to)

    def to_twin(k, w):
        return send(
            p.at[index_of(k, w, 1 - c)], twin_in.at[k * SIDE + w], twin_sent.at[k * SIDE + w], twin_got.at[k * SIDE + w], twin
        )

    def to_side(k):
        return send(p.at[index_of(k, 1 - x, c)], side_in.at[k], side_sent.at[k], side_got.at[k], side)

    def to_up(k):
        return send(p.at[index_of(k, x, c)], up_in.at[k], up_sent.at[k], up_got.at[k], up)

    def to_down(k):
        return send(p.at[index_of(k, x, c)], down_in.at[k], down_sent.at[k], down_got.at[k], down)

    def add(slot, ref):
        rows = p.shape[1]
        chunk = next(r for r in (32, 16, 8) if rows % r == 0)

        @pl.loop(0, rows // chunk)
        def _(i):
            at = pl.ds(pl.multiple_of(i * chunk, chunk), chunk)
            p[slot, at, :] = (p[slot, at, :].astype(F32) + ref[at, :].astype(F32)).astype(p.dtype)

    for k in steps:
        to_twin(k, x).start()
        to_twin(k, 1 - x).start()
    for k in range(n_e):

        @pl.loop(1, members)
        def _(d):
            exchange_copy(k, d).start()

        into[k].wait()
        out_of[k].start()
    for k in steps:
        w = 1 - x
        to_twin(k, w).wait_recv()
        add(index_of(k, w, c), twin_in.at[k * SIDE + w])
        to_side(k).start()
        to_twin(k, x).wait_recv()
        add(index_of(k, x, c), twin_in.at[k * SIDE + x])
    for s, k in enumerate(steps):
        mine = index_of(k, x, c)
        to_side(k).wait_recv()
        add(mine, side_in.at[k])
        if s < levels - 1:

            @pl.when((k > z) & (z > 0))
            def _():
                to_up(k).wait_recv()
                add(mine, up_in.at[k])

            @pl.when((k < z) & (z < levels - 1))
            def _():
                to_down(k).wait_recv()
                add(mine, down_in.at[k])

            @pl.when(k > z)
            def _():
                to_up(k).start()

            @pl.when(k < z)
            def _():
                to_down(k).start()

        else:

            @pl.when(z > 0)
            def _():
                to_up(k).wait_recv()
                add(mine, up_in.at[k])

            @pl.when(z < levels - 1)
            def _():
                to_down(k).wait_recv()
                add(mine, down_in.at[k])

            out[...] = p[mine]
    for s, k in enumerate(steps):
        to_twin(k, x).wait_send()
        to_twin(k, 1 - x).wait_send()
        to_side(k).wait_send()
        if s < levels - 1:

            @pl.when(k > z)
            def _():
                to_up(k).wait_send()

            @pl.when(k < z)
            def _():
                to_down(k).wait_send()

    for k in range(n_e):

        @pl.loop(1, members)
        def _(d):
            exchange_copy(k, d).wait()

        out_of[k].wait()


def reduce_blocks(p, extra, members, collective_id):
    extra = list(extra)
    n_e = len(extra)
    anywhere = pl.BlockSpec(memory_space=pl.ANY)
    _, r, c = p.shape
    levels = members // (SIDE * CORES)
    sem = pltpu.SemaphoreType.DMA
    vmem = pl.BlockSpec(memory_space=pltpu.VMEM)
    out, *landed = pl.pallas_call(
        functools.partial(reduce_kernel, members=members, n_e=n_e),
        in_specs=[vmem] + [anywhere] * n_e,
        out_specs=[vmem] + [anywhere] * n_e,
        out_shape=[jax.ShapeDtypeStruct((r, c), p.dtype)] + [jax.ShapeDtypeStruct(e.shape, e.dtype) for e in extra],
        scratch_shapes=[
            pltpu.VMEM((members // CORES, r, c), p.dtype),
            pltpu.VMEM((levels, r, c), p.dtype),
            pltpu.VMEM((levels, r, c), p.dtype),
            pltpu.VMEM((levels, r, c), p.dtype),
        ]
        + [sem((members // CORES,))] * 2
        + [sem((levels,))] * 6
        + [pltpu.VMEM(e.shape[1:], e.dtype) for e in extra]
        + [sem] * n_e
        + [sem((members,)), sem((members,))] * n_e,
        compiler_params=pltpu.CompilerParams(
            collective_id=collective_id, has_side_effects=True, vmem_limit_bytes=60 * 1024 * 1024
        ),
        cost_estimate=pl.CostEstimate(flops=0, bytes_accessed=members * r * c * 16, transcendentals=0),
        name=f"reduce_{collective_id}",
    )(p, *extra)
    return out, landed


def spread_kernel(src, out, stage, sent, got, local, *, members, sequences):
    me, mine = lax.axis_index("grp"), lax.axis_index("rep")
    barrier = pltpu.get_barrier_semaphore()
    into = pltpu.make_async_copy(src.at[me], stage, local)
    out_of = pltpu.make_async_copy(stage, out.at[mine, me], local)
    into.start()

    def other(n):
        return lax.rem(mine + n // members, sequences), lax.rem(me + n % members, members)

    @pl.loop(1, members * sequences)
    def _(n):
        r, to = other(n)
        pl.semaphore_signal(barrier, 1, device_id={"rep": r, "grp": to}, device_id_type=pl.DeviceIdType.MESH)

    pl.semaphore_wait(barrier, members * sequences - 1)

    def copy(n):
        r, to = other(n)
        return pltpu.make_async_remote_copy(
            src_ref=src.at[to],
            dst_ref=out.at[mine, me],
            send_sem=sent.at[n],
            recv_sem=got.at[n],
            device_id={"rep": r, "grp": to},
            device_id_type=pl.DeviceIdType.MESH,
        )

    @pl.loop(1, members * sequences)
    def _(n):
        copy(n).start()

    into.wait()
    out_of.start()

    @pl.loop(1, members * sequences)
    def _(n):
        copy(n).wait()

    out_of.wait()


def spread_blocks(v, members, sequences, collective_id):
    anywhere = pl.BlockSpec(memory_space=pl.ANY)
    sem = pltpu.SemaphoreType.DMA
    return pl.pallas_call(
        functools.partial(spread_kernel, members=members, sequences=sequences),
        in_specs=[anywhere],
        out_specs=anywhere,
        out_shape=jax.ShapeDtypeStruct((sequences, *v.shape), v.dtype),
        scratch_shapes=[pltpu.VMEM(v.shape[1:], v.dtype), sem((members * sequences,)), sem((members * sequences,)), sem],
        compiler_params=pltpu.CompilerParams(collective_id=collective_id, has_side_effects=True),
        cost_estimate=pl.CostEstimate(flops=0, bytes_accessed=v.size * 16, transcendentals=0),
        name=f"spread_{collective_id}",
    )(v)


def gather(v):
    return lax.all_gather(v, "grp", axis=0, tiled=True)


def exchange(v):
    return lax.all_to_all(v, "grp", split_axis=0, concat_axis=0, tiled=True)


def scatter_sum(v):
    return lax.psum_scatter(v, "grp", scatter_dimension=0, tiled=True)


def after(v, *others):
    return lax.optimization_barrier((v, *others))[0]


def block_of(length):
    return next(b for b in (512, 384, 256, 128) if length % b == 0)


def attend_kernel(prefix_ref, q_ref, k_ref, v_ref, o_ref, lse_ref, *, block, factor):
    i = pl.program_id(0)
    prefix = prefix_ref[0]
    start = i * block
    q = q_ref[...]
    seen = jnp.where(start < prefix, (prefix + block - 1) // block, 0)
    stop = jnp.maximum(i + 1, seen)
    rows = start + lax.broadcasted_iota(jnp.int32, (block, block), 0)

    def step(j, carry):
        top, total, acc = carry
        at = pl.multiple_of(j * block, block)
        k = k_ref[pl.ds(at, block), :]
        v = v_ref[pl.ds(at, block), :]
        s = dot_t(q, k) * factor
        cols = at + lax.broadcasted_iota(jnp.int32, (block, block), 1)
        limit = jnp.where(rows < prefix, jnp.maximum(rows, prefix - 1), rows)
        s = jnp.where(cols <= limit, s, -1e30)
        fresh = jnp.maximum(top, jnp.max(s, axis=1, keepdims=True))
        p = jnp.exp(s - fresh)
        scale = jnp.exp(top - fresh)
        total = total * scale + jnp.sum(p, axis=1, keepdims=True)
        acc = acc * scale + dot(p.astype(BF16), v)
        return fresh, total, acc

    top, total, acc = lax.fori_loop(
        0,
        stop,
        step,
        (
            jnp.full((block, 1), -1e30, F32),
            jnp.zeros((block, 1), F32),
            jnp.zeros((block, VD), F32),
        ),
    )
    o_ref[...] = acc / total
    lse_ref[...] = top + jnp.log(total)


def attend(prefix, q, k, v):
    length = q.shape[0]
    block = block_of(length)
    return pl.pallas_call(
        functools.partial(attend_kernel, block=block, factor=QK**-0.5),
        grid=(length // block,),
        in_specs=[
            pl.BlockSpec(memory_space=pltpu.SMEM),
            pl.BlockSpec((block, QK), lambda i: (i, 0)),
            pl.BlockSpec((length, QK), lambda i: (0, 0)),
            pl.BlockSpec((length, VD), lambda i: (0, 0)),
        ],
        out_specs=[
            pl.BlockSpec((block, VD), lambda i: (i, 0)),
            pl.BlockSpec((block, 1), lambda i: (i, 0)),
        ],
        out_shape=[
            jax.ShapeDtypeStruct((length, VD), F32),
            jax.ShapeDtypeStruct((length, 1), F32),
        ],
        cost_estimate=pl.CostEstimate(
            flops=length * length * (QK + VD), bytes_accessed=length * 1000, transcendentals=length * length // 2
        ),
        name="attend",
    )(prefix, q, k, v)


def attend_back_kernel(
    prefix_ref, q_ref, k_ref, v_ref, d_ref, lse_ref, delta_ref, dq_ref, dk_ref, dv_ref, *, block, factor
):
    i = pl.program_id(0)
    prefix = prefix_ref[0]
    start = i * block

    @pl.when(i == 0)
    def _():
        dk_ref[...] = jnp.zeros_like(dk_ref)
        dv_ref[...] = jnp.zeros_like(dv_ref)

    q = q_ref[...]
    d = d_ref[...]
    lse = lse_ref[...]
    delta = delta_ref[...]
    seen = jnp.where(start < prefix, (prefix + block - 1) // block, 0)
    stop = jnp.maximum(i + 1, seen)
    rows = start + lax.broadcasted_iota(jnp.int32, (block, block), 1)

    def step(j, dq):
        at = pl.multiple_of(j * block, block)
        k = k_ref[pl.ds(at, block), :]
        v = v_ref[pl.ds(at, block), :]
        s = dot_t(k, q) * factor
        cols = at + lax.broadcasted_iota(jnp.int32, (block, block), 0)
        limit = jnp.where(rows < prefix, jnp.maximum(rows, prefix - 1), rows)
        p = jnp.where(cols <= limit, jnp.exp(s - lse), 0.0)
        dp = dot_t(v, d)
        ds = (p * (dp - delta)).astype(BF16)
        dv_ref[pl.ds(at, block), :] += dot(p.astype(BF16), d)
        dk_ref[pl.ds(at, block), :] += dot(ds, q) * factor
        return dq + t_dot(ds, k)

    dq = lax.fori_loop(0, stop, step, jnp.zeros((block, QK), F32))
    dq_ref[...] = dq * factor


def attend_back(prefix, q, k, v, d, lse, delta):
    length = q.shape[0]
    block = block_of(length)
    whole = lambda i: (0, 0)
    return pl.pallas_call(
        functools.partial(attend_back_kernel, block=block, factor=QK**-0.5),
        grid=(length // block,),
        in_specs=[
            pl.BlockSpec(memory_space=pltpu.SMEM),
            pl.BlockSpec((block, QK), lambda i: (i, 0)),
            pl.BlockSpec((length, QK), whole),
            pl.BlockSpec((length, VD), whole),
            pl.BlockSpec((block, VD), lambda i: (i, 0)),
            pl.BlockSpec((1, block), lambda i: (0, i)),
            pl.BlockSpec((1, block), lambda i: (0, i)),
        ],
        out_specs=[
            pl.BlockSpec((block, QK), lambda i: (i, 0)),
            pl.BlockSpec((length, QK), whole),
            pl.BlockSpec((length, VD), whole),
        ],
        out_shape=[
            jax.ShapeDtypeStruct((length, QK), F32),
            jax.ShapeDtypeStruct((length, QK), F32),
            jax.ShapeDtypeStruct((length, VD), F32),
        ],
        cost_estimate=pl.CostEstimate(
            flops=length * length * (3 * QK + 2 * VD), bytes_accessed=length * 2000, transcendentals=length * length // 2
        ),
        name="attend_back",
    )(prefix, q, k, v, d, lse, delta)


def pack(v):
    half = v.shape[1] // 2
    rope = jnp.concatenate([v[:, :half, NOPE:], v[:, half:, NOPE:]], axis=-1)
    return jnp.concatenate([v[:, :, :NOPE], rope], axis=1)


def unpack(v):
    rows = v.shape[1] * 2 // 3
    rope = jnp.concatenate([v[:, rows:, :ROPE], v[:, rows:, ROPE:]], axis=1)
    return jnp.concatenate([v[:, :rows], rope], axis=-1)


def per_device(
    hidden,
    grad_out,
    expert_ids,
    prefix_len,
    adapter_id,
    attn_gain,
    kv_gain,
    ffn_gain,
    w_q,
    w_kva,
    w_kvb,
    w_o,
    w_router,
    shared_gate,
    shared_up,
    shared_down,
    expert_gate,
    expert_up_weight,
    expert_down,
    q_down,
    q_up,
    o_down,
    o_up,
):
    tokens = hidden.shape[1]
    width = hidden.shape[2]
    members = lax.axis_size("grp")
    length = tokens * members
    experts = expert_gate.shape[0] * members
    capacity = tokens * TOP * 5 // (4 * experts)
    slots = -(-capacity // 16) * 16
    me = lax.axis_index("grp")

    inputs = hidden[0].astype(F32)
    cotangent = grad_out[0]
    c32 = cotangent.astype(F32)
    routes = expert_ids[0]
    adapter = adapter_id[0]
    pick = lambda table: lax.dynamic_index_in_dim(table, adapter, 0, keepdims=False)
    qa_down, qa_up, oa_down, oa_up = pick(q_down), pick(q_up), pick(o_down), pick(o_up)

    chosen_by = jnp.sum(
        (routes[:, :, None] == jnp.arange(experts, dtype=jnp.int32)[None, None, :]).astype(F32), axis=1
    )
    (all_kva, all_q, all_router), (kvb_parts, chosen_all) = communicate(
        [w_kva, w_q, w_router],
        [
            w_kvb.reshape(w_kvb.shape[0], members, -1).transpose(1, 0, 2),
            jnp.broadcast_to(chosen_by.T[:, None, :], (experts, 8, tokens)),
        ],
        members,
        1,
    )
    full_kva, full_q, full_router = (v.reshape(-1, v.shape[2]) for v in (all_kva, all_q, all_router))
    own_kvb = kvb_parts.reshape(KVR, -1)
    hidden_slice = shared_down.shape[0]
    shared = after(jnp.stack([shared_gate, shared_up], axis=1), all_q)
    shared = shared.reshape(shared.shape[0], 2, members, hidden_slice).transpose(2, 0, 1, 3)
    own_shared = exchange(shared.reshape(members, -1, 2 * hidden_slice)).reshape(width, 2 * hidden_slice)
    full_o = gather(after(w_o, all_q))

    positions = me * tokens + jnp.arange(tokens, dtype=jnp.int32)
    cosine, sine = angles(positions, ROPE)
    normed = root_norm(inputs, attn_gain).astype(BF16)
    latent = dot(normed, full_kva)
    compressed = root_norm(latent[:, :KVR], kv_gain).astype(BF16)
    k_rope = rotate(latent[:, KVR:], cosine, sine).astype(BF16)
    q_small = dot(normed, qa_down).astype(BF16)
    query = (dot(normed, full_q) + dot(q_small, qa_up)).reshape(tokens, H, QK)
    query = jnp.concatenate(
        [query[:, :, :NOPE], rotate(query[:, :, NOPE:], cosine[:, None], sine[:, None])], axis=-1
    ).astype(BF16)
    (all_latent,), (q_packed,) = communicate(
        [jnp.concatenate([compressed, k_rope], axis=-1)], [pack(query.transpose(1, 0, 2))], members, 2
    )
    all_latent = all_latent.reshape(length, KVR + ROPE)
    q_head = unpack(q_packed).reshape(length, QK)
    expanded = dot(all_latent[:, :KVR], own_kvb).astype(BF16)
    k_head = jnp.concatenate([expanded[:, :NOPE], all_latent[:, KVR:]], axis=-1)
    v_head = expanded[:, NOPE:]
    mixture, lse = attend(prefix_len, q_head, k_head, v_head)
    _, (mixed,) = communicate([], [mixture.astype(BF16).reshape(members, tokens, VD)], members, 3)
    mixed = mixed.transpose(1, 0, 2).reshape(tokens, H * VD)
    o_small = dot(mixed, oa_down).astype(BF16)
    middle = inputs + dot(mixed, full_o) + dot(o_small, oa_up)
    ffn_in = root_norm(middle, ffn_gain).astype(BF16)
    route_probs = jax.nn.softmax(dot(ffn_in, full_router), axis=-1)

    (all_in,), (prob_parts,) = communicate(
        [ffn_in],
        [jnp.broadcast_to(route_probs.T[:, None, :], (experts, 8, tokens))],
        members,
        4,
    )
    all_c = gather(after(cotangent, all_in))
    ffn_all = all_in.reshape(length, width)
    probs = prob_parts[:, 0]
    chosen = chosen_all[:, 0] > 0.5
    order = jnp.arange(tokens, dtype=jnp.int32)
    before = (order[:, None] < order[None, :]).astype(BF16)
    rank = dot(chosen.astype(BF16), before).astype(jnp.int32)
    place = (rank[:, None, :] == jnp.arange(slots, dtype=jnp.int32)[None, :, None]) & chosen[:, None, :]
    select = place.astype(BF16)
    weight_rows = jnp.sum(jnp.where(place, probs[:, None, :], 0.0), axis=-1)

    def compact(rows):
        return lax.dot_general(
            select,
            rows.reshape(members, tokens, width),
            (((2,), (1,)), ((0,), (0,))),
            preferred_element_type=F32,
        ).astype(BF16).reshape(members * slots, width)

    def spread(rows):
        return lax.dot_general(
            select,
            rows.reshape(members, slots, width),
            (((1,), (1,)), ((0,), (0,))),
            preferred_element_type=F32,
        ).reshape(length, width)

    rows_in = compact(ffn_all)
    e_gate = dot(rows_in, expert_gate[0])
    e_up = dot(rows_in, expert_up_weight[0])
    e_hidden = (jax.nn.silu(e_gate) * e_up).astype(BF16)
    e_out = dot(e_hidden, expert_down[0]).astype(BF16)
    gates = weight_rows.reshape(members * slots, 1)
    s_gate = dot(ffn_all, own_shared[:, :hidden_slice])
    s_up = dot(ffn_all, own_shared[:, hidden_slice:])
    s_hidden = (jax.nn.silu(s_gate) * s_up).astype(BF16)
    partial = spread((gates * e_out.astype(F32)).astype(BF16)) + dot(s_hidden, shared_down)
    ffn_out = scatter_sum(partial.astype(BF16))
    output = (middle + ffn_out.astype(F32)).astype(BF16)

    rows_c = compact(all_c)
    rows_c32 = rows_c.astype(F32)
    d_gate = jnp.sum(rows_c32 * e_out.astype(F32), axis=-1).reshape(members, slots)
    d_eout = (gates * rows_c32).astype(BF16)
    d_eh = dot_t(d_eout, expert_down[0])
    d_egate = (d_eh * e_up * gated_slope(e_gate)).astype(BF16)
    d_eup = (d_eh * jax.nn.silu(e_gate)).astype(BF16)
    d_rows = (dot_t(d_egate, expert_gate[0]) + dot_t(d_eup, expert_up_weight[0])).astype(BF16)
    d_sh = dot_t(all_c, shared_down)
    d_sgate = (d_sh * s_up * gated_slope(s_gate)).astype(BF16)
    d_sup = (d_sh * jax.nn.silu(s_gate)).astype(BF16)
    d_shared = jnp.concatenate([d_sgate, d_sup], axis=-1)
    d_partial = spread(d_rows) + dot_t(d_shared, own_shared)
    d_gate_all = jnp.sum(jnp.where(place, d_gate[:, :, None], 0.0), axis=1)
    d_own, (d_route,) = reduce_blocks(
        d_partial.astype(BF16).reshape(members, tokens, width),
        [jnp.broadcast_to(d_gate_all[:, None, :], (members, 8, tokens))],
        members,
        5,
    )
    d_route = d_route[:, 0].T
    d_logits = (
        route_probs * (d_route - jnp.sum(route_probs * d_route, axis=-1, keepdims=True))
    ).astype(BF16)
    d_ffn = d_own.astype(F32) + dot_t(d_logits, full_router)
    d_middle = c32 + norm_back(middle, ffn_gain, d_ffn)
    d_attn = d_middle.astype(BF16)
    grad_oup = t_dot(o_small, d_attn)
    d_osmall = dot_t(d_attn, oa_up).astype(BF16)
    grad_odown = t_dot(d_osmall, mixed)
    d_mixed = (dot_t(d_attn, full_o) + dot_t(d_osmall, oa_down)).astype(BF16)
    _, (d_head,) = communicate([], [d_mixed.reshape(tokens, H, VD).transpose(1, 0, 2)], members, 6)
    d_head = d_head.reshape(length, VD)
    delta = jnp.sum(d_head.astype(F32) * mixture, axis=-1)
    dq, dk, dv = attend_back(
        prefix_len, q_head, k_head, v_head, d_head, lse.reshape(1, length), delta.reshape(1, length)
    )
    d_expanded = jnp.concatenate([dk[:, :NOPE], dv], axis=-1).astype(BF16)
    d_latents, (d_query,) = reduce_blocks(
        jnp.concatenate([dot_t(d_expanded, own_kvb), dk[:, NOPE:]], axis=-1)
        .astype(BF16)
        .reshape(members, tokens, KVR + ROPE),
        [pack(dq.astype(BF16).reshape(members, tokens, QK))],
        members,
        7,
    )
    d_latents = d_latents.astype(F32)
    d_query = unpack(d_query).transpose(1, 0, 2).astype(F32)
    d_latent = jnp.concatenate(
        [
            norm_back(latent[:, :KVR], kv_gain, d_latents[:, :KVR]),
            unrotate(d_latents[:, KVR:], cosine, sine),
        ],
        axis=-1,
    ).astype(BF16)
    d_query = (
        jnp.concatenate(
            [d_query[:, :, :NOPE], unrotate(d_query[:, :, NOPE:], cosine[:, None], sine[:, None])],
            axis=-1,
        )
        .reshape(tokens, H * QK)
        .astype(BF16)
    )
    grad_qup = t_dot(q_small, d_query)
    d_qsmall = dot_t(d_query, qa_up).astype(BF16)
    grad_qdown = t_dot(d_qsmall, normed)
    d_normed = dot_t(d_query, full_q) + dot_t(d_qsmall, qa_down) + dot_t(d_latent, full_kva)
    grad_inputs = (d_middle + norm_back(inputs, attn_gain, d_normed)).astype(BF16)

    rank_of = qa_up.shape[0]
    parts = [
        g.astype(BF16).reshape(rank_of, members, -1).transpose(1, 0, 2)
        for g in (grad_qdown, grad_qup, grad_odown, grad_oup)
    ]
    sizes = [g.shape[2] for g in parts]
    lanes = 128
    named = jnp.broadcast_to(adapter.astype(BF16), (members, rank_of, lanes))
    sequences = lax.axis_size("rep")
    shares = spread_blocks(jnp.concatenate(parts + [named], axis=-1), members, sequences, 8)
    numbers = shares[:, 0, 0, -1].astype(jnp.int32)
    share = jnp.sum(shares[..., :-lanes].astype(F32), axis=1)
    selector = (jnp.arange(q_down.shape[0], dtype=jnp.int32)[:, None] == numbers[None, :]).astype(F32)
    summed = jnp.sum(selector[:, :, None, None] * share[None], axis=1)
    ends = [sum(sizes[: n + 1]) for n in range(4)]
    outs = [summed[:, :, e - s : e] for e, s in zip(ends, sizes)]
    return (
        output[None],
        grad_inputs[None],
        outs[0].transpose(0, 2, 1),
        outs[1],
        outs[2].transpose(0, 2, 1),
        outs[3],
    )


def solution(mesh):
    seq = P("rep", "grp", None)
    rows = P("grp", None)
    in_specs = (
        (seq, seq, seq, P("rep"), P("rep"), P(), P(), P())
        + (rows,) * 8
        + (P("grp", None, None),) * 3
        + (P(),) * 4
    )
    out_specs = (
        seq,
        seq,
        P(None, "grp", None),
        P(None, None, "grp"),
        P(None, "grp", None),
        P(None, None, "grp"),
    )
    return jax.shard_map(
        per_device, mesh=mesh, in_specs=in_specs, out_specs=out_specs, check_vma=False
    )
```

```python
import functools

import jax
import jax.numpy as jnp
from jax import lax
from jax.experimental import pallas as pl
from jax.experimental.pallas import tpu as pltpu
from jax.sharding import PartitionSpec as P

H = 16
NOPE = 128
ROPE = 64
VD = 128
KVR = 512
TOP = 6
QK = NOPE + ROPE
EPS = 1e-06
F32 = jnp.float32
BF16 = jnp.bfloat16


def dot(former, latter):
    return jnp.dot(former, latter, preferred_element_type=F32)


def dot_t(former, latter):
    return lax.dot_general(
        former, latter, (((1,), (1,)), ((), ())), preferred_element_type=F32
    )


def t_dot(former, latter):
    return lax.dot_general(
        former, latter, (((0,), (0,)), ((), ())), preferred_element_type=F32
    )


def root_norm(v, gains):
    factor = lax.rsqrt(jnp.mean(v * v, axis=-1, keepdims=True) + EPS)
    return v * factor * gains


def norm_back(v, gains, gradient):
    factor = lax.rsqrt(jnp.mean(v * v, axis=-1, keepdims=True) + EPS)
    weighted = gradient * gains
    return factor * weighted - v * (factor * factor * factor) * jnp.mean(
        weighted * v, axis=-1, keepdims=True
    )


def angles(positions, width):
    frequency = 10000.0 ** (-jnp.arange(0, width, 2, dtype=F32) / width)
    phases = positions.astype(F32)[:, None] * frequency[None, :]
    return (jnp.cos(phases), jnp.sin(phases))


def rotate(v, cosine, sine):
    half = v.shape[-1] // 2
    a, b = v[..., :half], v[..., half:]
    return jnp.concatenate([a * cosine - b * sine, b * cosine + a * sine], axis=-1)


def unrotate(v, cosine, sine):
    half = v.shape[-1] // 2
    a, b = v[..., :half], v[..., half:]
    return jnp.concatenate([a * cosine + b * sine, b * cosine - a * sine], axis=-1)


SIDE = 2
CORES = 2
MESH = pl.DeviceIdType.MESH


def place_of():
    me = lax.axis_index("grp")
    return me // (SIDE * CORES), (me // CORES) % SIDE, me % CORES


def index_of(z, x, c):
    return (z * SIDE + x) * CORES + c


def send(src, dst, sent, got, to):
    return pltpu.make_async_remote_copy(
        src_ref=src,
        dst_ref=dst,
        send_sem=sent,
        recv_sem=got,
        device_id=to if isinstance(to, dict) else {"grp": to},
        device_id_type=MESH,
    )


def meet(members, partner=None):
    barrier = pltpu.get_barrier_semaphore()
    me = lax.axis_index("grp")

    @pl.loop(1, members)
    def _(d):
        pl.semaphore_signal(barrier, 1, device_id={"grp": lax.rem(me + d, members)}, device_id_type=MESH)

    if partner is not None:
        pl.semaphore_signal(barrier, 1, device_id=partner, device_id_type=MESH)
    pl.semaphore_wait(barrier, members - 1 + (partner is not None))


def pick_from(table, z, s):
    v = 0
    for i, row in enumerate(table):
        for j, entry in enumerate(row):
            if entry:
                v = v + jnp.where((z == i) & (s == j), entry, 0)
    return v


def near_first(levels):
    return [sorted(range(levels), key=lambda v: (abs(v - k), v)) for k in range(levels)]


def far_first(levels):
    return [sorted((v for v in range(levels) if v != k), key=lambda v: (-abs(v - k), v)) + [k] for k in range(levels)]


class Gather:
    def __init__(self, src, out, sent, got, members, split=0):
        self.src, self.out, self.sent, self.got = src, out, sent, got
        self.members, self.split = members, split
        self.levels = members // (SIDE * CORES)
        self.z, self.x, self.c = z, x, c = place_of()
        self.me = lax.axis_index("grp")
        self.up, self.down = index_of(z + 1, x, c), index_of(z - 1, x, c)
        self.side, self.twin = index_of(z, 1 - x, c), index_of(z, x, 1 - c)
        if split:
            rows = src.shape[0]
            rep = lax.axis_index("rep")
            odd = rep % 2
            self.partner = {"rep": rep + 1 - 2 * odd, "grp": self.me}
            self.window = pl.ds(pl.multiple_of(odd * split, 16), rows - split)
            self.given = pl.ds(pl.multiple_of(odd * (rows - split), 16), split)
            self.lacked = pl.ds(pl.multiple_of((1 - odd) * (rows - split), 16), split)

    def copy(self, slot, kind, to, own=False, rows=None):
        rows = rows or (self.window if self.split else None)
        other = rows is not None and self.split and rows is not self.window
        src = self.src if own else self.out.at[slot]
        dst = self.out.at[slot]
        if rows is not None:
            src, dst = src.at[rows], dst.at[rows]
        return send(src, dst, self.sent.at[kind, slot], self.got.at[int(bool(other)), slot], to)

    def arrive(self, slot):
        self.copy(slot, 0, self.twin).wait_recv()

    def to_partner(self, slot):
        return self.copy(slot, 4, self.partner, rows=self.given)

    def lacked_to_twin(self, slot, own=False):
        return self.copy(slot, 5, self.twin, own, rows=self.lacked)

    def first(self):
        @pl.when(self.z < self.levels - 1)
        def _():
            self.copy(self.me, 0, self.up, True).start()

        @pl.when(self.z > 0)
        def _():
            self.copy(self.me, 1, self.down, True).start()

        self.copy(self.me, 2, self.side, True).start()
        self.copy(self.me, 3, self.twin, True).start()
        if self.split:
            self.lacked_to_twin(self.me, True).start()

    def relay(self, s):
        @pl.when(self.z >= s)
        def _():
            slot = index_of(self.z - s, self.x, self.c)
            self.arrive(slot)

            @pl.when(self.z < self.levels - 1)
            def _():
                self.copy(slot, 0, self.up).start()

            self.spread(slot)

        @pl.when(self.z + s < self.levels)
        def _():
            slot = index_of(self.z + s, self.x, self.c)
            self.arrive(slot)

            @pl.when(self.z > 0)
            def _():
                self.copy(slot, 1, self.down).start()

            self.spread(slot)

    def spread(self, slot):
        self.copy(slot, 2, self.side).start()
        self.copy(slot, 3, self.twin).start()
        if self.split:
            self.to_partner(slot).start()

    def pass_on(self, k):
        slot = index_of(k, 1 - self.x, self.c)
        self.arrive(slot)
        self.copy(slot, 3, self.twin).start()
        if self.split:
            self.to_partner(slot).start()

    def take_lacked(self, k, x):
        slot = index_of(k, x, self.c)

        @pl.when(slot != self.me)
        def _():
            self.copy(slot, 4, self.partner, rows=self.lacked).wait_recv()
            self.lacked_to_twin(slot).start()

    def take_twin(self, k):
        for x in range(SIDE):
            self.arrive(index_of(k, x, 1 - self.c))

    def take_twin_lacked(self):
        @pl.loop(0, self.members // CORES)
        def _(i):
            self.lacked_to_twin(i * CORES + 1 - self.c).wait_recv()

    def finish(self):
        @pl.loop(0, self.levels)
        def _(k):
            slot = index_of(k, self.x, self.c)
            self.copy(slot, 2, self.side).wait_send()

            @pl.when((k <= self.z) & (self.z < self.levels - 1))
            def _():
                self.copy(slot, 0, self.up).wait_send()

            @pl.when((k >= self.z) & (self.z > 0))
            def _():
                self.copy(slot, 1, self.down).wait_send()

        @pl.loop(0, self.members // CORES)
        def _(i):
            slot = i * CORES + self.c
            self.copy(slot, 3, self.twin).wait_send()
            if self.split:
                self.lacked_to_twin(slot).wait_send()

                @pl.when(slot != self.me)
                def _():
                    self.to_partner(slot).wait_send()


class Exchange:
    def __init__(self, src, out, sent, got, members):
        self.src, self.out, self.sent, self.got, self.members = src, out, sent, got, members
        self.me = lax.axis_index("grp")

    def copy(self, d):
        to = lax.rem(self.me + d, self.members)
        return send(self.src.at[to], self.out.at[self.me], self.sent.at[d], self.got.at[d], to)

    def start(self):
        @pl.loop(1, self.members)
        def _(d):
            self.copy(d).start()

    def wait(self):
        @pl.loop(1, self.members)
        def _(d):
            self.copy(d).wait()


def comm_kernel(*refs, members, splits, n_e):
    n_g = len(splits)
    n = n_g + n_e
    ins, outs = refs[:n], refs[n : 2 * n]
    stage = refs[2 * n : 3 * n]
    local = refs[3 * n]
    sems = refs[3 * n + 1 :]
    me = lax.axis_index("grp")
    into = [
        pltpu.make_async_copy(r if k < n_g else r.at[me], stage[k], local.at[k]) for k, r in enumerate(ins)
    ]
    out_of = [pltpu.make_async_copy(stage[k], outs[k].at[me], local.at[k]) for k in range(n)]
    gathers = [
        Gather(ins[k], outs[k], sems[2 * k], sems[2 * k + 1], members, splits[k]) for k in range(n_g)
    ]
    exchanges = [Exchange(ins[k], outs[k], sems[2 * k], sems[2 * k + 1], members) for k in range(n_g, n)]
    for copy in into:
        copy.start()
    split = [g for g in gathers if g.split]
    meet(members, split[0].partner if split else None)
    for g in gathers:
        g.first()
    for e in exchanges:
        e.start()
    for a, b in zip(into, out_of):
        a.wait()
        b.start()
    levels = members // (SIDE * CORES)
    z = me // (SIDE * CORES)
    order = near_first(levels)
    for s in range(1, levels):
        for g in gathers:
            g.relay(s)
    for s in range(levels):
        for g in gathers:
            g.pass_on(pick_from(order, z, s))
    for g in split:

        @pl.loop(0, levels)
        def _(s):
            k = pick_from(order, z, s)
            g.take_lacked(k, g.x)
            g.take_lacked(k, 1 - g.x)

    for g in gathers:

        @pl.loop(0, levels)
        def _(k):
            g.take_twin(k)

        if g.split:
            g.take_twin_lacked()
        g.finish()
    for e in exchanges:
        e.wait()
    for copy in out_of:
        copy.wait()


def communicate(gathers, exchanges, members, collective_id, splits=None):
    gathers, exchanges = list(gathers), list(exchanges)
    n_g, n_e = len(gathers), len(exchanges)
    splits = splits or [0] * n_g
    blocks = [g.shape for g in gathers] + [e.shape[1:] for e in exchanges]
    kinds = [a.dtype for a in gathers + exchanges]
    anywhere = pl.BlockSpec(memory_space=pl.ANY)
    sem = pltpu.SemaphoreType.DMA
    moved = sum(members * b[0] * b[1] * 2 for b in blocks)
    outs = pl.pallas_call(
        functools.partial(comm_kernel, members=members, splits=tuple(splits), n_e=n_e),
        in_specs=[anywhere] * (n_g + n_e),
        out_specs=[anywhere] * (n_g + n_e),
        out_shape=[jax.ShapeDtypeStruct((members, *b), k) for b, k in zip(blocks, kinds)],
        scratch_shapes=[pltpu.VMEM(b, k) for b, k in zip(blocks, kinds)]
        + [sem((n_g + n_e,))]
        + [sem((6, members)), sem((2, members))] * n_g
        + [sem((members,)), sem((members,))] * n_e,
        compiler_params=pltpu.CompilerParams(collective_id=collective_id, has_side_effects=True),
        cost_estimate=pl.CostEstimate(flops=0, bytes_accessed=moved * 8, transcendentals=0),
        name=f"communicate_{collective_id}",
    )(*gathers, *exchanges)
    return outs[:n_g], outs[n_g:]


class Reduce:
    def __init__(self, p, twin_in, side_in, line_in, sems, members):
        self.p, self.twin_in, self.side_in, self.line_in = p, twin_in, side_in, line_in
        self.sems = sems
        self.levels = members // (SIDE * CORES)
        self.z, self.x, self.c = place_of()

    def copy(self, kind, slot, dst, n, to):
        sent, got = self.sems[2 * kind], self.sems[2 * kind + 1]
        return send(self.p.at[slot], dst.at[n], sent.at[n], got.at[n], to)

    def to_twin(self, k, w):
        twin = index_of(self.z, self.x, 1 - self.c)
        return self.copy(0, index_of(k, w, 1 - self.c), self.twin_in, k * SIDE + w, twin)

    def to_side(self, k):
        return self.copy(1, index_of(k, 1 - self.x, self.c), self.side_in, k, index_of(self.z, 1 - self.x, self.c))

    def to_up(self, k):
        return self.copy(2, index_of(k, self.x, self.c), self.line_in, k + 1, index_of(self.z + 1, self.x, self.c))

    def to_down(self, k):
        return self.copy(3, index_of(k, self.x, self.c), self.line_in, k, index_of(self.z - 1, self.x, self.c))

    def add(self, slot, ref):
        rows = self.p.shape[1]
        chunk = next(r for r in (32, 16, 8) if rows % r == 0)

        @pl.loop(0, rows // chunk)
        def _(i):
            at = pl.ds(pl.multiple_of(i * chunk, chunk), chunk)
            self.p[slot, at, :] = (self.p[slot, at, :].astype(F32) + ref[at, :].astype(F32)).astype(self.p.dtype)

    def start(self, k):
        self.to_twin(k, self.x).start()
        self.to_twin(k, 1 - self.x).start()

    def chip(self, k):
        w = 1 - self.x
        self.to_twin(k, w).wait_recv()
        self.add(index_of(k, w, self.c), self.twin_in.at[k * SIDE + w])
        self.to_side(k).start()
        self.to_twin(k, self.x).wait_recv()
        self.add(index_of(k, self.x, self.c), self.twin_in.at[k * SIDE + self.x])

    def line(self, k):
        z, mine = self.z, index_of(k, self.x, self.c)
        self.to_side(k).wait_recv()
        self.add(mine, self.side_in.at[k])

        @pl.when((k > z) & (z > 0))
        def _():
            self.to_up(k).wait_recv()
            self.add(mine, self.line_in.at[k + 1])

        @pl.when((k < z) & (z < self.levels - 1))
        def _():
            self.to_down(k).wait_recv()
            self.add(mine, self.line_in.at[k])

        @pl.when(k > z)
        def _():
            self.to_up(k).start()

        @pl.when(k < z)
        def _():
            self.to_down(k).start()

    def last(self, out):
        z, mine = self.z, index_of(self.z, self.x, self.c)
        self.to_side(z).wait_recv()
        self.add(mine, self.side_in.at[z])

        @pl.when(z > 0)
        def _():
            self.to_up(z).wait_recv()
            self.add(mine, self.line_in.at[z + 1])

        @pl.when(z < self.levels - 1)
        def _():
            self.to_down(z).wait_recv()
            self.add(mine, self.line_in.at[z])

        out[...] = self.p[mine]

    def finish(self):
        z = self.z

        @pl.loop(0, self.levels)
        def _(k):
            self.to_twin(k, 0).wait_send()
            self.to_twin(k, 1).wait_send()
            self.to_side(k).wait_send()

            @pl.when(k > z)
            def _():
                self.to_up(k).wait_send()

            @pl.when(k < z)
            def _():
                self.to_down(k).wait_send()

    @staticmethod
    def scratch(members, r, c, kind):
        levels = members // (SIDE * CORES)
        sem = pltpu.SemaphoreType.DMA
        return [
            pltpu.VMEM((members // CORES, r, c), kind),
            pltpu.VMEM((levels, r, c), kind),
            pltpu.VMEM((levels + 1, r, c), kind),
        ] + [sem((n,)) for n in (members // CORES,) * 2 + (levels,) * 2 + (levels + 1,) * 4]


def reduce_kernel(*refs, members, n_e):
    p, extra, out, landed = refs[0], refs[1 : 1 + n_e], refs[1 + n_e], refs[2 + n_e : 2 + 2 * n_e]
    bufs = refs[2 + 2 * n_e :]
    r = Reduce(p, *bufs[:3], bufs[3:11], members)
    stage, local, sems = bufs[11 : 11 + n_e], bufs[11 + n_e : 11 + 2 * n_e], bufs[11 + 2 * n_e :]
    me = lax.axis_index("grp")
    order = far_first(r.levels)
    into = [pltpu.make_async_copy(extra[k].at[me], stage[k], local[k]) for k in range(n_e)]
    out_of = [pltpu.make_async_copy(stage[k], landed[k].at[me], local[k]) for k in range(n_e)]
    exchanges = [Exchange(extra[k], landed[k], sems[2 * k], sems[2 * k + 1], members) for k in range(n_e)]
    for k in range(n_e):
        into[k].start()
    meet(members)

    @pl.loop(0, r.levels)
    def _(s):
        r.start(pick_from(order, r.z, s))

    for k in range(n_e):
        exchanges[k].start()
        into[k].wait()
        out_of[k].start()

    @pl.loop(0, r.levels)
    def _(s):
        r.chip(pick_from(order, r.z, s))

    @pl.loop(0, r.levels - 1)
    def _(s):
        r.line(pick_from(order, r.z, s))

    r.last(out)
    r.finish()
    for k in range(n_e):
        exchanges[k].wait()
        out_of[k].wait()


def reduce_blocks(p, extra, members, collective_id):
    extra = list(extra)
    n_e = len(extra)
    anywhere = pl.BlockSpec(memory_space=pl.ANY)
    _, r, c = p.shape
    sem = pltpu.SemaphoreType.DMA
    vmem = pl.BlockSpec(memory_space=pltpu.VMEM)
    out, *landed = pl.pallas_call(
        functools.partial(reduce_kernel, members=members, n_e=n_e),
        in_specs=[vmem] + [anywhere] * n_e,
        out_specs=[vmem] + [anywhere] * n_e,
        out_shape=[jax.ShapeDtypeStruct((r, c), p.dtype)] + [jax.ShapeDtypeStruct(e.shape, e.dtype) for e in extra],
        scratch_shapes=Reduce.scratch(members, r, c, p.dtype)
        + [pltpu.VMEM(e.shape[1:], e.dtype) for e in extra]
        + [sem] * n_e
        + [sem((members,)), sem((members,))] * n_e,
        compiler_params=pltpu.CompilerParams(
            collective_id=collective_id, has_side_effects=True, vmem_limit_bytes=60 * 1024 * 1024
        ),
        cost_estimate=pl.CostEstimate(flops=0, bytes_accessed=members * r * c * 16, transcendentals=0),
        name=f"reduce_{collective_id}",
    )(p, *extra)
    return out, landed


def spread_kernel(src, out, stage, sent, got, local, *, members, sequences):
    me, mine = lax.axis_index("grp"), lax.axis_index("rep")
    barrier = pltpu.get_barrier_semaphore()
    into = pltpu.make_async_copy(src.at[me], stage, local)
    out_of = pltpu.make_async_copy(stage, out.at[mine, me], local)
    into.start()

    def other(n):
        return lax.rem(mine + n // members, sequences), lax.rem(me + n % members, members)

    @pl.loop(1, members * sequences)
    def _(n):
        r, to = other(n)
        pl.semaphore_signal(barrier, 1, device_id={"rep": r, "grp": to}, device_id_type=MESH)

    pl.semaphore_wait(barrier, members * sequences - 1)

    def copy(n):
        r, to = other(n)
        return pltpu.make_async_remote_copy(
            src_ref=src.at[to],
            dst_ref=out.at[mine, me],
            send_sem=sent.at[n],
            recv_sem=got.at[n],
            device_id={"rep": r, "grp": to},
            device_id_type=MESH,
        )

    @pl.loop(1, members * sequences)
    def _(n):
        copy(n).start()

    into.wait()
    out_of.start()

    @pl.loop(1, members * sequences)
    def _(n):
        copy(n).wait()

    out_of.wait()


def spread_blocks(v, members, sequences, collective_id):
    anywhere = pl.BlockSpec(memory_space=pl.ANY)
    sem = pltpu.SemaphoreType.DMA
    return pl.pallas_call(
        functools.partial(spread_kernel, members=members, sequences=sequences),
        in_specs=[anywhere],
        out_specs=anywhere,
        out_shape=jax.ShapeDtypeStruct((sequences, *v.shape), v.dtype),
        scratch_shapes=[pltpu.VMEM(v.shape[1:], v.dtype), sem((members * sequences,)), sem((members * sequences,)), sem],
        compiler_params=pltpu.CompilerParams(collective_id=collective_id, has_side_effects=True),
        cost_estimate=pl.CostEstimate(flops=0, bytes_accessed=v.size * 16, transcendentals=0),
        name=f"spread_{collective_id}",
    )(v)


def gather(v):
    return lax.all_gather(v, "grp", axis=0, tiled=True)


def exchange(v):
    return lax.all_to_all(v, "grp", split_axis=0, concat_axis=0, tiled=True)


def scatter_sum(v):
    return lax.psum_scatter(v, "grp", scatter_dimension=0, tiled=True)


def after(v, *others):
    return lax.optimization_barrier((v, *others))[0]


def block_of(length):
    return next(b for b in (512, 384, 256, 128) if length % b == 0)


def attend_kernel(prefix_ref, q_ref, k_ref, v_ref, o_ref, lse_ref, *, block, factor):
    i = pl.program_id(0)
    prefix = prefix_ref[0]
    start = i * block
    q = q_ref[...]
    seen = jnp.where(start < prefix, (prefix + block - 1) // block, 0)
    stop = jnp.maximum(i + 1, seen)
    rows = start + lax.broadcasted_iota(jnp.int32, (block, block), 0)

    def step(j, carry):
        top, total, acc = carry
        at = pl.multiple_of(j * block, block)
        k = k_ref[pl.ds(at, block), :]
        v = v_ref[pl.ds(at, block), :]
        s = dot_t(q, k) * factor
        cols = at + lax.broadcasted_iota(jnp.int32, (block, block), 1)
        limit = jnp.where(rows < prefix, jnp.maximum(rows, prefix - 1), rows)
        s = jnp.where(cols <= limit, s, -1e30)
        fresh = jnp.maximum(top, jnp.max(s, axis=1, keepdims=True))
        p = jnp.exp(s - fresh)
        scale = jnp.exp(top - fresh)
        total = total * scale + jnp.sum(p, axis=1, keepdims=True)
        acc = acc * scale + dot(p.astype(BF16), v)
        return fresh, total, acc

    top, total, acc = lax.fori_loop(
        0,
        stop,
        step,
        (
            jnp.full((block, 1), -1e30, F32),
            jnp.zeros((block, 1), F32),
            jnp.zeros((block, VD), F32),
        ),
    )
    o_ref[...] = acc / total
    lse_ref[...] = top + jnp.log(total)


def attend(prefix, q, k, v):
    length = q.shape[0]
    block = block_of(length)
    return pl.pallas_call(
        functools.partial(attend_kernel, block=block, factor=QK**-0.5),
        grid=(length // block,),
        in_specs=[
            pl.BlockSpec(memory_space=pltpu.SMEM),
            pl.BlockSpec((block, QK), lambda i: (i, 0)),
            pl.BlockSpec((length, QK), lambda i: (0, 0)),
            pl.BlockSpec((length, VD), lambda i: (0, 0)),
        ],
        out_specs=[
            pl.BlockSpec((block, VD), lambda i: (i, 0)),
            pl.BlockSpec((block, 1), lambda i: (i, 0)),
        ],
        out_shape=[
            jax.ShapeDtypeStruct((length, VD), F32),
            jax.ShapeDtypeStruct((length, 1), F32),
        ],
        cost_estimate=pl.CostEstimate(
            flops=length * length * (QK + VD), bytes_accessed=length * 1000, transcendentals=length * length // 2
        ),
        name="attend",
    )(prefix, q, k, v)


def attend_back_kernel(
    prefix_ref, q_ref, k_ref, v_ref, d_ref, lse_ref, delta_ref, dq_ref, dk_ref, dv_ref, *, block, factor
):
    i = pl.program_id(0)
    prefix = prefix_ref[0]
    start = i * block

    @pl.when(i == 0)
    def _():
        dk_ref[...] = jnp.zeros_like(dk_ref)
        dv_ref[...] = jnp.zeros_like(dv_ref)

    q = q_ref[...]
    d = d_ref[...]
    lse = lse_ref[...]
    delta = delta_ref[...]
    seen = jnp.where(start < prefix, (prefix + block - 1) // block, 0)
    stop = jnp.maximum(i + 1, seen)
    rows = start + lax.broadcasted_iota(jnp.int32, (block, block), 1)

    def step(j, dq):
        at = pl.multiple_of(j * block, block)
        k = k_ref[pl.ds(at, block), :]
        v = v_ref[pl.ds(at, block), :]
        s = dot_t(k, q) * factor
        cols = at + lax.broadcasted_iota(jnp.int32, (block, block), 0)
        limit = jnp.where(rows < prefix, jnp.maximum(rows, prefix - 1), rows)
        p = jnp.where(cols <= limit, jnp.exp(s - lse), 0.0)
        dp = dot_t(v, d)
        ds = (p * (dp - delta)).astype(BF16)
        dv_ref[pl.ds(at, block), :] += dot(p.astype(BF16), d)
        dk_ref[pl.ds(at, block), :] += dot(ds, q) * factor
        return dq + t_dot(ds, k)

    dq = lax.fori_loop(0, stop, step, jnp.zeros((block, QK), F32))
    dq_ref[...] = dq * factor


def attend_back(prefix, q, k, v, d, lse, delta):
    length = q.shape[0]
    block = block_of(length)
    whole = lambda i: (0, 0)
    return pl.pallas_call(
        functools.partial(attend_back_kernel, block=block, factor=QK**-0.5),
        grid=(length // block,),
        in_specs=[
            pl.BlockSpec(memory_space=pltpu.SMEM),
            pl.BlockSpec((block, QK), lambda i: (i, 0)),
            pl.BlockSpec((length, QK), whole),
            pl.BlockSpec((length, VD), whole),
            pl.BlockSpec((block, VD), lambda i: (i, 0)),
            pl.BlockSpec((1, block), lambda i: (0, i)),
            pl.BlockSpec((1, block), lambda i: (0, i)),
        ],
        out_specs=[
            pl.BlockSpec((block, QK), lambda i: (i, 0)),
            pl.BlockSpec((length, QK), whole),
            pl.BlockSpec((length, VD), whole),
        ],
        out_shape=[
            jax.ShapeDtypeStruct((length, QK), F32),
            jax.ShapeDtypeStruct((length, QK), F32),
            jax.ShapeDtypeStruct((length, VD), F32),
        ],
        cost_estimate=pl.CostEstimate(
            flops=length * length * (3 * QK + 2 * VD), bytes_accessed=length * 2000, transcendentals=length * length // 2
        ),
        name="attend_back",
    )(prefix, q, k, v, d, lse, delta)


def silu_parts(v):
    logistic = 1.0 / (1.0 + jnp.exp(-v))
    return v * logistic, logistic * (1.0 + v * (1.0 - logistic))


def picks(rank, slots):
    at = lax.broadcasted_iota(jnp.int32, (slots, rank.shape[1]), 0).astype(F32)
    return at == rank


def picks_back(rank, slots):
    at = lax.broadcasted_iota(jnp.int32, (rank.shape[0], slots), 1).astype(F32)
    return at == rank


def tiles(width, size):
    return pl.ds(pl.multiple_of(width * size, size), size)


def experts_kernel(
    x_hbm, prob_hbm, rank_ref, back_ref, gate_hbm, up_hbm, down_hbm, own_hbm, sdown_hbm,
    part_hbm, eg_hbm, eu_hbm, eo_hbm, sh_hbm, prob_out,
    xs, probs, gate, up, down, own, sdown, tail, rows, acts, part_st, eg_st, eu_st, eo_st, sh_st,
    sent, got, e_sent, e_got, load, store,
    *, members, slots, tile, wide
):
    me = lax.axis_index("grp")
    levels = members // (SIDE * CORES)
    group = SIDE * CORES
    width, hidden = gate.shape
    half, whole = hidden % tile, hidden // tile
    units = own.shape[1] // 2
    z = me // group
    order = near_first(levels)
    loads = [
        pltpu.make_async_copy(a, b, load.at[n])
        for n, (a, b) in enumerate(
            [
                (x_hbm, xs.at[me]),
                (prob_hbm.at[me], probs.at[me]),
                (own_hbm, own),
                (gate_hbm, gate),
                (up_hbm, up),
                (down_hbm, down),
                (sdown_hbm, sdown),
            ]
        )
    ]
    gather = Gather(x_hbm, xs, sent, got, members)
    exchange = Exchange(prob_hbm, probs, e_sent, e_got, members)
    for copy in loads:
        copy.start()
    meet(members)
    gather.first()
    exchange.start()
    for copy in loads:
        copy.wait()
    tail[:, :half] = gate[:, hidden - half :]
    tail[:, half:] = up[:, hidden - half :]
    gather.pass_on(z)
    gather.relay(1)
    exchange.wait()
    prob_out[...] = probs[...]

    def stores(s, k):
        n = s % 2
        return [
            pltpu.make_async_copy(a.at[n], b.at[k], store.at[n, m])
            for m, (a, b) in enumerate(
                [(part_st, part_hbm), (eg_st, eg_hbm), (eu_st, eu_hbm), (eo_st, eo_hbm), (sh_st, sh_hbm)]
            )
        ]

    @pl.loop(0, levels)
    def _(s):
        k = pick_from(order, z, s)
        n = s % 2
        gather.take_twin(k)

        @pl.when(s >= 2)
        def _():
            for copy in stores(s, pick_from(order, z, s - 2)):
                copy.wait()

        for b in range(group):
            pick = picks(rank_ref[k * group + b, 0:1, :], slots).astype(BF16)
            rows[b * slots : (b + 1) * slots, :] = dot(pick, xs[k * group + b]).astype(BF16)

        def keep(at, g, u):
            eg_st[n, :, at] = g.astype(BF16)
            eu_st[n, :, at] = u.astype(BF16)
            acts[:, at] = (silu_parts(g)[0] * u).astype(BF16)

        @pl.loop(0, whole)
        def _(j):
            at = tiles(j, tile)
            x = rows[...]
            keep(at, dot(x, gate[:, at]), dot(x, up[:, at]))

        last = dot(rows[...], tail[...])
        keep(pl.ds(whole * tile, half), last[:, :half], last[:, half:])

        gather.relay(s + 2)

        @pl.when(s + 1 < levels)
        def _():
            gather.pass_on(pick_from(order, z, s + 1))

        @pl.loop(0, width // wide)
        def _(j):
            at = tiles(j, wide)
            eo_st[n, :, at] = dot(acts[...], down[:, at]).astype(BF16)

        for b in range(group):
            i = k * group + b
            pick = picks(rank_ref[i, 0:1, :], slots)
            back = picks_back(back_ref[i], slots).astype(BF16)
            g = jnp.sum(jnp.where(pick, probs[i, 0:1, :], 0.0), axis=1, keepdims=True)
            pre = dot(xs[i], own[...])
            sh_st[n, b] = pre.astype(BF16)
            act = (silu_parts(pre[:, :units])[0] * pre[:, units:]).astype(BF16)

            @pl.loop(0, width // wide)
            def _(j):
                at = tiles(j, wide)
                weighted = (g * eo_st[n, b * slots : (b + 1) * slots, at].astype(F32)).astype(BF16)
                part_st[n, b, :, at] = (dot(back, weighted) + dot(act, sdown[:, at])).astype(BF16)

        for copy in stores(s, k):
            copy.start()

    @pl.loop(levels - 2, levels)
    def _(s):
        for copy in stores(s, pick_from(order, z, s)):
            copy.wait()

    gather.finish()


def experts_forward(x, prob, rank, back, gate, up, down, own, sdown, slots, members, collective_id):
    tokens, width = x.shape
    hidden = gate.shape[1]
    group = SIDE * CORES
    levels = members // group
    packed = group * slots
    anywhere = pl.BlockSpec(memory_space=pl.ANY)
    vmem = pl.BlockSpec(memory_space=pltpu.VMEM)
    sem = pltpu.SemaphoreType.DMA
    tile = 256
    shapes = [
        (levels, group, tokens, width),
        (levels, packed, hidden),
        (levels, packed, hidden),
        (levels, packed, width),
        (levels, group, tokens, own.shape[1]),
    ]
    return pl.pallas_call(
        functools.partial(experts_kernel, members=members, slots=slots, tile=tile, wide=512),
        in_specs=[anywhere, anywhere, vmem, vmem] + [anywhere] * 5,
        out_specs=[anywhere] * 5 + [vmem],
        out_shape=[jax.ShapeDtypeStruct(s, BF16) for s in shapes] + [jax.ShapeDtypeStruct(prob.shape, F32)],
        scratch_shapes=[
            pltpu.VMEM((members, tokens, width), BF16),
            pltpu.VMEM(prob.shape, F32),
            pltpu.VMEM(gate.shape, BF16),
            pltpu.VMEM(up.shape, BF16),
            pltpu.VMEM(down.shape, BF16),
            pltpu.VMEM(own.shape, BF16),
            pltpu.VMEM(sdown.shape, BF16),
            pltpu.VMEM((width, tile), BF16),
            pltpu.VMEM((packed, width), BF16),
            pltpu.VMEM((packed, hidden), BF16),
        ]
        + [pltpu.VMEM((2, *s[1:]), BF16) for s in shapes]
        + [sem((6, members)), sem((2, members)), sem((members,)), sem((members,)), sem((7,)), sem((2, 5))],
        compiler_params=pltpu.CompilerParams(
            collective_id=collective_id, has_side_effects=True, vmem_limit_bytes=63 * 1024 * 1024
        ),
        cost_estimate=pl.CostEstimate(
            flops=12 * members * slots * width * hidden, bytes_accessed=60_000_000, transcendentals=0
        ),
        name="experts_forward",
    )(x, prob, rank, back, gate, up, down, own, sdown)


def experts_back_kernel(
    c_hbm, rank_ref, back_ref, prob_ref, eg_hbm, eu_hbm, eo_hbm, sh_hbm, gate_hbm, up_hbm, down_hbm, own_hbm, sdown_hbm,
    out, dg_out,
    part, cs, eg, eu, eo, sh, gate, up, down, own, sdown, rows, d_gate, d_up, dg_st, dg_in,
    *sems, members, slots, tile, wide
):
    twin_in, side_in, line_in = sems[:3]
    e_sent, e_got, load, fetch = sems[11:15]
    me = lax.axis_index("grp")
    levels = members // (SIDE * CORES)
    group = SIDE * CORES
    width, hidden = gate.shape
    half, whole = hidden % tile, hidden // tile
    units = own.shape[1] // 2
    z = me // group
    order = far_first(levels)
    reduce = Reduce(part, twin_in, side_in, line_in, sems[3:11], members)
    exchange = Exchange(dg_st, dg_in, e_sent, e_got, members)

    def cotangents(s):
        return pltpu.make_async_copy(c_hbm.at[pick_from(order, z, s)], cs.at[s % 2], fetch.at[s % 2])

    def kept(s):
        k = pick_from(order, z, s)
        return [
            pltpu.make_async_copy(a.at[k], b, fetch.at[2 + m])
            for m, (a, b) in enumerate([(eo_hbm, eo), (eg_hbm, eg), (eu_hbm, eu), (sh_hbm, sh)])
        ]

    loads = [
        pltpu.make_async_copy(a, b, load.at[n])
        for n, (a, b) in enumerate(
            [(down_hbm, down), (gate_hbm, gate), (up_hbm, up), (own_hbm, own), (sdown_hbm, sdown)]
        )
    ]
    cotangents(0).start()
    for copy in kept(0):
        copy.start()
    for copy in loads:
        copy.start()
    meet(members)

    def early(s):
        return (z == 0) | (z == levels - 1)

    @pl.loop(0, levels)
    def _(s):
        k = pick_from(order, z, s)
        n = s % 2
        cotangents(s).wait()
        load_eo, load_eg, load_eu, load_sh = kept(s)

        @pl.when(s + 1 < levels)
        def _():
            cotangents(s + 1).start()

        load_eo.wait()
        for b in range(group):
            i = k * group + b
            at = slice(b * slots, (b + 1) * slots)
            pick = picks(rank_ref[i, 0:1, :], slots)
            c = dot(pick.astype(BF16), cs[n, b])
            g = jnp.sum(jnp.where(pick, prob_ref[i, 0:1, :], 0.0), axis=1, keepdims=True)
            along = jnp.sum(c * eo[at, :].astype(F32), axis=1, keepdims=True)
            dg_st[i] = jnp.broadcast_to(
                jnp.sum(jnp.where(pick, along, 0.0), axis=0, keepdims=True), dg_st.shape[1:]
            )
            rows[at, :] = (g * c).astype(BF16)

        @pl.when(s == 0)
        def _():
            for copy in loads:
                copy.wait()

        load_eg.wait()
        load_eu.wait()

        def slopes(at):
            d = dot_t(rows[...], down[at, :])
            act, slope = silu_parts(eg[:, at].astype(F32))
            d_gate[:, at] = (d * eu[:, at].astype(F32) * slope).astype(BF16)
            d_up[:, at] = (d * act).astype(BF16)

        @pl.loop(0, whole)
        def _(j):
            slopes(tiles(j, tile))

        slopes(pl.ds(whole * tile, half))

        @pl.when(s >= 1)
        def _():
            reduce.chip(pick_from(order, z, s - 1))

        @pl.when((s >= 2) & ~early(s))
        def _():
            reduce.line(pick_from(order, z, s - 2))

        @pl.loop(0, width // tile)
        def _(j):
            at = tiles(j, tile)
            eo[:, at] = (dot_t(d_gate[...], gate[at, :]) + dot_t(d_up[...], up[at, :])).astype(BF16)

        load_sh.wait()
        for b in range(group):
            i = k * group + b
            back = picks_back(back_ref[i], slots).astype(BF16)
            d = dot_t(cs[n, b], sdown[...])
            pre = sh[b].astype(F32)
            act, slope = silu_parts(pre[:, :units])
            both = jnp.concatenate([d * pre[:, units:] * slope, d * act], axis=1).astype(BF16)

            @pl.loop(0, width // wide)
            def _(j):
                at = tiles(j, wide)
                part[i, :, at] = (
                    dot(back, eo[b * slots : (b + 1) * slots, at]) + dot_t(both, own[at, :])
                ).astype(BF16)

        reduce.start(k)

        @pl.when(s + 1 < levels)
        def _():
            for copy in kept(s + 1):
                copy.start()

        @pl.when((s >= 1) & early(s))
        def _():
            reduce.line(pick_from(order, z, s - 1))

    exchange.start()
    dg_in[me] = dg_st[me]
    reduce.chip(z)

    @pl.when(~early(0))
    def _():
        reduce.line(pick_from(order, z, levels - 2))

    reduce.last(out)
    reduce.finish()
    exchange.wait()
    dg_out[...] = dg_in[...]


def experts_backward(c, rank, back, prob, kept, gate, up, down, own, sdown, slots, members, collective_id):
    _, tokens, width = c.shape
    hidden = gate.shape[1]
    group = SIDE * CORES
    levels = members // group
    packed = group * slots
    anywhere = pl.BlockSpec(memory_space=pl.ANY)
    vmem = pl.BlockSpec(memory_space=pltpu.VMEM)
    sem = pltpu.SemaphoreType.DMA
    eg, eu, eo, sh = kept
    return pl.pallas_call(
        functools.partial(experts_back_kernel, members=members, slots=slots, tile=256, wide=512),
        in_specs=[anywhere, vmem, vmem, vmem] + [anywhere] * 9,
        out_specs=[vmem, vmem],
        out_shape=[
            jax.ShapeDtypeStruct((tokens, width), BF16),
            jax.ShapeDtypeStruct((members, 8, tokens), F32),
        ],
        scratch_shapes=[
            pltpu.VMEM((members, tokens, width), BF16),
            pltpu.VMEM((2, group, tokens, width), BF16),
            pltpu.VMEM(eg.shape[1:], BF16),
            pltpu.VMEM(eu.shape[1:], BF16),
            pltpu.VMEM(eo.shape[1:], BF16),
            pltpu.VMEM(sh.shape[1:], BF16),
            pltpu.VMEM(gate.shape, BF16),
            pltpu.VMEM(up.shape, BF16),
            pltpu.VMEM(down.shape, BF16),
            pltpu.VMEM(own.shape, BF16),
            pltpu.VMEM(sdown.shape, BF16),
            pltpu.VMEM((packed, width), BF16),
            pltpu.VMEM((packed, hidden), BF16),
            pltpu.VMEM((packed, hidden), BF16),
            pltpu.VMEM((members, 8, tokens), F32),
            pltpu.VMEM((members, 8, tokens), F32),
        ]
        + Reduce.scratch(members, tokens, width, BF16)
        + [sem((members,)), sem((members,)), sem((5,)), sem((6,))],
        compiler_params=pltpu.CompilerParams(
            collective_id=collective_id, has_side_effects=True, vmem_limit_bytes=67_043_328
        ),
        cost_estimate=pl.CostEstimate(
            flops=12 * members * slots * width * hidden, bytes_accessed=60_000_000, transcendentals=0
        ),
        name="experts_backward",
    )(c.reshape(levels, group, tokens, width), rank, back, prob, *kept, gate, up, down, own, sdown)


def pack(v):
    half = v.shape[1] // 2
    rope = jnp.concatenate([v[:, :half, NOPE:], v[:, half:, NOPE:]], axis=-1)
    return jnp.concatenate([v[:, :, :NOPE], rope], axis=1)


def unpack(v):
    rows = v.shape[1] * 2 // 3
    rope = jnp.concatenate([v[:, rows:, :ROPE], v[:, rows:, ROPE:]], axis=1)
    return jnp.concatenate([v[:, :rows], rope], axis=-1)


def per_device(
    hidden,
    grad_out,
    expert_ids,
    prefix_len,
    adapter_id,
    attn_gain,
    kv_gain,
    ffn_gain,
    w_q,
    w_kva,
    w_kvb,
    w_o,
    w_router,
    shared_gate,
    shared_up,
    shared_down,
    expert_gate,
    expert_up_weight,
    expert_down,
    q_down,
    q_up,
    o_down,
    o_up,
):
    tokens = hidden.shape[1]
    width = hidden.shape[2]
    members = lax.axis_size("grp")
    length = tokens * members
    experts = expert_gate.shape[0] * members
    capacity = tokens * TOP * 5 // (4 * experts)
    slots = -(-capacity // 16) * 16
    me = lax.axis_index("grp")

    inputs = hidden[0].astype(F32)
    cotangent = grad_out[0]
    c32 = cotangent.astype(F32)
    routes = expert_ids[0]
    adapter = adapter_id[0]
    pick = lambda table: lax.dynamic_index_in_dim(table, adapter, 0, keepdims=False)
    qa_down, qa_up, oa_down, oa_up = pick(q_down), pick(q_up), pick(o_down), pick(o_up)

    chosen_by = jnp.sum(
        (routes[:, :, None] == jnp.arange(experts, dtype=jnp.int32)[None, None, :]).astype(F32), axis=1
    )
    sequences = lax.axis_size("rep")
    split = w_q.shape[0] * 3 // 128 * 16 if sequences % 2 == 0 else 0
    (all_kva, all_q, all_o, all_router), (kvb_parts, chosen_all) = communicate(
        [w_kva, w_q, w_o, w_router],
        [
            w_kvb.reshape(w_kvb.shape[0], members, -1).transpose(1, 0, 2),
            jnp.broadcast_to(chosen_by.T[:, None, :], (experts, 8, tokens)),
        ],
        members,
        1,
        [split, split, split, 0],
    )
    full_kva, full_q, full_o, full_router = (
        v.reshape(-1, v.shape[2]) for v in (all_kva, all_q, all_o, all_router)
    )
    own_kvb = kvb_parts.reshape(KVR, -1)
    hidden_slice = shared_down.shape[0]
    shared = after(jnp.stack([shared_gate, shared_up], axis=1), all_q)
    shared = shared.reshape(shared.shape[0], 2, members, hidden_slice).transpose(2, 0, 1, 3)
    own_shared = exchange(shared.reshape(members, -1, 2 * hidden_slice)).reshape(width, 2 * hidden_slice)

    positions = me * tokens + jnp.arange(tokens, dtype=jnp.int32)
    cosine, sine = angles(positions, ROPE)
    normed = root_norm(inputs, attn_gain).astype(BF16)
    latent = dot(normed, full_kva)
    compressed = root_norm(latent[:, :KVR], kv_gain).astype(BF16)
    k_rope = rotate(latent[:, KVR:], cosine, sine).astype(BF16)
    q_small = dot(normed, qa_down).astype(BF16)
    query = (dot(normed, full_q) + dot(q_small, qa_up)).reshape(tokens, H, QK)
    query = jnp.concatenate(
        [query[:, :, :NOPE], rotate(query[:, :, NOPE:], cosine[:, None], sine[:, None])], axis=-1
    ).astype(BF16)
    (all_latent,), (q_packed,) = communicate(
        [jnp.concatenate([compressed, k_rope], axis=-1)], [pack(query.transpose(1, 0, 2))], members, 2
    )
    all_latent = all_latent.reshape(length, KVR + ROPE)
    q_head = unpack(q_packed).reshape(length, QK)
    expanded = dot(all_latent[:, :KVR], own_kvb).astype(BF16)
    k_head = jnp.concatenate([expanded[:, :NOPE], all_latent[:, KVR:]], axis=-1)
    v_head = expanded[:, NOPE:]
    mixture, lse = attend(prefix_len, q_head, k_head, v_head)
    _, (mixed,) = communicate([], [mixture.astype(BF16).reshape(members, tokens, VD)], members, 3)
    mixed = mixed.transpose(1, 0, 2).reshape(tokens, H * VD)
    o_small = dot(mixed, oa_down).astype(BF16)
    middle = inputs + dot(mixed, full_o) + dot(o_small, oa_up)
    ffn_in = root_norm(middle, ffn_gain).astype(BF16)
    route_probs = jax.nn.softmax(dot(ffn_in, full_router), axis=-1)

    all_c = gather(after(cotangent, q_head))
    chosen = chosen_all[:, 0] > 0.5
    order = jnp.arange(tokens, dtype=jnp.int32)
    before = (order[:, None] < order[None, :]).astype(BF16)
    rank = jnp.where(chosen, dot(chosen.astype(BF16), before), -1.0)
    back = rank[:, :, None]
    rank = jnp.broadcast_to(rank[:, None, :], (members, 8, tokens))
    weights = (expert_gate[0], expert_up_weight[0], expert_down[0], own_shared, shared_down)
    prob_blocks = jnp.broadcast_to(route_probs.T[:, None, :], (experts, 8, tokens))
    partial, *kept, prob_parts = experts_forward(
        ffn_in, prob_blocks, rank, back, *weights, slots, members, 4
    )
    ffn_out = scatter_sum(partial.reshape(length, width))
    output = (middle + ffn_out.astype(F32)).astype(BF16)
    d_own, d_route = experts_backward(
        all_c.reshape(members, tokens, width), rank, back, prob_parts, kept, *weights, slots, members, 5
    )
    d_route = d_route[:, 0].T
    d_logits = (
        route_probs * (d_route - jnp.sum(route_probs * d_route, axis=-1, keepdims=True))
    ).astype(BF16)
    d_ffn = d_own.astype(F32) + dot_t(d_logits, full_router)
    d_middle = c32 + norm_back(middle, ffn_gain, d_ffn)
    d_attn = d_middle.astype(BF16)
    grad_oup = t_dot(o_small, d_attn)
    d_osmall = dot_t(d_attn, oa_up).astype(BF16)
    grad_odown = t_dot(d_osmall, mixed)
    d_mixed = (dot_t(d_attn, full_o) + dot_t(d_osmall, oa_down)).astype(BF16)
    _, (d_head,) = communicate([], [d_mixed.reshape(tokens, H, VD).transpose(1, 0, 2)], members, 6)
    d_head = d_head.reshape(length, VD)
    delta = jnp.sum(d_head.astype(F32) * mixture, axis=-1)
    dq, dk, dv = attend_back(
        prefix_len, q_head, k_head, v_head, d_head, lse.reshape(1, length), delta.reshape(1, length)
    )
    d_expanded = jnp.concatenate([dk[:, :NOPE], dv], axis=-1).astype(BF16)
    d_latents, (d_query,) = reduce_blocks(
        jnp.concatenate([dot_t(d_expanded, own_kvb), dk[:, NOPE:]], axis=-1)
        .astype(BF16)
        .reshape(members, tokens, KVR + ROPE),
        [pack(dq.astype(BF16).reshape(members, tokens, QK))],
        members,
        7,
    )
    d_latents = d_latents.astype(F32)
    d_query = unpack(d_query).transpose(1, 0, 2).astype(F32)
    d_latent = jnp.concatenate(
        [
            norm_back(latent[:, :KVR], kv_gain, d_latents[:, :KVR]),
            unrotate(d_latents[:, KVR:], cosine, sine),
        ],
        axis=-1,
    ).astype(BF16)
    d_query = (
        jnp.concatenate(
            [d_query[:, :, :NOPE], unrotate(d_query[:, :, NOPE:], cosine[:, None], sine[:, None])],
            axis=-1,
        )
        .reshape(tokens, H * QK)
        .astype(BF16)
    )
    grad_qup = t_dot(q_small, d_query)
    d_qsmall = dot_t(d_query, qa_up).astype(BF16)
    grad_qdown = t_dot(d_qsmall, normed)
    d_normed = dot_t(d_query, full_q) + dot_t(d_qsmall, qa_down) + dot_t(d_latent, full_kva)
    grad_inputs = (d_middle + norm_back(inputs, attn_gain, d_normed)).astype(BF16)

    rank_of = qa_up.shape[0]
    parts = [
        g.astype(BF16).reshape(rank_of, members, -1).transpose(1, 0, 2)
        for g in (grad_qdown, grad_qup, grad_odown, grad_oup)
    ]
    sizes = [g.shape[2] for g in parts]
    lanes = 128
    named = jnp.broadcast_to(adapter.astype(BF16), (members, rank_of, lanes))
    shares = spread_blocks(jnp.concatenate(parts + [named], axis=-1), members, sequences, 8)
    numbers = shares[:, 0, 0, -1].astype(jnp.int32)
    share = jnp.sum(shares[..., :-lanes].astype(F32), axis=1)
    selector = (jnp.arange(q_down.shape[0], dtype=jnp.int32)[:, None] == numbers[None, :]).astype(F32)
    summed = jnp.sum(selector[:, :, None, None] * share[None], axis=1)
    ends = [sum(sizes[: n + 1]) for n in range(4)]
    outs = [summed[:, :, e - s : e] for e, s in zip(ends, sizes)]
    return (
        output[None],
        grad_inputs[None],
        outs[0].transpose(0, 2, 1),
        outs[1],
        outs[2].transpose(0, 2, 1),
        outs[3],
    )


def solution(mesh):
    seq = P("rep", "grp", None)
    rows = P("grp", None)
    in_specs = (
        (seq, seq, seq, P("rep"), P("rep"), P(), P(), P())
        + (rows,) * 8
        + (P("grp", None, None),) * 3
        + (P(),) * 4
    )
    out_specs = (
        seq,
        seq,
        P(None, "grp", None),
        P(None, None, "grp"),
        P(None, "grp", None),
        P(None, None, "grp"),
    )
    return jax.shard_map(
        per_device, mesh=mesh, in_specs=in_specs, out_specs=out_specs, check_vma=False
    )
```

```python
import functools
import math

import jax
import jax.numpy as jnp
from jax import lax
from jax.experimental import pallas as pl
from jax.experimental.pallas import tpu as pltpu
from jax.sharding import PartitionSpec as P

H = 16
NOPE = 128
ROPE = 64
VD = 128
KVR = 512
TOP = 6
QK = NOPE + ROPE
EPS = 1e-06
F32 = jnp.float32
BF16 = jnp.bfloat16


def dot(former, latter):
    return jnp.dot(former, latter, preferred_element_type=F32)


def dot_t(former, latter):
    return lax.dot_general(
        former, latter, (((1,), (1,)), ((), ())), preferred_element_type=F32
    )


def t_dot(former, latter):
    return lax.dot_general(
        former, latter, (((0,), (0,)), ((), ())), preferred_element_type=F32
    )


def root_norm(v, gains):
    factor = lax.rsqrt(jnp.mean(v * v, axis=-1, keepdims=True) + EPS)
    return v * factor * gains


def norm_back(v, gains, gradient):
    factor = lax.rsqrt(jnp.mean(v * v, axis=-1, keepdims=True) + EPS)
    weighted = gradient * gains
    return factor * weighted - v * (factor * factor * factor) * jnp.mean(
        weighted * v, axis=-1, keepdims=True
    )


def angles(positions, width):
    frequency = 10000.0 ** (-jnp.arange(0, width, 2, dtype=F32) / width)
    phases = positions.astype(F32)[:, None] * frequency[None, :]
    return (jnp.cos(phases), jnp.sin(phases))


def rotate(v, cosine, sine):
    half = v.shape[-1] // 2
    a, b = v[..., :half], v[..., half:]
    return jnp.concatenate([a * cosine - b * sine, b * cosine + a * sine], axis=-1)


def unrotate(v, cosine, sine):
    half = v.shape[-1] // 2
    a, b = v[..., :half], v[..., half:]
    return jnp.concatenate([a * cosine + b * sine, b * cosine - a * sine], axis=-1)


SIDE = 2
CORES = 2
MESH = pl.DeviceIdType.MESH


def place_of():
    me = lax.axis_index("grp")
    return me // (SIDE * CORES), (me // CORES) % SIDE, me % CORES


def index_of(z, x, c):
    return (z * SIDE + x) * CORES + c


def send(src, dst, sent, got, to):
    return pltpu.make_async_remote_copy(
        src_ref=src,
        dst_ref=dst,
        send_sem=sent,
        recv_sem=got,
        device_id=to if isinstance(to, dict) else {"grp": to},
        device_id_type=MESH,
    )


def meet(members, partner=None):
    barrier = pltpu.get_barrier_semaphore()
    me = lax.axis_index("grp")

    @pl.loop(1, members)
    def _(d):
        pl.semaphore_signal(barrier, 1, device_id={"grp": lax.rem(me + d, members)}, device_id_type=MESH)

    if partner is not None:
        pl.semaphore_signal(barrier, 1, device_id=partner, device_id_type=MESH)
    pl.semaphore_wait(barrier, members - 1 + (partner is not None))


def pick_from(table, z, s):
    v = 0
    for i, row in enumerate(table):
        for j, entry in enumerate(row):
            if entry:
                v = v + jnp.where((z == i) & (s == j), entry, 0)
    return v


def near_first(levels):
    return [sorted(range(levels), key=lambda v: (abs(v - k), v)) for k in range(levels)]


def far_first(levels):
    return [sorted((v for v in range(levels) if v != k), key=lambda v: (-abs(v - k), v)) + [k] for k in range(levels)]


class Gather:
    def __init__(self, src, out, sent, got, members, split=0):
        self.src, self.out, self.sent, self.got = src, out, sent, got
        self.members, self.split = members, split
        self.levels = members // (SIDE * CORES)
        self.z, self.x, self.c = z, x, c = place_of()
        self.me = lax.axis_index("grp")
        self.up, self.down = index_of(z + 1, x, c), index_of(z - 1, x, c)
        self.side, self.twin = index_of(z, 1 - x, c), index_of(z, x, 1 - c)
        if split:
            rows = src.shape[0]
            rep = lax.axis_index("rep")
            odd = rep % 2
            self.partner = {"rep": rep + 1 - 2 * odd, "grp": self.me}
            self.window = pl.ds(pl.multiple_of(odd * split, 16), rows - split)
            self.given = pl.ds(pl.multiple_of(odd * (rows - split), 16), split)
            self.lacked = pl.ds(pl.multiple_of((1 - odd) * (rows - split), 16), split)

    def copy(self, slot, kind, to, own=False, rows=None):
        rows = rows or (self.window if self.split else None)
        other = rows is not None and self.split and rows is not self.window
        src = self.src if own else self.out.at[slot]
        dst = self.out.at[slot]
        if rows is not None:
            src, dst = src.at[rows], dst.at[rows]
        return send(src, dst, self.sent.at[kind, slot], self.got.at[int(bool(other)), slot], to)

    def arrive(self, slot):
        self.copy(slot, 0, self.twin).wait_recv()

    def to_partner(self, slot):
        return self.copy(slot, 4, self.partner, rows=self.given)

    def lacked_to_twin(self, slot, own=False):
        return self.copy(slot, 5, self.twin, own, rows=self.lacked)

    def first(self):
        @pl.when(self.z < self.levels - 1)
        def _():
            self.copy(self.me, 0, self.up, True).start()

        @pl.when(self.z > 0)
        def _():
            self.copy(self.me, 1, self.down, True).start()

        self.copy(self.me, 2, self.side, True).start()
        self.copy(self.me, 3, self.twin, True).start()
        if self.split:
            self.lacked_to_twin(self.me, True).start()

    def relay(self, s):
        @pl.when(self.z >= s)
        def _():
            slot = index_of(self.z - s, self.x, self.c)
            self.arrive(slot)

            @pl.when(self.z < self.levels - 1)
            def _():
                self.copy(slot, 0, self.up).start()

            self.spread(slot)

        @pl.when(self.z + s < self.levels)
        def _():
            slot = index_of(self.z + s, self.x, self.c)
            self.arrive(slot)

            @pl.when(self.z > 0)
            def _():
                self.copy(slot, 1, self.down).start()

            self.spread(slot)

    def spread(self, slot):
        self.copy(slot, 2, self.side).start()
        self.copy(slot, 3, self.twin).start()
        if self.split:
            self.to_partner(slot).start()

    def pass_on(self, k):
        slot = index_of(k, 1 - self.x, self.c)
        self.arrive(slot)
        self.copy(slot, 3, self.twin).start()
        if self.split:
            self.to_partner(slot).start()

    def take_lacked(self, k, x):
        slot = index_of(k, x, self.c)

        @pl.when(slot != self.me)
        def _():
            self.copy(slot, 4, self.partner, rows=self.lacked).wait_recv()
            self.lacked_to_twin(slot).start()

    def take_twin(self, k):
        for x in range(SIDE):
            self.arrive(index_of(k, x, 1 - self.c))

    def take_twin_lacked(self):
        @pl.loop(0, self.members // CORES)
        def _(i):
            self.lacked_to_twin(i * CORES + 1 - self.c).wait_recv()

    def finish(self):
        @pl.loop(0, self.levels)
        def _(k):
            slot = index_of(k, self.x, self.c)
            self.copy(slot, 2, self.side).wait_send()

            @pl.when((k <= self.z) & (self.z < self.levels - 1))
            def _():
                self.copy(slot, 0, self.up).wait_send()

            @pl.when((k >= self.z) & (self.z > 0))
            def _():
                self.copy(slot, 1, self.down).wait_send()

        @pl.loop(0, self.members // CORES)
        def _(i):
            slot = i * CORES + self.c
            self.copy(slot, 3, self.twin).wait_send()
            if self.split:
                self.lacked_to_twin(slot).wait_send()

                @pl.when(slot != self.me)
                def _():
                    self.to_partner(slot).wait_send()


class Exchange:
    def __init__(self, src, out, sent, got, members):
        self.src, self.out, self.sent, self.got, self.members = src, out, sent, got, members
        self.me = lax.axis_index("grp")

    def copy(self, d):
        to = lax.rem(self.me + d, self.members)
        return send(self.src.at[to], self.out.at[self.me], self.sent.at[d], self.got.at[d], to)

    def start(self):
        @pl.loop(1, self.members)
        def _(d):
            self.copy(d).start()

    def wait(self):
        @pl.loop(1, self.members)
        def _(d):
            self.copy(d).wait()


def comm_kernel(*refs, members, splits, n_e):
    n_g = len(splits)
    n = n_g + n_e
    ins, outs = refs[:n], refs[n : 2 * n]
    stage = refs[2 * n : 3 * n]
    local = refs[3 * n]
    sems = refs[3 * n + 1 :]
    me = lax.axis_index("grp")
    into = [
        pltpu.make_async_copy(r if k < n_g else r.at[me], stage[k], local.at[k]) for k, r in enumerate(ins)
    ]
    out_of = [pltpu.make_async_copy(stage[k], outs[k].at[me], local.at[k]) for k in range(n)]
    gathers = [
        Gather(ins[k], outs[k], sems[2 * k], sems[2 * k + 1], members, splits[k]) for k in range(n_g)
    ]
    exchanges = [Exchange(ins[k], outs[k], sems[2 * k], sems[2 * k + 1], members) for k in range(n_g, n)]
    for copy in into:
        copy.start()
    split = [g for g in gathers if g.split]
    meet(members, split[0].partner if split else None)
    for g in gathers:
        g.first()
    for e in exchanges:
        e.start()
    for a, b in zip(into, out_of):
        a.wait()
        b.start()
    levels = members // (SIDE * CORES)
    z = me // (SIDE * CORES)
    order = near_first(levels)

    def lacked(g, s):
        k = pick_from(order, z, s)
        g.take_lacked(k, g.x)
        g.take_lacked(k, 1 - g.x)

    if gathers:

        @pl.loop(0, levels)
        def _(s):
            for g in gathers:
                g.relay(s + 1)
            for g in gathers:
                g.pass_on(pick_from(order, z, s))

            @pl.when(s >= 1)
            def _():
                for g in split:
                    lacked(g, s - 1)

    for g in split:
        lacked(g, levels - 1)
    for g in gathers:

        @pl.loop(0, levels)
        def _(k):
            g.take_twin(k)

        if g.split:
            g.take_twin_lacked()
        g.finish()
    for e in exchanges:
        e.wait()
    for copy in out_of:
        copy.wait()


def communicate(gathers, exchanges, members, collective_id, splits=None):
    gathers, exchanges = list(gathers), list(exchanges)
    n_g, n_e = len(gathers), len(exchanges)
    splits = splits or [0] * n_g
    blocks = [g.shape for g in gathers] + [e.shape[1:] for e in exchanges]
    kinds = [a.dtype for a in gathers + exchanges]
    anywhere = pl.BlockSpec(memory_space=pl.ANY)
    sem = pltpu.SemaphoreType.DMA
    moved = sum(members * b[0] * b[1] * 2 for b in blocks)
    outs = pl.pallas_call(
        functools.partial(comm_kernel, members=members, splits=tuple(splits), n_e=n_e),
        in_specs=[anywhere] * (n_g + n_e),
        out_specs=[anywhere] * (n_g + n_e),
        out_shape=[jax.ShapeDtypeStruct((members, *b), k) for b, k in zip(blocks, kinds)],
        scratch_shapes=[pltpu.VMEM(b, k) for b, k in zip(blocks, kinds)]
        + [sem((n_g + n_e,))]
        + [sem((6, members)), sem((2, members))] * n_g
        + [sem((members,)), sem((members,))] * n_e,
        compiler_params=pltpu.CompilerParams(collective_id=collective_id, has_side_effects=True),
        cost_estimate=pl.CostEstimate(flops=0, bytes_accessed=moved * 8, transcendentals=0),
        name=f"communicate_{collective_id}",
    )(*gathers, *exchanges)
    return outs[:n_g], outs[n_g:]


class Reduce:
    def __init__(self, p, twin_in, side_in, line_in, sems, members):
        self.p, self.twin_in, self.side_in, self.line_in = p, twin_in, side_in, line_in
        self.sems = sems
        self.levels = members // (SIDE * CORES)
        self.z, self.x, self.c = place_of()

    def copy(self, kind, slot, dst, n, to):
        sent, got = self.sems[2 * kind], self.sems[2 * kind + 1]
        return send(self.p.at[slot], dst.at[n], sent.at[n], got.at[n], to)

    def to_twin(self, k, w):
        twin = index_of(self.z, self.x, 1 - self.c)
        return self.copy(0, index_of(k, w, 1 - self.c), self.twin_in, k * SIDE + w, twin)

    def to_side(self, k):
        return self.copy(1, index_of(k, 1 - self.x, self.c), self.side_in, k, index_of(self.z, 1 - self.x, self.c))

    def to_up(self, k):
        return self.copy(2, index_of(k, self.x, self.c), self.line_in, k + 1, index_of(self.z + 1, self.x, self.c))

    def to_down(self, k):
        return self.copy(3, index_of(k, self.x, self.c), self.line_in, k, index_of(self.z - 1, self.x, self.c))

    def add(self, slot, ref):
        rows = self.p.shape[1]
        chunk = next(r for r in (32, 16, 8) if rows % r == 0)

        @pl.loop(0, rows // chunk)
        def _(i):
            at = pl.ds(pl.multiple_of(i * chunk, chunk), chunk)
            self.p[slot, at, :] = (self.p[slot, at, :].astype(F32) + ref[at, :].astype(F32)).astype(self.p.dtype)

    def start(self, k):
        self.to_twin(k, self.x).start()
        self.to_twin(k, 1 - self.x).start()

    def chip(self, k):
        w = 1 - self.x
        self.to_twin(k, w).wait_recv()
        self.add(index_of(k, w, self.c), self.twin_in.at[k * SIDE + w])
        self.to_side(k).start()
        self.to_twin(k, self.x).wait_recv()
        self.add(index_of(k, self.x, self.c), self.twin_in.at[k * SIDE + self.x])

    def line(self, k):
        z, mine = self.z, index_of(k, self.x, self.c)
        self.to_side(k).wait_recv()
        self.add(mine, self.side_in.at[k])

        @pl.when((k > z) & (z > 0))
        def _():
            self.to_up(k).wait_recv()
            self.add(mine, self.line_in.at[k + 1])

        @pl.when((k < z) & (z < self.levels - 1))
        def _():
            self.to_down(k).wait_recv()
            self.add(mine, self.line_in.at[k])

        @pl.when(k > z)
        def _():
            self.to_up(k).start()

        @pl.when(k < z)
        def _():
            self.to_down(k).start()

    def last(self, out):
        z, mine = self.z, index_of(self.z, self.x, self.c)
        self.to_side(z).wait_recv()
        self.add(mine, self.side_in.at[z])

        @pl.when(z > 0)
        def _():
            self.to_up(z).wait_recv()
            self.add(mine, self.line_in.at[z + 1])

        @pl.when(z < self.levels - 1)
        def _():
            self.to_down(z).wait_recv()
            self.add(mine, self.line_in.at[z])

        out[...] = self.p[mine]

    def finish(self):
        z = self.z

        @pl.loop(0, self.levels)
        def _(k):
            self.to_twin(k, 0).wait_send()
            self.to_twin(k, 1).wait_send()
            self.to_side(k).wait_send()

            @pl.when(k > z)
            def _():
                self.to_up(k).wait_send()

            @pl.when(k < z)
            def _():
                self.to_down(k).wait_send()

    @staticmethod
    def scratch(members, r, c, kind):
        levels = members // (SIDE * CORES)
        sem = pltpu.SemaphoreType.DMA
        return [
            pltpu.VMEM((members // CORES, r, c), kind),
            pltpu.VMEM((levels, r, c), kind),
            pltpu.VMEM((levels + 1, r, c), kind),
        ] + [sem((n,)) for n in (members // CORES,) * 2 + (levels,) * 2 + (levels + 1,) * 4]


def reduce_kernel(*refs, members, n_e):
    p, extra, out, landed = refs[0], refs[1 : 1 + n_e], refs[1 + n_e], refs[2 + n_e : 2 + 2 * n_e]
    bufs = refs[2 + 2 * n_e :]
    r = Reduce(p, *bufs[:3], bufs[3:11], members)
    stage, local, sems = bufs[11 : 11 + n_e], bufs[11 + n_e : 11 + 2 * n_e], bufs[11 + 2 * n_e :]
    me = lax.axis_index("grp")
    order = far_first(r.levels)
    into = [pltpu.make_async_copy(extra[k].at[me], stage[k], local[k]) for k in range(n_e)]
    out_of = [pltpu.make_async_copy(stage[k], landed[k].at[me], local[k]) for k in range(n_e)]
    exchanges = [Exchange(extra[k], landed[k], sems[2 * k], sems[2 * k + 1], members) for k in range(n_e)]
    for k in range(n_e):
        into[k].start()
    meet(members)

    @pl.loop(0, r.levels)
    def _(s):
        r.start(pick_from(order, r.z, s))

    for k in range(n_e):
        exchanges[k].start()
        into[k].wait()
        out_of[k].start()

    @pl.loop(0, r.levels)
    def _(s):
        r.chip(pick_from(order, r.z, s))

    @pl.loop(0, r.levels - 1)
    def _(s):
        r.line(pick_from(order, r.z, s))

    r.last(out)
    r.finish()
    for k in range(n_e):
        exchanges[k].wait()
        out_of[k].wait()


def reduce_blocks(p, extra, members, collective_id):
    extra = list(extra)
    n_e = len(extra)
    anywhere = pl.BlockSpec(memory_space=pl.ANY)
    _, r, c = p.shape
    sem = pltpu.SemaphoreType.DMA
    vmem = pl.BlockSpec(memory_space=pltpu.VMEM)
    out, *landed = pl.pallas_call(
        functools.partial(reduce_kernel, members=members, n_e=n_e),
        in_specs=[vmem] + [anywhere] * n_e,
        out_specs=[vmem] + [anywhere] * n_e,
        out_shape=[jax.ShapeDtypeStruct((r, c), p.dtype)] + [jax.ShapeDtypeStruct(e.shape, e.dtype) for e in extra],
        scratch_shapes=Reduce.scratch(members, r, c, p.dtype)
        + [pltpu.VMEM(e.shape[1:], e.dtype) for e in extra]
        + [sem] * n_e
        + [sem((members,)), sem((members,))] * n_e,
        compiler_params=pltpu.CompilerParams(
            collective_id=collective_id, has_side_effects=True, vmem_limit_bytes=60 * 1024 * 1024
        ),
        cost_estimate=pl.CostEstimate(flops=0, bytes_accessed=members * r * c * 16, transcendentals=0),
        name=f"reduce_{collective_id}",
    )(p, *extra)
    return out, landed


def spread_kernel(src, common, out, commons, stage, stage2, sent, got, sent2, got2, local, *, members, sequences):
    me, mine = lax.axis_index("grp"), lax.axis_index("rep")
    barrier = pltpu.get_barrier_semaphore()
    into = [
        pltpu.make_async_copy(src.at[me], stage, local.at[0]),
        pltpu.make_async_copy(common, stage2, local.at[1]),
    ]
    out_of = [
        pltpu.make_async_copy(stage, out.at[mine, me], local.at[0]),
        pltpu.make_async_copy(stage2, commons.at[mine], local.at[1]),
    ]
    for copy in into:
        copy.start()

    def other(n):
        return lax.rem(mine + n // members, sequences), lax.rem(me + n % members, members)

    @pl.loop(1, members * sequences)
    def _(n):
        r, to = other(n)
        pl.semaphore_signal(barrier, 1, device_id={"rep": r, "grp": to}, device_id_type=MESH)

    pl.semaphore_wait(barrier, members * sequences - 1)

    def block(n):
        r, to = other(n)
        return send(src.at[to], out.at[mine, me], sent.at[n], got.at[n], {"rep": r, "grp": to})

    def whole(n):
        r, to = other(n * members)
        return send(common, commons.at[mine], sent2.at[n], got2.at[n], {"rep": r, "grp": to})

    @pl.loop(1, sequences)
    def _(n):
        whole(n).start()

    @pl.loop(1, members * sequences)
    def _(n):
        block(n).start()

    for a, b in zip(into, out_of):
        a.wait()
        b.start()

    @pl.loop(1, sequences)
    def _(n):
        whole(n).wait()

    @pl.loop(1, members * sequences)
    def _(n):
        block(n).wait()

    for copy in out_of:
        copy.wait()


def spread_blocks(v, common, members, sequences, collective_id):
    anywhere = pl.BlockSpec(memory_space=pl.ANY)
    sem = pltpu.SemaphoreType.DMA
    return pl.pallas_call(
        functools.partial(spread_kernel, members=members, sequences=sequences),
        in_specs=[anywhere, anywhere],
        out_specs=[anywhere, anywhere],
        out_shape=[
            jax.ShapeDtypeStruct((sequences, *v.shape), v.dtype),
            jax.ShapeDtypeStruct((sequences, *common.shape), common.dtype),
        ],
        scratch_shapes=[
            pltpu.VMEM(v.shape[1:], v.dtype),
            pltpu.VMEM(common.shape, common.dtype),
            sem((members * sequences,)),
            sem((members * sequences,)),
            sem((sequences,)),
            sem((sequences,)),
            sem((2,)),
        ],
        compiler_params=pltpu.CompilerParams(collective_id=collective_id, has_side_effects=True),
        cost_estimate=pl.CostEstimate(flops=0, bytes_accessed=v.size * 16, transcendentals=0),
        name=f"spread_{collective_id}",
    )(v, common)


def gather(v):
    return lax.all_gather(v, "grp", axis=0, tiled=True)


def exchange(v):
    return lax.all_to_all(v, "grp", split_axis=0, concat_axis=0, tiled=True)


def scatter_sum(v):
    return lax.psum_scatter(v, "grp", scatter_dimension=0, tiled=True)


def after(v, *others):
    return lax.optimization_barrier((v, *others))[0]


def tie(v, other):
    first = other[(0,) * other.ndim]
    return v + jnp.minimum(jnp.abs(first), 0).astype(v.dtype)


def block_of(length):
    return next(b for b in (512, 384, 256, 128) if length % b == 0)


def attend_kernel(prefix_ref, q_ref, k_ref, v_ref, o_ref, lse_ref, *, block, unit):
    i = pl.program_id(0)
    prefix = prefix_ref[0]
    start = i * block
    q = q_ref[...]
    inside = start < prefix
    stop = jnp.maximum(i + 1, jnp.where(inside, (prefix + block - 1) // block, 0))
    full = (jnp.where(inside, prefix - 1, start) + 1) // block
    rows = start + lax.broadcasted_iota(jnp.int32, (block, 1), 0)
    limit = jnp.where(rows < prefix, prefix - 1, rows)

    def step(j, carry, masked):
        top, total, acc = carry
        at = pl.multiple_of(j * block, block)
        k = k_ref[pl.ds(at, block), :]
        v = v_ref[pl.ds(at, block), :]
        s = dot_t(q, k)
        if masked:
            cols = at + lax.broadcasted_iota(jnp.int32, (1, block), 1)
            s = jnp.where(cols <= limit, s, -1e30)
        fresh = jnp.maximum(top, jnp.max(s, axis=1, keepdims=True))
        p = jnp.exp2((s - fresh) * unit)
        scale = jnp.exp2((top - fresh) * unit)
        total = total * scale + jnp.sum(p, axis=1, keepdims=True)
        acc = acc * scale + dot(p.astype(BF16), v)
        return fresh, total, acc

    carry = (
        jnp.full((block, 1), -1e30, F32),
        jnp.zeros((block, 1), F32),
        jnp.zeros((block, VD), F32),
    )
    carry = lax.fori_loop(0, full, functools.partial(step, masked=False), carry)
    top, total, acc = lax.fori_loop(full, stop, functools.partial(step, masked=True), carry)
    o_ref[...] = acc / total
    lse_ref[...] = top * unit + jnp.log2(total)


def attend(prefix, q, k, v):
    length = q.shape[0]
    block = block_of(length)
    return pl.pallas_call(
        functools.partial(attend_kernel, block=block, unit=QK**-0.5 * math.log2(math.e)),
        grid=(length // block,),
        in_specs=[
            pl.BlockSpec(memory_space=pltpu.SMEM),
            pl.BlockSpec((block, QK), lambda i: (i, 0)),
            pl.BlockSpec((length, QK), lambda i: (0, 0)),
            pl.BlockSpec((length, VD), lambda i: (0, 0)),
        ],
        out_specs=[
            pl.BlockSpec((block, VD), lambda i: (i, 0)),
            pl.BlockSpec((block, 1), lambda i: (i, 0)),
        ],
        out_shape=[
            jax.ShapeDtypeStruct((length, VD), F32),
            jax.ShapeDtypeStruct((length, 1), F32),
        ],
        cost_estimate=pl.CostEstimate(
            flops=length * length * (QK + VD), bytes_accessed=length * 1000, transcendentals=length * length // 2
        ),
        name="attend",
    )(prefix, q, k, v)


def attend_back_kernel(
    prefix_ref, q_ref, k_ref, v_ref, d_ref, lse_ref, delta_ref, dq_ref, dk_ref, dv_ref, *, block, factor, unit
):
    i = pl.program_id(0)
    prefix = prefix_ref[0]
    start = i * block

    @pl.when(i == 0)
    def _():
        dk_ref[...] = jnp.zeros_like(dk_ref)
        dv_ref[...] = jnp.zeros_like(dv_ref)

    q = q_ref[...]
    d = d_ref[...]
    lse = lse_ref[...]
    delta = delta_ref[...]
    inside = start < prefix
    stop = jnp.maximum(i + 1, jnp.where(inside, (prefix + block - 1) // block, 0))
    full = (jnp.where(inside, prefix - 1, start) + 1) // block
    rows = start + lax.broadcasted_iota(jnp.int32, (1, block), 1)
    limit = jnp.where(rows < prefix, prefix - 1, rows)

    def step(j, dq, masked):
        at = pl.multiple_of(j * block, block)
        k = k_ref[pl.ds(at, block), :]
        v = v_ref[pl.ds(at, block), :]
        p = jnp.exp2(dot_t(k, q) * unit - lse)
        if masked:
            cols = at + lax.broadcasted_iota(jnp.int32, (block, 1), 0)
            p = jnp.where(cols <= limit, p, 0.0)
        dp = dot_t(v, d)
        ds = (p * (dp - delta)).astype(BF16)
        dv_ref[pl.ds(at, block), :] += dot(p.astype(BF16), d)
        dk_ref[pl.ds(at, block), :] += dot(ds, q)
        return dq + t_dot(ds, k)

    dq = lax.fori_loop(0, full, functools.partial(step, masked=False), jnp.zeros((block, QK), F32))
    dq = lax.fori_loop(full, stop, functools.partial(step, masked=True), dq)
    dq_ref[...] = (dq * factor).astype(dq_ref.dtype)

    @pl.when(i == pl.num_programs(0) - 1)
    def _():
        dk_ref[...] = dk_ref[...] * factor


def attend_back(prefix, q, k, v, d, lse, delta):
    length = q.shape[0]
    block = block_of(length)
    whole = lambda i: (0, 0)
    factor = QK**-0.5
    return pl.pallas_call(
        functools.partial(attend_back_kernel, block=block, factor=factor, unit=factor * math.log2(math.e)),
        grid=(length // block,),
        in_specs=[
            pl.BlockSpec(memory_space=pltpu.SMEM),
            pl.BlockSpec((block, QK), lambda i: (i, 0)),
            pl.BlockSpec((length, QK), whole),
            pl.BlockSpec((length, VD), whole),
            pl.BlockSpec((block, VD), lambda i: (i, 0)),
            pl.BlockSpec((1, block), lambda i: (0, i)),
            pl.BlockSpec((1, block), lambda i: (0, i)),
        ],
        out_specs=[
            pl.BlockSpec((block, QK), lambda i: (i, 0)),
            pl.BlockSpec((length, QK), whole),
            pl.BlockSpec((length, VD), whole),
        ],
        out_shape=[
            jax.ShapeDtypeStruct((length, QK), BF16),
            jax.ShapeDtypeStruct((length, QK), F32),
            jax.ShapeDtypeStruct((length, VD), F32),
        ],
        cost_estimate=pl.CostEstimate(
            flops=length * length * (3 * QK + 2 * VD), bytes_accessed=length * 2000, transcendentals=length * length // 2
        ),
        name="attend_back",
    )(prefix, q, k, v, d, lse, delta)


def silu_parts(v):
    logistic = 1.0 / (1.0 + jnp.exp(-v))
    return v * logistic, logistic * (1.0 + v * (1.0 - logistic))


def picks(rank, slots):
    at = lax.broadcasted_iota(jnp.int32, (slots, rank.shape[1]), 0).astype(F32)
    return at == rank


def picks_back(rank, slots):
    at = lax.broadcasted_iota(jnp.int32, (rank.shape[0], slots), 1).astype(F32)
    return at == rank


def tiles(width, size):
    return pl.ds(pl.multiple_of(width * size, size), size)


def experts_kernel(
    x_hbm, prob_hbm, rank_ref, back_ref, gate_hbm, up_hbm, down_hbm, own_hbm, sdown_hbm,
    part_hbm, part2_hbm, eg_hbm, eu_hbm, eo_hbm, sh_hbm, prob_out,
    xs, probs, gate, up, down, own, sdown, tail, rows, acts, sacts, part_st, eg_st, eu_st, eo_st, sh_st,
    sent, got, e_sent, e_got, load, store,
    *, members, slots, tile, wide
):
    me = lax.axis_index("grp")
    levels = members // (SIDE * CORES)
    group = SIDE * CORES
    width, hidden = gate.shape
    half, whole = hidden % tile, hidden // tile
    units = own.shape[1] // 2
    z = me // group
    order = near_first(levels)
    loads = [
        pltpu.make_async_copy(a, b, load.at[n])
        for n, (a, b) in enumerate(
            [
                (x_hbm, xs.at[me]),
                (prob_hbm.at[me], probs.at[me]),
                (own_hbm, own),
                (gate_hbm, gate),
                (up_hbm, up),
                (down_hbm, down),
                (sdown_hbm, sdown),
            ]
        )
    ]
    gather = Gather(x_hbm, xs, sent, got, members)
    exchange = Exchange(prob_hbm, probs, e_sent, e_got, members)
    for copy in loads:
        copy.start()
    meet(members)
    gather.first()
    exchange.start()
    for copy in loads:
        copy.wait()
    tail[:, :half] = gate[:, hidden - half :]
    tail[:, half:] = up[:, hidden - half :]
    gather.pass_on(z)
    gather.relay(1)
    exchange.wait()
    prob_out[...] = probs[...]

    def stores(s, k):
        n = s % 2
        return [
            pltpu.make_async_copy(a, b.at[k], store.at[n, m])
            for m, (a, b) in enumerate(
                [
                    (part_st.at[n, :, :, pl.ds(0, width // 2)], part_hbm),
                    (part_st.at[n, :, :, pl.ds(width // 2, width // 2)], part2_hbm),
                    (eg_st.at[n], eg_hbm),
                    (eu_st.at[n], eu_hbm),
                    (eo_st.at[n], eo_hbm),
                    (sh_st.at[n], sh_hbm),
                ]
            )
        ]

    @pl.loop(0, levels)
    def _(s):
        k = pick_from(order, z, s)
        n = s % 2
        gather.take_twin(k)

        @pl.when(s >= 2)
        def _():
            for copy in stores(s, pick_from(order, z, s - 2)):
                copy.wait()

        @pl.loop(0, group)
        def _(b):
            pick = picks(rank_ref[k * group + b, 0:1, :], slots).astype(BF16)
            rows[tiles(b, slots), :] = dot(pick, xs[k * group + b]).astype(BF16)

        def keep(at, g, u):
            eg_st[n, :, at] = g.astype(BF16)
            eu_st[n, :, at] = u.astype(BF16)
            acts[:, at] = (silu_parts(g)[0] * u).astype(BF16)

        @pl.loop(0, whole)
        def _(j):
            at = tiles(j, tile)
            x = rows[...]
            keep(at, dot(x, gate[:, at]), dot(x, up[:, at]))

        last = dot(rows[...], tail[...])
        keep(pl.ds(whole * tile, half), last[:, :half], last[:, half:])

        gather.relay(s + 2)

        @pl.when(s + 1 < levels)
        def _():
            gather.pass_on(pick_from(order, z, s + 1))

        @pl.loop(0, width // wide)
        def _(j):
            at = tiles(j, wide)
            eo_st[n, :, at] = dot(acts[...], down[:, at]).astype(BF16)

        @pl.loop(0, group // 2)
        def _(h):
            x = xs[pl.ds(k * group + 2 * h, 2)].reshape(-1, width)
            pre = dot(x, own[...])
            sh_st[n, pl.ds(2 * h, 2)] = pre.astype(BF16).reshape(2, -1, 2 * units)
            act = (silu_parts(pre[:, :units])[0] * pre[:, units:]).astype(BF16)
            sacts[pl.ds(2 * h, 2)] = act.reshape(2, -1, units)

        @pl.loop(0, group)
        def _(b):
            i = k * group + b
            pick = picks(rank_ref[i, 0:1, :], slots)
            back = picks_back(back_ref[i], slots).astype(BF16)
            g = jnp.sum(jnp.where(pick, probs[i, 0:1, :], 0.0), axis=1, keepdims=True)
            act = sacts[b]
            for j in range(width // wide):
                at = slice(j * wide, (j + 1) * wide)
                weighted = (g * eo_st[n, tiles(b, slots), at].astype(F32)).astype(BF16)
                part_st[n, b, :, at] = (dot(back, weighted) + dot(act, sdown[:, at])).astype(BF16)

        for copy in stores(s, k):
            copy.start()

    @pl.loop(levels - 2, levels)
    def _(s):
        for copy in stores(s, pick_from(order, z, s)):
            copy.wait()

    gather.finish()


def experts_forward(x, prob, rank, back, gate, up, down, own, sdown, slots, members, collective_id):
    tokens, width = x.shape
    hidden = gate.shape[1]
    group = SIDE * CORES
    levels = members // group
    packed = group * slots
    anywhere = pl.BlockSpec(memory_space=pl.ANY)
    vmem = pl.BlockSpec(memory_space=pltpu.VMEM)
    sem = pltpu.SemaphoreType.DMA
    tile = 256
    shapes = [
        (levels, group, tokens, width),
        (levels, packed, hidden),
        (levels, packed, hidden),
        (levels, packed, width),
        (levels, group, tokens, own.shape[1]),
    ]
    return pl.pallas_call(
        functools.partial(experts_kernel, members=members, slots=slots, tile=tile, wide=512),
        in_specs=[anywhere, anywhere, vmem, vmem] + [anywhere] * 5,
        out_specs=[anywhere] * 6 + [vmem],
        out_shape=[jax.ShapeDtypeStruct((*shapes[0][:3], width // 2), BF16)] * 2
        + [jax.ShapeDtypeStruct(s, BF16) for s in shapes[1:]] + [jax.ShapeDtypeStruct(prob.shape, F32)],
        scratch_shapes=[
            pltpu.VMEM((members, tokens, width), BF16),
            pltpu.VMEM(prob.shape, F32),
            pltpu.VMEM(gate.shape, BF16),
            pltpu.VMEM(up.shape, BF16),
            pltpu.VMEM(down.shape, BF16),
            pltpu.VMEM(own.shape, BF16),
            pltpu.VMEM(sdown.shape, BF16),
            pltpu.VMEM((width, tile), BF16),
            pltpu.VMEM((packed, width), BF16),
            pltpu.VMEM((packed, hidden), BF16),
            pltpu.VMEM((group, tokens, own.shape[1] // 2), BF16),
        ]
        + [pltpu.VMEM((2, *s[1:]), BF16) for s in shapes]
        + [sem((6, members)), sem((2, members)), sem((members,)), sem((members,)), sem((7,)), sem((2, 6))],
        compiler_params=pltpu.CompilerParams(
            collective_id=collective_id, has_side_effects=True, vmem_limit_bytes=63 * 1024 * 1024
        ),
        cost_estimate=pl.CostEstimate(
            flops=12 * members * slots * width * hidden, bytes_accessed=60_000_000, transcendentals=0
        ),
        name="experts_forward",
    )(x, prob, rank, back, gate, up, down, own, sdown)


def experts_back_kernel(
    c_hbm, c2_hbm, rank_ref, back_ref, prob_ref, eg_hbm, eu_hbm, eo_hbm, sh_hbm, gate_hbm, up_hbm, down_hbm, own_hbm, sdown_hbm,
    out, dg_out,
    part, cs, eg, eu, eo, sh, gate, up, down, own, sdown, rows, d_gate, d_up, dg_st, dg_in,
    *sems, members, slots, tile, wide
):
    twin_in, side_in, line_in = sems[:3]
    e_sent, e_got, load, fetch = sems[11:15]
    me = lax.axis_index("grp")
    levels = members // (SIDE * CORES)
    group = SIDE * CORES
    width, hidden = gate.shape
    half, whole = hidden % tile, hidden // tile
    units = own.shape[1] // 2
    z = me // group
    order = far_first(levels)
    reduce = Reduce(part, twin_in, side_in, line_in, sems[3:11], members)
    exchange = Exchange(dg_st, dg_in, e_sent, e_got, members)

    def cotangents(s):
        k = pick_from(order, z, s)
        return [
            pltpu.make_async_copy(
                a.at[k], cs.at[s % 2, :, :, pl.ds(h * (width // 2), width // 2)], fetch.at[4 + s % 2 * 2 + h]
            )
            for h, a in enumerate([c_hbm, c2_hbm])
        ]

    def kept(s):
        k = pick_from(order, z, s)
        return [
            pltpu.make_async_copy(a.at[k], b, fetch.at[m])
            for m, (a, b) in enumerate([(eo_hbm, eo), (eg_hbm, eg), (eu_hbm, eu), (sh_hbm, sh)])
        ]

    loads = [
        pltpu.make_async_copy(a, b, load.at[n])
        for n, (a, b) in enumerate(
            [(down_hbm, down), (gate_hbm, gate), (up_hbm, up), (own_hbm, own), (sdown_hbm, sdown)]
        )
    ]
    for copy in cotangents(0) + kept(0):
        copy.start()
    for copy in loads:
        copy.start()
    meet(members)

    def early(s):
        return (z == 0) | (z == levels - 1)

    @pl.loop(0, levels)
    def _(s):
        k = pick_from(order, z, s)
        n = s % 2
        for copy in cotangents(s):
            copy.wait()
        load_eo, load_eg, load_eu, load_sh = kept(s)

        @pl.when(s + 1 < levels)
        def _():
            for copy in cotangents(s + 1):
                copy.start()

        load_eo.wait()
        @pl.loop(0, group)
        def _(b):
            i = k * group + b
            at = tiles(b, slots)
            pick = picks(rank_ref[i, 0:1, :], slots)
            c = dot(pick.astype(BF16), cs[n, b])
            g = jnp.sum(jnp.where(pick, prob_ref[i, 0:1, :], 0.0), axis=1, keepdims=True)
            along = jnp.sum(c * eo[at, :].astype(F32), axis=1, keepdims=True)
            dg_st[i] = jnp.broadcast_to(
                jnp.sum(jnp.where(pick, along, 0.0), axis=0, keepdims=True), dg_st.shape[1:]
            )
            rows[at, :] = (g * c).astype(BF16)

        @pl.when(s == 0)
        def _():
            for copy in loads:
                copy.wait()

        load_eg.wait()
        load_eu.wait()

        def slopes(at):
            d = dot_t(rows[...], down[at, :])
            act, slope = silu_parts(eg[:, at].astype(F32))
            d_gate[:, at] = (d * eu[:, at].astype(F32) * slope).astype(BF16)
            d_up[:, at] = (d * act).astype(BF16)

        @pl.loop(0, whole)
        def _(j):
            slopes(tiles(j, tile))

        slopes(pl.ds(whole * tile, half))

        @pl.when(s >= 1)
        def _():
            reduce.chip(pick_from(order, z, s - 1))

        @pl.when((s >= 2) & ~early(s))
        def _():
            reduce.line(pick_from(order, z, s - 2))

        @pl.loop(0, width // tile)
        def _(j):
            at = tiles(j, tile)
            eo[:, at] = (dot_t(d_gate[...], gate[at, :]) + dot_t(d_up[...], up[at, :])).astype(BF16)

        load_sh.wait()
        @pl.loop(0, group)
        def _(b):
            i = k * group + b
            back = picks_back(back_ref[i], slots).astype(BF16)
            d = dot_t(cs[n, b], sdown[...])
            pre = sh[b].astype(F32)
            act, slope = silu_parts(pre[:, :units])
            both = jnp.concatenate([d * pre[:, units:] * slope, d * act], axis=1).astype(BF16)
            for j in range(width // wide):
                at = slice(j * wide, (j + 1) * wide)
                part[i, :, at] = (
                    dot(back, eo[tiles(b, slots), at]) + dot_t(both, own[at, :])
                ).astype(BF16)

        reduce.start(k)

        @pl.when(s + 1 < levels)
        def _():
            for copy in kept(s + 1):
                copy.start()

        @pl.when((s >= 1) & early(s))
        def _():
            reduce.line(pick_from(order, z, s - 1))

    exchange.start()
    dg_in[me] = dg_st[me]
    reduce.chip(z)

    @pl.when(~early(0))
    def _():
        reduce.line(pick_from(order, z, levels - 2))

    reduce.last(out)
    reduce.finish()
    exchange.wait()
    dg_out[...] = dg_in[...]


def experts_backward(cs, rank, back, prob, kept, gate, up, down, own, sdown, slots, members, collective_id):
    tokens, width = cs[0].shape[1], cs[0].shape[2] * 2
    hidden = gate.shape[1]
    group = SIDE * CORES
    levels = members // group
    packed = group * slots
    anywhere = pl.BlockSpec(memory_space=pl.ANY)
    vmem = pl.BlockSpec(memory_space=pltpu.VMEM)
    sem = pltpu.SemaphoreType.DMA
    eg, eu, eo, sh = kept
    return pl.pallas_call(
        functools.partial(experts_back_kernel, members=members, slots=slots, tile=256, wide=512),
        in_specs=[anywhere, anywhere, vmem, vmem, vmem] + [anywhere] * 9,
        out_specs=[vmem, vmem],
        out_shape=[
            jax.ShapeDtypeStruct((tokens, width), BF16),
            jax.ShapeDtypeStruct((members, 8, tokens), F32),
        ],
        scratch_shapes=[
            pltpu.VMEM((members, tokens, width), BF16),
            pltpu.VMEM((2, group, tokens, width), BF16),
            pltpu.VMEM(eg.shape[1:], BF16),
            pltpu.VMEM(eu.shape[1:], BF16),
            pltpu.VMEM(eo.shape[1:], BF16),
            pltpu.VMEM(sh.shape[1:], BF16),
            pltpu.VMEM(gate.shape, BF16),
            pltpu.VMEM(up.shape, BF16),
            pltpu.VMEM(down.shape, BF16),
            pltpu.VMEM(own.shape, BF16),
            pltpu.VMEM(sdown.shape, BF16),
            pltpu.VMEM((packed, width), BF16),
            pltpu.VMEM((packed, hidden), BF16),
            pltpu.VMEM((packed, hidden), BF16),
            pltpu.VMEM((members, 8, tokens), F32),
            pltpu.VMEM((members, 8, tokens), F32),
        ]
        + Reduce.scratch(members, tokens, width, BF16)
        + [sem((members,)), sem((members,)), sem((5,)), sem((8,))],
        compiler_params=pltpu.CompilerParams(
            collective_id=collective_id, has_side_effects=True, vmem_limit_bytes=67_043_328
        ),
        cost_estimate=pl.CostEstimate(
            flops=12 * members * slots * width * hidden, bytes_accessed=60_000_000, transcendentals=0
        ),
        name="experts_backward",
    )(*(c.reshape(levels, group, tokens, -1) for c in cs), rank, back, prob, *kept, gate, up, down, own, sdown)


def by_owner(gradient, members):
    return gradient.astype(BF16).reshape(gradient.shape[0], members, -1).transpose(1, 0, 2)


def pack(v):
    half = v.shape[1] // 2
    rope = jnp.concatenate([v[:, :half, NOPE:], v[:, half:, NOPE:]], axis=-1)
    return jnp.concatenate([v[:, :, :NOPE], rope], axis=1)


def unpack(v):
    rows = v.shape[1] * 2 // 3
    rope = jnp.concatenate([v[:, rows:, :ROPE], v[:, rows:, ROPE:]], axis=1)
    return jnp.concatenate([v[:, :rows], rope], axis=-1)


def per_device(
    hidden,
    grad_out,
    expert_ids,
    prefix_len,
    adapter_id,
    attn_gain,
    kv_gain,
    ffn_gain,
    w_q,
    w_kva,
    w_kvb,
    w_o,
    w_router,
    shared_gate,
    shared_up,
    shared_down,
    expert_gate,
    expert_up_weight,
    expert_down,
    q_down,
    q_up,
    o_down,
    o_up,
):
    tokens = hidden.shape[1]
    width = hidden.shape[2]
    members = lax.axis_size("grp")
    length = tokens * members
    experts = expert_gate.shape[0] * members
    capacity = tokens * TOP * 5 // (4 * experts)
    slots = -(-capacity // 16) * 16
    me = lax.axis_index("grp")

    inputs = hidden[0].astype(F32)
    cotangent = grad_out[0]
    c32 = cotangent.astype(F32)
    routes = expert_ids[0]
    adapter = adapter_id[0]
    pick = lambda table: lax.dynamic_index_in_dim(table, adapter, 0, keepdims=False)
    qa_down, qa_up, oa_down, oa_up = pick(q_down), pick(q_up), pick(o_down), pick(o_up)

    chosen_by = jnp.sum(
        (routes[:, :, None] == jnp.arange(experts, dtype=jnp.int32)[None, None, :]).astype(F32), axis=1
    )
    sequences = lax.axis_size("rep")
    split = w_q.shape[0] * 3 // 128 * 16 if sequences % 2 == 0 else 0
    (all_kva, all_q, all_o, all_router), (kvb_parts, chosen_all) = communicate(
        [w_kva, w_q, w_o, w_router],
        [
            w_kvb.reshape(w_kvb.shape[0], members, -1).transpose(1, 0, 2),
            jnp.broadcast_to(chosen_by.T[:, None, :], (experts, 8, tokens)),
        ],
        members,
        1,
        [split, split, split, 0],
    )
    full_kva, full_q, full_o, full_router = (
        v.reshape(-1, v.shape[2]) for v in (all_kva, all_q, all_o, all_router)
    )
    own_kvb = kvb_parts.reshape(KVR, -1)
    hidden_slice = shared_down.shape[0]
    shared = after(jnp.stack([shared_gate, shared_up], axis=1), all_q)
    shared = shared.reshape(shared.shape[0], 2, members, hidden_slice).transpose(2, 0, 1, 3)
    own_shared = exchange(shared.reshape(members, -1, 2 * hidden_slice)).reshape(width, 2 * hidden_slice)

    positions = me * tokens + jnp.arange(tokens, dtype=jnp.int32)
    cosine, sine = angles(positions, ROPE)
    normed = root_norm(inputs, attn_gain).astype(BF16)
    latent = dot(normed, full_kva)
    compressed = root_norm(latent[:, :KVR], kv_gain).astype(BF16)
    k_rope = rotate(latent[:, KVR:], cosine, sine).astype(BF16)
    q_small = dot(normed, qa_down).astype(BF16)
    query = (dot(normed, full_q) + dot(q_small, qa_up)).reshape(tokens, H, QK)
    query = jnp.concatenate(
        [query[:, :, :NOPE], rotate(query[:, :, NOPE:], cosine[:, None], sine[:, None])], axis=-1
    ).astype(BF16)
    (all_latent,), (q_packed,) = communicate(
        [jnp.concatenate([compressed, k_rope], axis=-1)], [after(pack(query.transpose(1, 0, 2)), own_shared)], members, 2
    )
    all_latent = all_latent.reshape(length, KVR + ROPE)
    q_head = unpack(q_packed).reshape(length, QK)
    q_head, c_first = lax.optimization_barrier((q_head, cotangent[:, : width // 2]))
    expanded = dot(all_latent[:, :KVR], own_kvb).astype(BF16)
    k_head = jnp.concatenate([expanded[:, :NOPE], all_latent[:, KVR:]], axis=-1)
    v_head = expanded[:, NOPE:]
    mixture, lse = attend(prefix_len, q_head, k_head, v_head)
    _, (mixed_parts,) = communicate([], [mixture.astype(BF16).reshape(members, tokens, VD)], members, 3)
    mixed = mixed_parts.transpose(1, 0, 2).reshape(tokens, H * VD)
    o_small = dot(mixed, oa_down).astype(BF16)
    middle = inputs + dot(mixed, full_o) + dot(o_small, oa_up)
    ffn_in = root_norm(middle, ffn_gain).astype(BF16)
    route_probs = jax.nn.softmax(dot(ffn_in, full_router), axis=-1)

    half = width // 2
    all_c = [
        gather(c_first).reshape(members, tokens, half),
        gather(tie(cotangent[:, half:], mixed_parts)).reshape(members, tokens, half),
    ]
    chosen = chosen_all[:, 0] > 0.5
    order = jnp.arange(tokens, dtype=jnp.int32)
    before = (order[:, None] < order[None, :]).astype(BF16)
    rank = jnp.where(chosen, dot(chosen.astype(BF16), before), -1.0)
    back = rank[:, :, None]
    rank = jnp.broadcast_to(rank[:, None, :], (members, 8, tokens))
    weights = (expert_gate[0], expert_up_weight[0], expert_down[0], own_shared, shared_down)
    prob_blocks = jnp.broadcast_to(route_probs.T[:, None, :], (experts, 8, tokens))
    *partial, kept_gate, kept_up, kept_out, kept_shared, prob_parts = experts_forward(
        ffn_in, prob_blocks, rank, back, *weights, slots, members, 4
    )
    kept = (kept_gate, kept_up, kept_out, kept_shared)
    partial = [part.reshape(length, half) for part in partial]
    ffn_out = [scatter_sum(partial[0])]
    d_own, d_route = experts_backward(
        all_c, rank, back, prob_parts, kept, *weights, slots, members, 5
    )
    ffn_out.append(scatter_sum(after(partial[1], d_own)))
    d_route = d_route[:, 0].T
    d_logits = (
        route_probs * (d_route - jnp.sum(route_probs * d_route, axis=-1, keepdims=True))
    ).astype(BF16)
    d_ffn = d_own.astype(F32) + dot_t(d_logits, full_router)
    d_middle = c32 + norm_back(middle, ffn_gain, d_ffn)
    d_attn = d_middle.astype(BF16)
    grad_oup = t_dot(o_small, d_attn)
    d_osmall = dot_t(d_attn, oa_up).astype(BF16)
    grad_odown = t_dot(d_osmall, mixed)
    d_mixed = (dot_t(d_attn, full_o) + dot_t(d_osmall, oa_down)).astype(BF16)
    _, (d_head,) = communicate([], [d_mixed.reshape(tokens, H, VD).transpose(1, 0, 2)], members, 6)
    d_head = d_head.reshape(length, VD)
    delta = jnp.sum(d_head.astype(F32) * mixture, axis=-1)
    dq, dk, dv = attend_back(
        prefix_len, q_head, k_head, v_head, d_head, lse.reshape(1, length), delta.reshape(1, length)
    )
    d_expanded = jnp.concatenate([dk[:, :NOPE], dv], axis=-1).astype(BF16)
    o_parts = jnp.concatenate([by_owner(g, members) for g in (grad_odown, grad_oup)], axis=-1)
    d_latents, (d_query, o_landed) = reduce_blocks(
        jnp.concatenate([dot_t(d_expanded, own_kvb), dk[:, NOPE:]], axis=-1)
        .astype(BF16)
        .reshape(members, tokens, KVR + ROPE),
        [pack(dq.reshape(members, tokens, QK)), o_parts],
        members,
        7,
    )
    d_latents = d_latents.astype(F32)
    d_query = unpack(d_query).transpose(1, 0, 2).astype(F32)
    d_latent = jnp.concatenate(
        [
            norm_back(latent[:, :KVR], kv_gain, d_latents[:, :KVR]),
            unrotate(d_latents[:, KVR:], cosine, sine),
        ],
        axis=-1,
    ).astype(BF16)
    d_query = (
        jnp.concatenate(
            [d_query[:, :, :NOPE], unrotate(d_query[:, :, NOPE:], cosine[:, None], sine[:, None])],
            axis=-1,
        )
        .reshape(tokens, H * QK)
        .astype(BF16)
    )
    first, second, _ = lax.optimization_barrier((*ffn_out, d_query))
    output = (middle + jnp.concatenate([first, second], axis=-1).astype(F32)).astype(BF16)
    grad_qup = t_dot(q_small, d_query)
    d_qsmall = dot_t(d_query, qa_up).astype(BF16)
    grad_qdown = t_dot(d_qsmall, normed)
    d_normed = dot_t(d_query, full_q) + dot_t(d_qsmall, qa_down) + dot_t(d_latent, full_kva)
    grad_inputs = (d_middle + norm_back(inputs, attn_gain, d_normed)).astype(BF16)

    q_parts = jnp.concatenate([by_owner(g, members) for g in (grad_qdown, grad_qup)], axis=-1)
    o_share = jnp.sum(o_landed.astype(F32), axis=0)
    named = jnp.broadcast_to(adapter.astype(F32), (o_share.shape[0], 128))
    q_shares, o_shares = spread_blocks(
        q_parts, jnp.concatenate([o_share, named], axis=-1), members, sequences, 8
    )
    numbers = o_shares[:, 0, -1].astype(jnp.int32)
    shares = jnp.concatenate([jnp.sum(q_shares.astype(F32), axis=1), o_shares[:, :, :-128]], axis=-1)
    selector = (jnp.arange(q_down.shape[0], dtype=jnp.int32)[:, None] == numbers[None, :]).astype(F32)
    summed = jnp.sum(selector[:, :, None, None] * shares[None], axis=1)
    sizes = [g.shape[1] // members for g in (grad_qdown, grad_qup, grad_odown, grad_oup)]
    ends = [sum(sizes[: n + 1]) for n in range(4)]
    outs = [summed[:, :, e - s : e] for e, s in zip(ends, sizes)]
    return (
        output[None],
        grad_inputs[None],
        outs[0].transpose(0, 2, 1),
        outs[1],
        outs[2].transpose(0, 2, 1),
        outs[3],
    )


def solution(mesh):
    seq = P("rep", "grp", None)
    rows = P("grp", None)
    in_specs = (
        (seq, seq, seq, P("rep"), P("rep"), P(), P(), P())
        + (rows,) * 8
        + (P("grp", None, None),) * 3
        + (P(),) * 4
    )
    out_specs = (
        seq,
        seq,
        P(None, "grp", None),
        P(None, None, "grp"),
        P(None, "grp", None),
        P(None, None, "grp"),
    )
    return jax.shard_map(
        per_device, mesh=mesh, in_specs=in_specs, out_specs=out_specs, check_vma=False
    )
```

```python
import functools
import math

import jax
import jax.numpy as jnp
from jax import lax
from jax.experimental import pallas as pl
from jax.experimental.pallas import tpu as pltpu
from jax.sharding import PartitionSpec as P

H = 16
NOPE = 128
ROPE = 64
VD = 128
KVR = 512
TOP = 6
QK = NOPE + ROPE
EPS = 1e-06
F32 = jnp.float32
BF16 = jnp.bfloat16


def dot(former, latter):
    return jnp.dot(former, latter, preferred_element_type=F32)


def dot_t(former, latter):
    return lax.dot_general(
        former, latter, (((1,), (1,)), ((), ())), preferred_element_type=F32
    )


def t_dot(former, latter):
    return lax.dot_general(
        former, latter, (((0,), (0,)), ((), ())), preferred_element_type=F32
    )


def root_norm(v, gains):
    factor = lax.rsqrt(jnp.mean(v * v, axis=-1, keepdims=True) + EPS)
    return v * factor * gains


def norm_back(v, gains, gradient):
    factor = lax.rsqrt(jnp.mean(v * v, axis=-1, keepdims=True) + EPS)
    weighted = gradient * gains
    return factor * weighted - v * (factor * factor * factor) * jnp.mean(
        weighted * v, axis=-1, keepdims=True
    )


def angles(positions, width):
    frequency = 10000.0 ** (-jnp.arange(0, width, 2, dtype=F32) / width)
    phases = positions.astype(F32)[:, None] * frequency[None, :]
    return (jnp.cos(phases), jnp.sin(phases))


def rotate(v, cosine, sine):
    half = v.shape[-1] // 2
    a, b = v[..., :half], v[..., half:]
    return jnp.concatenate([a * cosine - b * sine, b * cosine + a * sine], axis=-1)


def unrotate(v, cosine, sine):
    half = v.shape[-1] // 2
    a, b = v[..., :half], v[..., half:]
    return jnp.concatenate([a * cosine + b * sine, b * cosine - a * sine], axis=-1)


SIDE = 2
CORES = 2
MESH = pl.DeviceIdType.MESH


def place_of():
    me = lax.axis_index("grp")
    return me // (SIDE * CORES), (me // CORES) % SIDE, me % CORES


def index_of(z, x, c):
    return (z * SIDE + x) * CORES + c


def send(src, dst, sent, got, to):
    return pltpu.make_async_remote_copy(
        src_ref=src,
        dst_ref=dst,
        send_sem=sent,
        recv_sem=got,
        device_id=to if isinstance(to, dict) else {"grp": to},
        device_id_type=MESH,
    )


def meet(members, partner=None):
    barrier = pltpu.get_barrier_semaphore()
    me = lax.axis_index("grp")

    @pl.loop(1, members)
    def _(d):
        pl.semaphore_signal(barrier, 1, device_id={"grp": lax.rem(me + d, members)}, device_id_type=MESH)

    if partner is not None:
        pl.semaphore_signal(barrier, 1, device_id=partner, device_id_type=MESH)
    pl.semaphore_wait(barrier, members - 1 + (partner is not None))


def pick_from(table, z, s):
    v = 0
    for i, row in enumerate(table):
        for j, entry in enumerate(row):
            if entry:
                v = v + jnp.where((z == i) & (s == j), entry, 0)
    return v


def near_first(levels):
    return [sorted(range(levels), key=lambda v: (abs(v - k), v)) for k in range(levels)]


def far_first(levels):
    return [sorted((v for v in range(levels) if v != k), key=lambda v: (-abs(v - k), v)) + [k] for k in range(levels)]


class Gather:
    def __init__(self, src, out, sent, got, members, split=0):
        self.src, self.out, self.sent, self.got = src, out, sent, got
        self.members, self.split = members, split
        self.levels = members // (SIDE * CORES)
        self.z, self.x, self.c = z, x, c = place_of()
        self.me = lax.axis_index("grp")
        self.up, self.down = index_of(z + 1, x, c), index_of(z - 1, x, c)
        self.side, self.twin = index_of(z, 1 - x, c), index_of(z, x, 1 - c)
        if split:
            rows = src.shape[0]
            rep = lax.axis_index("rep")
            odd = rep % 2
            self.partner = {"rep": rep + 1 - 2 * odd, "grp": self.me}
            self.window = pl.ds(pl.multiple_of(odd * split, 16), rows - split)
            self.given = pl.ds(pl.multiple_of(odd * (rows - split), 16), split)
            self.lacked = pl.ds(pl.multiple_of((1 - odd) * (rows - split), 16), split)

    def copy(self, slot, kind, to, own=False, rows=None):
        rows = rows or (self.window if self.split else None)
        other = rows is not None and self.split and rows is not self.window
        src = self.src if own else self.out.at[slot]
        dst = self.out.at[slot]
        if rows is not None:
            src, dst = src.at[rows], dst.at[rows]
        return send(src, dst, self.sent.at[kind, slot], self.got.at[int(bool(other)), slot], to)

    def arrive(self, slot):
        self.copy(slot, 0, self.twin).wait_recv()

    def to_partner(self, slot):
        return self.copy(slot, 4, self.partner, rows=self.given)

    def lacked_to_twin(self, slot, own=False):
        return self.copy(slot, 5, self.twin, own, rows=self.lacked)

    def first(self):
        @pl.when(self.z < self.levels - 1)
        def _():
            self.copy(self.me, 0, self.up, True).start()

        @pl.when(self.z > 0)
        def _():
            self.copy(self.me, 1, self.down, True).start()

        self.copy(self.me, 2, self.side, True).start()
        self.copy(self.me, 3, self.twin, True).start()
        if self.split:
            self.lacked_to_twin(self.me, True).start()

    def relay(self, s):
        @pl.when(self.z >= s)
        def _():
            slot = index_of(self.z - s, self.x, self.c)
            self.arrive(slot)

            @pl.when(self.z < self.levels - 1)
            def _():
                self.copy(slot, 0, self.up).start()

            self.spread(slot)

        @pl.when(self.z + s < self.levels)
        def _():
            slot = index_of(self.z + s, self.x, self.c)
            self.arrive(slot)

            @pl.when(self.z > 0)
            def _():
                self.copy(slot, 1, self.down).start()

            self.spread(slot)

    def spread(self, slot):
        self.copy(slot, 2, self.side).start()
        self.copy(slot, 3, self.twin).start()
        if self.split:
            self.to_partner(slot).start()

    def pass_on(self, k):
        slot = index_of(k, 1 - self.x, self.c)
        self.arrive(slot)
        self.copy(slot, 3, self.twin).start()
        if self.split:
            self.to_partner(slot).start()

    def take_lacked(self, k, x):
        slot = index_of(k, x, self.c)

        @pl.when(slot != self.me)
        def _():
            self.copy(slot, 4, self.partner, rows=self.lacked).wait_recv()
            self.lacked_to_twin(slot).start()

    def take_twin(self, k):
        for x in range(SIDE):
            self.arrive(index_of(k, x, 1 - self.c))

    def take_twin_lacked(self):
        @pl.loop(0, self.members // CORES)
        def _(i):
            self.lacked_to_twin(i * CORES + 1 - self.c).wait_recv()

    def finish(self):
        @pl.loop(0, self.levels)
        def _(k):
            slot = index_of(k, self.x, self.c)
            self.copy(slot, 2, self.side).wait_send()

            @pl.when((k <= self.z) & (self.z < self.levels - 1))
            def _():
                self.copy(slot, 0, self.up).wait_send()

            @pl.when((k >= self.z) & (self.z > 0))
            def _():
                self.copy(slot, 1, self.down).wait_send()

        @pl.loop(0, self.members // CORES)
        def _(i):
            slot = i * CORES + self.c
            self.copy(slot, 3, self.twin).wait_send()
            if self.split:
                self.lacked_to_twin(slot).wait_send()

                @pl.when(slot != self.me)
                def _():
                    self.to_partner(slot).wait_send()


class Exchange:
    def __init__(self, src, out, sent, got, members):
        self.src, self.out, self.sent, self.got, self.members = src, out, sent, got, members
        self.me = lax.axis_index("grp")

    def copy(self, d):
        to = lax.rem(self.me + d, self.members)
        return send(self.src.at[to], self.out.at[self.me], self.sent.at[d], self.got.at[d], to)

    def start(self):
        @pl.loop(1, self.members)
        def _(d):
            self.copy(d).start()

    def wait(self):
        @pl.loop(1, self.members)
        def _(d):
            self.copy(d).wait()


def comm_kernel(*refs, members, splits, n_e):
    n_g = len(splits)
    n = n_g + n_e
    ins, outs = refs[:n], refs[n : 2 * n]
    stage = refs[2 * n : 3 * n]
    local = refs[3 * n]
    sems = refs[3 * n + 1 :]
    me = lax.axis_index("grp")
    into = [
        pltpu.make_async_copy(r if k < n_g else r.at[me], stage[k], local.at[k]) for k, r in enumerate(ins)
    ]
    out_of = [pltpu.make_async_copy(stage[k], outs[k].at[me], local.at[k]) for k in range(n)]
    gathers = [
        Gather(ins[k], outs[k], sems[2 * k], sems[2 * k + 1], members, splits[k]) for k in range(n_g)
    ]
    exchanges = [Exchange(ins[k], outs[k], sems[2 * k], sems[2 * k + 1], members) for k in range(n_g, n)]
    for copy in into:
        copy.start()
    split = [g for g in gathers if g.split]
    meet(members, split[0].partner if split else None)
    for g in gathers:
        g.first()
    for e in exchanges:
        e.start()
    for a, b in zip(into, out_of):
        a.wait()
        b.start()
    levels = members // (SIDE * CORES)
    z = me // (SIDE * CORES)
    order = near_first(levels)

    def lacked(g, s):
        k = pick_from(order, z, s)
        g.take_lacked(k, g.x)
        g.take_lacked(k, 1 - g.x)

    if gathers:

        @pl.loop(0, levels)
        def _(s):
            for g in gathers:
                g.relay(s + 1)
            for g in gathers:
                g.pass_on(pick_from(order, z, s))

            @pl.when(s >= 1)
            def _():
                for g in split:
                    lacked(g, s - 1)

    for g in split:
        lacked(g, levels - 1)
    for g in gathers:

        @pl.loop(0, levels)
        def _(k):
            g.take_twin(k)

        if g.split:
            g.take_twin_lacked()
        g.finish()
    for e in exchanges:
        e.wait()
    for copy in out_of:
        copy.wait()


def communicate(gathers, exchanges, members, collective_id, splits=None):
    gathers, exchanges = list(gathers), list(exchanges)
    n_g, n_e = len(gathers), len(exchanges)
    splits = splits or [0] * n_g
    blocks = [g.shape for g in gathers] + [e.shape[1:] for e in exchanges]
    kinds = [a.dtype for a in gathers + exchanges]
    anywhere = pl.BlockSpec(memory_space=pl.ANY)
    sem = pltpu.SemaphoreType.DMA
    moved = sum(members * b[0] * b[1] * 2 for b in blocks)
    outs = pl.pallas_call(
        functools.partial(comm_kernel, members=members, splits=tuple(splits), n_e=n_e),
        in_specs=[anywhere] * (n_g + n_e),
        out_specs=[anywhere] * (n_g + n_e),
        out_shape=[jax.ShapeDtypeStruct((members, *b), k) for b, k in zip(blocks, kinds)],
        scratch_shapes=[pltpu.VMEM(b, k) for b, k in zip(blocks, kinds)]
        + [sem((n_g + n_e,))]
        + [sem((6, members)), sem((2, members))] * n_g
        + [sem((members,)), sem((members,))] * n_e,
        compiler_params=pltpu.CompilerParams(collective_id=collective_id, has_side_effects=True),
        cost_estimate=pl.CostEstimate(flops=0, bytes_accessed=moved * 8, transcendentals=0),
        name=f"communicate_{collective_id}",
    )(*gathers, *exchanges)
    return outs[:n_g], outs[n_g:]


class Reduce:
    def __init__(self, p, twin_in, side_in, line_in, sems, members):
        self.p, self.twin_in, self.side_in, self.line_in = p, twin_in, side_in, line_in
        self.sems = sems
        self.levels = members // (SIDE * CORES)
        self.z, self.x, self.c = place_of()

    def copy(self, kind, slot, dst, n, to):
        sent, got = self.sems[2 * kind], self.sems[2 * kind + 1]
        return send(self.p.at[slot], dst.at[n], sent.at[n], got.at[n], to)

    def to_twin(self, k, w):
        twin = index_of(self.z, self.x, 1 - self.c)
        return self.copy(0, index_of(k, w, 1 - self.c), self.twin_in, k * SIDE + w, twin)

    def to_side(self, k):
        return self.copy(1, index_of(k, 1 - self.x, self.c), self.side_in, k, index_of(self.z, 1 - self.x, self.c))

    def to_up(self, k):
        return self.copy(2, index_of(k, self.x, self.c), self.line_in, k + 1, index_of(self.z + 1, self.x, self.c))

    def to_down(self, k):
        return self.copy(3, index_of(k, self.x, self.c), self.line_in, k, index_of(self.z - 1, self.x, self.c))

    def add(self, slot, ref):
        rows = self.p.shape[1]
        chunk = next(r for r in (32, 16, 8) if rows % r == 0)

        @pl.loop(0, rows // chunk)
        def _(i):
            at = pl.ds(pl.multiple_of(i * chunk, chunk), chunk)
            self.p[slot, at, :] = (self.p[slot, at, :].astype(F32) + ref[at, :].astype(F32)).astype(self.p.dtype)

    def start(self, k):
        self.to_twin(k, self.x).start()
        self.to_twin(k, 1 - self.x).start()

    def chip(self, k):
        w = 1 - self.x
        self.to_twin(k, w).wait_recv()
        self.add(index_of(k, w, self.c), self.twin_in.at[k * SIDE + w])
        self.to_side(k).start()
        self.to_twin(k, self.x).wait_recv()
        self.add(index_of(k, self.x, self.c), self.twin_in.at[k * SIDE + self.x])

    def line(self, k):
        z, mine = self.z, index_of(k, self.x, self.c)
        self.to_side(k).wait_recv()
        self.add(mine, self.side_in.at[k])

        @pl.when((k > z) & (z > 0))
        def _():
            self.to_up(k).wait_recv()
            self.add(mine, self.line_in.at[k + 1])

        @pl.when((k < z) & (z < self.levels - 1))
        def _():
            self.to_down(k).wait_recv()
            self.add(mine, self.line_in.at[k])

        @pl.when(k > z)
        def _():
            self.to_up(k).start()

        @pl.when(k < z)
        def _():
            self.to_down(k).start()

    def last(self, out):
        z, mine = self.z, index_of(self.z, self.x, self.c)
        self.to_side(z).wait_recv()
        self.add(mine, self.side_in.at[z])

        @pl.when(z > 0)
        def _():
            self.to_up(z).wait_recv()
            self.add(mine, self.line_in.at[z + 1])

        @pl.when(z < self.levels - 1)
        def _():
            self.to_down(z).wait_recv()
            self.add(mine, self.line_in.at[z])

        out[...] = self.p[mine]

    def finish(self):
        z = self.z

        @pl.loop(0, self.levels)
        def _(k):
            self.to_twin(k, 0).wait_send()
            self.to_twin(k, 1).wait_send()
            self.to_side(k).wait_send()

            @pl.when(k > z)
            def _():
                self.to_up(k).wait_send()

            @pl.when(k < z)
            def _():
                self.to_down(k).wait_send()

    @staticmethod
    def scratch(members, r, c, kind):
        levels = members // (SIDE * CORES)
        sem = pltpu.SemaphoreType.DMA
        return [
            pltpu.VMEM((members // CORES, r, c), kind),
            pltpu.VMEM((levels, r, c), kind),
            pltpu.VMEM((levels + 1, r, c), kind),
        ] + [sem((n,)) for n in (members // CORES,) * 2 + (levels,) * 2 + (levels + 1,) * 4]


def reduce_kernel(*refs, members, n_e):
    p, extra, out, landed = refs[0], refs[1 : 1 + n_e], refs[1 + n_e], refs[2 + n_e : 2 + 2 * n_e]
    bufs = refs[2 + 2 * n_e :]
    r = Reduce(p, *bufs[:3], bufs[3:11], members)
    stage, local, sems = bufs[11 : 11 + n_e], bufs[11 + n_e : 11 + 2 * n_e], bufs[11 + 2 * n_e :]
    me = lax.axis_index("grp")
    order = far_first(r.levels)
    into = [pltpu.make_async_copy(extra[k].at[me], stage[k], local[k]) for k in range(n_e)]
    out_of = [pltpu.make_async_copy(stage[k], landed[k].at[me], local[k]) for k in range(n_e)]
    exchanges = [Exchange(extra[k], landed[k], sems[2 * k], sems[2 * k + 1], members) for k in range(n_e)]
    for k in range(n_e):
        into[k].start()
    meet(members)

    @pl.loop(0, r.levels)
    def _(s):
        r.start(pick_from(order, r.z, s))

    for k in range(n_e):
        exchanges[k].start()
        into[k].wait()
        out_of[k].start()

    @pl.loop(0, r.levels)
    def _(s):
        r.chip(pick_from(order, r.z, s))

    @pl.loop(0, r.levels - 1)
    def _(s):
        r.line(pick_from(order, r.z, s))

    r.last(out)
    r.finish()
    for k in range(n_e):
        exchanges[k].wait()
        out_of[k].wait()


def reduce_blocks(p, extra, members, collective_id):
    extra = list(extra)
    n_e = len(extra)
    anywhere = pl.BlockSpec(memory_space=pl.ANY)
    _, r, c = p.shape
    sem = pltpu.SemaphoreType.DMA
    vmem = pl.BlockSpec(memory_space=pltpu.VMEM)
    out, *landed = pl.pallas_call(
        functools.partial(reduce_kernel, members=members, n_e=n_e),
        in_specs=[vmem] + [anywhere] * n_e,
        out_specs=[vmem] + [anywhere] * n_e,
        out_shape=[jax.ShapeDtypeStruct((r, c), p.dtype)] + [jax.ShapeDtypeStruct(e.shape, e.dtype) for e in extra],
        scratch_shapes=Reduce.scratch(members, r, c, p.dtype)
        + [pltpu.VMEM(e.shape[1:], e.dtype) for e in extra]
        + [sem] * n_e
        + [sem((members,)), sem((members,))] * n_e,
        compiler_params=pltpu.CompilerParams(
            collective_id=collective_id, has_side_effects=True, vmem_limit_bytes=60 * 1024 * 1024
        ),
        cost_estimate=pl.CostEstimate(flops=0, bytes_accessed=members * r * c * 16, transcendentals=0),
        name=f"reduce_{collective_id}",
    )(p, *extra)
    return out, landed


def spread_kernel(src, common, out, commons, stage, stage2, sent, got, sent2, got2, local, *, members, sequences):
    me, mine = lax.axis_index("grp"), lax.axis_index("rep")
    barrier = pltpu.get_barrier_semaphore()
    into = [
        pltpu.make_async_copy(src.at[me], stage, local.at[0]),
        pltpu.make_async_copy(common, stage2, local.at[1]),
    ]
    out_of = [
        pltpu.make_async_copy(stage, out.at[mine, me], local.at[0]),
        pltpu.make_async_copy(stage2, commons.at[mine], local.at[1]),
    ]
    for copy in into:
        copy.start()

    def other(n):
        return lax.rem(mine + n // members, sequences), lax.rem(me + n % members, members)

    @pl.loop(1, members * sequences)
    def _(n):
        r, to = other(n)
        pl.semaphore_signal(barrier, 1, device_id={"rep": r, "grp": to}, device_id_type=MESH)

    pl.semaphore_wait(barrier, members * sequences - 1)

    def block(n):
        r, to = other(n)
        return send(src.at[to], out.at[mine, me], sent.at[n], got.at[n], {"rep": r, "grp": to})

    def whole(n):
        r, to = other(n * members)
        return send(common, commons.at[mine], sent2.at[n], got2.at[n], {"rep": r, "grp": to})

    @pl.loop(1, sequences)
    def _(n):
        whole(n).start()

    @pl.loop(1, members * sequences)
    def _(n):
        block(n).start()

    for a, b in zip(into, out_of):
        a.wait()
        b.start()

    @pl.loop(1, sequences)
    def _(n):
        whole(n).wait()

    @pl.loop(1, members * sequences)
    def _(n):
        block(n).wait()

    for copy in out_of:
        copy.wait()


def spread_blocks(v, common, members, sequences, collective_id):
    anywhere = pl.BlockSpec(memory_space=pl.ANY)
    sem = pltpu.SemaphoreType.DMA
    return pl.pallas_call(
        functools.partial(spread_kernel, members=members, sequences=sequences),
        in_specs=[anywhere, anywhere],
        out_specs=[anywhere, anywhere],
        out_shape=[
            jax.ShapeDtypeStruct((sequences, *v.shape), v.dtype),
            jax.ShapeDtypeStruct((sequences, *common.shape), common.dtype),
        ],
        scratch_shapes=[
            pltpu.VMEM(v.shape[1:], v.dtype),
            pltpu.VMEM(common.shape, common.dtype),
            sem((members * sequences,)),
            sem((members * sequences,)),
            sem((sequences,)),
            sem((sequences,)),
            sem((2,)),
        ],
        compiler_params=pltpu.CompilerParams(collective_id=collective_id, has_side_effects=True),
        cost_estimate=pl.CostEstimate(flops=0, bytes_accessed=v.size * 16, transcendentals=0),
        name=f"spread_{collective_id}",
    )(v, common)


def gather(v):
    return lax.all_gather(v, "grp", axis=0, tiled=True)


def exchange(v):
    return lax.all_to_all(v, "grp", split_axis=0, concat_axis=0, tiled=True)


def scatter_sum(v):
    return lax.psum_scatter(v, "grp", scatter_dimension=0, tiled=True)


def after(v, *others):
    return lax.optimization_barrier((v, *others))[0]


def tie(v, other):
    first = other[(0,) * other.ndim]
    return v + jnp.minimum(jnp.abs(first), 0).astype(v.dtype)


def key_blocks(start, rows, keys, length):
    end = start + rows
    end = jnp.where(start < length // 2, jnp.maximum(end, length // 2), end)
    return (start + 1) // keys, (end + keys - 1) // keys


def attend_kernel(prefix_ref, q_ref, k_ref, v_ref, o_ref, lse_ref, mixed, blocks, sent, got, local, *, members, unit):
    me = lax.axis_index("grp")
    tokens = blocks.shape[1]
    block, keys = 2 * tokens, 4 * tokens
    turns = members // 2
    prefix = prefix_ref[0]

    def block_to(n):
        return send(blocks.at[n], mixed.at[me], sent.at[n], got.at[me], n)

    def from_device(n):
        return send(blocks.at[n], mixed.at[n], sent.at[n], got.at[n], n)

    own = pltpu.make_async_copy(blocks.at[me], mixed.at[me], local)
    meet(members)

    @pl.loop(0, turns)
    def _(n):
        i = lax.rem(me // 2 + n, turns)
        start = pl.multiple_of(i * block, block)
        here = pl.ds(start, block)
        q = q_ref[here, :]
        rows = start + lax.broadcasted_iota(jnp.int32, (block, 1), 0)
        limit = jnp.where(rows < prefix, prefix - 1, rows)
        limit = jnp.maximum(limit, rows)

        def step(j, carry, masked):
            top, total, acc = carry
            at = pl.multiple_of(j * keys, keys)
            k = k_ref[pl.ds(at, keys), :]
            v = v_ref[pl.ds(at, keys), :]
            s = dot_t(q, k)
            if masked:
                cols = at + lax.broadcasted_iota(jnp.int32, (1, keys), 1)
                s = jnp.where(cols <= limit, s, -1e30)
            fresh = jnp.maximum(top, jnp.max(s, axis=1, keepdims=True))
            p = jnp.exp2((s - fresh) * unit)
            scale = jnp.exp2((top - fresh) * unit)
            total = total * scale + jnp.sum(p, axis=1, keepdims=True)
            acc = acc * scale + dot(p.astype(BF16), v)
            return fresh, total, acc

        carry = (
            jnp.full((block, 1), -1e30, F32),
            jnp.zeros((block, 1), F32),
            jnp.zeros((block, VD), F32),
        )
        full, stop = key_blocks(start, block, keys, q_ref.shape[0])
        carry = lax.fori_loop(0, full, functools.partial(step, masked=False), carry)
        top, total, acc = lax.fori_loop(full, stop, functools.partial(step, masked=True), carry)
        o = acc / total
        o_ref[here, :] = o
        lse_ref[here, :] = top * unit + jnp.log2(total)
        blocks[pl.ds(2 * i, 2)] = o.astype(BF16).reshape(2, tokens, VD)
        for t in range(2):
            to = 2 * i + t

            @pl.when(to == me)
            def _():
                own.start()

            @pl.when(to != me)
            def _():
                block_to(to).start()

    own.wait()

    @pl.loop(1, members)
    def _(d):
        n = lax.rem(me + d, members)
        from_device(n).wait_recv()
        block_to(n).wait_send()


def attend(prefix, q, k, v, members, collective_id):
    length = q.shape[0]
    tokens = length // members
    vmem = pl.BlockSpec(memory_space=pltpu.VMEM)
    sem = pltpu.SemaphoreType.DMA
    return pl.pallas_call(
        functools.partial(attend_kernel, members=members, unit=QK**-0.5 * math.log2(math.e)),
        in_specs=[pl.BlockSpec(memory_space=pltpu.SMEM), vmem, vmem, vmem],
        out_specs=[vmem, vmem, pl.BlockSpec(memory_space=pl.ANY)],
        out_shape=[
            jax.ShapeDtypeStruct((length, VD), F32),
            jax.ShapeDtypeStruct((length, 1), F32),
            jax.ShapeDtypeStruct((members, tokens, VD), BF16),
        ],
        scratch_shapes=[pltpu.VMEM((members, tokens, VD), BF16), sem((members,)), sem((members,)), sem],
        compiler_params=pltpu.CompilerParams(
            collective_id=collective_id, has_side_effects=True, vmem_limit_bytes=40 * 1024 * 1024
        ),
        cost_estimate=pl.CostEstimate(
            flops=length * length * (QK + VD), bytes_accessed=length * 1000, transcendentals=length * length // 2
        ),
        name="attend",
    )(prefix, q, k, v)


def attend_back_kernel(
    prefix_ref, q_ref, k_ref, v_ref, o_ref, lse_ref, d_hbm, kvb_ref, part_ref, dq_out,
    ds_in, blocks, dk, dv, sent, got, q_sent, q_got, local, local2,
    *, members, factor, unit
):
    me = lax.axis_index("grp")
    tokens = blocks.shape[1] * 2 // 3
    block, keys = 2 * tokens, 4 * tokens
    turns = members // 2
    prefix = prefix_ref[0]
    exchange = Exchange(d_hbm, ds_in, sent, got, members)
    into = pltpu.make_async_copy(d_hbm.at[me], ds_in.at[me], local)
    own = pltpu.make_async_copy(blocks.at[me], dq_out.at[me], local2)

    def block_to(n):
        return send(blocks.at[n], dq_out.at[me], q_sent.at[n], q_got.at[me], n)

    def from_device(n):
        return send(blocks.at[n], dq_out.at[n], q_sent.at[n], q_got.at[n], n)

    into.start()
    meet(members)
    exchange.start()
    dk[...] = jnp.zeros_like(dk)
    dv[...] = jnp.zeros_like(dv)
    into.wait()

    @pl.loop(0, turns)
    def _(n):
        i = lax.rem(me // 2 + n, turns)
        start = pl.multiple_of(i * block, block)
        here = pl.ds(start, block)
        for t in range(2):
            source = 2 * i + t

            @pl.when(source != me)
            def _():
                send(ds_in.at[source], ds_in.at[source], sent.at[0], got.at[lax.rem(me - source + members, members)], source).wait_recv()

        d = ds_in[pl.ds(2 * i, 2)].reshape(block, VD)
        q = q_ref[here, :]
        lse = lse_ref[pl.ds(i, 1), 0, :]
        along = d.astype(F32) * o_ref[here, :]
        high = along.astype(BF16)
        low = (along - high.astype(F32)).astype(BF16)
        ones = jnp.ones((8, VD), BF16)
        delta = (dot_t(ones, high) + dot_t(ones, low))[0:1, :]
        rows = start + lax.broadcasted_iota(jnp.int32, (1, block), 1)
        limit = jnp.maximum(jnp.where(rows < prefix, prefix - 1, rows), rows)

        def step(j, dq, masked):
            at = pl.multiple_of(j * keys, keys)
            k = k_ref[pl.ds(at, keys), :]
            v = v_ref[pl.ds(at, keys), :]
            p = jnp.exp2(dot_t(k, q) * unit - lse)
            if masked:
                cols = at + lax.broadcasted_iota(jnp.int32, (keys, 1), 0)
                p = jnp.where(cols <= limit, p, 0.0)
            dp = dot_t(v, d)
            ds = (p * (dp - delta)).astype(BF16)
            dv[pl.ds(at, keys), :] += dot(p.astype(BF16), d)
            dk[pl.ds(at, keys), :] += dot(ds, q)
            return dq + t_dot(ds, k)

        full, stop = key_blocks(start, block, keys, q_ref.shape[0])
        dq = lax.fori_loop(0, full, functools.partial(step, masked=False), jnp.zeros((block, QK), F32))
        dq = lax.fori_loop(full, stop, functools.partial(step, masked=True), dq)
        dq = (dq * factor).astype(BF16)
        half = tokens // 2
        for t in range(2):
            to = 2 * i + t
            r = t * tokens
            blocks[to, :tokens, :] = dq[r : r + tokens, :NOPE]
            blocks[to, tokens:, :ROPE] = dq[r : r + half, NOPE:]
            blocks[to, tokens:, ROPE:] = dq[r + half : r + tokens, NOPE:]

            @pl.when(to == me)
            def _():
                own.start()

            @pl.when(to != me)
            def _():
                block_to(to).start()

    @pl.loop(0, members)
    def _(b):
        at = pl.ds(pl.multiple_of(b * tokens, tokens), tokens)
        d = jnp.concatenate([dk[at, :NOPE] * factor, dv[at, :]], axis=1).astype(BF16)
        part_ref[b, :, :KVR] = dot_t(d, kvb_ref[...]).astype(BF16)
        part_ref[b, :, KVR:] = (dk[at, NOPE:] * factor).astype(BF16)

    own.wait()

    @pl.loop(1, members)
    def _(d):
        n = lax.rem(me + d, members)
        from_device(n).wait_recv()
        block_to(n).wait_send()
        exchange.copy(d).wait_send()


def attend_back(prefix, q, k, v, o, lse, d, kvb, members, collective_id):
    length = q.shape[0]
    tokens = length // members
    vmem = pl.BlockSpec(memory_space=pltpu.VMEM)
    anywhere = pl.BlockSpec(memory_space=pl.ANY)
    sem = pltpu.SemaphoreType.DMA
    factor = QK**-0.5
    packed = tokens + tokens // 2
    return pl.pallas_call(
        functools.partial(attend_back_kernel, members=members, factor=factor, unit=factor * math.log2(math.e)),
        in_specs=[pl.BlockSpec(memory_space=pltpu.SMEM)] + [vmem] * 5 + [anywhere, vmem],
        out_specs=[vmem, anywhere],
        out_shape=[
            jax.ShapeDtypeStruct((members, tokens, KVR + ROPE), BF16),
            jax.ShapeDtypeStruct((members, packed, NOPE), BF16),
        ],
        scratch_shapes=[
            pltpu.VMEM((members, tokens, VD), BF16),
            pltpu.VMEM((members, packed, NOPE), BF16),
            pltpu.VMEM((length, QK), F32),
            pltpu.VMEM((length, VD), F32),
            sem((members,)), sem((members,)), sem((members,)), sem((members,)), sem, sem,
        ],
        compiler_params=pltpu.CompilerParams(
            collective_id=collective_id, has_side_effects=True, vmem_limit_bytes=50 * 1024 * 1024
        ),
        cost_estimate=pl.CostEstimate(
            flops=length * length * (3 * QK + 2 * VD), bytes_accessed=length * 2000, transcendentals=length * length // 2
        ),
        name="attend_back",
    )(prefix, q, k, v, o, lse, d, kvb)


def silu_parts(v):
    logistic = 0.5 * jnp.tanh(0.5 * v) + 0.5
    return v * logistic, logistic * (1.0 + v * (1.0 - logistic))


def picks(rank, slots):
    at = lax.broadcasted_iota(jnp.int32, (slots, rank.shape[1]), 0).astype(F32)
    return at == rank


def picks_back(rank, slots):
    at = lax.broadcasted_iota(jnp.int32, (rank.shape[0], slots), 1).astype(F32)
    return at == rank


def tiles(width, size):
    return pl.ds(pl.multiple_of(width * size, size), size)


def experts_kernel(
    x_hbm, prob_hbm, c_hbm, rank_ref, back_ref, gate_hbm, up_hbm, down_hbm, own_hbm, sdown_hbm,
    part_hbm, eg_hbm, eu_hbm, eo_hbm, sh_hbm, c_out, prob_out,
    xs, probs, gate, up, down, own, sdown, tail, rows, acts, sacts, part_st, eg_st, eu_st, eo_st, sh_st,
    c_st, sent, got, e_sent, e_got, c_sent, c_got, load, store,
    *, members, slots, tile, wide
):
    me = lax.axis_index("grp")
    levels = members // (SIDE * CORES)
    group = SIDE * CORES
    width, hidden = gate.shape
    half, whole = hidden % tile, hidden // tile
    units = own.shape[1] // 2
    z = me // group
    order = near_first(levels)
    loads = [
        pltpu.make_async_copy(a, b, load.at[n])
        for n, (a, b) in enumerate(
            [
                (x_hbm, xs.at[me]),
                (prob_hbm.at[me], probs.at[me]),
                (own_hbm, own),
                (gate_hbm, gate),
                (up_hbm, up),
                (down_hbm, down),
                (sdown_hbm, sdown),
                (c_hbm, c_st),
            ]
        )
    ]
    gather = Gather(x_hbm, xs, sent, got, members)
    behind = Gather(c_hbm, c_out, c_sent, c_got, members)
    own_c = pltpu.make_async_copy(c_st, c_out.at[me], load.at[7])
    exchange = Exchange(prob_hbm, probs, e_sent, e_got, members)
    for copy in loads:
        copy.start()
    meet(members)
    gather.first()
    exchange.start()
    for copy in loads:
        copy.wait()
    own_c.start()
    tail[:, :half] = gate[:, hidden - half :]
    tail[:, half:] = up[:, hidden - half :]
    gather.pass_on(z)
    gather.relay(1)
    exchange.wait()
    prob_out[...] = probs[...]

    def stores(s, k):
        n = s % 2
        return [
            pltpu.make_async_copy(a, b.at[k], store.at[n, m])
            for m, (a, b) in enumerate(
                [
                    (part_st.at[n], part_hbm),
                    (eg_st.at[n], eg_hbm),
                    (eu_st.at[n], eu_hbm),
                    (eo_st.at[n], eo_hbm),
                    (sh_st.at[n], sh_hbm),
                ]
            )
        ]

    @pl.loop(0, levels)
    def _(s):
        k = pick_from(order, z, s)
        n = s % 2
        gather.take_twin(k)

        @pl.when(s >= 2)
        def _():
            for copy in stores(s, pick_from(order, z, s - 2)):
                copy.wait()

        @pl.loop(0, group)
        def _(b):
            pick = picks(rank_ref[k * group + b, 0:1, :], slots).astype(BF16)
            rows[tiles(b, slots), :] = dot(pick, xs[k * group + b]).astype(BF16)

        def keep(at, g, u):
            eg_st[n, :, at] = g.astype(BF16)
            eu_st[n, :, at] = u.astype(BF16)
            acts[:, at] = (silu_parts(g)[0] * u).astype(BF16)

        @pl.loop(0, whole)
        def _(j):
            at = tiles(j, tile)
            x = rows[...]
            keep(at, dot(x, gate[:, at]), dot(x, up[:, at]))

        last = dot(rows[...], tail[...])
        keep(pl.ds(whole * tile, half), last[:, :half], last[:, half:])

        gather.relay(s + 2)

        @pl.when(s + 1 < levels)
        def _():
            gather.pass_on(pick_from(order, z, s + 1))

        @pl.when(s == levels - 3)
        def _():
            behind.first()

        @pl.when(s >= levels - 2)
        def _():
            behind.relay(s - levels + 3)
            behind.pass_on(pick_from(order, z, s - levels + 2))

        @pl.loop(0, width // wide)
        def _(j):
            at = tiles(j, wide)
            eo_st[n, :, at] = dot(acts[...], down[:, at]).astype(BF16)

        @pl.loop(0, group // 2)
        def _(h):
            x = xs[pl.ds(k * group + 2 * h, 2)].reshape(-1, width)
            pre = dot(x, own[...])
            sh_st[n, pl.ds(2 * h, 2)] = pre.astype(BF16).reshape(2, -1, 2 * units)
            act = (silu_parts(pre[:, :units])[0] * pre[:, units:]).astype(BF16)
            sacts[pl.ds(2 * h, 2)] = act.reshape(2, -1, units)

        @pl.loop(0, group)
        def _(b):
            i = k * group + b
            pick = picks(rank_ref[i, 0:1, :], slots)
            back = picks_back(back_ref[i], slots).astype(BF16)
            g = jnp.sum(jnp.where(pick, probs[i, 0:1, :], 0.0), axis=1, keepdims=True)
            act = sacts[b]
            for j in range(width // wide):
                at = slice(j * wide, (j + 1) * wide)
                weighted = (g * eo_st[n, tiles(b, slots), at].astype(F32)).astype(BF16)
                part_st[n, b, :, at] = (dot(back, weighted) + dot(act, sdown[:, at])).astype(BF16)

        for copy in stores(s, k):
            copy.start()

    @pl.loop(2, levels)
    def _(s):
        behind.relay(s + 1)
        behind.pass_on(pick_from(order, z, s))

    @pl.loop(levels - 2, levels)
    def _(s):
        for copy in stores(s, pick_from(order, z, s)):
            copy.wait()

    @pl.loop(0, levels)
    def _(k):
        behind.take_twin(k)

    own_c.wait()
    gather.finish()
    behind.finish()


def experts_forward(x, prob, c, rank, back, gate, up, down, own, sdown, slots, members, collective_id):
    tokens, width = x.shape
    hidden = gate.shape[1]
    group = SIDE * CORES
    levels = members // group
    packed = group * slots
    anywhere = pl.BlockSpec(memory_space=pl.ANY)
    vmem = pl.BlockSpec(memory_space=pltpu.VMEM)
    sem = pltpu.SemaphoreType.DMA
    tile = 256
    shapes = [
        (levels, group, tokens, width),
        (levels, packed, hidden),
        (levels, packed, hidden),
        (levels, packed, width),
        (levels, group, tokens, own.shape[1]),
    ]
    return pl.pallas_call(
        functools.partial(experts_kernel, members=members, slots=slots, tile=tile, wide=512),
        in_specs=[anywhere, anywhere, anywhere, vmem, vmem] + [anywhere] * 5,
        out_specs=[anywhere] * 6 + [vmem],
        out_shape=[jax.ShapeDtypeStruct(s, BF16) for s in shapes]
        + [jax.ShapeDtypeStruct((members, *c.shape), BF16)]
        + [jax.ShapeDtypeStruct(prob.shape, F32)],
        scratch_shapes=[
            pltpu.VMEM((members, tokens, width), BF16),
            pltpu.VMEM(prob.shape, F32),
            pltpu.VMEM(gate.shape, BF16),
            pltpu.VMEM(up.shape, BF16),
            pltpu.VMEM(down.shape, BF16),
            pltpu.VMEM(own.shape, BF16),
            pltpu.VMEM(sdown.shape, BF16),
            pltpu.VMEM((width, tile), BF16),
            pltpu.VMEM((packed, width), BF16),
            pltpu.VMEM((packed, hidden), BF16),
            pltpu.VMEM((group, tokens, own.shape[1] // 2), BF16),
        ]
        + [pltpu.VMEM((2, *s[1:]), BF16) for s in shapes]
        + [pltpu.VMEM(c.shape, BF16)]
        + [sem((6, members)), sem((2, members)), sem((members,)), sem((members,))]
        + [sem((6, members)), sem((2, members)), sem((8,)), sem((2, 5))],
        compiler_params=pltpu.CompilerParams(
            collective_id=collective_id, has_side_effects=True, vmem_limit_bytes=63 * 1024 * 1024
        ),
        cost_estimate=pl.CostEstimate(
            flops=12 * members * slots * width * hidden, bytes_accessed=60_000_000, transcendentals=0
        ),
        name="experts_forward",
    )(x, prob, c, rank, back, gate, up, down, own, sdown)


def experts_back_kernel(
    c_hbm, c2_hbm, rank_ref, back_ref, prob_ref, eg_hbm, eu_hbm, eo_hbm, sh_hbm, gate_hbm, up_hbm, down_hbm, own_hbm, sdown_hbm,
    out, dg_out,
    part, cs, eg, eu, eo, sh, gate, up, down, own, sdown, rows, d_gate, d_up, dg_st, dg_in,
    *sems, members, slots, tile, wide
):
    twin_in, side_in, line_in = sems[:3]
    e_sent, e_got, load, fetch = sems[11:15]
    me = lax.axis_index("grp")
    levels = members // (SIDE * CORES)
    group = SIDE * CORES
    width, hidden = gate.shape
    half, whole = hidden % tile, hidden // tile
    units = own.shape[1] // 2
    z = me // group
    order = far_first(levels)
    reduce = Reduce(part, twin_in, side_in, line_in, sems[3:11], members)
    exchange = Exchange(dg_st, dg_in, e_sent, e_got, members)

    def cotangents(s):
        k = pick_from(order, z, s)
        return [
            pltpu.make_async_copy(
                a.at[k], cs.at[s % 2, :, :, pl.ds(h * (width // 2), width // 2)], fetch.at[4 + s % 2 * 2 + h]
            )
            for h, a in enumerate([c_hbm, c2_hbm])
        ]

    def kept(s):
        k = pick_from(order, z, s)
        return [
            pltpu.make_async_copy(a.at[k], b, fetch.at[m])
            for m, (a, b) in enumerate([(eo_hbm, eo), (eg_hbm, eg), (eu_hbm, eu), (sh_hbm, sh)])
        ]

    loads = [
        pltpu.make_async_copy(a, b, load.at[n])
        for n, (a, b) in enumerate(
            [(down_hbm, down), (gate_hbm, gate), (up_hbm, up), (own_hbm, own), (sdown_hbm, sdown)]
        )
    ]
    for copy in cotangents(0) + kept(0):
        copy.start()
    for copy in loads:
        copy.start()
    meet(members)

    def early(s):
        return (z == 0) | (z == levels - 1)

    @pl.loop(0, levels)
    def _(s):
        k = pick_from(order, z, s)
        n = s % 2
        for copy in cotangents(s):
            copy.wait()
        load_eo, load_eg, load_eu, load_sh = kept(s)

        @pl.when(s + 1 < levels)
        def _():
            for copy in cotangents(s + 1):
                copy.start()

        load_eo.wait()
        @pl.loop(0, group)
        def _(b):
            i = k * group + b
            at = tiles(b, slots)
            pick = picks(rank_ref[i, 0:1, :], slots)
            c = dot(pick.astype(BF16), cs[n, b])
            g = jnp.sum(jnp.where(pick, prob_ref[i, 0:1, :], 0.0), axis=1, keepdims=True)
            along = jnp.sum(c * eo[at, :].astype(F32), axis=1, keepdims=True)
            dg_st[i] = jnp.broadcast_to(
                jnp.sum(jnp.where(pick, along, 0.0), axis=0, keepdims=True), dg_st.shape[1:]
            )
            rows[at, :] = (g * c).astype(BF16)

        @pl.when(s == 0)
        def _():
            for copy in loads:
                copy.wait()

        load_eg.wait()
        load_eu.wait()

        def slopes(at):
            d = dot_t(rows[...], down[at, :])
            act, slope = silu_parts(eg[:, at].astype(F32))
            d_gate[:, at] = (d * eu[:, at].astype(F32) * slope).astype(BF16)
            d_up[:, at] = (d * act).astype(BF16)

        @pl.loop(0, whole)
        def _(j):
            slopes(tiles(j, tile))

        slopes(pl.ds(whole * tile, half))

        @pl.when(s >= 1)
        def _():
            reduce.chip(pick_from(order, z, s - 1))

        @pl.when((s >= 2) & ~early(s))
        def _():
            reduce.line(pick_from(order, z, s - 2))

        @pl.loop(0, width // tile)
        def _(j):
            at = tiles(j, tile)
            eo[:, at] = (dot_t(d_gate[...], gate[at, :]) + dot_t(d_up[...], up[at, :])).astype(BF16)

        load_sh.wait()
        @pl.loop(0, group)
        def _(b):
            i = k * group + b
            back = picks_back(back_ref[i], slots).astype(BF16)
            d = dot_t(cs[n, b], sdown[...])
            pre = sh[b].astype(F32)
            act, slope = silu_parts(pre[:, :units])
            both = jnp.concatenate([d * pre[:, units:] * slope, d * act], axis=1).astype(BF16)
            for j in range(width // wide):
                at = slice(j * wide, (j + 1) * wide)
                part[i, :, at] = (
                    dot(back, eo[tiles(b, slots), at]) + dot_t(both, own[at, :])
                ).astype(BF16)

        reduce.start(k)

        @pl.when(s + 1 < levels)
        def _():
            for copy in kept(s + 1):
                copy.start()

        @pl.when((s >= 1) & early(s))
        def _():
            reduce.line(pick_from(order, z, s - 1))

    exchange.start()
    dg_in[me] = dg_st[me]
    reduce.chip(z)

    @pl.when(~early(0))
    def _():
        reduce.line(pick_from(order, z, levels - 2))

    reduce.last(out)
    reduce.finish()
    exchange.wait()
    dg_out[...] = dg_in[...]


def experts_backward(cs, rank, back, prob, kept, gate, up, down, own, sdown, slots, members, collective_id):
    tokens, width = cs[0].shape[1], cs[0].shape[2] * 2
    hidden = gate.shape[1]
    group = SIDE * CORES
    levels = members // group
    packed = group * slots
    anywhere = pl.BlockSpec(memory_space=pl.ANY)
    vmem = pl.BlockSpec(memory_space=pltpu.VMEM)
    sem = pltpu.SemaphoreType.DMA
    eg, eu, eo, sh = kept
    return pl.pallas_call(
        functools.partial(experts_back_kernel, members=members, slots=slots, tile=256, wide=512),
        in_specs=[anywhere, anywhere, vmem, vmem, vmem] + [anywhere] * 9,
        out_specs=[vmem, vmem],
        out_shape=[
            jax.ShapeDtypeStruct((tokens, width), BF16),
            jax.ShapeDtypeStruct((members, 8, tokens), F32),
        ],
        scratch_shapes=[
            pltpu.VMEM((members, tokens, width), BF16),
            pltpu.VMEM((2, group, tokens, width), BF16),
            pltpu.VMEM(eg.shape[1:], BF16),
            pltpu.VMEM(eu.shape[1:], BF16),
            pltpu.VMEM(eo.shape[1:], BF16),
            pltpu.VMEM(sh.shape[1:], BF16),
            pltpu.VMEM(gate.shape, BF16),
            pltpu.VMEM(up.shape, BF16),
            pltpu.VMEM(down.shape, BF16),
            pltpu.VMEM(own.shape, BF16),
            pltpu.VMEM(sdown.shape, BF16),
            pltpu.VMEM((packed, width), BF16),
            pltpu.VMEM((packed, hidden), BF16),
            pltpu.VMEM((packed, hidden), BF16),
            pltpu.VMEM((members, 8, tokens), F32),
            pltpu.VMEM((members, 8, tokens), F32),
        ]
        + Reduce.scratch(members, tokens, width, BF16)
        + [sem((members,)), sem((members,)), sem((5,)), sem((8,))],
        compiler_params=pltpu.CompilerParams(
            collective_id=collective_id, has_side_effects=True, vmem_limit_bytes=67_043_328
        ),
        cost_estimate=pl.CostEstimate(
            flops=12 * members * slots * width * hidden, bytes_accessed=60_000_000, transcendentals=0
        ),
        name="experts_backward",
    )(*(c.reshape(levels, group, tokens, -1) for c in cs), rank, back, prob, *kept, gate, up, down, own, sdown)


def by_owner(gradient, members):
    return gradient.astype(BF16).reshape(gradient.shape[0], members, -1).transpose(1, 0, 2)


def pack(v):
    half = v.shape[1] // 2
    rope = jnp.concatenate([v[:, :half, NOPE:], v[:, half:, NOPE:]], axis=-1)
    return jnp.concatenate([v[:, :, :NOPE], rope], axis=1)


def unpack(v):
    rows = v.shape[1] * 2 // 3
    rope = jnp.concatenate([v[:, rows:, :ROPE], v[:, rows:, ROPE:]], axis=1)
    return jnp.concatenate([v[:, :rows], rope], axis=-1)


def per_device(
    hidden,
    grad_out,
    expert_ids,
    prefix_len,
    adapter_id,
    attn_gain,
    kv_gain,
    ffn_gain,
    w_q,
    w_kva,
    w_kvb,
    w_o,
    w_router,
    shared_gate,
    shared_up,
    shared_down,
    expert_gate,
    expert_up_weight,
    expert_down,
    q_down,
    q_up,
    o_down,
    o_up,
):
    tokens = hidden.shape[1]
    width = hidden.shape[2]
    members = lax.axis_size("grp")
    length = tokens * members
    experts = expert_gate.shape[0] * members
    capacity = tokens * TOP * 5 // (4 * experts)
    slots = -(-capacity // 16) * 16
    me = lax.axis_index("grp")

    inputs = hidden[0].astype(F32)
    cotangent = grad_out[0]
    c32 = cotangent.astype(F32)
    routes = expert_ids[0]
    adapter = adapter_id[0]
    pick = lambda table: lax.dynamic_index_in_dim(table, adapter, 0, keepdims=False)
    qa_down, qa_up, oa_down, oa_up = pick(q_down), pick(q_up), pick(o_down), pick(o_up)

    chosen_by = jnp.sum(
        (routes[:, :, None] == jnp.arange(experts, dtype=jnp.int32)[None, None, :]).astype(F32), axis=1
    )
    sequences = lax.axis_size("rep")
    split = w_q.shape[0] * 3 // 128 * 16 if sequences % 2 == 0 else 0
    (all_kva, all_q, all_o), _ = communicate([w_kva, w_q, w_o], [], members, 1, [split] * 3)
    full_kva, full_q, full_o = (v.reshape(-1, v.shape[2]) for v in (all_kva, all_q, all_o))
    hidden_slice = shared_down.shape[0]
    shared = after(jnp.stack([shared_gate, shared_up], axis=1), all_q)
    shared = shared.reshape(shared.shape[0], 2, members, hidden_slice).transpose(2, 0, 1, 3)
    own_shared = exchange(shared.reshape(members, -1, 2 * hidden_slice)).reshape(width, 2 * hidden_slice)

    positions = me * tokens + jnp.arange(tokens, dtype=jnp.int32)
    cosine, sine = angles(positions, ROPE)
    normed = root_norm(inputs, attn_gain).astype(BF16)
    latent = dot(normed, full_kva)
    compressed = root_norm(latent[:, :KVR], kv_gain).astype(BF16)
    k_rope = rotate(latent[:, KVR:], cosine, sine).astype(BF16)
    q_small = dot(normed, qa_down).astype(BF16)
    query = (dot(normed, full_q) + dot(q_small, qa_up)).reshape(tokens, H, QK)
    query = jnp.concatenate(
        [query[:, :, :NOPE], rotate(query[:, :, NOPE:], cosine[:, None], sine[:, None])], axis=-1
    ).astype(BF16)
    (all_latent, all_router), (q_packed, kvb_parts, chosen_all) = communicate(
        [jnp.concatenate([compressed, k_rope], axis=-1), w_router],
        [
            after(pack(query.transpose(1, 0, 2)), own_shared),
            w_kvb.reshape(w_kvb.shape[0], members, -1).transpose(1, 0, 2),
            jnp.broadcast_to(chosen_by.T[:, None, :], (experts, 8, tokens)),
        ],
        members,
        2,
    )
    full_router = all_router.reshape(width, -1)
    own_kvb = kvb_parts.reshape(KVR, -1)
    all_latent = all_latent.reshape(length, KVR + ROPE)
    q_head = unpack(q_packed).reshape(length, QK)
    q_head, c_first = lax.optimization_barrier((q_head, cotangent[:, : width // 2]))
    expanded = dot(all_latent[:, :KVR], own_kvb).astype(BF16)
    k_head = jnp.concatenate([expanded[:, :NOPE], all_latent[:, KVR:]], axis=-1)
    v_head = expanded[:, NOPE:]
    mixture, lse, mixed_parts = attend(prefix_len, q_head, k_head, v_head, members, 3)
    mixed = mixed_parts.transpose(1, 0, 2).reshape(tokens, H * VD)
    o_small = dot(mixed, oa_down).astype(BF16)
    middle = inputs + dot(mixed, full_o) + dot(o_small, oa_up)
    ffn_in = root_norm(middle, ffn_gain).astype(BF16)
    route_probs = jax.nn.softmax(dot(ffn_in, full_router), axis=-1)

    half = width // 2
    first_c = gather(c_first).reshape(members, tokens, half)
    chosen = chosen_all[:, 0] > 0.5
    order = jnp.arange(tokens, dtype=jnp.int32)
    before = (order[:, None] < order[None, :]).astype(BF16)
    rank = jnp.where(chosen, dot(chosen.astype(BF16), before), -1.0)
    back = rank[:, :, None]
    rank = jnp.broadcast_to(rank[:, None, :], (members, 8, tokens))
    weights = (expert_gate[0], expert_up_weight[0], expert_down[0], own_shared, shared_down)
    prob_blocks = jnp.broadcast_to(route_probs.T[:, None, :], (experts, 8, tokens))
    partial, kept_gate, kept_up, kept_out, kept_shared, second_c, prob_parts = experts_forward(
        ffn_in, prob_blocks, cotangent[:, half:], rank, back, *weights, slots, members, 4
    )
    kept = (kept_gate, kept_up, kept_out, kept_shared)
    ffn_out = scatter_sum(partial.reshape(length, width))
    d_own, d_route = experts_backward(
        (first_c, second_c), rank, back, prob_parts, kept, *weights, slots, members, 5
    )
    d_route = d_route[:, 0].T
    d_logits = (
        route_probs * (d_route - jnp.sum(route_probs * d_route, axis=-1, keepdims=True))
    ).astype(BF16)
    d_ffn = d_own.astype(F32) + dot_t(d_logits, full_router)
    d_middle = c32 + norm_back(middle, ffn_gain, d_ffn)
    d_attn = d_middle.astype(BF16)
    grad_oup = t_dot(o_small, d_attn)
    d_osmall = dot_t(d_attn, oa_up).astype(BF16)
    grad_odown = t_dot(d_osmall, mixed)
    d_mixed = (dot_t(d_attn, full_o) + dot_t(d_osmall, oa_down)).astype(BF16)
    d_latents, d_query = attend_back(
        prefix_len,
        q_head,
        k_head,
        v_head,
        mixture,
        lse.reshape(members // 2, 1, 2 * tokens),
        d_mixed.reshape(tokens, H, VD).transpose(1, 0, 2),
        own_kvb,
        members,
        6,
    )
    o_parts = jnp.concatenate([by_owner(g, members) for g in (grad_odown, grad_oup)], axis=-1)
    d_latents, (o_landed,) = reduce_blocks(d_latents, [o_parts], members, 7)
    d_latents = d_latents.astype(F32)
    d_query = unpack(d_query).transpose(1, 0, 2).astype(F32)
    d_latent = jnp.concatenate(
        [
            norm_back(latent[:, :KVR], kv_gain, d_latents[:, :KVR]),
            unrotate(d_latents[:, KVR:], cosine, sine),
        ],
        axis=-1,
    ).astype(BF16)
    d_query = (
        jnp.concatenate(
            [d_query[:, :, :NOPE], unrotate(d_query[:, :, NOPE:], cosine[:, None], sine[:, None])],
            axis=-1,
        )
        .reshape(tokens, H * QK)
        .astype(BF16)
    )
    ffn_out, _ = lax.optimization_barrier((ffn_out, d_query))
    output = (middle + ffn_out.astype(F32)).astype(BF16)
    grad_qup = t_dot(q_small, d_query)
    d_qsmall = dot_t(d_query, qa_up).astype(BF16)
    grad_qdown = t_dot(d_qsmall, normed)
    d_normed = dot_t(d_query, full_q) + dot_t(d_qsmall, qa_down) + dot_t(d_latent, full_kva)
    grad_inputs = (d_middle + norm_back(inputs, attn_gain, d_normed)).astype(BF16)

    q_parts = jnp.concatenate([by_owner(g, members) for g in (grad_qdown, grad_qup)], axis=-1)
    o_share = jnp.sum(o_landed.astype(F32), axis=0)
    named = jnp.broadcast_to(adapter.astype(F32), (o_share.shape[0], 128))
    q_shares, o_shares = spread_blocks(
        q_parts, jnp.concatenate([o_share, named], axis=-1), members, sequences, 8
    )
    numbers = o_shares[:, 0, -1].astype(jnp.int32)
    shares = jnp.concatenate([jnp.sum(q_shares.astype(F32), axis=1), o_shares[:, :, :-128]], axis=-1)
    selector = (jnp.arange(q_down.shape[0], dtype=jnp.int32)[:, None] == numbers[None, :]).astype(F32)
    summed = jnp.sum(selector[:, :, None, None] * shares[None], axis=1)
    sizes = [g.shape[1] // members for g in (grad_qdown, grad_qup, grad_odown, grad_oup)]
    ends = [sum(sizes[: n + 1]) for n in range(4)]
    outs = [summed[:, :, e - s : e] for e, s in zip(ends, sizes)]
    return (
        output[None],
        grad_inputs[None],
        outs[0].transpose(0, 2, 1),
        outs[1],
        outs[2].transpose(0, 2, 1),
        outs[3],
    )


def solution(mesh):
    seq = P("rep", "grp", None)
    rows = P("grp", None)
    in_specs = (
        (seq, seq, seq, P("rep"), P("rep"), P(), P(), P())
        + (rows,) * 8
        + (P("grp", None, None),) * 3
        + (P(),) * 4
    )
    out_specs = (
        seq,
        seq,
        P(None, "grp", None),
        P(None, None, "grp"),
        P(None, "grp", None),
        P(None, None, "grp"),
    )
    return jax.shard_map(
        per_device, mesh=mesh, in_specs=in_specs, out_specs=out_specs, check_vma=False
    )
```

```python
import functools
import math

import jax
import jax.numpy as jnp
from jax import lax
from jax.experimental import pallas as pl
from jax.experimental.pallas import tpu as pltpu
from jax.sharding import PartitionSpec as P

H = 16
NOPE = 128
ROPE = 64
VD = 128
KVR = 512
TOP = 6
QK = NOPE + ROPE
EPS = 1e-06
F32 = jnp.float32
BF16 = jnp.bfloat16


def dot(former, latter):
    return jnp.dot(former, latter, preferred_element_type=F32)


def dot_t(former, latter):
    return lax.dot_general(
        former, latter, (((1,), (1,)), ((), ())), preferred_element_type=F32
    )


def t_dot(former, latter):
    return lax.dot_general(
        former, latter, (((0,), (0,)), ((), ())), preferred_element_type=F32
    )


def root_norm(v, gains):
    factor = lax.rsqrt(jnp.mean(v * v, axis=-1, keepdims=True) + EPS)
    return v * factor * gains


def norm_back(v, gains, gradient):
    factor = lax.rsqrt(jnp.mean(v * v, axis=-1, keepdims=True) + EPS)
    weighted = gradient * gains
    return factor * weighted - v * (factor * factor * factor) * jnp.mean(
        weighted * v, axis=-1, keepdims=True
    )


def angles(positions, width):
    frequency = 10000.0 ** (-jnp.arange(0, width, 2, dtype=F32) / width)
    phases = positions.astype(F32)[:, None] * frequency[None, :]
    return (jnp.cos(phases), jnp.sin(phases))


def rotate(v, cosine, sine):
    half = v.shape[-1] // 2
    a, b = v[..., :half], v[..., half:]
    return jnp.concatenate([a * cosine - b * sine, b * cosine + a * sine], axis=-1)


def unrotate(v, cosine, sine):
    half = v.shape[-1] // 2
    a, b = v[..., :half], v[..., half:]
    return jnp.concatenate([a * cosine + b * sine, b * cosine - a * sine], axis=-1)


SIDE = 2
CORES = 2
MESH = pl.DeviceIdType.MESH


def place_of():
    me = lax.axis_index("grp")
    return me // (SIDE * CORES), (me // CORES) % SIDE, me % CORES


def index_of(z, x, c):
    return (z * SIDE + x) * CORES + c


def send(src, dst, sent, got, to):
    return pltpu.make_async_remote_copy(
        src_ref=src,
        dst_ref=dst,
        send_sem=sent,
        recv_sem=got,
        device_id=to if isinstance(to, dict) else {"grp": to},
        device_id_type=MESH,
    )


def meet(members, partner=None):
    barrier = pltpu.get_barrier_semaphore()
    me = lax.axis_index("grp")

    @pl.loop(1, members)
    def _(d):
        pl.semaphore_signal(barrier, 1, device_id={"grp": lax.rem(me + d, members)}, device_id_type=MESH)

    if partner is not None:
        pl.semaphore_signal(barrier, 1, device_id=partner, device_id_type=MESH)
    pl.semaphore_wait(barrier, members - 1 + (partner is not None))


def pick_from(table, z, s):
    v = 0
    for i, row in enumerate(table):
        for j, entry in enumerate(row):
            if entry:
                v = v + jnp.where((z == i) & (s == j), entry, 0)
    return v


def near_first(levels):
    return [sorted(range(levels), key=lambda v: (abs(v - k), v)) for k in range(levels)]


def far_first(levels):
    return [sorted((v for v in range(levels) if v != k), key=lambda v: (-abs(v - k), v)) + [k] for k in range(levels)]


class Gather:
    def __init__(self, src, out, sent, got, members, split=0):
        self.src, self.out, self.sent, self.got = src, out, sent, got
        self.members, self.split = members, split
        self.levels = members // (SIDE * CORES)
        self.z, self.x, self.c = z, x, c = place_of()
        self.me = lax.axis_index("grp")
        self.up, self.down = index_of(z + 1, x, c), index_of(z - 1, x, c)
        self.side, self.twin = index_of(z, 1 - x, c), index_of(z, x, 1 - c)
        if split:
            rows = src.shape[0]
            rep = lax.axis_index("rep")
            odd = rep % 2
            self.partner = {"rep": rep + 1 - 2 * odd, "grp": self.me}
            self.window = pl.ds(pl.multiple_of(odd * split, 16), rows - split)
            self.given = pl.ds(pl.multiple_of(odd * (rows - split), 16), split)
            self.lacked = pl.ds(pl.multiple_of((1 - odd) * (rows - split), 16), split)

    def copy(self, slot, kind, to, own=False, rows=None):
        rows = rows or (self.window if self.split else None)
        other = rows is not None and self.split and rows is not self.window
        src = self.src if own else self.out.at[slot]
        dst = self.out.at[slot]
        if rows is not None:
            src, dst = src.at[rows], dst.at[rows]
        return send(src, dst, self.sent.at[kind, slot], self.got.at[int(bool(other)), slot], to)

    def arrive(self, slot):
        self.copy(slot, 0, self.twin).wait_recv()

    def to_partner(self, slot):
        return self.copy(slot, 4, self.partner, rows=self.given)

    def lacked_to_twin(self, slot, own=False):
        return self.copy(slot, 5, self.twin, own, rows=self.lacked)

    def first(self):
        @pl.when(self.z < self.levels - 1)
        def _():
            self.copy(self.me, 0, self.up, True).start()

        @pl.when(self.z > 0)
        def _():
            self.copy(self.me, 1, self.down, True).start()

        self.copy(self.me, 2, self.side, True).start()
        self.copy(self.me, 3, self.twin, True).start()
        if self.split:
            self.lacked_to_twin(self.me, True).start()

    def relay(self, s):
        @pl.when(self.z >= s)
        def _():
            slot = index_of(self.z - s, self.x, self.c)
            self.arrive(slot)

            @pl.when(self.z < self.levels - 1)
            def _():
                self.copy(slot, 0, self.up).start()

            self.spread(slot)

        @pl.when(self.z + s < self.levels)
        def _():
            slot = index_of(self.z + s, self.x, self.c)
            self.arrive(slot)

            @pl.when(self.z > 0)
            def _():
                self.copy(slot, 1, self.down).start()

            self.spread(slot)

    def spread(self, slot):
        self.copy(slot, 2, self.side).start()
        self.copy(slot, 3, self.twin).start()
        if self.split:
            self.to_partner(slot).start()

    def pass_on(self, k):
        slot = index_of(k, 1 - self.x, self.c)
        self.arrive(slot)
        self.copy(slot, 3, self.twin).start()
        if self.split:
            self.to_partner(slot).start()

    def take_lacked(self, k, x):
        slot = index_of(k, x, self.c)

        @pl.when(slot != self.me)
        def _():
            self.copy(slot, 4, self.partner, rows=self.lacked).wait_recv()
            self.lacked_to_twin(slot).start()

    def take_twin(self, k):
        for x in range(SIDE):
            self.arrive(index_of(k, x, 1 - self.c))

    def take_twin_lacked(self):
        @pl.loop(0, self.members // CORES)
        def _(i):
            self.lacked_to_twin(i * CORES + 1 - self.c).wait_recv()

    def finish(self):
        @pl.loop(0, self.levels)
        def _(k):
            slot = index_of(k, self.x, self.c)
            self.copy(slot, 2, self.side).wait_send()

            @pl.when((k <= self.z) & (self.z < self.levels - 1))
            def _():
                self.copy(slot, 0, self.up).wait_send()

            @pl.when((k >= self.z) & (self.z > 0))
            def _():
                self.copy(slot, 1, self.down).wait_send()

        @pl.loop(0, self.members // CORES)
        def _(i):
            slot = i * CORES + self.c
            self.copy(slot, 3, self.twin).wait_send()
            if self.split:
                self.lacked_to_twin(slot).wait_send()

                @pl.when(slot != self.me)
                def _():
                    self.to_partner(slot).wait_send()


class Exchange:
    def __init__(self, src, out, sent, got, members):
        self.src, self.out, self.sent, self.got, self.members = src, out, sent, got, members
        self.me = lax.axis_index("grp")

    def copy(self, d):
        to = lax.rem(self.me + d, self.members)
        return send(self.src.at[to], self.out.at[self.me], self.sent.at[d], self.got.at[d], to)

    def start(self):
        @pl.loop(1, self.members)
        def _(d):
            self.copy(d).start()

    def wait(self):
        @pl.loop(1, self.members)
        def _(d):
            self.copy(d).wait()


def comm_kernel(*refs, members, splits, n_e):
    n_g = len(splits)
    n = n_g + n_e
    ins, outs = refs[:n], refs[n : 2 * n]
    stage = refs[2 * n : 3 * n]
    local = refs[3 * n]
    sems = refs[3 * n + 1 :]
    me = lax.axis_index("grp")
    into = [
        pltpu.make_async_copy(r if k < n_g else r.at[me], stage[k], local.at[k]) for k, r in enumerate(ins)
    ]
    out_of = [pltpu.make_async_copy(stage[k], outs[k].at[me], local.at[k]) for k in range(n)]
    gathers = [
        Gather(ins[k], outs[k], sems[2 * k], sems[2 * k + 1], members, splits[k]) for k in range(n_g)
    ]
    exchanges = [Exchange(ins[k], outs[k], sems[2 * k], sems[2 * k + 1], members) for k in range(n_g, n)]
    for copy in into:
        copy.start()
    split = [g for g in gathers if g.split]
    meet(members, split[0].partner if split else None)
    for g in gathers:
        g.first()
    for e in exchanges:
        e.start()
    for a, b in zip(into, out_of):
        a.wait()
        b.start()
    levels = members // (SIDE * CORES)
    z = me // (SIDE * CORES)
    order = near_first(levels)

    def lacked(g, s):
        k = pick_from(order, z, s)
        g.take_lacked(k, g.x)
        g.take_lacked(k, 1 - g.x)

    if gathers:

        @pl.loop(0, levels)
        def _(s):
            for g in gathers:
                g.relay(s + 1)
            for g in gathers:
                g.pass_on(pick_from(order, z, s))

            @pl.when(s >= 1)
            def _():
                for g in split:
                    lacked(g, s - 1)

    for g in split:
        lacked(g, levels - 1)
    for g in gathers:

        @pl.loop(0, levels)
        def _(k):
            g.take_twin(k)

        if g.split:
            g.take_twin_lacked()
        g.finish()
    for e in exchanges:
        e.wait()
    for copy in out_of:
        copy.wait()


def communicate(gathers, exchanges, members, collective_id, splits=None):
    gathers, exchanges = list(gathers), list(exchanges)
    n_g, n_e = len(gathers), len(exchanges)
    splits = splits or [0] * n_g
    blocks = [g.shape for g in gathers] + [e.shape[1:] for e in exchanges]
    kinds = [a.dtype for a in gathers + exchanges]
    anywhere = pl.BlockSpec(memory_space=pl.ANY)
    sem = pltpu.SemaphoreType.DMA
    moved = sum(members * b[0] * b[1] * 2 for b in blocks)
    outs = pl.pallas_call(
        functools.partial(comm_kernel, members=members, splits=tuple(splits), n_e=n_e),
        in_specs=[anywhere] * (n_g + n_e),
        out_specs=[anywhere] * (n_g + n_e),
        out_shape=[jax.ShapeDtypeStruct((members, *b), k) for b, k in zip(blocks, kinds)],
        scratch_shapes=[pltpu.VMEM(b, k) for b, k in zip(blocks, kinds)]
        + [sem((n_g + n_e,))]
        + [sem((6, members)), sem((2, members))] * n_g
        + [sem((members,)), sem((members,))] * n_e,
        compiler_params=pltpu.CompilerParams(collective_id=collective_id, has_side_effects=True),
        cost_estimate=pl.CostEstimate(flops=0, bytes_accessed=moved * 8, transcendentals=0),
        name=f"communicate_{collective_id}",
    )(*gathers, *exchanges)
    return outs[:n_g], outs[n_g:]


class Reduce:
    def __init__(self, p, twin_in, side_in, line_in, sems, members):
        self.p, self.twin_in, self.side_in, self.line_in = p, twin_in, side_in, line_in
        self.sems = sems
        self.levels = members // (SIDE * CORES)
        self.z, self.x, self.c = place_of()

    def copy(self, kind, slot, dst, n, to):
        sent, got = self.sems[2 * kind], self.sems[2 * kind + 1]
        return send(self.p.at[slot], dst.at[n], sent.at[n], got.at[n], to)

    def to_twin(self, k, w):
        twin = index_of(self.z, self.x, 1 - self.c)
        return self.copy(0, index_of(k, w, 1 - self.c), self.twin_in, k * SIDE + w, twin)

    def to_side(self, k):
        return self.copy(1, index_of(k, 1 - self.x, self.c), self.side_in, k, index_of(self.z, 1 - self.x, self.c))

    def to_up(self, k):
        return self.copy(2, index_of(k, self.x, self.c), self.line_in, k + 1, index_of(self.z + 1, self.x, self.c))

    def to_down(self, k):
        return self.copy(3, index_of(k, self.x, self.c), self.line_in, k, index_of(self.z - 1, self.x, self.c))

    def add(self, slot, ref):
        rows = self.p.shape[1]
        chunk = next(r for r in (32, 16, 8) if rows % r == 0)

        @pl.loop(0, rows // chunk)
        def _(i):
            at = pl.ds(pl.multiple_of(i * chunk, chunk), chunk)
            self.p[slot, at, :] = (self.p[slot, at, :].astype(F32) + ref[at, :].astype(F32)).astype(self.p.dtype)

    def start(self, k):
        self.to_twin(k, self.x).start()
        self.to_twin(k, 1 - self.x).start()

    def chip(self, k):
        w = 1 - self.x
        self.to_twin(k, w).wait_recv()
        self.add(index_of(k, w, self.c), self.twin_in.at[k * SIDE + w])
        self.to_side(k).start()
        self.to_twin(k, self.x).wait_recv()
        self.add(index_of(k, self.x, self.c), self.twin_in.at[k * SIDE + self.x])

    def line(self, k):
        z, mine = self.z, index_of(k, self.x, self.c)
        self.to_side(k).wait_recv()
        self.add(mine, self.side_in.at[k])

        @pl.when((k > z) & (z > 0))
        def _():
            self.to_up(k).wait_recv()
            self.add(mine, self.line_in.at[k + 1])

        @pl.when((k < z) & (z < self.levels - 1))
        def _():
            self.to_down(k).wait_recv()
            self.add(mine, self.line_in.at[k])

        @pl.when(k > z)
        def _():
            self.to_up(k).start()

        @pl.when(k < z)
        def _():
            self.to_down(k).start()

    def last(self, out):
        z, mine = self.z, index_of(self.z, self.x, self.c)
        self.to_side(z).wait_recv()
        self.add(mine, self.side_in.at[z])

        @pl.when(z > 0)
        def _():
            self.to_up(z).wait_recv()
            self.add(mine, self.line_in.at[z + 1])

        @pl.when(z < self.levels - 1)
        def _():
            self.to_down(z).wait_recv()
            self.add(mine, self.line_in.at[z])

        out[...] = self.p[mine]

    def finish(self):
        z = self.z

        @pl.loop(0, self.levels)
        def _(k):
            self.to_twin(k, 0).wait_send()
            self.to_twin(k, 1).wait_send()
            self.to_side(k).wait_send()

            @pl.when(k > z)
            def _():
                self.to_up(k).wait_send()

            @pl.when(k < z)
            def _():
                self.to_down(k).wait_send()

    @staticmethod
    def scratch(members, r, c, kind):
        levels = members // (SIDE * CORES)
        sem = pltpu.SemaphoreType.DMA
        return [
            pltpu.VMEM((members // CORES, r, c), kind),
            pltpu.VMEM((levels, r, c), kind),
            pltpu.VMEM((levels + 1, r, c), kind),
        ] + [sem((n,)) for n in (members // CORES,) * 2 + (levels,) * 2 + (levels + 1,) * 4]


def gather(v):
    return lax.all_gather(v, "grp", axis=0, tiled=True)


def exchange(v):
    return lax.all_to_all(v, "grp", split_axis=0, concat_axis=0, tiled=True)


def scatter_sum(v):
    return lax.psum_scatter(v, "grp", scatter_dimension=0, tiled=True)


def after(v, *others):
    return lax.optimization_barrier((v, *others))[0]


def tie(v, other):
    first = other[(0,) * other.ndim]
    return v + jnp.minimum(jnp.abs(first), 0).astype(v.dtype)


def key_blocks(start, rows, keys, length):
    end = start + rows
    end = jnp.where(start < length // 2, jnp.maximum(end, length // 2), end)
    return (start + 1) // keys, (end + keys - 1) // keys


def attend_kernel(prefix_ref, q_ref, k_ref, v_ref, o_ref, lse_ref, mixed, blocks, sent, got, local, *, members, unit):
    me = lax.axis_index("grp")
    tokens = blocks.shape[1]
    block, keys = 2 * tokens, 4 * tokens
    turns = members // 2
    prefix = prefix_ref[0]

    def block_to(n):
        return send(blocks.at[n], mixed.at[me], sent.at[n], got.at[me], n)

    def from_device(n):
        return send(blocks.at[n], mixed.at[n], sent.at[n], got.at[n], n)

    own = pltpu.make_async_copy(blocks.at[me], mixed.at[me], local)
    meet(members)

    @pl.loop(0, turns)
    def _(n):
        i = lax.rem(me // 2 + n, turns)
        start = pl.multiple_of(i * block, block)
        here = pl.ds(start, block)
        q = q_ref[here, :]
        rows = start + lax.broadcasted_iota(jnp.int32, (block, 1), 0)
        limit = jnp.where(rows < prefix, prefix - 1, rows)
        limit = jnp.maximum(limit, rows)

        def step(j, carry, masked):
            top, total, acc = carry
            at = pl.multiple_of(j * keys, keys)
            k = k_ref[pl.ds(at, keys), :]
            v = v_ref[pl.ds(at, keys), :]
            s = dot_t(q, k)
            if masked:
                cols = at + lax.broadcasted_iota(jnp.int32, (1, keys), 1)
                s = jnp.where(cols <= limit, s, -1e30)
            fresh = jnp.maximum(top, jnp.max(s, axis=1, keepdims=True))
            p = jnp.exp2((s - fresh) * unit)
            scale = jnp.exp2((top - fresh) * unit)
            total = total * scale + jnp.sum(p, axis=1, keepdims=True)
            acc = acc * scale + dot(p.astype(BF16), v)
            return fresh, total, acc

        carry = (
            jnp.full((block, 1), -1e30, F32),
            jnp.zeros((block, 1), F32),
            jnp.zeros((block, VD), F32),
        )
        full, stop = key_blocks(start, block, keys, q_ref.shape[0])
        carry = lax.fori_loop(0, full, functools.partial(step, masked=False), carry)
        top, total, acc = lax.fori_loop(full, stop, functools.partial(step, masked=True), carry)
        o = acc / total
        o_ref[here, :] = o
        lse_ref[here, :] = top * unit + jnp.log2(total)
        blocks[pl.ds(2 * i, 2)] = o.astype(BF16).reshape(2, tokens, VD)
        for t in range(2):
            to = 2 * i + t

            @pl.when(to == me)
            def _():
                own.start()

            @pl.when(to != me)
            def _():
                block_to(to).start()

    own.wait()

    @pl.loop(1, members)
    def _(d):
        n = lax.rem(me + d, members)
        from_device(n).wait_recv()
        block_to(n).wait_send()


def attend(prefix, q, k, v, members, collective_id):
    length = q.shape[0]
    tokens = length // members
    vmem = pl.BlockSpec(memory_space=pltpu.VMEM)
    sem = pltpu.SemaphoreType.DMA
    return pl.pallas_call(
        functools.partial(attend_kernel, members=members, unit=QK**-0.5 * math.log2(math.e)),
        in_specs=[pl.BlockSpec(memory_space=pltpu.SMEM), vmem, vmem, vmem],
        out_specs=[vmem, vmem, pl.BlockSpec(memory_space=pl.ANY)],
        out_shape=[
            jax.ShapeDtypeStruct((length, VD), F32),
            jax.ShapeDtypeStruct((length, 1), F32),
            jax.ShapeDtypeStruct((members, tokens, VD), BF16),
        ],
        scratch_shapes=[pltpu.VMEM((members, tokens, VD), BF16), sem((members,)), sem((members,)), sem],
        compiler_params=pltpu.CompilerParams(
            collective_id=collective_id, has_side_effects=True, vmem_limit_bytes=40 * 1024 * 1024
        ),
        cost_estimate=pl.CostEstimate(
            flops=length * length * (QK + VD), bytes_accessed=length * 1000, transcendentals=length * length // 2
        ),
        name="attend",
    )(prefix, q, k, v)


def attend_back_kernel(
    prefix_ref, q_ref, k_ref, v_ref, o_ref, lse_ref, d_hbm, kvb_ref, part_ref, dq_out,
    ds_in, blocks, dk, dv, sent, got, q_sent, q_got, local, local2,
    *, members, factor, unit
):
    me = lax.axis_index("grp")
    tokens = blocks.shape[1] * 2 // 3
    block, keys = 2 * tokens, 4 * tokens
    turns = members // 2
    prefix = prefix_ref[0]
    exchange = Exchange(d_hbm, ds_in, sent, got, members)
    into = pltpu.make_async_copy(d_hbm.at[me], ds_in.at[me], local)
    own = pltpu.make_async_copy(blocks.at[me], dq_out.at[me], local2)

    def block_to(n):
        return send(blocks.at[n], dq_out.at[me], q_sent.at[n], q_got.at[me], n)

    def from_device(n):
        return send(blocks.at[n], dq_out.at[n], q_sent.at[n], q_got.at[n], n)

    into.start()
    meet(members)
    exchange.start()
    dk[...] = jnp.zeros_like(dk)
    dv[...] = jnp.zeros_like(dv)
    into.wait()

    @pl.loop(0, turns)
    def _(n):
        i = lax.rem(me // 2 + n, turns)
        start = pl.multiple_of(i * block, block)
        here = pl.ds(start, block)
        for t in range(2):
            source = 2 * i + t

            @pl.when(source != me)
            def _():
                send(ds_in.at[source], ds_in.at[source], sent.at[0], got.at[lax.rem(me - source + members, members)], source).wait_recv()

        d = ds_in[pl.ds(2 * i, 2)].reshape(block, VD)
        q = q_ref[here, :]
        lse = lse_ref[pl.ds(i, 1), 0, :]
        along = d.astype(F32) * o_ref[here, :]
        high = along.astype(BF16)
        low = (along - high.astype(F32)).astype(BF16)
        ones = jnp.ones((8, VD), BF16)
        delta = (dot_t(ones, high) + dot_t(ones, low))[0:1, :]
        rows = start + lax.broadcasted_iota(jnp.int32, (1, block), 1)
        limit = jnp.maximum(jnp.where(rows < prefix, prefix - 1, rows), rows)

        def step(j, dq, masked):
            at = pl.multiple_of(j * keys, keys)
            k = k_ref[pl.ds(at, keys), :]
            v = v_ref[pl.ds(at, keys), :]
            p = jnp.exp2(dot_t(k, q) * unit - lse)
            if masked:
                cols = at + lax.broadcasted_iota(jnp.int32, (keys, 1), 0)
                p = jnp.where(cols <= limit, p, 0.0)
            dp = dot_t(v, d)
            ds = (p * (dp - delta)).astype(BF16)
            dv[pl.ds(at, keys), :] += dot(p.astype(BF16), d)
            dk[pl.ds(at, keys), :] += dot(ds, q)
            return dq + t_dot(ds, k)

        full, stop = key_blocks(start, block, keys, q_ref.shape[0])
        dq = lax.fori_loop(0, full, functools.partial(step, masked=False), jnp.zeros((block, QK), F32))
        dq = lax.fori_loop(full, stop, functools.partial(step, masked=True), dq)
        dq = (dq * factor).astype(BF16)
        half = tokens // 2
        for t in range(2):
            to = 2 * i + t
            r = t * tokens
            blocks[to, :tokens, :] = dq[r : r + tokens, :NOPE]
            blocks[to, tokens:, :ROPE] = dq[r : r + half, NOPE:]
            blocks[to, tokens:, ROPE:] = dq[r + half : r + tokens, NOPE:]

            @pl.when(to == me)
            def _():
                own.start()

            @pl.when(to != me)
            def _():
                block_to(to).start()

    @pl.loop(0, members)
    def _(b):
        at = pl.ds(pl.multiple_of(b * tokens, tokens), tokens)
        d = jnp.concatenate([dk[at, :NOPE] * factor, dv[at, :]], axis=1).astype(BF16)
        part_ref[b, :, :KVR] = dot_t(d, kvb_ref[...]).astype(BF16)
        part_ref[b, :, KVR:] = (dk[at, NOPE:] * factor).astype(BF16)

    own.wait()

    @pl.loop(1, members)
    def _(d):
        n = lax.rem(me + d, members)
        from_device(n).wait_recv()
        block_to(n).wait_send()
        exchange.copy(d).wait_send()


def attend_back(prefix, q, k, v, o, lse, d, kvb, members, collective_id):
    length = q.shape[0]
    tokens = length // members
    vmem = pl.BlockSpec(memory_space=pltpu.VMEM)
    anywhere = pl.BlockSpec(memory_space=pl.ANY)
    sem = pltpu.SemaphoreType.DMA
    factor = QK**-0.5
    packed = tokens + tokens // 2
    return pl.pallas_call(
        functools.partial(attend_back_kernel, members=members, factor=factor, unit=factor * math.log2(math.e)),
        in_specs=[pl.BlockSpec(memory_space=pltpu.SMEM)] + [vmem] * 5 + [anywhere, vmem],
        out_specs=[vmem, anywhere],
        out_shape=[
            jax.ShapeDtypeStruct((members, tokens, KVR + ROPE), BF16),
            jax.ShapeDtypeStruct((members, packed, NOPE), BF16),
        ],
        scratch_shapes=[
            pltpu.VMEM((members, tokens, VD), BF16),
            pltpu.VMEM((members, packed, NOPE), BF16),
            pltpu.VMEM((length, QK), F32),
            pltpu.VMEM((length, VD), F32),
            sem((members,)), sem((members,)), sem((members,)), sem((members,)), sem, sem,
        ],
        compiler_params=pltpu.CompilerParams(
            collective_id=collective_id, has_side_effects=True, vmem_limit_bytes=50 * 1024 * 1024
        ),
        cost_estimate=pl.CostEstimate(
            flops=length * length * (3 * QK + 2 * VD), bytes_accessed=length * 2000, transcendentals=length * length // 2
        ),
        name="attend_back",
    )(prefix, q, k, v, o, lse, d, kvb)


def silu_parts(v):
    logistic = 0.5 * jnp.tanh(0.5 * v) + 0.5
    return v * logistic, logistic * (1.0 + v * (1.0 - logistic))


def picks(rank, slots):
    at = lax.broadcasted_iota(jnp.int32, (slots, rank.shape[1]), 0).astype(F32)
    return at == rank


def picks_back(rank, slots):
    at = lax.broadcasted_iota(jnp.int32, (rank.shape[0], slots), 1).astype(F32)
    return at == rank


def tiles(width, size):
    return pl.ds(pl.multiple_of(width * size, size), size)


def experts_kernel(
    x_hbm, prob_hbm, c_hbm, rank_ref, back_ref, gate_hbm, up_hbm, down_hbm, own_hbm, sdown_hbm,
    part_hbm, eg_hbm, eu_hbm, eo_hbm, sh_hbm, c_out, prob_out,
    xs, probs, gate, up, down, own, sdown, tail, rows, acts, sacts, part_st, eg_st, eu_st, eo_st, sh_st,
    c_st, sent, got, e_sent, e_got, c_sent, c_got, load, store,
    *, members, slots, tile, wide
):
    me = lax.axis_index("grp")
    levels = members // (SIDE * CORES)
    group = SIDE * CORES
    width, hidden = gate.shape
    half, whole = hidden % tile, hidden // tile
    units = own.shape[1] // 2
    z = me // group
    order = near_first(levels)
    loads = [
        pltpu.make_async_copy(a, b, load.at[n])
        for n, (a, b) in enumerate(
            [
                (x_hbm, xs.at[me]),
                (prob_hbm.at[me], probs.at[me]),
                (own_hbm, own),
                (gate_hbm, gate),
                (up_hbm, up),
                (down_hbm, down),
                (sdown_hbm, sdown),
                (c_hbm, c_st),
            ]
        )
    ]
    gather = Gather(x_hbm, xs, sent, got, members)
    behind = Gather(c_hbm, c_out, c_sent, c_got, members)
    own_c = pltpu.make_async_copy(c_st, c_out.at[me], load.at[7])
    exchange = Exchange(prob_hbm, probs, e_sent, e_got, members)
    for copy in loads:
        copy.start()
    meet(members)
    gather.first()
    exchange.start()
    for copy in loads:
        copy.wait()
    own_c.start()
    tail[:, :half] = gate[:, hidden - half :]
    tail[:, half:] = up[:, hidden - half :]
    gather.pass_on(z)
    gather.relay(1)
    exchange.wait()
    prob_out[...] = probs[...]

    def stores(s, k):
        n = s % 2
        return [
            pltpu.make_async_copy(a, b.at[k], store.at[n, m])
            for m, (a, b) in enumerate(
                [
                    (part_st.at[n], part_hbm),
                    (eg_st.at[n], eg_hbm),
                    (eu_st.at[n], eu_hbm),
                    (eo_st.at[n], eo_hbm),
                    (sh_st.at[n], sh_hbm),
                ]
            )
        ]

    @pl.loop(0, levels)
    def _(s):
        k = pick_from(order, z, s)
        n = s % 2
        gather.take_twin(k)

        @pl.when(s >= 2)
        def _():
            for copy in stores(s, pick_from(order, z, s - 2)):
                copy.wait()

        @pl.loop(0, group)
        def _(b):
            pick = picks(rank_ref[k * group + b, 0:1, :], slots).astype(BF16)
            rows[tiles(b, slots), :] = dot(pick, xs[k * group + b]).astype(BF16)

        def keep(at, g, u):
            eg_st[n, :, at] = g.astype(BF16)
            eu_st[n, :, at] = u.astype(BF16)
            acts[:, at] = (silu_parts(g)[0] * u).astype(BF16)

        @pl.loop(0, whole)
        def _(j):
            at = tiles(j, tile)
            x = rows[...]
            keep(at, dot(x, gate[:, at]), dot(x, up[:, at]))

        last = dot(rows[...], tail[...])
        keep(pl.ds(whole * tile, half), last[:, :half], last[:, half:])

        gather.relay(s + 2)

        @pl.when(s + 1 < levels)
        def _():
            gather.pass_on(pick_from(order, z, s + 1))

        @pl.when(s == levels - 3)
        def _():
            behind.first()

        @pl.when(s >= levels - 2)
        def _():
            behind.relay(s - levels + 3)
            behind.pass_on(pick_from(order, z, s - levels + 2))

        @pl.loop(0, width // wide)
        def _(j):
            at = tiles(j, wide)
            eo_st[n, :, at] = dot(acts[...], down[:, at]).astype(BF16)

        @pl.loop(0, group // 2)
        def _(h):
            x = xs[pl.ds(k * group + 2 * h, 2)].reshape(-1, width)
            pre = dot(x, own[...])
            sh_st[n, pl.ds(2 * h, 2)] = pre.astype(BF16).reshape(2, -1, 2 * units)
            act = (silu_parts(pre[:, :units])[0] * pre[:, units:]).astype(BF16)
            sacts[pl.ds(2 * h, 2)] = act.reshape(2, -1, units)

        @pl.loop(0, group)
        def _(b):
            i = k * group + b
            pick = picks(rank_ref[i, 0:1, :], slots)
            back = picks_back(back_ref[i], slots).astype(BF16)
            g = jnp.sum(jnp.where(pick, probs[i, 0:1, :], 0.0), axis=1, keepdims=True)
            act = sacts[b]
            for j in range(width // wide):
                at = slice(j * wide, (j + 1) * wide)
                weighted = (g * eo_st[n, tiles(b, slots), at].astype(F32)).astype(BF16)
                part_st[n, b, :, at] = (dot(back, weighted) + dot(act, sdown[:, at])).astype(BF16)

        for copy in stores(s, k):
            copy.start()

    @pl.loop(2, levels)
    def _(s):
        behind.relay(s + 1)
        behind.pass_on(pick_from(order, z, s))

    @pl.loop(levels - 2, levels)
    def _(s):
        for copy in stores(s, pick_from(order, z, s)):
            copy.wait()

    @pl.loop(0, levels)
    def _(k):
        behind.take_twin(k)

    own_c.wait()
    gather.finish()
    behind.finish()


def experts_forward(x, prob, c, rank, back, gate, up, down, own, sdown, slots, members, collective_id):
    tokens, width = x.shape
    hidden = gate.shape[1]
    group = SIDE * CORES
    levels = members // group
    packed = group * slots
    anywhere = pl.BlockSpec(memory_space=pl.ANY)
    vmem = pl.BlockSpec(memory_space=pltpu.VMEM)
    sem = pltpu.SemaphoreType.DMA
    tile = 256
    shapes = [
        (levels, group, tokens, width),
        (levels, packed, hidden),
        (levels, packed, hidden),
        (levels, packed, width),
        (levels, group, tokens, own.shape[1]),
    ]
    return pl.pallas_call(
        functools.partial(experts_kernel, members=members, slots=slots, tile=tile, wide=512),
        in_specs=[anywhere, anywhere, anywhere, vmem, vmem] + [anywhere] * 5,
        out_specs=[anywhere] * 6 + [vmem],
        out_shape=[jax.ShapeDtypeStruct(s, BF16) for s in shapes]
        + [jax.ShapeDtypeStruct((members, *c.shape), BF16)]
        + [jax.ShapeDtypeStruct(prob.shape, F32)],
        scratch_shapes=[
            pltpu.VMEM((members, tokens, width), BF16),
            pltpu.VMEM(prob.shape, F32),
            pltpu.VMEM(gate.shape, BF16),
            pltpu.VMEM(up.shape, BF16),
            pltpu.VMEM(down.shape, BF16),
            pltpu.VMEM(own.shape, BF16),
            pltpu.VMEM(sdown.shape, BF16),
            pltpu.VMEM((width, tile), BF16),
            pltpu.VMEM((packed, width), BF16),
            pltpu.VMEM((packed, hidden), BF16),
            pltpu.VMEM((group, tokens, own.shape[1] // 2), BF16),
        ]
        + [pltpu.VMEM((2, *s[1:]), BF16) for s in shapes]
        + [pltpu.VMEM(c.shape, BF16)]
        + [sem((6, members)), sem((2, members)), sem((members,)), sem((members,))]
        + [sem((6, members)), sem((2, members)), sem((8,)), sem((2, 5))],
        compiler_params=pltpu.CompilerParams(
            collective_id=collective_id, has_side_effects=True, vmem_limit_bytes=63 * 1024 * 1024
        ),
        cost_estimate=pl.CostEstimate(
            flops=12 * members * slots * width * hidden, bytes_accessed=60_000_000, transcendentals=0
        ),
        name="experts_forward",
    )(x, prob, c, rank, back, gate, up, down, own, sdown)


def experts_back_kernel(
    c_hbm, c2_hbm, rank_ref, back_ref, prob_ref, eg_hbm, eu_hbm, eo_hbm, sh_hbm, gate_hbm, up_hbm, down_hbm, own_hbm, sdown_hbm,
    out, dg_out,
    part, cs, eg, eu, eo, sh, gate, up, down, own, sdown, rows, d_gate, d_up, dg_st, dg_in,
    *sems, members, slots, tile, wide
):
    twin_in, side_in, line_in = sems[:3]
    e_sent, e_got, load, fetch = sems[11:15]
    me = lax.axis_index("grp")
    levels = members // (SIDE * CORES)
    group = SIDE * CORES
    width, hidden = gate.shape
    half, whole = hidden % tile, hidden // tile
    units = own.shape[1] // 2
    z = me // group
    order = far_first(levels)
    reduce = Reduce(part, twin_in, side_in, line_in, sems[3:11], members)
    exchange = Exchange(dg_st, dg_in, e_sent, e_got, members)

    def cotangents(s):
        k = pick_from(order, z, s)
        return [
            pltpu.make_async_copy(
                a.at[k], cs.at[s % 2, :, :, pl.ds(h * (width // 2), width // 2)], fetch.at[4 + s % 2 * 2 + h]
            )
            for h, a in enumerate([c_hbm, c2_hbm])
        ]

    def kept(s):
        k = pick_from(order, z, s)
        return [
            pltpu.make_async_copy(a.at[k], b, fetch.at[m])
            for m, (a, b) in enumerate([(eo_hbm, eo), (eg_hbm, eg), (eu_hbm, eu), (sh_hbm, sh)])
        ]

    loads = [
        pltpu.make_async_copy(a, b, load.at[n])
        for n, (a, b) in enumerate(
            [(down_hbm, down), (gate_hbm, gate), (up_hbm, up), (own_hbm, own), (sdown_hbm, sdown)]
        )
    ]
    for copy in cotangents(0) + kept(0):
        copy.start()
    for copy in loads:
        copy.start()
    meet(members)

    def early(s):
        return (z == 0) | (z == levels - 1)

    @pl.loop(0, levels)
    def _(s):
        k = pick_from(order, z, s)
        n = s % 2
        for copy in cotangents(s):
            copy.wait()
        load_eo, load_eg, load_eu, load_sh = kept(s)

        @pl.when(s + 1 < levels)
        def _():
            for copy in cotangents(s + 1):
                copy.start()

        load_eo.wait()
        @pl.loop(0, group)
        def _(b):
            i = k * group + b
            at = tiles(b, slots)
            pick = picks(rank_ref[i, 0:1, :], slots)
            c = dot(pick.astype(BF16), cs[n, b])
            g = jnp.sum(jnp.where(pick, prob_ref[i, 0:1, :], 0.0), axis=1, keepdims=True)
            along = jnp.sum(c * eo[at, :].astype(F32), axis=1, keepdims=True)
            dg_st[i] = jnp.broadcast_to(
                jnp.sum(jnp.where(pick, along, 0.0), axis=0, keepdims=True), dg_st.shape[1:]
            )
            rows[at, :] = (g * c).astype(BF16)

        @pl.when(s == 0)
        def _():
            for copy in loads:
                copy.wait()

        load_eg.wait()
        load_eu.wait()

        def slopes(at):
            d = dot_t(rows[...], down[at, :])
            act, slope = silu_parts(eg[:, at].astype(F32))
            d_gate[:, at] = (d * eu[:, at].astype(F32) * slope).astype(BF16)
            d_up[:, at] = (d * act).astype(BF16)

        @pl.loop(0, whole)
        def _(j):
            slopes(tiles(j, tile))

        slopes(pl.ds(whole * tile, half))

        @pl.when(s >= 1)
        def _():
            reduce.chip(pick_from(order, z, s - 1))

        @pl.when((s >= 2) & ~early(s))
        def _():
            reduce.line(pick_from(order, z, s - 2))

        @pl.loop(0, width // tile)
        def _(j):
            at = tiles(j, tile)
            eo[:, at] = (dot_t(d_gate[...], gate[at, :]) + dot_t(d_up[...], up[at, :])).astype(BF16)

        load_sh.wait()
        @pl.loop(0, group)
        def _(b):
            i = k * group + b
            back = picks_back(back_ref[i], slots).astype(BF16)
            d = dot_t(cs[n, b], sdown[...])
            pre = sh[b].astype(F32)
            act, slope = silu_parts(pre[:, :units])
            both = jnp.concatenate([d * pre[:, units:] * slope, d * act], axis=1).astype(BF16)
            for j in range(width // wide):
                at = slice(j * wide, (j + 1) * wide)
                part[i, :, at] = (
                    dot(back, eo[tiles(b, slots), at]) + dot_t(both, own[at, :])
                ).astype(BF16)

        reduce.start(k)

        @pl.when(s + 1 < levels)
        def _():
            for copy in kept(s + 1):
                copy.start()

        @pl.when((s >= 1) & early(s))
        def _():
            reduce.line(pick_from(order, z, s - 1))

    exchange.start()
    dg_in[me] = dg_st[me]
    reduce.chip(z)

    @pl.when(~early(0))
    def _():
        reduce.line(pick_from(order, z, levels - 2))

    reduce.last(out)
    reduce.finish()
    exchange.wait()
    dg_out[...] = dg_in[...]


def experts_backward(cs, rank, back, prob, kept, gate, up, down, own, sdown, slots, members, collective_id):
    tokens, width = cs[0].shape[1], cs[0].shape[2] * 2
    hidden = gate.shape[1]
    group = SIDE * CORES
    levels = members // group
    packed = group * slots
    anywhere = pl.BlockSpec(memory_space=pl.ANY)
    vmem = pl.BlockSpec(memory_space=pltpu.VMEM)
    sem = pltpu.SemaphoreType.DMA
    eg, eu, eo, sh = kept
    return pl.pallas_call(
        functools.partial(experts_back_kernel, members=members, slots=slots, tile=256, wide=512),
        in_specs=[anywhere, anywhere, vmem, vmem, vmem] + [anywhere] * 9,
        out_specs=[vmem, vmem],
        out_shape=[
            jax.ShapeDtypeStruct((tokens, width), BF16),
            jax.ShapeDtypeStruct((members, 8, tokens), F32),
        ],
        scratch_shapes=[
            pltpu.VMEM((members, tokens, width), BF16),
            pltpu.VMEM((2, group, tokens, width), BF16),
            pltpu.VMEM(eg.shape[1:], BF16),
            pltpu.VMEM(eu.shape[1:], BF16),
            pltpu.VMEM(eo.shape[1:], BF16),
            pltpu.VMEM(sh.shape[1:], BF16),
            pltpu.VMEM(gate.shape, BF16),
            pltpu.VMEM(up.shape, BF16),
            pltpu.VMEM(down.shape, BF16),
            pltpu.VMEM(own.shape, BF16),
            pltpu.VMEM(sdown.shape, BF16),
            pltpu.VMEM((packed, width), BF16),
            pltpu.VMEM((packed, hidden), BF16),
            pltpu.VMEM((packed, hidden), BF16),
            pltpu.VMEM((members, 8, tokens), F32),
            pltpu.VMEM((members, 8, tokens), F32),
        ]
        + Reduce.scratch(members, tokens, width, BF16)
        + [sem((members,)), sem((members,)), sem((5,)), sem((8,))],
        compiler_params=pltpu.CompilerParams(
            collective_id=collective_id, has_side_effects=True, vmem_limit_bytes=67_043_328
        ),
        cost_estimate=pl.CostEstimate(
            flops=12 * members * slots * width * hidden, bytes_accessed=60_000_000, transcendentals=0
        ),
        name="experts_backward",
    )(*(c.reshape(levels, group, tokens, -1) for c in cs), rank, back, prob, *kept, gate, up, down, own, sdown)


class Spread:
    def __init__(self, src, out, common, commons, sems, members, sequences):
        self.src, self.out, self.common, self.commons = src, out, common, commons
        self.sent, self.got, self.sent2, self.got2 = sems
        self.members, self.sequences = members, sequences
        self.me, self.mine = lax.axis_index("grp"), lax.axis_index("rep")

    def other(self, n):
        r = lax.rem(self.mine + n // self.members, self.sequences)
        return {"rep": r, "grp": lax.rem(self.me + n % self.members, self.members)}

    def meet(self):
        barrier = pltpu.get_barrier_semaphore()
        count = self.members * self.sequences

        @pl.loop(1, count)
        def _(n):
            pl.semaphore_signal(barrier, 1, device_id=self.other(n), device_id_type=MESH)

        pl.semaphore_wait(barrier, count - 1)

    def block(self, n):
        to = self.other(n)
        return send(self.src.at[to["grp"]], self.out.at[self.mine, self.me], self.sent.at[n], self.got.at[n], to)

    def whole(self, n):
        return send(self.common, self.commons.at[self.mine], self.sent2.at[n], self.got2.at[n], self.other(n * self.members))

    def start_blocks(self):
        @pl.loop(1, self.members * self.sequences)
        def _(n):
            self.block(n).start()

    def start_common(self):
        @pl.loop(1, self.sequences)
        def _(n):
            self.whole(n).start()

    def wait(self):
        @pl.loop(1, self.members * self.sequences)
        def _(n):
            self.block(n).wait()

        @pl.loop(1, self.sequences)
        def _(n):
            self.whole(n).wait()


def finish_kernel(
    part, o_src, dq_ref, cos_ref, sin_ref, q_hbm, kva_ref, up_ref, down_ref, small_ref, normed_ref, latent_ref, kvg_ref,
    x_ref, xg_ref, dmid_ref, name_ref,
    out, q_out, o_out,
    *bufs, members, sequences
):
    twin_in, side_in, line_in = bufs[:3]
    o_in, o_common, q_parts, d_query, wq, dn, d_lat, d_latent, ds_ref = bufs[11:20]
    o_sent, o_got, b_sent, b_got, w_sent, w_got, local = bufs[20:]
    reduce = Reduce(part, twin_in, side_in, line_in, bufs[3:11], members)
    exchange = Exchange(o_src, o_in, o_sent, o_got, members)
    spread = Spread(q_parts, q_out, o_common, o_out, (b_sent, b_got, w_sent, w_got), members, sequences)
    me, mine = spread.me, spread.mine
    order = far_first(reduce.levels)
    z, levels = reduce.z, reduce.levels
    tokens, width = x_ref.shape
    tile = 256
    load = pltpu.make_async_copy(q_hbm, wq, local.at[0])
    own = [
        pltpu.make_async_copy(q_parts.at[me], q_out.at[mine, me], local.at[1]),
        pltpu.make_async_copy(o_common, o_out.at[mine], local.at[2]),
    ]
    load.start()
    spread.meet()

    @pl.loop(0, levels)
    def _(s):
        reduce.start(pick_from(order, z, s))

    exchange.start()
    o_in[me] = o_src[me]
    cosine, sine = cos_ref[...], sin_ref[...]
    half = ROPE // 2
    for pair in range(dq_ref.shape[0] // 2):
        pieces = []
        for h in (2 * pair, 2 * pair + 1):
            rope = jnp.concatenate([dq_ref[h, tokens:, :ROPE], dq_ref[h, tokens:, ROPE:]], axis=0).astype(F32)
            turned = jnp.concatenate([rope[:, half:], rope[:, :half]], axis=1)
            pieces += [dq_ref[h, :tokens, :], (rope * cosine + turned * sine).astype(BF16)]
        d_query[:, pair * 2 * QK : (pair + 1) * 2 * QK] = jnp.concatenate(pieces, axis=1)

    @pl.loop(0, levels)
    def _(s):
        reduce.chip(pick_from(order, z, s))

    grad_up = t_dot(small_ref[...], d_query[...])
    ds_ref[...] = dot_t(d_query[...], up_ref[...]).astype(BF16)
    grad_down = t_dot(ds_ref[...], normed_ref[...])
    rows = width // members
    for g in range(members):
        first = g // 2 * 2 * QK
        q_parts[g] = jnp.concatenate(
            [grad_down[:, g * rows : (g + 1) * rows], grad_up[:, first : first + 2 * QK]], axis=1
        ).astype(BF16)
    spread.start_blocks()
    own[0].start()
    exchange.wait()
    total = jnp.zeros(o_in.shape[1:], F32)
    for g in range(members):
        total = total + o_in[g].astype(F32)
    o_common[...] = jnp.concatenate([total, name_ref[...]], axis=1)
    spread.start_common()
    own[1].start()
    load.wait()
    every = width // tile // (levels - 1)

    @pl.loop(0, width // tile)
    def _(j):
        dn[:, tiles(j, tile)] = dot_t(d_query[...], wq[pl.ds(j * (tile // rows), tile // rows)].reshape(tile, -1))

        @pl.when((j % every == every - 1) & (j // every < levels - 1))
        def _():
            reduce.line(pick_from(order, z, j // every))

    reduce.last(d_lat)
    gradient = d_lat[...].astype(F32)
    latent = latent_ref[...]
    d_latent[:, :KVR] = norm_back(latent[:, :KVR], kvg_ref[...], gradient[:, :KVR]).astype(BF16)
    rope = gradient[:, KVR:]
    turned = jnp.concatenate([rope[:, half:], rope[:, :half]], axis=1)
    d_latent[:, KVR:] = (rope * cosine + turned * sine).astype(BF16)

    @pl.loop(0, width // tile)
    def _(j):
        at = tiles(j, tile)
        dn[:, at] += dot_t(d_latent[...], kva_ref[at, :]) + dot_t(ds_ref[...], down_ref[at, :])

    out[...] = (dmid_ref[...] + norm_back(x_ref[...].astype(F32), xg_ref[...], dn[...])).astype(BF16)
    reduce.finish()
    spread.wait()
    for copy in own:
        copy.wait()


def finish(part, o_parts, dq, cosine, sine, all_q, kva, up, down, small, normed, latent, kvg, x, xg, dmid, name, sequences, collective_id):
    members, tokens, c = part.shape
    width = x.shape[1]
    rank = o_parts.shape[1]
    vmem = pl.BlockSpec(memory_space=pltpu.VMEM)
    anywhere = pl.BlockSpec(memory_space=pl.ANY)
    sem = pltpu.SemaphoreType.DMA
    share = width // members + 2 * QK
    common = (rank, o_parts.shape[2] + name.shape[1])
    return pl.pallas_call(
        functools.partial(finish_kernel, members=members, sequences=sequences),
        in_specs=[vmem] * 5 + [anywhere] + [vmem] * 11,
        out_specs=[vmem, anywhere, anywhere],
        out_shape=[
            jax.ShapeDtypeStruct((tokens, width), BF16),
            jax.ShapeDtypeStruct((sequences, members, rank, share), BF16),
            jax.ShapeDtypeStruct((sequences, *common), F32),
        ],
        scratch_shapes=Reduce.scratch(members, tokens, c, BF16)
        + [
            pltpu.VMEM(o_parts.shape, BF16),
            pltpu.VMEM(common, F32),
            pltpu.VMEM((members, rank, share), BF16),
            pltpu.VMEM((tokens, H * QK), BF16),
            pltpu.VMEM(all_q.shape, BF16),
            pltpu.VMEM((tokens, width), F32),
            pltpu.VMEM((tokens, c), BF16),
            pltpu.VMEM((tokens, c), BF16),
            pltpu.VMEM((tokens, rank), BF16),
        ]
        + [sem((n,)) for n in (members,) * 2 + (members * sequences,) * 2 + (sequences,) * 2 + (3,)],
        compiler_params=pltpu.CompilerParams(
            collective_id=collective_id, has_side_effects=True, vmem_limit_bytes=56 * 1024 * 1024
        ),
        cost_estimate=pl.CostEstimate(flops=4 * tokens * width * H * QK, bytes_accessed=40_000_000, transcendentals=0),
        name="finish",
    )(part, o_parts, dq, cosine, sine, all_q, kva, up, down, small, normed, latent, kvg, x, xg, dmid, name)


def by_owner(gradient, members):
    return gradient.astype(BF16).reshape(gradient.shape[0], members, -1).transpose(1, 0, 2)


def pack(v):
    half = v.shape[1] // 2
    rope = jnp.concatenate([v[:, :half, NOPE:], v[:, half:, NOPE:]], axis=-1)
    return jnp.concatenate([v[:, :, :NOPE], rope], axis=1)


def unpack(v):
    rows = v.shape[1] * 2 // 3
    rope = jnp.concatenate([v[:, rows:, :ROPE], v[:, rows:, ROPE:]], axis=1)
    return jnp.concatenate([v[:, :rows], rope], axis=-1)


def per_device(
    hidden,
    grad_out,
    expert_ids,
    prefix_len,
    adapter_id,
    attn_gain,
    kv_gain,
    ffn_gain,
    w_q,
    w_kva,
    w_kvb,
    w_o,
    w_router,
    shared_gate,
    shared_up,
    shared_down,
    expert_gate,
    expert_up_weight,
    expert_down,
    q_down,
    q_up,
    o_down,
    o_up,
):
    tokens = hidden.shape[1]
    width = hidden.shape[2]
    members = lax.axis_size("grp")
    length = tokens * members
    experts = expert_gate.shape[0] * members
    capacity = tokens * TOP * 5 // (4 * experts)
    slots = -(-capacity // 16) * 16
    me = lax.axis_index("grp")

    inputs = hidden[0].astype(F32)
    cotangent = grad_out[0]
    c32 = cotangent.astype(F32)
    routes = expert_ids[0]
    adapter = adapter_id[0]
    pick = lambda table: lax.dynamic_index_in_dim(table, adapter, 0, keepdims=False)
    qa_down, qa_up, oa_down, oa_up = pick(q_down), pick(q_up), pick(o_down), pick(o_up)

    chosen_by = jnp.sum(
        (routes[:, :, None] == jnp.arange(experts, dtype=jnp.int32)[None, None, :]).astype(F32), axis=1
    )
    sequences = lax.axis_size("rep")
    split = w_q.shape[0] * 3 // 128 * 16 if sequences % 2 == 0 else 0
    (all_kva, all_q, all_o), _ = communicate([w_kva, w_q, w_o], [], members, 1, [split] * 3)
    full_kva, full_q, full_o = (v.reshape(-1, v.shape[2]) for v in (all_kva, all_q, all_o))
    hidden_slice = shared_down.shape[0]
    shared = after(jnp.stack([shared_gate, shared_up], axis=1), all_q)
    shared = shared.reshape(shared.shape[0], 2, members, hidden_slice).transpose(2, 0, 1, 3)
    own_shared = exchange(shared.reshape(members, -1, 2 * hidden_slice)).reshape(width, 2 * hidden_slice)

    positions = me * tokens + jnp.arange(tokens, dtype=jnp.int32)
    cosine, sine = angles(positions, ROPE)
    normed = root_norm(inputs, attn_gain).astype(BF16)
    latent = dot(normed, full_kva)
    compressed = root_norm(latent[:, :KVR], kv_gain).astype(BF16)
    k_rope = rotate(latent[:, KVR:], cosine, sine).astype(BF16)
    q_small = dot(normed, qa_down).astype(BF16)
    query = (dot(normed, full_q) + dot(q_small, qa_up)).reshape(tokens, H, QK)
    query = jnp.concatenate(
        [query[:, :, :NOPE], rotate(query[:, :, NOPE:], cosine[:, None], sine[:, None])], axis=-1
    ).astype(BF16)
    (all_latent, all_router), (q_packed, kvb_parts, chosen_all) = communicate(
        [jnp.concatenate([compressed, k_rope], axis=-1), w_router],
        [
            after(pack(query.transpose(1, 0, 2)), own_shared),
            w_kvb.reshape(w_kvb.shape[0], members, -1).transpose(1, 0, 2),
            jnp.broadcast_to(chosen_by.T[:, None, :], (experts, 8, tokens)),
        ],
        members,
        2,
    )
    full_router = all_router.reshape(width, -1)
    own_kvb = kvb_parts.reshape(KVR, -1)
    all_latent = all_latent.reshape(length, KVR + ROPE)
    q_head = unpack(q_packed).reshape(length, QK)
    q_head, c_first = lax.optimization_barrier((q_head, cotangent[:, : width // 2]))
    expanded = dot(all_latent[:, :KVR], own_kvb).astype(BF16)
    k_head = jnp.concatenate([expanded[:, :NOPE], all_latent[:, KVR:]], axis=-1)
    v_head = expanded[:, NOPE:]
    mixture, lse, mixed_parts = attend(prefix_len, q_head, k_head, v_head, members, 3)
    mixed = mixed_parts.transpose(1, 0, 2).reshape(tokens, H * VD)
    o_small = dot(mixed, oa_down).astype(BF16)
    middle = inputs + dot(mixed, full_o) + dot(o_small, oa_up)
    ffn_in = root_norm(middle, ffn_gain).astype(BF16)
    route_probs = jax.nn.softmax(dot(ffn_in, full_router), axis=-1)

    half = width // 2
    first_c = gather(c_first).reshape(members, tokens, half)
    chosen = chosen_all[:, 0] > 0.5
    order = jnp.arange(tokens, dtype=jnp.int32)
    before = (order[:, None] < order[None, :]).astype(BF16)
    rank = jnp.where(chosen, dot(chosen.astype(BF16), before), -1.0)
    back = rank[:, :, None]
    rank = jnp.broadcast_to(rank[:, None, :], (members, 8, tokens))
    weights = (expert_gate[0], expert_up_weight[0], expert_down[0], own_shared, shared_down)
    prob_blocks = jnp.broadcast_to(route_probs.T[:, None, :], (experts, 8, tokens))
    partial, kept_gate, kept_up, kept_out, kept_shared, second_c, prob_parts = experts_forward(
        ffn_in, prob_blocks, cotangent[:, half:], rank, back, *weights, slots, members, 4
    )
    kept = (kept_gate, kept_up, kept_out, kept_shared)
    ffn_out = scatter_sum(partial.reshape(length, width))
    d_own, d_route = experts_backward(
        (first_c, second_c), rank, back, prob_parts, kept, *weights, slots, members, 5
    )
    d_route = d_route[:, 0].T
    d_logits = (
        route_probs * (d_route - jnp.sum(route_probs * d_route, axis=-1, keepdims=True))
    ).astype(BF16)
    d_ffn = d_own.astype(F32) + dot_t(d_logits, full_router)
    d_middle = c32 + norm_back(middle, ffn_gain, d_ffn)
    d_attn = d_middle.astype(BF16)
    grad_oup = t_dot(o_small, d_attn)
    d_osmall = dot_t(d_attn, oa_up).astype(BF16)
    grad_odown = t_dot(d_osmall, mixed)
    d_mixed = (dot_t(d_attn, full_o) + dot_t(d_osmall, oa_down)).astype(BF16)
    d_latents, d_query = attend_back(
        prefix_len,
        q_head,
        k_head,
        v_head,
        mixture,
        lse.reshape(members // 2, 1, 2 * tokens),
        d_mixed.reshape(tokens, H, VD).transpose(1, 0, 2),
        own_kvb,
        members,
        6,
    )
    o_parts = jnp.concatenate([by_owner(g, members) for g in (grad_odown, grad_oup)], axis=-1)
    name = jnp.broadcast_to(adapter.astype(F32), (qa_up.shape[0], 128))
    grad_inputs, q_shares, o_shares = finish(
        d_latents,
        o_parts,
        d_query,
        jnp.concatenate([cosine, cosine], axis=1),
        jnp.concatenate([sine, -sine], axis=1),
        all_q,
        full_kva,
        qa_up,
        qa_down,
        q_small,
        normed,
        latent,
        kv_gain[None],
        hidden[0],
        attn_gain[None],
        d_middle,
        name,
        sequences,
        7,
    )
    ffn_out, _ = lax.optimization_barrier((ffn_out, d_query))
    output = (middle + ffn_out.astype(F32)).astype(BF16)
    numbers = o_shares[:, 0, -1].astype(jnp.int32)
    q_share = jnp.sum(q_shares.astype(F32), axis=1)
    rows = width // members
    q_up_share = lax.dynamic_slice_in_dim(q_share[..., rows:], me % 2 * QK, QK, 2)
    shares = jnp.concatenate([q_share[..., :rows], q_up_share, o_shares[:, :, :-128]], axis=-1)
    selector = (jnp.arange(q_down.shape[0], dtype=jnp.int32)[:, None] == numbers[None, :]).astype(F32)
    summed = jnp.sum(selector[:, :, None, None] * shares[None], axis=1)
    sizes = [rows, QK, rows, rows]
    ends = [sum(sizes[: n + 1]) for n in range(4)]
    outs = [summed[:, :, e - s : e] for e, s in zip(ends, sizes)]
    return (
        output[None],
        grad_inputs[None],
        outs[0].transpose(0, 2, 1),
        outs[1],
        outs[2].transpose(0, 2, 1),
        outs[3],
    )


def solution(mesh):
    seq = P("rep", "grp", None)
    rows = P("grp", None)
    in_specs = (
        (seq, seq, seq, P("rep"), P("rep"), P(), P(), P())
        + (rows,) * 8
        + (P("grp", None, None),) * 3
        + (P(),) * 4
    )
    out_specs = (
        seq,
        seq,
        P(None, "grp", None),
        P(None, None, "grp"),
        P(None, "grp", None),
        P(None, None, "grp"),
    )
    return jax.shard_map(
        per_device, mesh=mesh, in_specs=in_specs, out_specs=out_specs, check_vma=False
    )
```

```python
import functools
import math

import jax
import jax.numpy as jnp
from jax import lax
from jax.experimental import pallas as pl
from jax.experimental.pallas import tpu as pltpu
from jax.sharding import PartitionSpec as P

H = 16
NOPE = 128
ROPE = 64
VD = 128
KVR = 512
TOP = 6
QK = NOPE + ROPE
EPS = 1e-06
F32 = jnp.float32
BF16 = jnp.bfloat16


def dot(former, latter):
    return jnp.dot(former, latter, preferred_element_type=F32)


def dot_t(former, latter):
    return lax.dot_general(
        former, latter, (((1,), (1,)), ((), ())), preferred_element_type=F32
    )


def t_dot(former, latter):
    return lax.dot_general(
        former, latter, (((0,), (0,)), ((), ())), preferred_element_type=F32
    )


def root_norm(v, gains):
    factor = lax.rsqrt(jnp.mean(v * v, axis=-1, keepdims=True) + EPS)
    return v * factor * gains


def norm_back(v, gains, gradient):
    factor = lax.rsqrt(jnp.mean(v * v, axis=-1, keepdims=True) + EPS)
    weighted = gradient * gains
    return factor * weighted - v * (factor * factor * factor) * jnp.mean(
        weighted * v, axis=-1, keepdims=True
    )


def angles(positions, width):
    frequency = 10000.0 ** (-jnp.arange(0, width, 2, dtype=F32) / width)
    phases = positions.astype(F32)[:, None] * frequency[None, :]
    return (jnp.cos(phases), jnp.sin(phases))


def rotate(v, cosine, sine):
    half = v.shape[-1] // 2
    a, b = v[..., :half], v[..., half:]
    return jnp.concatenate([a * cosine - b * sine, b * cosine + a * sine], axis=-1)


def unrotate(v, cosine, sine):
    half = v.shape[-1] // 2
    a, b = v[..., :half], v[..., half:]
    return jnp.concatenate([a * cosine + b * sine, b * cosine - a * sine], axis=-1)


SIDE = 2
CORES = 2
MESH = pl.DeviceIdType.MESH


def place_of():
    me = lax.axis_index("grp")
    return me // (SIDE * CORES), (me // CORES) % SIDE, me % CORES


def index_of(z, x, c):
    return (z * SIDE + x) * CORES + c


def send(src, dst, sent, got, to):
    return pltpu.make_async_remote_copy(
        src_ref=src,
        dst_ref=dst,
        send_sem=sent,
        recv_sem=got,
        device_id=to if isinstance(to, dict) else {"grp": to},
        device_id_type=MESH,
    )


def meet(members, partner=None):
    barrier = pltpu.get_barrier_semaphore()
    me = lax.axis_index("grp")

    @pl.loop(1, members)
    def _(d):
        pl.semaphore_signal(barrier, 1, device_id={"grp": lax.rem(me + d, members)}, device_id_type=MESH)

    if partner is not None:
        pl.semaphore_signal(barrier, 1, device_id=partner, device_id_type=MESH)
    pl.semaphore_wait(barrier, members - 1 + (partner is not None))


def pick_from(table, z, s):
    v = 0
    for i, row in enumerate(table):
        for j, entry in enumerate(row):
            if entry:
                v = v + jnp.where((z == i) & (s == j), entry, 0)
    return v


def near_first(levels):
    return [sorted(range(levels), key=lambda v: (abs(v - k), v)) for k in range(levels)]


def far_first(levels):
    return [sorted((v for v in range(levels) if v != k), key=lambda v: (-abs(v - k), v)) + [k] for k in range(levels)]


class Gather:
    def __init__(self, src, out, sent, got, members, split=0):
        self.src, self.out, self.sent, self.got = src, out, sent, got
        self.members, self.split = members, split
        self.levels = members // (SIDE * CORES)
        self.z, self.x, self.c = z, x, c = place_of()
        self.me = lax.axis_index("grp")
        self.up, self.down = index_of(z + 1, x, c), index_of(z - 1, x, c)
        self.side, self.twin = index_of(z, 1 - x, c), index_of(z, x, 1 - c)
        if split:
            rows = src.shape[0]
            rep = lax.axis_index("rep")
            odd = rep % 2
            self.partner = {"rep": rep + 1 - 2 * odd, "grp": self.me}
            self.window = pl.ds(pl.multiple_of(odd * split, 16), rows - split)
            self.given = pl.ds(pl.multiple_of(odd * (rows - split), 16), split)
            self.lacked = pl.ds(pl.multiple_of((1 - odd) * (rows - split), 16), split)

    def copy(self, slot, kind, to, own=False, rows=None):
        rows = rows or (self.window if self.split else None)
        other = rows is not None and self.split and rows is not self.window
        src = self.src if own else self.out.at[slot]
        dst = self.out.at[slot]
        if rows is not None:
            src, dst = src.at[rows], dst.at[rows]
        return send(src, dst, self.sent.at[kind, slot], self.got.at[int(bool(other)), slot], to)

    def arrive(self, slot):
        self.copy(slot, 0, self.twin).wait_recv()

    def to_partner(self, slot):
        return self.copy(slot, 4, self.partner, rows=self.given)

    def lacked_to_twin(self, slot, own=False):
        return self.copy(slot, 5, self.twin, own, rows=self.lacked)

    def first(self):
        @pl.when(self.z < self.levels - 1)
        def _():
            self.copy(self.me, 0, self.up, True).start()

        @pl.when(self.z > 0)
        def _():
            self.copy(self.me, 1, self.down, True).start()

        self.copy(self.me, 2, self.side, True).start()
        self.copy(self.me, 3, self.twin, True).start()
        if self.split:
            self.lacked_to_twin(self.me, True).start()

    def relay(self, s):
        @pl.when(self.z >= s)
        def _():
            slot = index_of(self.z - s, self.x, self.c)
            self.arrive(slot)

            @pl.when(self.z < self.levels - 1)
            def _():
                self.copy(slot, 0, self.up).start()

            self.spread(slot)

        @pl.when(self.z + s < self.levels)
        def _():
            slot = index_of(self.z + s, self.x, self.c)
            self.arrive(slot)

            @pl.when(self.z > 0)
            def _():
                self.copy(slot, 1, self.down).start()

            self.spread(slot)

    def spread(self, slot):
        self.copy(slot, 2, self.side).start()
        self.copy(slot, 3, self.twin).start()
        if self.split:
            self.to_partner(slot).start()

    def pass_on(self, k):
        slot = index_of(k, 1 - self.x, self.c)
        self.arrive(slot)
        self.copy(slot, 3, self.twin).start()
        if self.split:
            self.to_partner(slot).start()

    def take_lacked(self, k, x):
        slot = index_of(k, x, self.c)

        @pl.when(slot != self.me)
        def _():
            self.copy(slot, 4, self.partner, rows=self.lacked).wait_recv()
            self.lacked_to_twin(slot).start()

    def take_twin(self, k):
        for x in range(SIDE):
            self.arrive(index_of(k, x, 1 - self.c))

    def take_twin_lacked(self):
        @pl.loop(0, self.members // CORES)
        def _(i):
            self.lacked_to_twin(i * CORES + 1 - self.c).wait_recv()

    def finish(self):
        @pl.loop(0, self.levels)
        def _(k):
            slot = index_of(k, self.x, self.c)
            self.copy(slot, 2, self.side).wait_send()

            @pl.when((k <= self.z) & (self.z < self.levels - 1))
            def _():
                self.copy(slot, 0, self.up).wait_send()

            @pl.when((k >= self.z) & (self.z > 0))
            def _():
                self.copy(slot, 1, self.down).wait_send()

        @pl.loop(0, self.members // CORES)
        def _(i):
            slot = i * CORES + self.c
            self.copy(slot, 3, self.twin).wait_send()
            if self.split:
                self.lacked_to_twin(slot).wait_send()

                @pl.when(slot != self.me)
                def _():
                    self.to_partner(slot).wait_send()


class Exchange:
    def __init__(self, src, out, sent, got, members):
        self.src, self.out, self.sent, self.got, self.members = src, out, sent, got, members
        self.me = lax.axis_index("grp")

    def copy(self, d):
        to = lax.rem(self.me + d, self.members)
        return send(self.src.at[to], self.out.at[self.me], self.sent.at[d], self.got.at[d], to)

    def start(self):
        @pl.loop(1, self.members)
        def _(d):
            self.copy(d).start()

    def wait(self):
        @pl.loop(1, self.members)
        def _(d):
            self.copy(d).wait()


class Reduce:
    def __init__(self, p, twin_in, side_in, line_in, sems, members):
        self.p, self.twin_in, self.side_in, self.line_in = p, twin_in, side_in, line_in
        self.sems = sems
        self.levels = members // (SIDE * CORES)
        self.z, self.x, self.c = place_of()

    def copy(self, kind, slot, dst, n, to):
        sent, got = self.sems[2 * kind], self.sems[2 * kind + 1]
        return send(self.p.at[slot], dst.at[n], sent.at[n], got.at[n], to)

    def to_twin(self, k, w):
        twin = index_of(self.z, self.x, 1 - self.c)
        return self.copy(0, index_of(k, w, 1 - self.c), self.twin_in, k * SIDE + w, twin)

    def to_side(self, k):
        return self.copy(1, index_of(k, 1 - self.x, self.c), self.side_in, k, index_of(self.z, 1 - self.x, self.c))

    def to_up(self, k):
        return self.copy(2, index_of(k, self.x, self.c), self.line_in, k + 1, index_of(self.z + 1, self.x, self.c))

    def to_down(self, k):
        return self.copy(3, index_of(k, self.x, self.c), self.line_in, k, index_of(self.z - 1, self.x, self.c))

    def add(self, slot, ref):
        rows = self.p.shape[1]
        chunk = next(r for r in (32, 16, 8) if rows % r == 0)

        @pl.loop(0, rows // chunk)
        def _(i):
            at = pl.ds(pl.multiple_of(i * chunk, chunk), chunk)
            self.p[slot, at, :] = (self.p[slot, at, :].astype(F32) + ref[at, :].astype(F32)).astype(self.p.dtype)

    def start(self, k):
        self.to_twin(k, self.x).start()
        self.to_twin(k, 1 - self.x).start()

    def chip(self, k):
        w = 1 - self.x
        self.to_twin(k, w).wait_recv()
        self.add(index_of(k, w, self.c), self.twin_in.at[k * SIDE + w])
        self.to_side(k).start()
        self.to_twin(k, self.x).wait_recv()
        self.add(index_of(k, self.x, self.c), self.twin_in.at[k * SIDE + self.x])

    def line(self, k):
        z, mine = self.z, index_of(k, self.x, self.c)
        self.to_side(k).wait_recv()
        self.add(mine, self.side_in.at[k])

        @pl.when((k > z) & (z > 0))
        def _():
            self.to_up(k).wait_recv()
            self.add(mine, self.line_in.at[k + 1])

        @pl.when((k < z) & (z < self.levels - 1))
        def _():
            self.to_down(k).wait_recv()
            self.add(mine, self.line_in.at[k])

        @pl.when(k > z)
        def _():
            self.to_up(k).start()

        @pl.when(k < z)
        def _():
            self.to_down(k).start()

    def last(self, out):
        z, mine = self.z, index_of(self.z, self.x, self.c)
        self.to_side(z).wait_recv()
        self.add(mine, self.side_in.at[z])

        @pl.when(z > 0)
        def _():
            self.to_up(z).wait_recv()
            self.add(mine, self.line_in.at[z + 1])

        @pl.when(z < self.levels - 1)
        def _():
            self.to_down(z).wait_recv()
            self.add(mine, self.line_in.at[z])

        out[...] = self.p[mine]

    def finish(self):
        z = self.z

        @pl.loop(0, self.levels)
        def _(k):
            self.to_twin(k, 0).wait_send()
            self.to_twin(k, 1).wait_send()
            self.to_side(k).wait_send()

            @pl.when(k > z)
            def _():
                self.to_up(k).wait_send()

            @pl.when(k < z)
            def _():
                self.to_down(k).wait_send()

    @staticmethod
    def scratch(members, r, c, kind):
        levels = members // (SIDE * CORES)
        sem = pltpu.SemaphoreType.DMA
        return [
            pltpu.VMEM((members // CORES, r, c), kind),
            pltpu.VMEM((levels, r, c), kind),
            pltpu.VMEM((levels + 1, r, c), kind),
        ] + [sem((n,)) for n in (members // CORES,) * 2 + (levels,) * 2 + (levels + 1,) * 4]


def gather(v):
    return lax.all_gather(v, "grp", axis=0, tiled=True)


def scatter_sum(v):
    return lax.psum_scatter(v, "grp", scatter_dimension=0, tiled=True)


def after(v, *others):
    return lax.optimization_barrier((v, *others))[0]


def tie(v, other):
    first = other[(0,) * other.ndim]
    return v + jnp.minimum(jnp.abs(first), 0).astype(v.dtype)


def open_kernel(
    kva_src, q_src, o_src, router_src, kvb_src, chosen_src, shared_src,
    normed_ref, down_ref, up_ref, cos_ref, sin_ref, kvg_ref,
    all_kva, all_q, all_o, all_router, all_lat, q_out, kvb_out, chosen_out, shared_out, latent_ref, small_ref,
    *bufs, members, split
):
    stage = bufs[:7]
    kva, wq, lat_st, qm = bufs[7:11]
    sems = bufs[11:]
    local, load = sems[26:]
    pairs = [sems[2 * n : 2 * n + 2] for n in range(13)]
    me = lax.axis_index("grp")
    levels = members // (SIDE * CORES)
    z = me // (SIDE * CORES)
    order = near_first(levels)
    tokens, width = normed_ref.shape
    g_kva = Gather(kva_src, all_kva, *pairs[0], members, split)
    g_q = Gather(q_src, all_q, *pairs[1], members, split)
    g_o = Gather(o_src, all_o, *pairs[2], members, split)
    g_router = Gather(router_src, all_router, *pairs[3], members)
    g_lat = Gather(lat_st, all_lat, *pairs[4], members)
    e_kvb = Exchange(kvb_src, kvb_out, *pairs[5], members)
    e_chosen = Exchange(chosen_src, chosen_out, *pairs[6], members)
    e_shared = Exchange(shared_src, shared_out, *pairs[7], members)
    q_sent, q_got = pairs[8]
    sources = [kva_src, q_src, o_src, router_src, kvb_src.at[me], chosen_src.at[me], shared_src.at[me]]
    places = [all_kva, all_q, all_o, all_router, kvb_out, chosen_out, shared_out]
    into = [pltpu.make_async_copy(a, stage[n], local.at[n]) for n, a in enumerate(sources)]
    out_of = [pltpu.make_async_copy(stage[n], b.at[me], local.at[n]) for n, b in enumerate(places)]
    own_lat = pltpu.make_async_copy(lat_st, all_lat.at[me], local.at[7])
    own_q = pltpu.make_async_copy(qm.at[me], q_out.at[me], local.at[8])
    loads = [pltpu.make_async_copy(all_kva, kva, load.at[0]), pltpu.make_async_copy(all_q, wq, load.at[1])]

    def query_to(n):
        return send(qm.at[n], q_out.at[me], q_sent.at[n], q_got.at[me], n)

    def query_from(n):
        return send(qm.at[n], q_out.at[n], q_sent.at[n], q_got.at[n], n)

    def lacked(g, s):
        if g.split:
            k = pick_from(order, z, s)
            g.take_lacked(k, g.x)
            g.take_lacked(k, 1 - g.x)

    def events(gathers, s, before):
        for g in gathers:
            g.relay(s + 1)
        for g in gathers:
            g.pass_on(pick_from(order, z, s))

        @pl.when(before)
        def _():
            for g in gathers:
                lacked(g, s - 1)

    for copy in into:
        copy.start()
    meet(members, g_kva.partner if split else None)
    for g in (g_kva, g_q, g_router):
        g.first()
    e_kvb.start()
    e_chosen.start()
    for a, b in zip(into, out_of):
        a.wait()
        b.start()

    @pl.loop(0, levels)
    def _(s):
        events((g_kva, g_q, g_router), s, s >= 1)

    lacked(g_kva, levels - 1)
    lacked(g_q, levels - 1)
    g_o.first()
    e_shared.start()
    for g in (g_kva, g_q):

        @pl.loop(0, levels)
        def _(k):
            g.take_twin(k)

        if split:
            g.take_twin_lacked()
    for copy in out_of:
        copy.wait()
    for copy in loads:
        copy.start()
    loads[0].wait()
    latent = dot(normed_ref[...], kva[...].reshape(width, -1))
    latent_ref[...] = latent
    half = ROPE // 2

    def turn(v):
        turned = jnp.concatenate([v[:, half:], v[:, :half]], axis=1)
        return (v * cos_ref[...] - turned * sin_ref[...]).astype(BF16)

    lat_st[:, :KVR] = root_norm(latent[:, :KVR], kvg_ref[...]).astype(BF16)
    lat_st[:, KVR:] = turn(latent[:, KVR:])
    g_lat.first()
    own_lat.start()
    small_ref[...] = dot(normed_ref[...], down_ref[...]).astype(BF16)
    loads[1].wait()
    turns = members // 2

    @pl.loop(0, turns)
    def _(n):
        pair = lax.rem(me // 2 + n, turns)
        at = pl.ds(pl.multiple_of(pair * 2 * QK, 128), 2 * QK)
        both = dot(normed_ref[...], wq[:, :, at].reshape(width, 2 * QK)) + dot(small_ref[...], up_ref[:, at])
        for t in range(2):
            to = 2 * pair + t
            r = t * QK
            qm[to, :tokens, :] = both[:, r : r + NOPE].astype(BF16)
            rope = turn(both[:, r + NOPE : r + QK])
            qm[to, tokens:, :ROPE] = rope[: tokens // 2]
            qm[to, tokens:, ROPE:] = rope[tokens // 2 :]

            @pl.when(to == me)
            def _():
                own_q.start()

            @pl.when(to != me)
            def _():
                query_to(to).start()

        @pl.when(n == turns // 2)
        def _():
            events((g_lat, g_o), 0, False)

    @pl.loop(1, levels)
    def _(s):
        events((g_lat, g_o), s, s >= 1)

    lacked(g_o, levels - 1)
    for g in (g_lat, g_router, g_o):

        @pl.loop(0, levels)
        def _(k):
            g.take_twin(k)

        if g.split:
            g.take_twin_lacked()
    for g in (g_kva, g_q, g_router, g_lat, g_o):
        g.finish()

    @pl.loop(1, members)
    def _(d):
        n = lax.rem(me + d, members)
        query_from(n).wait_recv()
        query_to(n).wait_send()

    for e in (e_kvb, e_chosen, e_shared):
        e.wait()
    own_lat.wait()
    own_q.wait()


def opening(kva, q, o, router, kvb, chosen, shared, normed, down, up, cosine, sine, kvg, members, split, collective_id):
    tokens, width = normed.shape
    vmem = pl.BlockSpec(memory_space=pltpu.VMEM)
    anywhere = pl.BlockSpec(memory_space=pl.ANY)
    sem = pltpu.SemaphoreType.DMA
    packed = tokens + tokens // 2
    grown = lambda a: jax.ShapeDtypeStruct((members, *a.shape), a.dtype)
    same = lambda a: jax.ShapeDtypeStruct(a.shape, a.dtype)
    g_sems = [sem((6, members)), sem((2, members))]
    e_sems = [sem((members,)), sem((members,))]
    return pl.pallas_call(
        functools.partial(open_kernel, members=members, split=split),
        in_specs=[anywhere] * 7 + [vmem] * 6,
        out_specs=[anywhere] * 9 + [vmem] * 2,
        out_shape=[
            grown(kva), grown(q), grown(o), grown(router),
            jax.ShapeDtypeStruct((members, tokens, kva.shape[1]), BF16),
            jax.ShapeDtypeStruct((members, packed, NOPE), BF16),
            same(kvb), same(chosen), same(shared),
            jax.ShapeDtypeStruct((tokens, kva.shape[1]), F32),
            jax.ShapeDtypeStruct((tokens, down.shape[1]), BF16),
        ],
        scratch_shapes=[pltpu.VMEM(a.shape, a.dtype) for a in (kva, q, o, router)]
        + [pltpu.VMEM(a.shape[1:], a.dtype) for a in (kvb, chosen, shared)]
        + [
            pltpu.VMEM((members, *kva.shape), BF16),
            pltpu.VMEM((members, *q.shape), BF16),
            pltpu.VMEM((tokens, kva.shape[1]), BF16),
            pltpu.VMEM((members, packed, NOPE), BF16),
        ]
        + g_sems * 5
        + e_sems * 8
        + [sem((9,)), sem((2,))],
        compiler_params=pltpu.CompilerParams(
            collective_id=collective_id, has_side_effects=True, vmem_limit_bytes=48 * 1024 * 1024
        ),
        cost_estimate=pl.CostEstimate(flops=2 * tokens * width * q.shape[1], bytes_accessed=200_000_000, transcendentals=0),
        name="opening",
    )(kva, q, o, router, kvb, chosen, shared, normed, down, up, cosine, sine, kvg)


def key_blocks(start, rows, keys, length):
    end = start + rows
    end = jnp.where(start < length // 2, jnp.maximum(end, length // 2), end)
    return (start + 1) // keys, (end + keys - 1) // keys


def attend_kernel(prefix_ref, q_ref, k_ref, v_ref, o_ref, lse_ref, mixed, blocks, sent, got, local, *, members, unit):
    me = lax.axis_index("grp")
    tokens = blocks.shape[1]
    block, keys = 2 * tokens, 4 * tokens
    turns = members // 2
    prefix = prefix_ref[0]

    def block_to(n):
        return send(blocks.at[n], mixed.at[me], sent.at[n], got.at[me], n)

    def from_device(n):
        return send(blocks.at[n], mixed.at[n], sent.at[n], got.at[n], n)

    own = pltpu.make_async_copy(blocks.at[me], mixed.at[me], local)
    meet(members)

    @pl.loop(0, turns)
    def _(n):
        i = lax.rem(me // 2 + n, turns)
        start = pl.multiple_of(i * block, block)
        here = pl.ds(start, block)
        q = q_ref[here, :]
        rows = start + lax.broadcasted_iota(jnp.int32, (block, 1), 0)
        limit = jnp.where(rows < prefix, prefix - 1, rows)
        limit = jnp.maximum(limit, rows)

        def step(j, carry, masked):
            top, total, acc = carry
            at = pl.multiple_of(j * keys, keys)
            k = k_ref[pl.ds(at, keys), :]
            v = v_ref[pl.ds(at, keys), :]
            s = dot_t(q, k)
            if masked:
                cols = at + lax.broadcasted_iota(jnp.int32, (1, keys), 1)
                s = jnp.where(cols <= limit, s, -1e30)
            fresh = jnp.maximum(top, jnp.max(s, axis=1, keepdims=True))
            p = jnp.exp2((s - fresh) * unit)
            scale = jnp.exp2((top - fresh) * unit)
            total = total * scale + jnp.sum(p, axis=1, keepdims=True)
            acc = acc * scale + dot(p.astype(BF16), v)
            return fresh, total, acc

        carry = (
            jnp.full((block, 1), -1e30, F32),
            jnp.zeros((block, 1), F32),
            jnp.zeros((block, VD), F32),
        )
        full, stop = key_blocks(start, block, keys, q_ref.shape[0])
        carry = lax.fori_loop(0, full, functools.partial(step, masked=False), carry)
        top, total, acc = lax.fori_loop(full, stop, functools.partial(step, masked=True), carry)
        o = acc / total
        o_ref[here, :] = o
        lse_ref[here, :] = top * unit + jnp.log2(total)
        blocks[pl.ds(2 * i, 2)] = o.astype(BF16).reshape(2, tokens, VD)
        for t in range(2):
            to = 2 * i + t

            @pl.when(to == me)
            def _():
                own.start()

            @pl.when(to != me)
            def _():
                block_to(to).start()

    own.wait()

    @pl.loop(1, members)
    def _(d):
        n = lax.rem(me + d, members)
        from_device(n).wait_recv()
        block_to(n).wait_send()


def attend(prefix, q, k, v, members, collective_id):
    length = q.shape[0]
    tokens = length // members
    vmem = pl.BlockSpec(memory_space=pltpu.VMEM)
    sem = pltpu.SemaphoreType.DMA
    return pl.pallas_call(
        functools.partial(attend_kernel, members=members, unit=QK**-0.5 * math.log2(math.e)),
        in_specs=[pl.BlockSpec(memory_space=pltpu.SMEM), vmem, vmem, vmem],
        out_specs=[vmem, vmem, pl.BlockSpec(memory_space=pl.ANY)],
        out_shape=[
            jax.ShapeDtypeStruct((length, VD), F32),
            jax.ShapeDtypeStruct((length, 1), F32),
            jax.ShapeDtypeStruct((members, tokens, VD), BF16),
        ],
        scratch_shapes=[pltpu.VMEM((members, tokens, VD), BF16), sem((members,)), sem((members,)), sem],
        compiler_params=pltpu.CompilerParams(
            collective_id=collective_id, has_side_effects=True, vmem_limit_bytes=40 * 1024 * 1024
        ),
        cost_estimate=pl.CostEstimate(
            flops=length * length * (QK + VD), bytes_accessed=length * 1000, transcendentals=length * length // 2
        ),
        name="attend",
    )(prefix, q, k, v)


def attend_back_kernel(
    prefix_ref, q_ref, k_ref, v_ref, o_ref, lse_ref, d_hbm, kvb_ref, part_ref, dq_out,
    ds_in, blocks, dk, dv, sent, got, q_sent, q_got, local, local2,
    *, members, factor, unit
):
    me = lax.axis_index("grp")
    tokens = blocks.shape[1] * 2 // 3
    block, keys = 2 * tokens, 4 * tokens
    turns = members // 2
    prefix = prefix_ref[0]
    exchange = Exchange(d_hbm, ds_in, sent, got, members)
    into = pltpu.make_async_copy(d_hbm.at[me], ds_in.at[me], local)
    own = pltpu.make_async_copy(blocks.at[me], dq_out.at[me], local2)

    def block_to(n):
        return send(blocks.at[n], dq_out.at[me], q_sent.at[n], q_got.at[me], n)

    def from_device(n):
        return send(blocks.at[n], dq_out.at[n], q_sent.at[n], q_got.at[n], n)

    into.start()
    meet(members)
    exchange.start()
    dk[...] = jnp.zeros_like(dk)
    dv[...] = jnp.zeros_like(dv)
    into.wait()

    @pl.loop(0, turns)
    def _(n):
        i = lax.rem(me // 2 + n, turns)
        start = pl.multiple_of(i * block, block)
        here = pl.ds(start, block)
        for t in range(2):
            source = 2 * i + t

            @pl.when(source != me)
            def _():
                send(ds_in.at[source], ds_in.at[source], sent.at[0], got.at[lax.rem(me - source + members, members)], source).wait_recv()

        d = ds_in[pl.ds(2 * i, 2)].reshape(block, VD)
        q = q_ref[here, :]
        lse = lse_ref[pl.ds(i, 1), 0, :]
        along = d.astype(F32) * o_ref[here, :]
        high = along.astype(BF16)
        low = (along - high.astype(F32)).astype(BF16)
        ones = jnp.ones((8, VD), BF16)
        delta = (dot_t(ones, high) + dot_t(ones, low))[0:1, :]
        rows = start + lax.broadcasted_iota(jnp.int32, (1, block), 1)
        limit = jnp.maximum(jnp.where(rows < prefix, prefix - 1, rows), rows)

        def step(j, dq, masked):
            at = pl.multiple_of(j * keys, keys)
            k = k_ref[pl.ds(at, keys), :]
            v = v_ref[pl.ds(at, keys), :]
            p = jnp.exp2(dot_t(k, q) * unit - lse)
            if masked:
                cols = at + lax.broadcasted_iota(jnp.int32, (keys, 1), 0)
                p = jnp.where(cols <= limit, p, 0.0)
            dp = dot_t(v, d)
            ds = (p * (dp - delta)).astype(BF16)
            dv[pl.ds(at, keys), :] += dot(p.astype(BF16), d)
            dk[pl.ds(at, keys), :] += dot(ds, q)
            return dq + t_dot(ds, k)

        full, stop = key_blocks(start, block, keys, q_ref.shape[0])
        dq = lax.fori_loop(0, full, functools.partial(step, masked=False), jnp.zeros((block, QK), F32))
        dq = lax.fori_loop(full, stop, functools.partial(step, masked=True), dq)
        dq = (dq * factor).astype(BF16)
        half = tokens // 2
        for t in range(2):
            to = 2 * i + t
            r = t * tokens
            blocks[to, :tokens, :] = dq[r : r + tokens, :NOPE]
            blocks[to, tokens:, :ROPE] = dq[r : r + half, NOPE:]
            blocks[to, tokens:, ROPE:] = dq[r + half : r + tokens, NOPE:]

            @pl.when(to == me)
            def _():
                own.start()

            @pl.when(to != me)
            def _():
                block_to(to).start()

    @pl.loop(0, members)
    def _(b):
        at = pl.ds(pl.multiple_of(b * tokens, tokens), tokens)
        d = jnp.concatenate([dk[at, :NOPE] * factor, dv[at, :]], axis=1).astype(BF16)
        part_ref[b, :, :KVR] = dot_t(d, kvb_ref[...]).astype(BF16)
        part_ref[b, :, KVR:] = (dk[at, NOPE:] * factor).astype(BF16)

    own.wait()

    @pl.loop(1, members)
    def _(d):
        n = lax.rem(me + d, members)
        from_device(n).wait_recv()
        block_to(n).wait_send()
        exchange.copy(d).wait_send()


def attend_back(prefix, q, k, v, o, lse, d, kvb, members, collective_id):
    length = q.shape[0]
    tokens = length // members
    vmem = pl.BlockSpec(memory_space=pltpu.VMEM)
    anywhere = pl.BlockSpec(memory_space=pl.ANY)
    sem = pltpu.SemaphoreType.DMA
    factor = QK**-0.5
    packed = tokens + tokens // 2
    return pl.pallas_call(
        functools.partial(attend_back_kernel, members=members, factor=factor, unit=factor * math.log2(math.e)),
        in_specs=[pl.BlockSpec(memory_space=pltpu.SMEM)] + [vmem] * 5 + [anywhere, vmem],
        out_specs=[vmem, anywhere],
        out_shape=[
            jax.ShapeDtypeStruct((members, tokens, KVR + ROPE), BF16),
            jax.ShapeDtypeStruct((members, packed, NOPE), BF16),
        ],
        scratch_shapes=[
            pltpu.VMEM((members, tokens, VD), BF16),
            pltpu.VMEM((members, packed, NOPE), BF16),
            pltpu.VMEM((length, QK), F32),
            pltpu.VMEM((length, VD), F32),
            sem((members,)), sem((members,)), sem((members,)), sem((members,)), sem, sem,
        ],
        compiler_params=pltpu.CompilerParams(
            collective_id=collective_id, has_side_effects=True, vmem_limit_bytes=50 * 1024 * 1024
        ),
        cost_estimate=pl.CostEstimate(
            flops=length * length * (3 * QK + 2 * VD), bytes_accessed=length * 2000, transcendentals=length * length // 2
        ),
        name="attend_back",
    )(prefix, q, k, v, o, lse, d, kvb)


def silu_parts(v):
    logistic = 0.5 * jnp.tanh(0.5 * v) + 0.5
    return v * logistic, logistic * (1.0 + v * (1.0 - logistic))


def picks(rank, slots):
    at = lax.broadcasted_iota(jnp.int32, (slots, rank.shape[1]), 0).astype(F32)
    return at == rank


def picks_back(rank, slots):
    at = lax.broadcasted_iota(jnp.int32, (rank.shape[0], slots), 1).astype(F32)
    return at == rank


def tiles(width, size):
    return pl.ds(pl.multiple_of(width * size, size), size)


def experts_kernel(
    x_hbm, prob_hbm, c_hbm, rank_ref, back_ref, gate_hbm, up_hbm, down_hbm, own_hbm, sdown_hbm,
    part_hbm, eg_hbm, eu_hbm, eo_hbm, sh_hbm, c_out, prob_out,
    xs, probs, gate, up, down, own, sdown, tail, rows, acts, sacts, part_st, eg_st, eu_st, eo_st, sh_st,
    c_st, sent, got, e_sent, e_got, c_sent, c_got, load, store,
    *, members, slots, tile, wide
):
    me = lax.axis_index("grp")
    levels = members // (SIDE * CORES)
    group = SIDE * CORES
    width, hidden = gate.shape
    half, whole = hidden % tile, hidden // tile
    units = own.shape[1] // 2
    z = me // group
    order = near_first(levels)
    loads = [
        pltpu.make_async_copy(a, b, load.at[n])
        for n, (a, b) in enumerate(
            [
                (x_hbm, xs.at[me]),
                (prob_hbm.at[me], probs.at[me]),
                (own_hbm, own),
                (gate_hbm, gate),
                (up_hbm, up),
                (down_hbm, down),
                (sdown_hbm, sdown),
                (c_hbm, c_st),
            ]
        )
    ]
    gather = Gather(x_hbm, xs, sent, got, members)
    behind = Gather(c_hbm, c_out, c_sent, c_got, members)
    own_c = pltpu.make_async_copy(c_st, c_out.at[me], load.at[7])
    exchange = Exchange(prob_hbm, probs, e_sent, e_got, members)
    for copy in loads:
        copy.start()
    meet(members)
    gather.first()
    exchange.start()
    for copy in loads:
        copy.wait()
    own_c.start()
    tail[:, :half] = gate[:, hidden - half :]
    tail[:, half:] = up[:, hidden - half :]
    gather.pass_on(z)
    gather.relay(1)
    exchange.wait()
    prob_out[...] = probs[...]

    def stores(s, k):
        n = s % 2
        return [
            pltpu.make_async_copy(a, b.at[k], store.at[n, m])
            for m, (a, b) in enumerate(
                [
                    (part_st.at[n], part_hbm),
                    (eg_st.at[n], eg_hbm),
                    (eu_st.at[n], eu_hbm),
                    (eo_st.at[n], eo_hbm),
                    (sh_st.at[n], sh_hbm),
                ]
            )
        ]

    @pl.loop(0, levels)
    def _(s):
        k = pick_from(order, z, s)
        n = s % 2
        gather.take_twin(k)

        @pl.when(s >= 2)
        def _():
            for copy in stores(s, pick_from(order, z, s - 2)):
                copy.wait()

        @pl.loop(0, group)
        def _(b):
            pick = picks(rank_ref[k * group + b, 0:1, :], slots).astype(BF16)
            rows[tiles(b, slots), :] = dot(pick, xs[k * group + b]).astype(BF16)

        def keep(at, g, u):
            eg_st[n, :, at] = g.astype(BF16)
            eu_st[n, :, at] = u.astype(BF16)
            acts[:, at] = (silu_parts(g)[0] * u).astype(BF16)

        @pl.loop(0, whole)
        def _(j):
            at = tiles(j, tile)
            x = rows[...]
            keep(at, dot(x, gate[:, at]), dot(x, up[:, at]))

        last = dot(rows[...], tail[...])
        keep(pl.ds(whole * tile, half), last[:, :half], last[:, half:])

        gather.relay(s + 2)

        @pl.when(s + 1 < levels)
        def _():
            gather.pass_on(pick_from(order, z, s + 1))

        @pl.when(s == levels - 3)
        def _():
            behind.first()

        @pl.when(s >= levels - 2)
        def _():
            behind.relay(s - levels + 3)
            behind.pass_on(pick_from(order, z, s - levels + 2))

        @pl.loop(0, width // wide)
        def _(j):
            at = tiles(j, wide)
            eo_st[n, :, at] = dot(acts[...], down[:, at]).astype(BF16)

        @pl.loop(0, group // 2)
        def _(h):
            x = xs[pl.ds(k * group + 2 * h, 2)].reshape(-1, width)
            pre = dot(x, own[...])
            sh_st[n, pl.ds(2 * h, 2)] = pre.astype(BF16).reshape(2, -1, 2 * units)
            act = (silu_parts(pre[:, :units])[0] * pre[:, units:]).astype(BF16)
            sacts[pl.ds(2 * h, 2)] = act.reshape(2, -1, units)

        @pl.loop(0, group)
        def _(b):
            i = k * group + b
            pick = picks(rank_ref[i, 0:1, :], slots)
            back = picks_back(back_ref[i], slots).astype(BF16)
            g = jnp.sum(jnp.where(pick, probs[i, 0:1, :], 0.0), axis=1, keepdims=True)
            act = sacts[b]
            for j in range(width // wide):
                at = slice(j * wide, (j + 1) * wide)
                weighted = (g * eo_st[n, tiles(b, slots), at].astype(F32)).astype(BF16)
                part_st[n, b, :, at] = (dot(back, weighted) + dot(act, sdown[:, at])).astype(BF16)

        for copy in stores(s, k):
            copy.start()

    @pl.loop(2, levels)
    def _(s):
        behind.relay(s + 1)
        behind.pass_on(pick_from(order, z, s))

    @pl.loop(levels - 2, levels)
    def _(s):
        for copy in stores(s, pick_from(order, z, s)):
            copy.wait()

    @pl.loop(0, levels)
    def _(k):
        behind.take_twin(k)

    own_c.wait()
    gather.finish()
    behind.finish()


def experts_forward(x, prob, c, rank, back, gate, up, down, own, sdown, slots, members, collective_id):
    tokens, width = x.shape
    hidden = gate.shape[1]
    group = SIDE * CORES
    levels = members // group
    packed = group * slots
    anywhere = pl.BlockSpec(memory_space=pl.ANY)
    vmem = pl.BlockSpec(memory_space=pltpu.VMEM)
    sem = pltpu.SemaphoreType.DMA
    tile = 256
    shapes = [
        (levels, group, tokens, width),
        (levels, packed, hidden),
        (levels, packed, hidden),
        (levels, packed, width),
        (levels, group, tokens, own.shape[1]),
    ]
    return pl.pallas_call(
        functools.partial(experts_kernel, members=members, slots=slots, tile=tile, wide=512),
        in_specs=[anywhere, anywhere, anywhere, vmem, vmem] + [anywhere] * 5,
        out_specs=[anywhere] * 6 + [vmem],
        out_shape=[jax.ShapeDtypeStruct(s, BF16) for s in shapes]
        + [jax.ShapeDtypeStruct((members, *c.shape), BF16)]
        + [jax.ShapeDtypeStruct(prob.shape, F32)],
        scratch_shapes=[
            pltpu.VMEM((members, tokens, width), BF16),
            pltpu.VMEM(prob.shape, F32),
            pltpu.VMEM(gate.shape, BF16),
            pltpu.VMEM(up.shape, BF16),
            pltpu.VMEM(down.shape, BF16),
            pltpu.VMEM(own.shape, BF16),
            pltpu.VMEM(sdown.shape, BF16),
            pltpu.VMEM((width, tile), BF16),
            pltpu.VMEM((packed, width), BF16),
            pltpu.VMEM((packed, hidden), BF16),
            pltpu.VMEM((group, tokens, own.shape[1] // 2), BF16),
        ]
        + [pltpu.VMEM((2, *s[1:]), BF16) for s in shapes]
        + [pltpu.VMEM(c.shape, BF16)]
        + [sem((6, members)), sem((2, members)), sem((members,)), sem((members,))]
        + [sem((6, members)), sem((2, members)), sem((8,)), sem((2, 5))],
        compiler_params=pltpu.CompilerParams(
            collective_id=collective_id, has_side_effects=True, vmem_limit_bytes=63 * 1024 * 1024
        ),
        cost_estimate=pl.CostEstimate(
            flops=12 * members * slots * width * hidden, bytes_accessed=60_000_000, transcendentals=0
        ),
        name="experts_forward",
    )(x, prob, c, rank, back, gate, up, down, own, sdown)


def experts_back_kernel(
    c_hbm, c2_hbm, rank_ref, back_ref, prob_ref, eg_hbm, eu_hbm, eo_hbm, sh_hbm, gate_hbm, up_hbm, down_hbm, own_hbm, sdown_hbm,
    out, dg_out,
    part, cs, eg, eu, eo, sh, gate, up, down, own, sdown, rows, d_gate, d_up, dg_st, dg_in,
    *sems, members, slots, tile, wide
):
    twin_in, side_in, line_in = sems[:3]
    e_sent, e_got, load, fetch = sems[11:15]
    me = lax.axis_index("grp")
    levels = members // (SIDE * CORES)
    group = SIDE * CORES
    width, hidden = gate.shape
    half, whole = hidden % tile, hidden // tile
    units = own.shape[1] // 2
    z = me // group
    order = far_first(levels)
    reduce = Reduce(part, twin_in, side_in, line_in, sems[3:11], members)
    exchange = Exchange(dg_st, dg_in, e_sent, e_got, members)

    def cotangents(s):
        k = pick_from(order, z, s)
        return [
            pltpu.make_async_copy(
                a.at[k], cs.at[s % 2, :, :, pl.ds(h * (width // 2), width // 2)], fetch.at[4 + s % 2 * 2 + h]
            )
            for h, a in enumerate([c_hbm, c2_hbm])
        ]

    def kept(s):
        k = pick_from(order, z, s)
        return [
            pltpu.make_async_copy(a.at[k], b, fetch.at[m])
            for m, (a, b) in enumerate([(eo_hbm, eo), (eg_hbm, eg), (eu_hbm, eu), (sh_hbm, sh)])
        ]

    loads = [
        pltpu.make_async_copy(a, b, load.at[n])
        for n, (a, b) in enumerate(
            [(down_hbm, down), (gate_hbm, gate), (up_hbm, up), (own_hbm, own), (sdown_hbm, sdown)]
        )
    ]
    for copy in cotangents(0) + kept(0):
        copy.start()
    for copy in loads:
        copy.start()
    meet(members)

    def early(s):
        return (z == 0) | (z == levels - 1)

    @pl.loop(0, levels)
    def _(s):
        k = pick_from(order, z, s)
        n = s % 2
        for copy in cotangents(s):
            copy.wait()
        load_eo, load_eg, load_eu, load_sh = kept(s)

        @pl.when(s + 1 < levels)
        def _():
            for copy in cotangents(s + 1):
                copy.start()

        load_eo.wait()
        @pl.loop(0, group)
        def _(b):
            i = k * group + b
            at = tiles(b, slots)
            pick = picks(rank_ref[i, 0:1, :], slots)
            c = dot(pick.astype(BF16), cs[n, b])
            g = jnp.sum(jnp.where(pick, prob_ref[i, 0:1, :], 0.0), axis=1, keepdims=True)
            along = jnp.sum(c * eo[at, :].astype(F32), axis=1, keepdims=True)
            dg_st[i] = jnp.broadcast_to(
                jnp.sum(jnp.where(pick, along, 0.0), axis=0, keepdims=True), dg_st.shape[1:]
            )
            rows[at, :] = (g * c).astype(BF16)

        @pl.when(s == 0)
        def _():
            for copy in loads:
                copy.wait()

        load_eg.wait()
        load_eu.wait()

        def slopes(at):
            d = dot_t(rows[...], down[at, :])
            act, slope = silu_parts(eg[:, at].astype(F32))
            d_gate[:, at] = (d * eu[:, at].astype(F32) * slope).astype(BF16)
            d_up[:, at] = (d * act).astype(BF16)

        @pl.loop(0, whole)
        def _(j):
            slopes(tiles(j, tile))

        slopes(pl.ds(whole * tile, half))

        @pl.when(s >= 1)
        def _():
            reduce.chip(pick_from(order, z, s - 1))

        @pl.when((s >= 2) & ~early(s))
        def _():
            reduce.line(pick_from(order, z, s - 2))

        @pl.loop(0, width // tile)
        def _(j):
            at = tiles(j, tile)
            eo[:, at] = (dot_t(d_gate[...], gate[at, :]) + dot_t(d_up[...], up[at, :])).astype(BF16)

        load_sh.wait()
        @pl.loop(0, group)
        def _(b):
            i = k * group + b
            back = picks_back(back_ref[i], slots).astype(BF16)
            d = dot_t(cs[n, b], sdown[...])
            pre = sh[b].astype(F32)
            act, slope = silu_parts(pre[:, :units])
            both = jnp.concatenate([d * pre[:, units:] * slope, d * act], axis=1).astype(BF16)
            for j in range(width // wide):
                at = slice(j * wide, (j + 1) * wide)
                part[i, :, at] = (
                    dot(back, eo[tiles(b, slots), at]) + dot_t(both, own[at, :])
                ).astype(BF16)

        reduce.start(k)

        @pl.when(s + 1 < levels)
        def _():
            for copy in kept(s + 1):
                copy.start()

        @pl.when((s >= 1) & early(s))
        def _():
            reduce.line(pick_from(order, z, s - 1))

    exchange.start()
    dg_in[me] = dg_st[me]
    reduce.chip(z)

    @pl.when(~early(0))
    def _():
        reduce.line(pick_from(order, z, levels - 2))

    reduce.last(out)
    reduce.finish()
    exchange.wait()
    dg_out[...] = dg_in[...]


def experts_backward(cs, rank, back, prob, kept, gate, up, down, own, sdown, slots, members, collective_id):
    tokens, width = cs[0].shape[1], cs[0].shape[2] * 2
    hidden = gate.shape[1]
    group = SIDE * CORES
    levels = members // group
    packed = group * slots
    anywhere = pl.BlockSpec(memory_space=pl.ANY)
    vmem = pl.BlockSpec(memory_space=pltpu.VMEM)
    sem = pltpu.SemaphoreType.DMA
    eg, eu, eo, sh = kept
    return pl.pallas_call(
        functools.partial(experts_back_kernel, members=members, slots=slots, tile=256, wide=512),
        in_specs=[anywhere, anywhere, vmem, vmem, vmem] + [anywhere] * 9,
        out_specs=[vmem, vmem],
        out_shape=[
            jax.ShapeDtypeStruct((tokens, width), BF16),
            jax.ShapeDtypeStruct((members, 8, tokens), F32),
        ],
        scratch_shapes=[
            pltpu.VMEM((members, tokens, width), BF16),
            pltpu.VMEM((2, group, tokens, width), BF16),
            pltpu.VMEM(eg.shape[1:], BF16),
            pltpu.VMEM(eu.shape[1:], BF16),
            pltpu.VMEM(eo.shape[1:], BF16),
            pltpu.VMEM(sh.shape[1:], BF16),
            pltpu.VMEM(gate.shape, BF16),
            pltpu.VMEM(up.shape, BF16),
            pltpu.VMEM(down.shape, BF16),
            pltpu.VMEM(own.shape, BF16),
            pltpu.VMEM(sdown.shape, BF16),
            pltpu.VMEM((packed, width), BF16),
            pltpu.VMEM((packed, hidden), BF16),
            pltpu.VMEM((packed, hidden), BF16),
            pltpu.VMEM((members, 8, tokens), F32),
            pltpu.VMEM((members, 8, tokens), F32),
        ]
        + Reduce.scratch(members, tokens, width, BF16)
        + [sem((members,)), sem((members,)), sem((5,)), sem((8,))],
        compiler_params=pltpu.CompilerParams(
            collective_id=collective_id, has_side_effects=True, vmem_limit_bytes=67_043_328
        ),
        cost_estimate=pl.CostEstimate(
            flops=12 * members * slots * width * hidden, bytes_accessed=60_000_000, transcendentals=0
        ),
        name="experts_backward",
    )(*(c.reshape(levels, group, tokens, -1) for c in cs), rank, back, prob, *kept, gate, up, down, own, sdown)


class Spread:
    def __init__(self, src, out, common, commons, sems, members, sequences):
        self.src, self.out, self.common, self.commons = src, out, common, commons
        self.sent, self.got, self.sent2, self.got2 = sems
        self.members, self.sequences = members, sequences
        self.me, self.mine = lax.axis_index("grp"), lax.axis_index("rep")

    def other(self, n):
        r = lax.rem(self.mine + n // self.members, self.sequences)
        return {"rep": r, "grp": lax.rem(self.me + n % self.members, self.members)}

    def meet(self):
        barrier = pltpu.get_barrier_semaphore()
        count = self.members * self.sequences

        @pl.loop(1, count)
        def _(n):
            pl.semaphore_signal(barrier, 1, device_id=self.other(n), device_id_type=MESH)

        pl.semaphore_wait(barrier, count - 1)

    def block(self, n):
        to = self.other(n)
        return send(self.src.at[to["grp"]], self.out.at[self.mine, self.me], self.sent.at[n], self.got.at[n], to)

    def whole(self, n):
        return send(self.common, self.commons.at[self.mine], self.sent2.at[n], self.got2.at[n], self.other(n * self.members))

    def start_blocks(self):
        @pl.loop(1, self.members * self.sequences)
        def _(n):
            self.block(n).start()

    def start_common(self):
        @pl.loop(1, self.sequences)
        def _(n):
            self.whole(n).start()

    def wait(self):
        @pl.loop(1, self.members * self.sequences)
        def _(n):
            self.block(n).wait()

        @pl.loop(1, self.sequences)
        def _(n):
            self.whole(n).wait()


def finish_kernel(
    part, o_src, dq_ref, cos_ref, sin_ref, q_hbm, kva_ref, up_ref, down_ref, small_ref, normed_ref, latent_ref, kvg_ref,
    x_ref, xg_ref, dmid_ref, name_ref,
    out, q_out, o_out,
    *bufs, members, sequences
):
    twin_in, side_in, line_in = bufs[:3]
    o_in, o_common, q_parts, d_query, wq, dn, d_lat, d_latent, ds_ref = bufs[11:20]
    o_sent, o_got, b_sent, b_got, w_sent, w_got, local = bufs[20:]
    reduce = Reduce(part, twin_in, side_in, line_in, bufs[3:11], members)
    exchange = Exchange(o_src, o_in, o_sent, o_got, members)
    spread = Spread(q_parts, q_out, o_common, o_out, (b_sent, b_got, w_sent, w_got), members, sequences)
    me, mine = spread.me, spread.mine
    order = far_first(reduce.levels)
    z, levels = reduce.z, reduce.levels
    tokens, width = x_ref.shape
    tile = 256
    load = pltpu.make_async_copy(q_hbm, wq, local.at[0])
    own = [
        pltpu.make_async_copy(q_parts.at[me], q_out.at[mine, me], local.at[1]),
        pltpu.make_async_copy(o_common, o_out.at[mine], local.at[2]),
    ]
    load.start()
    spread.meet()

    @pl.loop(0, levels)
    def _(s):
        reduce.start(pick_from(order, z, s))

    exchange.start()
    o_in[me] = o_src[me]
    cosine, sine = cos_ref[...], sin_ref[...]
    half = ROPE // 2
    for pair in range(dq_ref.shape[0] // 2):
        pieces = []
        for h in (2 * pair, 2 * pair + 1):
            rope = jnp.concatenate([dq_ref[h, tokens:, :ROPE], dq_ref[h, tokens:, ROPE:]], axis=0).astype(F32)
            turned = jnp.concatenate([rope[:, half:], rope[:, :half]], axis=1)
            pieces += [dq_ref[h, :tokens, :], (rope * cosine + turned * sine).astype(BF16)]
        d_query[:, pair * 2 * QK : (pair + 1) * 2 * QK] = jnp.concatenate(pieces, axis=1)

    @pl.loop(0, levels)
    def _(s):
        reduce.chip(pick_from(order, z, s))

    grad_up = t_dot(small_ref[...], d_query[...])
    ds_ref[...] = dot_t(d_query[...], up_ref[...]).astype(BF16)
    grad_down = t_dot(ds_ref[...], normed_ref[...])
    rows = width // members
    for g in range(members):
        first = g // 2 * 2 * QK
        q_parts[g] = jnp.concatenate(
            [grad_down[:, g * rows : (g + 1) * rows], grad_up[:, first : first + 2 * QK]], axis=1
        ).astype(BF16)
    spread.start_blocks()
    own[0].start()
    exchange.wait()
    total = jnp.zeros(o_in.shape[1:], F32)
    for g in range(members):
        total = total + o_in[g].astype(F32)
    o_common[...] = jnp.concatenate([total, name_ref[...]], axis=1)
    spread.start_common()
    own[1].start()
    load.wait()
    every = width // tile // (levels - 1)

    @pl.loop(0, width // tile)
    def _(j):
        dn[:, tiles(j, tile)] = dot_t(d_query[...], wq[pl.ds(j * (tile // rows), tile // rows)].reshape(tile, -1))

        @pl.when((j % every == every - 1) & (j // every < levels - 1))
        def _():
            reduce.line(pick_from(order, z, j // every))

    reduce.last(d_lat)
    gradient = d_lat[...].astype(F32)
    latent = latent_ref[...]
    d_latent[:, :KVR] = norm_back(latent[:, :KVR], kvg_ref[...], gradient[:, :KVR]).astype(BF16)
    rope = gradient[:, KVR:]
    turned = jnp.concatenate([rope[:, half:], rope[:, :half]], axis=1)
    d_latent[:, KVR:] = (rope * cosine + turned * sine).astype(BF16)

    @pl.loop(0, width // tile)
    def _(j):
        at = tiles(j, tile)
        dn[:, at] += dot_t(d_latent[...], kva_ref[at, :]) + dot_t(ds_ref[...], down_ref[at, :])

    out[...] = (dmid_ref[...] + norm_back(x_ref[...].astype(F32), xg_ref[...], dn[...])).astype(BF16)
    reduce.finish()
    spread.wait()
    for copy in own:
        copy.wait()


def finish(part, o_parts, dq, cosine, sine, all_q, kva, up, down, small, normed, latent, kvg, x, xg, dmid, name, sequences, collective_id):
    members, tokens, c = part.shape
    width = x.shape[1]
    rank = o_parts.shape[1]
    vmem = pl.BlockSpec(memory_space=pltpu.VMEM)
    anywhere = pl.BlockSpec(memory_space=pl.ANY)
    sem = pltpu.SemaphoreType.DMA
    share = width // members + 2 * QK
    common = (rank, o_parts.shape[2] + name.shape[1])
    return pl.pallas_call(
        functools.partial(finish_kernel, members=members, sequences=sequences),
        in_specs=[vmem] * 5 + [anywhere] + [vmem] * 11,
        out_specs=[vmem, anywhere, anywhere],
        out_shape=[
            jax.ShapeDtypeStruct((tokens, width), BF16),
            jax.ShapeDtypeStruct((sequences, members, rank, share), BF16),
            jax.ShapeDtypeStruct((sequences, *common), F32),
        ],
        scratch_shapes=Reduce.scratch(members, tokens, c, BF16)
        + [
            pltpu.VMEM(o_parts.shape, BF16),
            pltpu.VMEM(common, F32),
            pltpu.VMEM((members, rank, share), BF16),
            pltpu.VMEM((tokens, H * QK), BF16),
            pltpu.VMEM(all_q.shape, BF16),
            pltpu.VMEM((tokens, width), F32),
            pltpu.VMEM((tokens, c), BF16),
            pltpu.VMEM((tokens, c), BF16),
            pltpu.VMEM((tokens, rank), BF16),
        ]
        + [sem((n,)) for n in (members,) * 2 + (members * sequences,) * 2 + (sequences,) * 2 + (3,)],
        compiler_params=pltpu.CompilerParams(
            collective_id=collective_id, has_side_effects=True, vmem_limit_bytes=56 * 1024 * 1024
        ),
        cost_estimate=pl.CostEstimate(flops=4 * tokens * width * H * QK, bytes_accessed=40_000_000, transcendentals=0),
        name="finish",
    )(part, o_parts, dq, cosine, sine, all_q, kva, up, down, small, normed, latent, kvg, x, xg, dmid, name)


def by_owner(gradient, members):
    return gradient.astype(BF16).reshape(gradient.shape[0], members, -1).transpose(1, 0, 2)


def pack(v):
    half = v.shape[1] // 2
    rope = jnp.concatenate([v[:, :half, NOPE:], v[:, half:, NOPE:]], axis=-1)
    return jnp.concatenate([v[:, :, :NOPE], rope], axis=1)


def unpack(v):
    rows = v.shape[1] * 2 // 3
    rope = jnp.concatenate([v[:, rows:, :ROPE], v[:, rows:, ROPE:]], axis=1)
    return jnp.concatenate([v[:, :rows], rope], axis=-1)


def per_device(
    hidden,
    grad_out,
    expert_ids,
    prefix_len,
    adapter_id,
    attn_gain,
    kv_gain,
    ffn_gain,
    w_q,
    w_kva,
    w_kvb,
    w_o,
    w_router,
    shared_gate,
    shared_up,
    shared_down,
    expert_gate,
    expert_up_weight,
    expert_down,
    q_down,
    q_up,
    o_down,
    o_up,
):
    tokens = hidden.shape[1]
    width = hidden.shape[2]
    members = lax.axis_size("grp")
    length = tokens * members
    experts = expert_gate.shape[0] * members
    capacity = tokens * TOP * 5 // (4 * experts)
    slots = -(-capacity // 16) * 16
    me = lax.axis_index("grp")

    inputs = hidden[0].astype(F32)
    cotangent = grad_out[0]
    c32 = cotangent.astype(F32)
    routes = expert_ids[0]
    adapter = adapter_id[0]
    pick = lambda table: lax.dynamic_index_in_dim(table, adapter, 0, keepdims=False)
    qa_down, qa_up, oa_down, oa_up = pick(q_down), pick(q_up), pick(o_down), pick(o_up)

    chosen_by = jnp.sum(
        (routes[:, :, None] == jnp.arange(experts, dtype=jnp.int32)[None, None, :]).astype(F32), axis=1
    )
    sequences = lax.axis_size("rep")
    split = w_q.shape[0] * 3 // 128 * 16 if sequences % 2 == 0 else 0
    hidden_slice = shared_down.shape[0]
    shared = jnp.stack([shared_gate, shared_up], axis=1)
    shared = shared.reshape(shared.shape[0], 2, members, hidden_slice).transpose(2, 0, 1, 3)
    positions = me * tokens + jnp.arange(tokens, dtype=jnp.int32)
    cosine, sine = angles(positions, ROPE)
    normed = root_norm(inputs, attn_gain).astype(BF16)
    cosine2 = jnp.concatenate([cosine, cosine], axis=1)
    sine2 = jnp.concatenate([sine, -sine], axis=1)
    (
        all_kva, all_q, all_o, all_router, all_latent, q_packed, kvb_parts, chosen_all, own_shared, latent, q_small
    ) = opening(
        w_kva,
        w_q,
        w_o,
        w_router,
        w_kvb.reshape(w_kvb.shape[0], members, -1).transpose(1, 0, 2),
        jnp.broadcast_to(chosen_by.T[:, None, :], (experts, 8, tokens)),
        shared.reshape(members, -1, 2 * hidden_slice),
        normed,
        qa_down,
        qa_up,
        cosine2,
        sine2,
        kv_gain[None],
        members,
        split,
        1,
    )
    full_kva, full_o, full_router = (v.reshape(-1, v.shape[2]) for v in (all_kva, all_o, all_router))
    own_kvb = kvb_parts.reshape(KVR, -1)
    own_shared = own_shared.reshape(width, -1)
    all_latent = all_latent.reshape(length, KVR + ROPE)
    q_head = unpack(q_packed).reshape(length, QK)
    q_head, c_first = lax.optimization_barrier((q_head, cotangent[:, : width // 2]))
    expanded = dot(all_latent[:, :KVR], own_kvb).astype(BF16)
    k_head = jnp.concatenate([expanded[:, :NOPE], all_latent[:, KVR:]], axis=-1)
    v_head = expanded[:, NOPE:]
    mixture, lse, mixed_parts = attend(prefix_len, q_head, k_head, v_head, members, 3)
    mixed = mixed_parts.transpose(1, 0, 2).reshape(tokens, H * VD)
    o_small = dot(mixed, oa_down).astype(BF16)
    middle = inputs + dot(mixed, full_o) + dot(o_small, oa_up)
    ffn_in = root_norm(middle, ffn_gain).astype(BF16)
    route_probs = jax.nn.softmax(dot(ffn_in, full_router), axis=-1)

    half = width // 2
    first_c = gather(c_first).reshape(members, tokens, half)
    chosen = chosen_all[:, 0] > 0.5
    order = jnp.arange(tokens, dtype=jnp.int32)
    before = (order[:, None] < order[None, :]).astype(BF16)
    rank = jnp.where(chosen, dot(chosen.astype(BF16), before), -1.0)
    back = rank[:, :, None]
    rank = jnp.broadcast_to(rank[:, None, :], (members, 8, tokens))
    weights = (expert_gate[0], expert_up_weight[0], expert_down[0], own_shared, shared_down)
    prob_blocks = jnp.broadcast_to(route_probs.T[:, None, :], (experts, 8, tokens))
    partial, kept_gate, kept_up, kept_out, kept_shared, second_c, prob_parts = experts_forward(
        ffn_in, prob_blocks, cotangent[:, half:], rank, back, *weights, slots, members, 4
    )
    kept = (kept_gate, kept_up, kept_out, kept_shared)
    ffn_out = scatter_sum(partial.reshape(length, width))
    d_own, d_route = experts_backward(
        (first_c, second_c), rank, back, prob_parts, kept, *weights, slots, members, 5
    )
    d_route = d_route[:, 0].T
    d_logits = (
        route_probs * (d_route - jnp.sum(route_probs * d_route, axis=-1, keepdims=True))
    ).astype(BF16)
    d_ffn = d_own.astype(F32) + dot_t(d_logits, full_router)
    d_middle = c32 + norm_back(middle, ffn_gain, d_ffn)
    d_attn = d_middle.astype(BF16)
    grad_oup = t_dot(o_small, d_attn)
    d_osmall = dot_t(d_attn, oa_up).astype(BF16)
    grad_odown = t_dot(d_osmall, mixed)
    d_mixed = (dot_t(d_attn, full_o) + dot_t(d_osmall, oa_down)).astype(BF16)
    d_latents, d_query = attend_back(
        prefix_len,
        q_head,
        k_head,
        v_head,
        mixture,
        lse.reshape(members // 2, 1, 2 * tokens),
        d_mixed.reshape(tokens, H, VD).transpose(1, 0, 2),
        own_kvb,
        members,
        6,
    )
    o_parts = jnp.concatenate([by_owner(g, members) for g in (grad_odown, grad_oup)], axis=-1)
    name = jnp.broadcast_to(adapter.astype(F32), (qa_up.shape[0], 128))
    grad_inputs, q_shares, o_shares = finish(
        d_latents,
        o_parts,
        d_query,
        cosine2,
        sine2,
        all_q,
        full_kva,
        qa_up,
        qa_down,
        q_small,
        normed,
        latent,
        kv_gain[None],
        hidden[0],
        attn_gain[None],
        d_middle,
        name,
        sequences,
        7,
    )
    ffn_out, _ = lax.optimization_barrier((ffn_out, d_query))
    output = (middle + ffn_out.astype(F32)).astype(BF16)
    numbers = o_shares[:, 0, -1].astype(jnp.int32)
    q_share = jnp.sum(q_shares.astype(F32), axis=1)
    rows = width // members
    q_up_share = lax.dynamic_slice_in_dim(q_share[..., rows:], me % 2 * QK, QK, 2)
    shares = jnp.concatenate([q_share[..., :rows], q_up_share, o_shares[:, :, :-128]], axis=-1)
    selector = (jnp.arange(q_down.shape[0], dtype=jnp.int32)[:, None] == numbers[None, :]).astype(F32)
    summed = jnp.sum(selector[:, :, None, None] * shares[None], axis=1)
    sizes = [rows, QK, rows, rows]
    ends = [sum(sizes[: n + 1]) for n in range(4)]
    outs = [summed[:, :, e - s : e] for e, s in zip(ends, sizes)]
    return (
        output[None],
        grad_inputs[None],
        outs[0].transpose(0, 2, 1),
        outs[1],
        outs[2].transpose(0, 2, 1),
        outs[3],
    )


def solution(mesh):
    seq = P("rep", "grp", None)
    rows = P("grp", None)
    in_specs = (
        (seq, seq, seq, P("rep"), P("rep"), P(), P(), P())
        + (rows,) * 8
        + (P("grp", None, None),) * 3
        + (P(),) * 4
    )
    out_specs = (
        seq,
        seq,
        P(None, "grp", None),
        P(None, None, "grp"),
        P(None, "grp", None),
        P(None, None, "grp"),
    )
    return jax.shard_map(
        per_device, mesh=mesh, in_specs=in_specs, out_specs=out_specs, check_vma=False
    )
```

```python
import functools
import math

import jax
import jax.numpy as jnp
from jax import lax
from jax.experimental import pallas as pl
from jax.experimental.pallas import tpu as pltpu
from jax.sharding import PartitionSpec as P

H = 16
NOPE = 128
ROPE = 64
VD = 128
KVR = 512
TOP = 6
QK = NOPE + ROPE
EPS = 1e-06
F32 = jnp.float32
BF16 = jnp.bfloat16


def dot(former, latter):
    return jnp.dot(former, latter, preferred_element_type=F32)


def dot_t(former, latter):
    return lax.dot_general(
        former, latter, (((1,), (1,)), ((), ())), preferred_element_type=F32
    )


def t_dot(former, latter):
    return lax.dot_general(
        former, latter, (((0,), (0,)), ((), ())), preferred_element_type=F32
    )


def root_norm(v, gains):
    factor = lax.rsqrt(jnp.mean(v * v, axis=-1, keepdims=True) + EPS)
    return v * factor * gains


def norm_back(v, gains, gradient):
    factor = lax.rsqrt(jnp.mean(v * v, axis=-1, keepdims=True) + EPS)
    weighted = gradient * gains
    return factor * weighted - v * (factor * factor * factor) * jnp.mean(
        weighted * v, axis=-1, keepdims=True
    )


def angles(positions, width):
    frequency = 10000.0 ** (-jnp.arange(0, width, 2, dtype=F32) / width)
    phases = positions.astype(F32)[:, None] * frequency[None, :]
    return (jnp.cos(phases), jnp.sin(phases))


def rotate(v, cosine, sine):
    half = v.shape[-1] // 2
    a, b = v[..., :half], v[..., half:]
    return jnp.concatenate([a * cosine - b * sine, b * cosine + a * sine], axis=-1)


def unrotate(v, cosine, sine):
    half = v.shape[-1] // 2
    a, b = v[..., :half], v[..., half:]
    return jnp.concatenate([a * cosine + b * sine, b * cosine - a * sine], axis=-1)


SIDE = 2
CORES = 2
MESH = pl.DeviceIdType.MESH


def place_of():
    me = lax.axis_index("grp")
    return me // (SIDE * CORES), (me // CORES) % SIDE, me % CORES


def index_of(z, x, c):
    return (z * SIDE + x) * CORES + c


def send(src, dst, sent, got, to):
    return pltpu.make_async_remote_copy(
        src_ref=src,
        dst_ref=dst,
        send_sem=sent,
        recv_sem=got,
        device_id=to if isinstance(to, dict) else {"grp": to},
        device_id_type=MESH,
    )


def meet(members, partner=None):
    barrier = pltpu.get_barrier_semaphore()
    me = lax.axis_index("grp")

    @pl.loop(1, members)
    def _(d):
        pl.semaphore_signal(barrier, 1, device_id={"grp": lax.rem(me + d, members)}, device_id_type=MESH)

    if partner is not None:
        pl.semaphore_signal(barrier, 1, device_id=partner, device_id_type=MESH)
    pl.semaphore_wait(barrier, members - 1 + (partner is not None))


def pick_from(table, z, s):
    v = 0
    for i, row in enumerate(table):
        for j, entry in enumerate(row):
            if entry:
                v = v + jnp.where((z == i) & (s == j), entry, 0)
    return v


def near_first(levels):
    return [sorted(range(levels), key=lambda v: (abs(v - k), v)) for k in range(levels)]


def far_first(levels):
    return [sorted((v for v in range(levels) if v != k), key=lambda v: (-abs(v - k), v)) + [k] for k in range(levels)]


class Gather:
    def __init__(self, src, out, sent, got, members, split=0):
        self.src, self.out, self.sent, self.got = src, out, sent, got
        self.members, self.split = members, split
        self.levels = members // (SIDE * CORES)
        self.z, self.x, self.c = z, x, c = place_of()
        self.me = lax.axis_index("grp")
        self.up, self.down = index_of(z + 1, x, c), index_of(z - 1, x, c)
        self.side, self.twin = index_of(z, 1 - x, c), index_of(z, x, 1 - c)
        if split:
            rows = src.shape[0]
            rep = lax.axis_index("rep")
            odd = rep % 2
            self.partner = {"rep": rep + 1 - 2 * odd, "grp": self.me}
            self.window = pl.ds(pl.multiple_of(odd * split, 16), rows - split)
            self.given = pl.ds(pl.multiple_of(odd * (rows - split), 16), split)
            self.lacked = pl.ds(pl.multiple_of((1 - odd) * (rows - split), 16), split)

    def copy(self, slot, kind, to, own=False, rows=None):
        rows = rows or (self.window if self.split else None)
        other = rows is not None and self.split and rows is not self.window
        src = self.src if own else self.out.at[slot]
        dst = self.out.at[slot]
        if rows is not None:
            src, dst = src.at[rows], dst.at[rows]
        return send(src, dst, self.sent.at[kind, slot], self.got.at[int(bool(other)), slot], to)

    def arrive(self, slot):
        self.copy(slot, 0, self.twin).wait_recv()

    def to_partner(self, slot):
        return self.copy(slot, 4, self.partner, rows=self.given)

    def lacked_to_twin(self, slot, own=False):
        return self.copy(slot, 5, self.twin, own, rows=self.lacked)

    def first(self):
        @pl.when(self.z < self.levels - 1)
        def _():
            self.copy(self.me, 0, self.up, True).start()

        @pl.when(self.z > 0)
        def _():
            self.copy(self.me, 1, self.down, True).start()

        self.copy(self.me, 2, self.side, True).start()
        self.copy(self.me, 3, self.twin, True).start()
        if self.split:
            self.lacked_to_twin(self.me, True).start()

    def relay(self, s):
        @pl.when(self.z >= s)
        def _():
            slot = index_of(self.z - s, self.x, self.c)
            self.arrive(slot)

            @pl.when(self.z < self.levels - 1)
            def _():
                self.copy(slot, 0, self.up).start()

            self.spread(slot)

        @pl.when(self.z + s < self.levels)
        def _():
            slot = index_of(self.z + s, self.x, self.c)
            self.arrive(slot)

            @pl.when(self.z > 0)
            def _():
                self.copy(slot, 1, self.down).start()

            self.spread(slot)

    def spread(self, slot):
        self.copy(slot, 2, self.side).start()
        self.copy(slot, 3, self.twin).start()
        if self.split:
            self.to_partner(slot).start()

    def pass_on(self, k):
        slot = index_of(k, 1 - self.x, self.c)
        self.arrive(slot)
        self.copy(slot, 3, self.twin).start()
        if self.split:
            self.to_partner(slot).start()

    def take_lacked(self, k, x):
        slot = index_of(k, x, self.c)

        @pl.when(slot != self.me)
        def _():
            self.copy(slot, 4, self.partner, rows=self.lacked).wait_recv()
            self.lacked_to_twin(slot).start()

    def take_twin(self, k):
        for x in range(SIDE):
            self.arrive(index_of(k, x, 1 - self.c))

    def take_twin_lacked(self):
        @pl.loop(0, self.members // CORES)
        def _(i):
            self.lacked_to_twin(i * CORES + 1 - self.c).wait_recv()

    def finish(self):
        @pl.loop(0, self.levels)
        def _(k):
            slot = index_of(k, self.x, self.c)
            self.copy(slot, 2, self.side).wait_send()

            @pl.when((k <= self.z) & (self.z < self.levels - 1))
            def _():
                self.copy(slot, 0, self.up).wait_send()

            @pl.when((k >= self.z) & (self.z > 0))
            def _():
                self.copy(slot, 1, self.down).wait_send()

        @pl.loop(0, self.members // CORES)
        def _(i):
            slot = i * CORES + self.c
            self.copy(slot, 3, self.twin).wait_send()
            if self.split:
                self.lacked_to_twin(slot).wait_send()

                @pl.when(slot != self.me)
                def _():
                    self.to_partner(slot).wait_send()


class SideFirst(Gather):
    def turn(self):
        slot = index_of(self.z, 1 - self.x, self.c)
        self.arrive(slot)

        @pl.when(self.z < self.levels - 1)
        def _():
            self.copy(slot, 0, self.up).start()

        @pl.when(self.z > 0)
        def _():
            self.copy(slot, 1, self.down).start()

        self.copy(slot, 3, self.twin).start()

    def relay(self, s):
        for x in (self.x, 1 - self.x):

            @pl.when(self.z >= s)
            def _():
                slot = index_of(self.z - s, x, self.c)
                self.arrive(slot)

                @pl.when(self.z < self.levels - 1)
                def _():
                    self.copy(slot, 0, self.up).start()

                self.copy(slot, 3, self.twin).start()

            @pl.when(self.z + s < self.levels)
            def _():
                slot = index_of(self.z + s, x, self.c)
                self.arrive(slot)

                @pl.when(self.z > 0)
                def _():
                    self.copy(slot, 1, self.down).start()

                self.copy(slot, 3, self.twin).start()

    def finish(self):
        self.copy(self.me, 2, self.side).wait_send()

        @pl.loop(0, self.members // CORES)
        def _(i):
            slot = i * CORES + self.c
            k = i // SIDE

            @pl.when((k <= self.z) & (self.z < self.levels - 1))
            def _():
                self.copy(slot, 0, self.up).wait_send()

            @pl.when((k >= self.z) & (self.z > 0))
            def _():
                self.copy(slot, 1, self.down).wait_send()

            self.copy(slot, 3, self.twin).wait_send()


class Exchange:
    def __init__(self, src, out, sent, got, members, halved=False):
        self.src, self.out, self.sent, self.got, self.members = src, out, sent, got, members
        self.me = lax.axis_index("grp")
        self.rows = None
        if halved:
            half = src.shape[1] // 2
            rep = lax.axis_index("rep")
            odd = rep % 2
            self.partner = {"rep": rep + 1 - 2 * odd, "grp": self.me}
            self.rows = pl.ds(pl.multiple_of(odd * half, 16), half)

    def copy(self, d):
        to = lax.rem(self.me + d, self.members)
        src, dst = self.src.at[to], self.out.at[self.me]
        if self.rows is not None:
            src, dst = src.at[self.rows], dst.at[self.rows]
        return send(src, dst, self.sent.at[d], self.got.at[d], to)

    def to_partner(self):
        ours = self.out.at[:, self.rows]
        return send(ours, ours, self.sent.at[0], self.got.at[0], self.partner)

    def start(self):
        @pl.loop(1, self.members)
        def _(d):
            self.copy(d).start()

    def wait(self):
        @pl.loop(1, self.members)
        def _(d):
            self.copy(d).wait()


class Reduce:
    def __init__(self, p, twin_in, side_in, line_in, sems, members):
        self.p, self.twin_in, self.side_in, self.line_in = p, twin_in, side_in, line_in
        self.sems = sems
        self.levels = members // (SIDE * CORES)
        self.z, self.x, self.c = place_of()

    def copy(self, kind, slot, dst, n, to):
        sent, got = self.sems[2 * kind], self.sems[2 * kind + 1]
        return send(self.p.at[slot], dst.at[n], sent.at[n], got.at[n], to)

    def to_twin(self, k, w):
        twin = index_of(self.z, self.x, 1 - self.c)
        return self.copy(0, index_of(k, w, 1 - self.c), self.twin_in, k * SIDE + w, twin)

    def to_side(self, k):
        return self.copy(1, index_of(k, 1 - self.x, self.c), self.side_in, k, index_of(self.z, 1 - self.x, self.c))

    def to_up(self, k):
        return self.copy(2, index_of(k, self.x, self.c), self.line_in, k + 1, index_of(self.z + 1, self.x, self.c))

    def to_down(self, k):
        return self.copy(3, index_of(k, self.x, self.c), self.line_in, k, index_of(self.z - 1, self.x, self.c))

    def add(self, slot, ref):
        rows = self.p.shape[1]
        chunk = next(r for r in (32, 16, 8) if rows % r == 0)

        @pl.loop(0, rows // chunk)
        def _(i):
            at = pl.ds(pl.multiple_of(i * chunk, chunk), chunk)
            self.p[slot, at, :] = (self.p[slot, at, :].astype(F32) + ref[at, :].astype(F32)).astype(self.p.dtype)

    def start(self, k):
        self.to_twin(k, self.x).start()
        self.to_twin(k, 1 - self.x).start()

    def chip(self, k):
        w = 1 - self.x
        self.to_twin(k, w).wait_recv()
        self.add(index_of(k, w, self.c), self.twin_in.at[k * SIDE + w])
        self.to_side(k).start()
        self.to_twin(k, self.x).wait_recv()
        self.add(index_of(k, self.x, self.c), self.twin_in.at[k * SIDE + self.x])

    def line(self, k):
        z, mine = self.z, index_of(k, self.x, self.c)
        self.to_side(k).wait_recv()
        self.add(mine, self.side_in.at[k])

        @pl.when((k > z) & (z > 0))
        def _():
            self.to_up(k).wait_recv()
            self.add(mine, self.line_in.at[k + 1])

        @pl.when((k < z) & (z < self.levels - 1))
        def _():
            self.to_down(k).wait_recv()
            self.add(mine, self.line_in.at[k])

        @pl.when(k > z)
        def _():
            self.to_up(k).start()

        @pl.when(k < z)
        def _():
            self.to_down(k).start()

    def last(self, out):
        z, mine = self.z, index_of(self.z, self.x, self.c)
        self.to_side(z).wait_recv()
        self.add(mine, self.side_in.at[z])

        @pl.when(z > 0)
        def _():
            self.to_up(z).wait_recv()
            self.add(mine, self.line_in.at[z + 1])

        @pl.when(z < self.levels - 1)
        def _():
            self.to_down(z).wait_recv()
            self.add(mine, self.line_in.at[z])

        out[...] = self.p[mine]

    def finish(self):
        z = self.z

        @pl.loop(0, self.levels)
        def _(k):
            self.to_twin(k, 0).wait_send()
            self.to_twin(k, 1).wait_send()
            self.to_side(k).wait_send()

            @pl.when(k > z)
            def _():
                self.to_up(k).wait_send()

            @pl.when(k < z)
            def _():
                self.to_down(k).wait_send()

    @staticmethod
    def scratch(members, r, c, kind):
        levels = members // (SIDE * CORES)
        sem = pltpu.SemaphoreType.DMA
        return [
            pltpu.VMEM((members // CORES, r, c), kind),
            pltpu.VMEM((levels, r, c), kind),
            pltpu.VMEM((levels + 1, r, c), kind),
        ] + [sem((n,)) for n in (members // CORES,) * 2 + (levels,) * 2 + (levels + 1,) * 4]


def gather(v):
    return lax.all_gather(v, "grp", axis=0, tiled=True)


def scatter_sum(v):
    return lax.psum_scatter(v, "grp", scatter_dimension=0, tiled=True)


def after(v, *others):
    return lax.optimization_barrier((v, *others))[0]


def tie(v, other):
    first = other[(0,) * other.ndim]
    return v + jnp.minimum(jnp.abs(first), 0).astype(v.dtype)


def open_kernel(
    kva_src, q_src, o_src, router_src, chosen_src, kvb_ref, sgate_ref, sup_ref,
    normed_ref, down_ref, up_ref, cos_ref, sin_ref, kvg_ref,
    all_kva, all_q, all_o, all_router, all_lat, q_out, kvb_out, chosen_out, shared_out, latent_ref, small_ref,
    *bufs, members, split
):
    stage = bufs[:5]
    kvb_src, shared_src, kva, wq, lat_st, qm = bufs[5:11]
    sems = bufs[11:]
    local, load = sems[26:]
    pairs = [sems[2 * n : 2 * n + 2] for n in range(13)]
    me = lax.axis_index("grp")
    levels = members // (SIDE * CORES)
    z = me // (SIDE * CORES)
    order = near_first(levels)
    tokens, width = normed_ref.shape
    g_kva = Gather(kva_src, all_kva, *pairs[0], members, split)
    g_q = Gather(q_src, all_q, *pairs[1], members, split)
    g_o = Gather(o_src, all_o, *pairs[2], members, o_src.shape[0] // 2 if split else 0)
    g_router = Gather(router_src, all_router, *pairs[3], members)
    g_lat = Gather(lat_st, all_lat, *pairs[4], members)
    e_kvb = Exchange(kvb_src, kvb_out, *pairs[5], members)
    e_chosen = Exchange(chosen_src, chosen_out, *pairs[6], members)
    e_shared = Exchange(shared_src, shared_out, *pairs[7], members, split > 0)
    q_sent, q_got = pairs[8]
    sources = [kva_src, q_src, o_src, router_src, chosen_src.at[me]]
    places = [all_kva, all_q, all_o, all_router, chosen_out]
    into = [pltpu.make_async_copy(a, stage[n], local.at[n]) for n, a in enumerate(sources)]
    out_of = [pltpu.make_async_copy(stage[n], b.at[me], local.at[n]) for n, b in enumerate(places)]
    cut, cut_out = shared_src.at[me], shared_out.at[me]
    if split:
        cut, cut_out = cut.at[e_shared.rows], cut_out.at[e_shared.rows]
    own_cut = [
        pltpu.make_async_copy(kvb_src.at[me], kvb_out.at[me], local.at[5]),
        pltpu.make_async_copy(cut, cut_out, local.at[6]),
    ]
    own_lat = pltpu.make_async_copy(lat_st, all_lat.at[me], local.at[7])
    own_q = pltpu.make_async_copy(qm.at[me], q_out.at[me], local.at[8])
    loads = [pltpu.make_async_copy(all_kva, kva, load.at[0]), pltpu.make_async_copy(all_q, wq, load.at[1])]

    def query_to(n):
        return send(qm.at[n], q_out.at[me], q_sent.at[n], q_got.at[me], n)

    def query_from(n):
        return send(qm.at[n], q_out.at[n], q_sent.at[n], q_got.at[n], n)

    def lacked(g, s):
        if g.split:
            k = pick_from(order, z, s)
            g.take_lacked(k, g.x)
            g.take_lacked(k, 1 - g.x)

    def events(gathers, s, before):
        for g in gathers:
            g.relay(s + 1)
        for g in gathers:
            g.pass_on(pick_from(order, z, s))

        @pl.when(before)
        def _():
            for g in gathers:
                lacked(g, s - 1)

    for copy in into:
        copy.start()
    meet(members, g_kva.partner if split else None)
    for g in (g_kva, g_q, g_router):
        g.first()
    e_chosen.start()
    cols, units = kvb_src.shape[2], shared_src.shape[2] // 2
    for g in range(members):
        kvb_src[g] = kvb_ref[:, g * cols : (g + 1) * cols]
        at = slice(g * units, (g + 1) * units)
        shared_src[g] = jnp.concatenate([sgate_ref[:, at], sup_ref[:, at]], axis=1)
    e_kvb.start()
    for copy in own_cut:
        copy.start()
    for a, b in zip(into, out_of):
        a.wait()
        b.start()

    @pl.loop(0, levels)
    def _(s):
        events((g_kva, g_q, g_router), s, s >= 1)

    lacked(g_kva, levels - 1)
    lacked(g_q, levels - 1)
    g_o.first()
    e_shared.start()
    for g in (g_kva, g_q):

        @pl.loop(0, levels)
        def _(k):
            g.take_twin(k)

        if split:
            g.take_twin_lacked()
    for copy in out_of + own_cut:
        copy.wait()
    for copy in loads:
        copy.start()
    loads[0].wait()
    latent = dot(normed_ref[...], kva[...].reshape(width, -1))
    latent_ref[...] = latent
    half = ROPE // 2

    def turn(v):
        turned = jnp.concatenate([v[:, half:], v[:, :half]], axis=1)
        return (v * cos_ref[...] - turned * sin_ref[...]).astype(BF16)

    lat_st[:, :KVR] = root_norm(latent[:, :KVR], kvg_ref[...]).astype(BF16)
    lat_st[:, KVR:] = turn(latent[:, KVR:])
    g_lat.first()
    own_lat.start()
    small_ref[...] = dot(normed_ref[...], down_ref[...]).astype(BF16)
    loads[1].wait()
    turns = members // 2

    @pl.loop(0, turns)
    def _(n):
        pair = lax.rem(me // 2 + n, turns)
        at = pl.ds(pl.multiple_of(pair * 2 * QK, 128), 2 * QK)
        both = dot(normed_ref[...], wq[:, :, at].reshape(width, 2 * QK)) + dot(small_ref[...], up_ref[:, at])
        for t in range(2):
            to = 2 * pair + t
            r = t * QK
            qm[to, :tokens, :] = both[:, r : r + NOPE].astype(BF16)
            rope = turn(both[:, r + NOPE : r + QK])
            qm[to, tokens:, :ROPE] = rope[: tokens // 2]
            qm[to, tokens:, ROPE:] = rope[tokens // 2 :]

            @pl.when(to == me)
            def _():
                own_q.start()

            @pl.when(to != me)
            def _():
                query_to(to).start()

        @pl.when(n == turns // 2)
        def _():
            events((g_lat, g_o), 0, False)

    @pl.loop(1, levels)
    def _(s):
        events((g_lat, g_o), s, s >= 1)

        @pl.when(s == 1)
        def _():
            e_shared.wait()
            if split:
                e_shared.to_partner().start()

    lacked(g_o, levels - 1)
    for g in (g_lat, g_router, g_o):

        @pl.loop(0, levels)
        def _(k):
            g.take_twin(k)

        if g.split:
            g.take_twin_lacked()
    for g in (g_kva, g_q, g_router, g_lat, g_o):
        g.finish()

    @pl.loop(1, members)
    def _(d):
        n = lax.rem(me + d, members)
        query_from(n).wait_recv()
        query_to(n).wait_send()

    for e in (e_kvb, e_chosen):
        e.wait()
    if split:
        e_shared.to_partner().wait()
    own_lat.wait()
    own_q.wait()


def opening(kva, q, o, router, chosen, kvb, sgate, sup, normed, down, up, cosine, sine, kvg, members, split, collective_id):
    tokens, width = normed.shape
    vmem = pl.BlockSpec(memory_space=pltpu.VMEM)
    anywhere = pl.BlockSpec(memory_space=pl.ANY)
    sem = pltpu.SemaphoreType.DMA
    packed = tokens + tokens // 2
    cut = (members, kvb.shape[0], kvb.shape[1] // members)
    slices = (members, sgate.shape[0], 2 * sgate.shape[1] // members)
    grown = lambda a: jax.ShapeDtypeStruct((members, *a.shape), a.dtype)
    same = lambda a: jax.ShapeDtypeStruct(a.shape, a.dtype)
    g_sems = [sem((6, members)), sem((2, members))]
    e_sems = [sem((members,)), sem((members,))]
    return pl.pallas_call(
        functools.partial(open_kernel, members=members, split=split),
        in_specs=[anywhere] * 5 + [vmem] * 9,
        out_specs=[anywhere] * 9 + [vmem] * 2,
        out_shape=[
            grown(kva), grown(q), grown(o), grown(router),
            jax.ShapeDtypeStruct((members, tokens, kva.shape[1]), BF16),
            jax.ShapeDtypeStruct((members, packed, NOPE), BF16),
            jax.ShapeDtypeStruct(cut, BF16), same(chosen), jax.ShapeDtypeStruct(slices, BF16),
            jax.ShapeDtypeStruct((tokens, kva.shape[1]), F32),
            jax.ShapeDtypeStruct((tokens, down.shape[1]), BF16),
        ],
        scratch_shapes=[pltpu.VMEM(a.shape, a.dtype) for a in (kva, q, o, router)]
        + [
            pltpu.VMEM(chosen.shape[1:], F32),
            pltpu.VMEM(cut, BF16),
            pltpu.VMEM(slices, BF16),
            pltpu.VMEM((members, *kva.shape), BF16),
            pltpu.VMEM((members, *q.shape), BF16),
            pltpu.VMEM((tokens, kva.shape[1]), BF16),
            pltpu.VMEM((members, packed, NOPE), BF16),
        ]
        + g_sems * 5
        + e_sems * 8
        + [sem((9,)), sem((2,))],
        compiler_params=pltpu.CompilerParams(
            collective_id=collective_id, has_side_effects=True, vmem_limit_bytes=48 * 1024 * 1024
        ),
        cost_estimate=pl.CostEstimate(flops=2 * tokens * width * q.shape[1], bytes_accessed=200_000_000, transcendentals=0),
        name="opening",
    )(kva, q, o, router, chosen, kvb, sgate, sup, normed, down, up, cosine, sine, kvg)


def key_blocks(start, rows, keys, length):
    end = start + rows
    end = jnp.where(start < length // 2, jnp.maximum(end, length // 2), end)
    return (start + 1) // keys, (end + keys - 1) // keys


def attend_kernel(
    prefix_ref, packed, lat_ref, kvb_ref, o_ref, lse_ref, q_ref, k_ref, v_ref, mixed, blocks, sent, got, local,
    *, members, unit
):
    me = lax.axis_index("grp")
    tokens = blocks.shape[1]
    block, keys = 2 * tokens, 4 * tokens
    turns = members // 2
    prefix = prefix_ref[0]

    def block_to(n):
        return send(blocks.at[n], mixed.at[me], sent.at[n], got.at[me], n)

    def from_device(n):
        return send(blocks.at[n], mixed.at[n], sent.at[n], got.at[n], n)

    own = pltpu.make_async_copy(blocks.at[me], mixed.at[me], local)
    half = tokens // 2

    @pl.loop(0, members)
    def _(b):
        at = pl.multiple_of(b * tokens, tokens)
        here = pl.ds(at, tokens)
        q_ref[here, :NOPE] = packed[b, :tokens, :]
        q_ref[pl.ds(at, half), NOPE:] = packed[b, tokens:, :ROPE]
        q_ref[pl.ds(at + half, half), NOPE:] = packed[b, tokens:, ROPE:]
        made = dot(lat_ref[b, :, :KVR], kvb_ref[...]).astype(BF16)
        k_ref[here, :NOPE] = made[:, :NOPE]
        k_ref[here, NOPE:] = lat_ref[b, :, KVR:]
        v_ref[here, :] = made[:, NOPE:]

    meet(members)

    @pl.loop(0, turns)
    def _(n):
        i = lax.rem(me // 2 + n, turns)
        start = pl.multiple_of(i * block, block)
        here = pl.ds(start, block)
        q = q_ref[here, :]
        rows = start + lax.broadcasted_iota(jnp.int32, (block, 1), 0)
        limit = jnp.where(rows < prefix, prefix - 1, rows)
        limit = jnp.maximum(limit, rows)

        def step(j, carry, masked):
            top, total, acc = carry
            at = pl.multiple_of(j * keys, keys)
            k = k_ref[pl.ds(at, keys), :]
            v = v_ref[pl.ds(at, keys), :]
            s = dot_t(q, k)
            if masked:
                cols = at + lax.broadcasted_iota(jnp.int32, (1, keys), 1)
                s = jnp.where(cols <= limit, s, -1e30)
            fresh = jnp.maximum(top, jnp.max(s, axis=1, keepdims=True))
            p = jnp.exp2((s - fresh) * unit)
            scale = jnp.exp2((top - fresh) * unit)
            total = total * scale + jnp.sum(p, axis=1, keepdims=True)
            acc = acc * scale + dot(p.astype(BF16), v)
            return fresh, total, acc

        carry = (
            jnp.full((block, 1), -1e30, F32),
            jnp.zeros((block, 1), F32),
            jnp.zeros((block, VD), F32),
        )
        full, stop = key_blocks(start, block, keys, q_ref.shape[0])
        carry = lax.fori_loop(0, full, functools.partial(step, masked=False), carry)
        top, total, acc = lax.fori_loop(full, stop, functools.partial(step, masked=True), carry)
        o = acc / total
        o_ref[here, :] = o
        lse_ref[here, :] = top * unit + jnp.log2(total)
        blocks[pl.ds(2 * i, 2)] = o.astype(BF16).reshape(2, tokens, VD)
        for t in range(2):
            to = 2 * i + t

            @pl.when(to == me)
            def _():
                own.start()

            @pl.when(to != me)
            def _():
                block_to(to).start()

    own.wait()

    @pl.loop(1, members)
    def _(d):
        n = lax.rem(me + d, members)
        from_device(n).wait_recv()
        block_to(n).wait_send()


def attend(prefix, packed, latents, kvb, members, collective_id):
    tokens = latents.shape[1]
    length = tokens * members
    vmem = pl.BlockSpec(memory_space=pltpu.VMEM)
    sem = pltpu.SemaphoreType.DMA
    return pl.pallas_call(
        functools.partial(attend_kernel, members=members, unit=QK**-0.5 * math.log2(math.e)),
        in_specs=[pl.BlockSpec(memory_space=pltpu.SMEM), vmem, vmem, vmem],
        out_specs=[vmem] * 5 + [pl.BlockSpec(memory_space=pl.ANY)],
        out_shape=[
            jax.ShapeDtypeStruct((length, VD), F32),
            jax.ShapeDtypeStruct((length, 1), F32),
            jax.ShapeDtypeStruct((length, QK), BF16),
            jax.ShapeDtypeStruct((length, QK), BF16),
            jax.ShapeDtypeStruct((length, VD), BF16),
            jax.ShapeDtypeStruct((members, tokens, VD), BF16),
        ],
        scratch_shapes=[pltpu.VMEM((members, tokens, VD), BF16), sem((members,)), sem((members,)), sem],
        compiler_params=pltpu.CompilerParams(
            collective_id=collective_id, has_side_effects=True, vmem_limit_bytes=40 * 1024 * 1024
        ),
        cost_estimate=pl.CostEstimate(
            flops=length * length * (QK + VD), bytes_accessed=length * 1000, transcendentals=length * length // 2
        ),
        name="attend",
    )(prefix, packed, latents, kvb)


def attend_back_kernel(
    prefix_ref, q_ref, k_ref, v_ref, o_ref, lse_ref, d_hbm, kvb_ref, part_ref, dq_out,
    ds_in, blocks, dk, dv, sent, got, q_sent, q_got, local, local2,
    *, members, factor, unit
):
    me = lax.axis_index("grp")
    tokens = blocks.shape[1] * 2 // 3
    block, keys = 2 * tokens, 4 * tokens
    turns = members // 2
    prefix = prefix_ref[0]
    exchange = Exchange(d_hbm, ds_in, sent, got, members)
    into = pltpu.make_async_copy(d_hbm.at[me], ds_in.at[me], local)
    own = pltpu.make_async_copy(blocks.at[me], dq_out.at[me], local2)

    def block_to(n):
        return send(blocks.at[n], dq_out.at[me], q_sent.at[n], q_got.at[me], n)

    def from_device(n):
        return send(blocks.at[n], dq_out.at[n], q_sent.at[n], q_got.at[n], n)

    into.start()
    meet(members)
    exchange.start()
    dk[...] = jnp.zeros_like(dk)
    dv[...] = jnp.zeros_like(dv)
    into.wait()

    @pl.loop(0, turns)
    def _(n):
        i = lax.rem(me // 2 + n, turns)
        start = pl.multiple_of(i * block, block)
        here = pl.ds(start, block)
        for t in range(2):
            source = 2 * i + t

            @pl.when(source != me)
            def _():
                send(ds_in.at[source], ds_in.at[source], sent.at[0], got.at[lax.rem(me - source + members, members)], source).wait_recv()

        d = ds_in[pl.ds(2 * i, 2)].reshape(block, VD)
        q = q_ref[here, :]
        lse = lse_ref[pl.ds(i, 1), 0, :]
        along = d.astype(F32) * o_ref[here, :]
        high = along.astype(BF16)
        low = (along - high.astype(F32)).astype(BF16)
        ones = jnp.ones((8, VD), BF16)
        delta = (dot_t(ones, high) + dot_t(ones, low))[0:1, :]
        rows = start + lax.broadcasted_iota(jnp.int32, (1, block), 1)
        limit = jnp.maximum(jnp.where(rows < prefix, prefix - 1, rows), rows)

        def step(j, dq, masked):
            at = pl.multiple_of(j * keys, keys)
            k = k_ref[pl.ds(at, keys), :]
            v = v_ref[pl.ds(at, keys), :]
            p = jnp.exp2(dot_t(k, q) * unit - lse)
            if masked:
                cols = at + lax.broadcasted_iota(jnp.int32, (keys, 1), 0)
                p = jnp.where(cols <= limit, p, 0.0)
            dp = dot_t(v, d)
            ds = (p * (dp - delta)).astype(BF16)
            dv[pl.ds(at, keys), :] += dot(p.astype(BF16), d)
            dk[pl.ds(at, keys), :] += dot(ds, q)
            return dq + t_dot(ds, k)

        full, stop = key_blocks(start, block, keys, q_ref.shape[0])
        dq = lax.fori_loop(0, full, functools.partial(step, masked=False), jnp.zeros((block, QK), F32))
        dq = lax.fori_loop(full, stop, functools.partial(step, masked=True), dq)
        dq = (dq * factor).astype(BF16)
        half = tokens // 2
        for t in range(2):
            to = 2 * i + t
            r = t * tokens
            blocks[to, :tokens, :] = dq[r : r + tokens, :NOPE]
            blocks[to, tokens:, :ROPE] = dq[r : r + half, NOPE:]
            blocks[to, tokens:, ROPE:] = dq[r + half : r + tokens, NOPE:]

            @pl.when(to == me)
            def _():
                own.start()

            @pl.when(to != me)
            def _():
                block_to(to).start()

    @pl.loop(0, members)
    def _(b):
        at = pl.ds(pl.multiple_of(b * tokens, tokens), tokens)
        d = jnp.concatenate([dk[at, :NOPE] * factor, dv[at, :]], axis=1).astype(BF16)
        part_ref[b, :, :KVR] = dot_t(d, kvb_ref[...]).astype(BF16)
        part_ref[b, :, KVR:] = (dk[at, NOPE:] * factor).astype(BF16)

    own.wait()

    @pl.loop(1, members)
    def _(d):
        n = lax.rem(me + d, members)
        from_device(n).wait_recv()
        block_to(n).wait_send()
        exchange.copy(d).wait_send()


def attend_back(prefix, q, k, v, o, lse, d, kvb, members, collective_id):
    length = q.shape[0]
    tokens = length // members
    vmem = pl.BlockSpec(memory_space=pltpu.VMEM)
    anywhere = pl.BlockSpec(memory_space=pl.ANY)
    sem = pltpu.SemaphoreType.DMA
    factor = QK**-0.5
    packed = tokens + tokens // 2
    return pl.pallas_call(
        functools.partial(attend_back_kernel, members=members, factor=factor, unit=factor * math.log2(math.e)),
        in_specs=[pl.BlockSpec(memory_space=pltpu.SMEM)] + [vmem] * 5 + [anywhere, vmem],
        out_specs=[vmem, anywhere],
        out_shape=[
            jax.ShapeDtypeStruct((members, tokens, KVR + ROPE), BF16),
            jax.ShapeDtypeStruct((members, packed, NOPE), BF16),
        ],
        scratch_shapes=[
            pltpu.VMEM((members, tokens, VD), BF16),
            pltpu.VMEM((members, packed, NOPE), BF16),
            pltpu.VMEM((length, QK), F32),
            pltpu.VMEM((length, VD), F32),
            sem((members,)), sem((members,)), sem((members,)), sem((members,)), sem, sem,
        ],
        compiler_params=pltpu.CompilerParams(
            collective_id=collective_id, has_side_effects=True, vmem_limit_bytes=50 * 1024 * 1024
        ),
        cost_estimate=pl.CostEstimate(
            flops=length * length * (3 * QK + 2 * VD), bytes_accessed=length * 2000, transcendentals=length * length // 2
        ),
        name="attend_back",
    )(prefix, q, k, v, o, lse, d, kvb)


def silu_parts(v):
    logistic = 0.5 * jnp.tanh(0.5 * v) + 0.5
    return v * logistic, logistic * (1.0 + v * (1.0 - logistic))


def picks(rank, slots):
    at = lax.broadcasted_iota(jnp.int32, (slots, rank.shape[1]), 0).astype(F32)
    return at == rank


def picks_back(rank, slots):
    at = lax.broadcasted_iota(jnp.int32, (rank.shape[0], slots), 1).astype(F32)
    return at == rank


def tiles(width, size):
    return pl.ds(pl.multiple_of(width * size, size), size)


def experts_kernel(
    x_hbm, prob_hbm, c_hbm, c2_hbm, rank_ref, back_ref, gate_hbm, up_hbm, down_hbm, own_hbm, sdown_hbm,
    part_hbm, eg_hbm, eu_hbm, eo_hbm, sh_hbm, c_out, c2_out, prob_out,
    xs, probs, gate, up, down, own, sdown, tail, rows, acts, sacts, part_st, eg_st, eu_st, eo_st, sh_st,
    c_st, c2_st, sent, got, e_sent, e_got, c_sent, c_got, c2_sent, c2_got, load, store,
    *, members, slots, tile, wide
):
    me = lax.axis_index("grp")
    levels = members // (SIDE * CORES)
    group = SIDE * CORES
    width, hidden = gate.shape
    half, whole = hidden % tile, hidden // tile
    units = own.shape[1] // 2
    z = me // group
    order = near_first(levels)
    loads = [
        pltpu.make_async_copy(a, b, load.at[n])
        for n, (a, b) in enumerate(
            [
                (x_hbm, xs.at[me]),
                (prob_hbm.at[me], probs.at[me]),
                (own_hbm, own),
                (gate_hbm, gate),
                (up_hbm, up),
                (down_hbm, down),
                (sdown_hbm, sdown),
                (c_hbm, c_st),
                (c2_hbm, c2_st),
            ]
        )
    ]
    gather = Gather(x_hbm, xs, sent, got, members)
    behind = Gather(c_hbm, c_out, c_sent, c_got, members)
    behind2 = SideFirst(c2_hbm, c2_out, c2_sent, c2_got, members)
    own_c = [
        pltpu.make_async_copy(c_st, c_out.at[me], load.at[7]),
        pltpu.make_async_copy(c2_st, c2_out.at[me], load.at[8]),
    ]
    exchange = Exchange(prob_hbm, probs, e_sent, e_got, members)
    for copy in loads:
        copy.start()
    meet(members)
    gather.first()
    exchange.start()
    for copy in loads:
        copy.wait()
    for copy in own_c:
        copy.start()
    tail[:, :half] = gate[:, hidden - half :]
    tail[:, half:] = up[:, hidden - half :]
    gather.pass_on(z)
    gather.relay(1)
    exchange.wait()
    prob_out[...] = probs[...]

    def stores(s, k):
        n = s % 2
        return [
            pltpu.make_async_copy(a, b.at[k], store.at[n, m])
            for m, (a, b) in enumerate(
                [
                    (part_st.at[n], part_hbm),
                    (eg_st.at[n], eg_hbm),
                    (eu_st.at[n], eu_hbm),
                    (eo_st.at[n], eo_hbm),
                    (sh_st.at[n], sh_hbm),
                ]
            )
        ]

    @pl.loop(0, levels)
    def _(s):
        k = pick_from(order, z, s)
        n = s % 2
        gather.take_twin(k)

        @pl.when(s >= 2)
        def _():
            for copy in stores(s, pick_from(order, z, s - 2)):
                copy.wait()

        @pl.loop(0, group)
        def _(b):
            pick = picks(rank_ref[k * group + b, 0:1, :], slots).astype(BF16)
            rows[tiles(b, slots), :] = dot(pick, xs[k * group + b]).astype(BF16)

        def keep(at, g, u):
            eg_st[n, :, at] = g.astype(BF16)
            eu_st[n, :, at] = u.astype(BF16)
            acts[:, at] = (silu_parts(g)[0] * u).astype(BF16)

        @pl.loop(0, whole)
        def _(j):
            at = tiles(j, tile)
            x = rows[...]
            keep(at, dot(x, gate[:, at]), dot(x, up[:, at]))

        last = dot(rows[...], tail[...])
        keep(pl.ds(whole * tile, half), last[:, :half], last[:, half:])

        gather.relay(s + 2)

        @pl.when(s + 1 < levels)
        def _():
            gather.pass_on(pick_from(order, z, s + 1))

        @pl.when(s == levels - 3)
        def _():
            behind.first()
            behind2.first()

        @pl.when(s >= levels - 2)
        def _():
            @pl.when(s == levels - 2)
            def _():
                behind2.turn()

            behind.relay(s - levels + 3)
            behind2.relay(s - levels + 3)
            behind.pass_on(pick_from(order, z, s - levels + 2))

        @pl.loop(0, width // wide)
        def _(j):
            at = tiles(j, wide)
            eo_st[n, :, at] = dot(acts[...], down[:, at]).astype(BF16)

        @pl.loop(0, group // 2)
        def _(h):
            x = xs[pl.ds(k * group + 2 * h, 2)].reshape(-1, width)
            pre = dot(x, own[...])
            sh_st[n, pl.ds(2 * h, 2)] = pre.astype(BF16).reshape(2, -1, 2 * units)
            act = (silu_parts(pre[:, :units])[0] * pre[:, units:]).astype(BF16)
            sacts[pl.ds(2 * h, 2)] = act.reshape(2, -1, units)

        @pl.loop(0, group)
        def _(b):
            i = k * group + b
            pick = picks(rank_ref[i, 0:1, :], slots)
            back = picks_back(back_ref[i], slots).astype(BF16)
            g = jnp.sum(jnp.where(pick, probs[i, 0:1, :], 0.0), axis=1, keepdims=True)
            act = sacts[b]
            for j in range(width // wide):
                at = slice(j * wide, (j + 1) * wide)
                weighted = (g * eo_st[n, tiles(b, slots), at].astype(F32)).astype(BF16)
                part_st[n, b, :, at] = (dot(back, weighted) + dot(act, sdown[:, at])).astype(BF16)

        for copy in stores(s, k):
            copy.start()

    @pl.loop(2, levels)
    def _(s):
        behind.relay(s + 1)
        behind2.relay(s + 1)
        behind.pass_on(pick_from(order, z, s))

    @pl.loop(levels - 2, levels)
    def _(s):
        for copy in stores(s, pick_from(order, z, s)):
            copy.wait()

    @pl.loop(0, levels)
    def _(k):
        behind.take_twin(k)
        behind2.take_twin(k)

    for copy in own_c:
        copy.wait()
    gather.finish()
    behind.finish()
    behind2.finish()


def experts_forward(x, prob, c, c2, rank, back, gate, up, down, own, sdown, slots, members, collective_id):
    tokens, width = x.shape
    hidden = gate.shape[1]
    group = SIDE * CORES
    levels = members // group
    packed = group * slots
    anywhere = pl.BlockSpec(memory_space=pl.ANY)
    vmem = pl.BlockSpec(memory_space=pltpu.VMEM)
    sem = pltpu.SemaphoreType.DMA
    tile = 256
    shapes = [
        (levels, group, tokens, width),
        (levels, packed, hidden),
        (levels, packed, hidden),
        (levels, packed, width),
        (levels, group, tokens, own.shape[1]),
    ]
    return pl.pallas_call(
        functools.partial(experts_kernel, members=members, slots=slots, tile=tile, wide=512),
        in_specs=[anywhere] * 4 + [vmem, vmem] + [anywhere] * 5,
        out_specs=[anywhere] * 7 + [vmem],
        out_shape=[jax.ShapeDtypeStruct(s, BF16) for s in shapes]
        + [jax.ShapeDtypeStruct((members, *a.shape), BF16) for a in (c, c2)]
        + [jax.ShapeDtypeStruct(prob.shape, F32)],
        scratch_shapes=[
            pltpu.VMEM((members, tokens, width), BF16),
            pltpu.VMEM(prob.shape, F32),
            pltpu.VMEM(gate.shape, BF16),
            pltpu.VMEM(up.shape, BF16),
            pltpu.VMEM(down.shape, BF16),
            pltpu.VMEM(own.shape, BF16),
            pltpu.VMEM(sdown.shape, BF16),
            pltpu.VMEM((width, tile), BF16),
            pltpu.VMEM((packed, width), BF16),
            pltpu.VMEM((packed, hidden), BF16),
            pltpu.VMEM((group, tokens, own.shape[1] // 2), BF16),
        ]
        + [pltpu.VMEM((2, *s[1:]), BF16) for s in shapes]
        + [pltpu.VMEM(c.shape, BF16), pltpu.VMEM(c2.shape, BF16)]
        + [sem((6, members)), sem((2, members)), sem((members,)), sem((members,))]
        + [sem((6, members)), sem((2, members))] * 2
        + [sem((9,)), sem((2, 5))],
        compiler_params=pltpu.CompilerParams(
            collective_id=collective_id, has_side_effects=True, vmem_limit_bytes=63 * 1024 * 1024
        ),
        cost_estimate=pl.CostEstimate(
            flops=12 * members * slots * width * hidden, bytes_accessed=60_000_000, transcendentals=0
        ),
        name="experts_forward",
    )(x, prob, c, c2, rank, back, gate, up, down, own, sdown)


def experts_back_kernel(
    c_hbm, c2_hbm, c3_hbm, rank_ref, back_ref, prob_ref, eg_hbm, eu_hbm, eo_hbm, sh_hbm, gate_hbm, up_hbm, down_hbm, own_hbm, sdown_hbm,
    out, dg_out,
    part, cs, eg, eu, eo, sh, gate, up, down, own, sdown, rows, d_gate, d_up, dg_st, dg_in,
    *sems, members, slots, tile, wide
):
    twin_in, side_in, line_in = sems[:3]
    e_sent, e_got, load, fetch = sems[11:15]
    me = lax.axis_index("grp")
    levels = members // (SIDE * CORES)
    group = SIDE * CORES
    width, hidden = gate.shape
    half, whole = hidden % tile, hidden // tile
    units = own.shape[1] // 2
    z = me // group
    order = far_first(levels)
    reduce = Reduce(part, twin_in, side_in, line_in, sems[3:11], members)
    exchange = Exchange(dg_st, dg_in, e_sent, e_got, members)

    def cotangents(s):
        k = pick_from(order, z, s)
        return [
            pltpu.make_async_copy(
                a.at[k], cs.at[s % 2, :, :, pl.ds(at, a.shape[3])], fetch.at[4 + s % 2 * 3 + h]
            )
            for h, (a, at) in enumerate([(c_hbm, 0), (c2_hbm, width // 2), (c3_hbm, width // 2 + c2_hbm.shape[3])])
        ]

    def kept(s):
        k = pick_from(order, z, s)
        return [
            pltpu.make_async_copy(a.at[k], b, fetch.at[m])
            for m, (a, b) in enumerate([(eo_hbm, eo), (eg_hbm, eg), (eu_hbm, eu), (sh_hbm, sh)])
        ]

    loads = [
        pltpu.make_async_copy(a, b, load.at[n])
        for n, (a, b) in enumerate(
            [(down_hbm, down), (gate_hbm, gate), (up_hbm, up), (own_hbm, own), (sdown_hbm, sdown)]
        )
    ]
    for copy in cotangents(0) + kept(0):
        copy.start()
    for copy in loads:
        copy.start()
    meet(members)

    def early(s):
        return (z == 0) | (z == levels - 1)

    @pl.loop(0, levels)
    def _(s):
        k = pick_from(order, z, s)
        n = s % 2
        for copy in cotangents(s):
            copy.wait()
        load_eo, load_eg, load_eu, load_sh = kept(s)

        @pl.when(s + 1 < levels)
        def _():
            for copy in cotangents(s + 1):
                copy.start()

        load_eo.wait()
        @pl.loop(0, group)
        def _(b):
            i = k * group + b
            at = tiles(b, slots)
            pick = picks(rank_ref[i, 0:1, :], slots)
            c = dot(pick.astype(BF16), cs[n, b])
            g = jnp.sum(jnp.where(pick, prob_ref[i, 0:1, :], 0.0), axis=1, keepdims=True)
            along = jnp.sum(c * eo[at, :].astype(F32), axis=1, keepdims=True)
            dg_st[i] = jnp.broadcast_to(
                jnp.sum(jnp.where(pick, along, 0.0), axis=0, keepdims=True), dg_st.shape[1:]
            )
            rows[at, :] = (g * c).astype(BF16)

        @pl.when(s == 0)
        def _():
            for copy in loads:
                copy.wait()

        load_eg.wait()
        load_eu.wait()

        def slopes(at):
            d = dot_t(rows[...], down[at, :])
            act, slope = silu_parts(eg[:, at].astype(F32))
            d_gate[:, at] = (d * eu[:, at].astype(F32) * slope).astype(BF16)
            d_up[:, at] = (d * act).astype(BF16)

        @pl.loop(0, whole)
        def _(j):
            slopes(tiles(j, tile))

        slopes(pl.ds(whole * tile, half))

        @pl.when(s >= 1)
        def _():
            reduce.chip(pick_from(order, z, s - 1))

        @pl.when((s >= 2) & ~early(s))
        def _():
            reduce.line(pick_from(order, z, s - 2))

        @pl.loop(0, width // tile)
        def _(j):
            at = tiles(j, tile)
            eo[:, at] = (dot_t(d_gate[...], gate[at, :]) + dot_t(d_up[...], up[at, :])).astype(BF16)

        load_sh.wait()
        @pl.loop(0, group)
        def _(b):
            i = k * group + b
            back = picks_back(back_ref[i], slots).astype(BF16)
            d = dot_t(cs[n, b], sdown[...])
            pre = sh[b].astype(F32)
            act, slope = silu_parts(pre[:, :units])
            both = jnp.concatenate([d * pre[:, units:] * slope, d * act], axis=1).astype(BF16)
            for j in range(width // wide):
                at = slice(j * wide, (j + 1) * wide)
                part[i, :, at] = (
                    dot(back, eo[tiles(b, slots), at]) + dot_t(both, own[at, :])
                ).astype(BF16)

        reduce.start(k)

        @pl.when(s + 1 < levels)
        def _():
            for copy in kept(s + 1):
                copy.start()

        @pl.when((s >= 1) & early(s))
        def _():
            reduce.line(pick_from(order, z, s - 1))

    exchange.start()
    dg_in[me] = dg_st[me]
    reduce.chip(z)

    @pl.when(~early(0))
    def _():
        reduce.line(pick_from(order, z, levels - 2))

    reduce.last(out)
    reduce.finish()
    exchange.wait()
    dg_out[...] = dg_in[...]


def experts_backward(cs, rank, back, prob, kept, gate, up, down, own, sdown, slots, members, collective_id):
    tokens, width = cs[0].shape[1], sum(c.shape[2] for c in cs)
    hidden = gate.shape[1]
    group = SIDE * CORES
    levels = members // group
    packed = group * slots
    anywhere = pl.BlockSpec(memory_space=pl.ANY)
    vmem = pl.BlockSpec(memory_space=pltpu.VMEM)
    sem = pltpu.SemaphoreType.DMA
    eg, eu, eo, sh = kept
    return pl.pallas_call(
        functools.partial(experts_back_kernel, members=members, slots=slots, tile=256, wide=512),
        in_specs=[anywhere] * 3 + [vmem] * 3 + [anywhere] * 9,
        out_specs=[vmem, vmem],
        out_shape=[
            jax.ShapeDtypeStruct((tokens, width), BF16),
            jax.ShapeDtypeStruct((members, 8, tokens), F32),
        ],
        scratch_shapes=[
            pltpu.VMEM((members, tokens, width), BF16),
            pltpu.VMEM((2, group, tokens, width), BF16),
            pltpu.VMEM(eg.shape[1:], BF16),
            pltpu.VMEM(eu.shape[1:], BF16),
            pltpu.VMEM(eo.shape[1:], BF16),
            pltpu.VMEM(sh.shape[1:], BF16),
            pltpu.VMEM(gate.shape, BF16),
            pltpu.VMEM(up.shape, BF16),
            pltpu.VMEM(down.shape, BF16),
            pltpu.VMEM(own.shape, BF16),
            pltpu.VMEM(sdown.shape, BF16),
            pltpu.VMEM((packed, width), BF16),
            pltpu.VMEM((packed, hidden), BF16),
            pltpu.VMEM((packed, hidden), BF16),
            pltpu.VMEM((members, 8, tokens), F32),
            pltpu.VMEM((members, 8, tokens), F32),
        ]
        + Reduce.scratch(members, tokens, width, BF16)
        + [sem((members,)), sem((members,)), sem((5,)), sem((10,))],
        compiler_params=pltpu.CompilerParams(
            collective_id=collective_id, has_side_effects=True, vmem_limit_bytes=67_043_328
        ),
        cost_estimate=pl.CostEstimate(
            flops=12 * members * slots * width * hidden, bytes_accessed=60_000_000, transcendentals=0
        ),
        name="experts_backward",
    )(*(c.reshape(levels, group, tokens, -1) for c in cs), rank, back, prob, *kept, gate, up, down, own, sdown)


class Spread:
    def __init__(self, src, out, common, commons, sems, members, sequences):
        self.src, self.out, self.common, self.commons = src, out, common, commons
        self.sent, self.got, self.sent2, self.got2 = sems
        self.members, self.sequences = members, sequences
        self.me, self.mine = lax.axis_index("grp"), lax.axis_index("rep")

    def other(self, n):
        r = lax.rem(self.mine + n // self.members, self.sequences)
        return {"rep": r, "grp": lax.rem(self.me + n % self.members, self.members)}

    def meet(self):
        barrier = pltpu.get_barrier_semaphore()
        count = self.members * self.sequences

        @pl.loop(1, count)
        def _(n):
            pl.semaphore_signal(barrier, 1, device_id=self.other(n), device_id_type=MESH)

        pl.semaphore_wait(barrier, count - 1)

    def block(self, n):
        to = self.other(n)
        return send(self.src.at[to["grp"]], self.out.at[self.mine, self.me], self.sent.at[n], self.got.at[n], to)

    def whole(self, n):
        return send(self.common, self.commons.at[self.mine], self.sent2.at[n], self.got2.at[n], self.other(n * self.members))

    def start_blocks(self):
        @pl.loop(1, self.members * self.sequences)
        def _(n):
            self.block(n).start()

    def start_common(self):
        @pl.loop(1, self.sequences)
        def _(n):
            self.whole(n).start()

    def wait(self):
        @pl.loop(1, self.members * self.sequences)
        def _(n):
            self.block(n).wait()

        @pl.loop(1, self.sequences)
        def _(n):
            self.whole(n).wait()


def finish_kernel(
    part, o_src, dq_ref, cos_ref, sin_ref, q_hbm, kva_ref, up_ref, down_ref, small_ref, normed_ref, latent_ref, kvg_ref,
    x_ref, xg_ref, dmid_ref, name_ref,
    out, gqd, gqu, god, gou,
    *bufs, members, sequences
):
    twin_in, side_in, line_in = bufs[:3]
    o_in, o_common, q_parts, d_query, wq, dn, d_lat, d_latent, ds_ref, q_out, o_out = bufs[11:22]
    o_sent, o_got, b_sent, b_got, w_sent, w_got, local = bufs[22:]
    reduce = Reduce(part, twin_in, side_in, line_in, bufs[3:11], members)
    exchange = Exchange(o_src, o_in, o_sent, o_got, members)
    spread = Spread(q_parts, q_out, o_common, o_out, (b_sent, b_got, w_sent, w_got), members, sequences)
    me, mine = spread.me, spread.mine
    order = far_first(reduce.levels)
    z, levels = reduce.z, reduce.levels
    tokens, width = x_ref.shape
    tile = 256
    load = pltpu.make_async_copy(q_hbm, wq, local.at[0])
    load.start()
    spread.meet()

    @pl.loop(0, levels)
    def _(s):
        reduce.start(pick_from(order, z, s))

    exchange.start()
    o_in[me] = o_src[me]
    cosine, sine = cos_ref[...], sin_ref[...]
    half = ROPE // 2
    for pair in range(dq_ref.shape[0] // 2):
        pieces = []
        for h in (2 * pair, 2 * pair + 1):
            rope = jnp.concatenate([dq_ref[h, tokens:, :ROPE], dq_ref[h, tokens:, ROPE:]], axis=0).astype(F32)
            turned = jnp.concatenate([rope[:, half:], rope[:, :half]], axis=1)
            pieces += [dq_ref[h, :tokens, :], (rope * cosine + turned * sine).astype(BF16)]
        d_query[:, pair * 2 * QK : (pair + 1) * 2 * QK] = jnp.concatenate(pieces, axis=1)

    @pl.loop(0, levels)
    def _(s):
        reduce.chip(pick_from(order, z, s))

    grad_up = t_dot(small_ref[...], d_query[...])
    ds_ref[...] = dot_t(d_query[...], up_ref[...]).astype(BF16)
    grad_down = t_dot(ds_ref[...], normed_ref[...])
    rows = width // members
    for g in range(members):
        first = g // 2 * 2 * QK
        q_parts[g] = jnp.concatenate(
            [grad_down[:, g * rows : (g + 1) * rows], grad_up[:, first : first + 2 * QK]], axis=1
        ).astype(BF16)
    spread.start_blocks()
    q_out[mine, me] = q_parts[me]
    exchange.wait()
    total = jnp.zeros(o_in.shape[1:], F32)
    for g in range(members):
        total = total + o_in[g].astype(F32)
    o_common[...] = jnp.concatenate([total, name_ref[...]], axis=1)
    spread.start_common()
    o_out[mine] = o_common[...]
    load.wait()
    every = width // tile // (levels - 1)

    @pl.loop(0, width // tile)
    def _(j):
        dn[:, tiles(j, tile)] = dot_t(d_query[...], wq[pl.ds(j * (tile // rows), tile // rows)].reshape(tile, -1))

        @pl.when((j % every == every - 1) & (j // every < levels - 1))
        def _():
            reduce.line(pick_from(order, z, j // every))

    reduce.last(d_lat)
    gradient = d_lat[...].astype(F32)
    latent = latent_ref[...]
    d_latent[:, :KVR] = norm_back(latent[:, :KVR], kvg_ref[...], gradient[:, :KVR]).astype(BF16)
    rope = gradient[:, KVR:]
    turned = jnp.concatenate([rope[:, half:], rope[:, :half]], axis=1)
    d_latent[:, KVR:] = (rope * cosine + turned * sine).astype(BF16)

    @pl.loop(0, width // tile)
    def _(j):
        at = tiles(j, tile)
        dn[:, at] += dot_t(d_latent[...], kva_ref[at, :]) + dot_t(ds_ref[...], down_ref[at, :])

    out[...] = (dmid_ref[...] + norm_back(x_ref[...].astype(F32), xg_ref[...], dn[...])).astype(BF16)
    reduce.finish()
    spread.wait()
    o_cols = gou.shape[2]
    shares = []
    for r in range(sequences):
        q_share = lax.fori_loop(
            0, members, lambda g, total: total + q_out[r, g].astype(F32), jnp.zeros(q_out.shape[2:], F32)
        )
        up_share = jnp.where(me % 2 == 0, q_share[:, rows : rows + QK], q_share[:, rows + QK :])
        o_share = o_out[r]
        number = o_share[:, 2 * o_cols : 2 * o_cols + 1]
        shares.append((number, q_share[:, :rows], up_share, o_share[:, :o_cols], o_share[:, o_cols : 2 * o_cols]))
    for a in range(gqd.shape[0]):
        sums = [jnp.zeros(part.shape, F32) for part in shares[0][1:]]
        for number, *parts in shares:
            chosen = number == a
            sums = [total + jnp.where(chosen, part, 0.0) for total, part in zip(sums, parts)]
        for ref, total in zip((gqd, gqu, god, gou), sums):
            ref[a] = total


def finish(part, o_parts, dq, cosine, sine, all_q, kva, up, down, small, normed, latent, kvg, x, xg, dmid, name, adapters, sequences, collective_id):
    members, tokens, c = part.shape
    width = x.shape[1]
    rank = o_parts.shape[1]
    vmem = pl.BlockSpec(memory_space=pltpu.VMEM)
    anywhere = pl.BlockSpec(memory_space=pl.ANY)
    sem = pltpu.SemaphoreType.DMA
    share = width // members + 2 * QK
    common = (rank, o_parts.shape[2] + name.shape[1])
    return pl.pallas_call(
        functools.partial(finish_kernel, members=members, sequences=sequences),
        in_specs=[vmem] * 5 + [anywhere] + [vmem] * 11,
        out_specs=[vmem] * 5,
        out_shape=[jax.ShapeDtypeStruct((tokens, width), BF16)]
        + [
            jax.ShapeDtypeStruct((adapters, rank, n), F32)
            for n in (width // members, QK, o_parts.shape[2] // 2, o_parts.shape[2] // 2)
        ],
        scratch_shapes=Reduce.scratch(members, tokens, c, BF16)
        + [
            pltpu.VMEM(o_parts.shape, BF16),
            pltpu.VMEM(common, F32),
            pltpu.VMEM((members, rank, share), BF16),
            pltpu.VMEM((tokens, H * QK), BF16),
            pltpu.VMEM(all_q.shape, BF16),
            pltpu.VMEM((tokens, width), F32),
            pltpu.VMEM((tokens, c), BF16),
            pltpu.VMEM((tokens, c), BF16),
            pltpu.VMEM((tokens, rank), BF16),
            pltpu.VMEM((sequences, members, rank, share), BF16),
            pltpu.VMEM((sequences, *common), F32),
        ]
        + [sem((n,)) for n in (members,) * 2 + (members * sequences,) * 2 + (sequences,) * 2 + (3,)],
        compiler_params=pltpu.CompilerParams(
            collective_id=collective_id, has_side_effects=True, vmem_limit_bytes=56 * 1024 * 1024
        ),
        cost_estimate=pl.CostEstimate(flops=4 * tokens * width * H * QK, bytes_accessed=40_000_000, transcendentals=0),
        name="finish",
    )(part, o_parts, dq, cosine, sine, all_q, kva, up, down, small, normed, latent, kvg, x, xg, dmid, name)


def by_owner(gradient, members):
    return gradient.astype(BF16).reshape(gradient.shape[0], members, -1).transpose(1, 0, 2)


def per_device(
    hidden,
    grad_out,
    expert_ids,
    prefix_len,
    adapter_id,
    attn_gain,
    kv_gain,
    ffn_gain,
    w_q,
    w_kva,
    w_kvb,
    w_o,
    w_router,
    shared_gate,
    shared_up,
    shared_down,
    expert_gate,
    expert_up_weight,
    expert_down,
    q_down,
    q_up,
    o_down,
    o_up,
):
    tokens = hidden.shape[1]
    width = hidden.shape[2]
    members = lax.axis_size("grp")
    length = tokens * members
    experts = expert_gate.shape[0] * members
    capacity = tokens * TOP * 5 // (4 * experts)
    slots = -(-capacity // 16) * 16
    me = lax.axis_index("grp")

    inputs = hidden[0].astype(F32)
    cotangent = grad_out[0]
    c32 = cotangent.astype(F32)
    routes = expert_ids[0]
    adapter = adapter_id[0]
    pick = lambda table: lax.dynamic_index_in_dim(table, adapter, 0, keepdims=False)
    qa_down, qa_up, oa_down, oa_up = pick(q_down), pick(q_up), pick(o_down), pick(o_up)

    chosen_by = jnp.sum(
        (routes[:, :, None] == jnp.arange(experts, dtype=jnp.int32)[None, None, :]).astype(F32), axis=1
    )
    sequences = lax.axis_size("rep")
    split = w_q.shape[0] * 3 // 128 * 16 if sequences % 2 == 0 else 0
    positions = me * tokens + jnp.arange(tokens, dtype=jnp.int32)
    cosine, sine = angles(positions, ROPE)
    normed = root_norm(inputs, attn_gain).astype(BF16)
    cosine2 = jnp.concatenate([cosine, cosine], axis=1)
    sine2 = jnp.concatenate([sine, -sine], axis=1)
    (
        all_kva, all_q, all_o, all_router, all_latent, q_packed, kvb_parts, chosen_all, own_shared, latent, q_small
    ) = opening(
        w_kva,
        w_q,
        w_o,
        w_router,
        jnp.broadcast_to(chosen_by.T[:, None, :], (experts, 8, tokens)),
        w_kvb,
        shared_gate,
        shared_up,
        normed,
        qa_down,
        qa_up,
        cosine2,
        sine2,
        kv_gain[None],
        members,
        split,
        1,
    )
    full_kva, full_o, full_router = (v.reshape(-1, v.shape[2]) for v in (all_kva, all_o, all_router))
    own_kvb = kvb_parts.reshape(KVR, -1)
    own_shared = own_shared.reshape(width, -1)
    q_packed, c_first = lax.optimization_barrier((q_packed, cotangent[:, : width // 2]))
    mixture, lse, q_head, k_head, v_head, mixed_parts = attend(prefix_len, q_packed, all_latent, own_kvb, members, 3)
    mixed = mixed_parts.transpose(1, 0, 2).reshape(tokens, H * VD)
    o_small = dot(mixed, oa_down).astype(BF16)
    middle = inputs + dot(mixed, full_o) + dot(o_small, oa_up)
    ffn_in = root_norm(middle, ffn_gain).astype(BF16)
    route_probs = jax.nn.softmax(dot(ffn_in, full_router), axis=-1)

    half = width // 2
    first_c = gather(c_first).reshape(members, tokens, half)
    chosen = chosen_all[:, 0] > 0.5
    order = jnp.arange(tokens, dtype=jnp.int32)
    before = (order[:, None] < order[None, :]).astype(BF16)
    rank = jnp.where(chosen, dot(chosen.astype(BF16), before), -1.0)
    back = rank[:, :, None]
    rank = jnp.broadcast_to(rank[:, None, :], (members, 8, tokens))
    weights = (expert_gate[0], expert_up_weight[0], expert_down[0], own_shared, shared_down)
    prob_blocks = jnp.broadcast_to(route_probs.T[:, None, :], (experts, 8, tokens))
    partial, kept_gate, kept_up, kept_out, kept_shared, second_c, third_c, prob_parts = experts_forward(
        ffn_in, prob_blocks, cotangent[:, half : half + half // 2], cotangent[:, half + half // 2 :], rank, back, *weights, slots, members, 4
    )
    kept = (kept_gate, kept_up, kept_out, kept_shared)
    ffn_out = scatter_sum(partial.reshape(length, width))
    d_own, d_route = experts_backward(
        (first_c, second_c, third_c), rank, back, prob_parts, kept, *weights, slots, members, 5
    )
    d_route = d_route[:, 0].T
    d_logits = (
        route_probs * (d_route - jnp.sum(route_probs * d_route, axis=-1, keepdims=True))
    ).astype(BF16)
    d_ffn = d_own.astype(F32) + dot_t(d_logits, full_router)
    d_middle = c32 + norm_back(middle, ffn_gain, d_ffn)
    d_attn = d_middle.astype(BF16)
    grad_oup = t_dot(o_small, d_attn)
    d_osmall = dot_t(d_attn, oa_up).astype(BF16)
    grad_odown = t_dot(d_osmall, mixed)
    d_mixed = (dot_t(d_attn, full_o) + dot_t(d_osmall, oa_down)).astype(BF16)
    d_latents, d_query = attend_back(
        prefix_len,
        q_head,
        k_head,
        v_head,
        mixture,
        lse.reshape(members // 2, 1, 2 * tokens),
        d_mixed.reshape(tokens, H, VD).transpose(1, 0, 2),
        own_kvb,
        members,
        6,
    )
    o_parts = jnp.concatenate([by_owner(g, members) for g in (grad_odown, grad_oup)], axis=-1)
    name = jnp.broadcast_to(adapter.astype(F32), (qa_up.shape[0], 128))
    grad_inputs, *outs = finish(
        d_latents,
        o_parts,
        d_query,
        cosine2,
        sine2,
        all_q,
        full_kva,
        qa_up,
        qa_down,
        q_small,
        normed,
        latent,
        kv_gain[None],
        hidden[0],
        attn_gain[None],
        d_middle,
        name,
        q_down.shape[0],
        sequences,
        7,
    )
    ffn_out, _ = lax.optimization_barrier((ffn_out, d_query))
    output = (middle + ffn_out.astype(F32)).astype(BF16)
    return (
        output[None],
        grad_inputs[None],
        outs[0].transpose(0, 2, 1),
        outs[1],
        outs[2].transpose(0, 2, 1),
        outs[3],
    )


def solution(mesh):
    seq = P("rep", "grp", None)
    rows = P("grp", None)
    in_specs = (
        (seq, seq, seq, P("rep"), P("rep"), P(), P(), P())
        + (rows,) * 8
        + (P("grp", None, None),) * 3
        + (P(),) * 4
    )
    out_specs = (
        seq,
        seq,
        P(None, "grp", None),
        P(None, None, "grp"),
        P(None, "grp", None),
        P(None, None, "grp"),
    )
    return jax.shard_map(
        per_device, mesh=mesh, in_specs=in_specs, out_specs=out_specs, check_vma=False
    )
```

```python
import functools
import math

import jax
import jax.numpy as jnp
from jax import lax
from jax.experimental import pallas as pl
from jax.experimental.pallas import tpu as pltpu
from jax.sharding import PartitionSpec as P

H = 16
NOPE = 128
ROPE = 64
VD = 128
KVR = 512
TOP = 6
QK = NOPE + ROPE
EPS = 1e-06
F32 = jnp.float32
BF16 = jnp.bfloat16


def dot(former, latter):
    return jnp.dot(former, latter, preferred_element_type=F32)


def dot_t(former, latter):
    return lax.dot_general(
        former, latter, (((1,), (1,)), ((), ())), preferred_element_type=F32
    )


def t_dot(former, latter):
    return lax.dot_general(
        former, latter, (((0,), (0,)), ((), ())), preferred_element_type=F32
    )


def root_norm(v, gains):
    factor = lax.rsqrt(jnp.mean(v * v, axis=-1, keepdims=True) + EPS)
    return v * factor * gains


def norm_back(v, gains, gradient):
    factor = lax.rsqrt(jnp.mean(v * v, axis=-1, keepdims=True) + EPS)
    weighted = gradient * gains
    return factor * weighted - v * (factor * factor * factor) * jnp.mean(
        weighted * v, axis=-1, keepdims=True
    )


def angles(positions, width):
    frequency = 10000.0 ** (-jnp.arange(0, width, 2, dtype=F32) / width)
    phases = positions.astype(F32)[:, None] * frequency[None, :]
    return (jnp.cos(phases), jnp.sin(phases))


def rotate(v, cosine, sine):
    half = v.shape[-1] // 2
    a, b = v[..., :half], v[..., half:]
    return jnp.concatenate([a * cosine - b * sine, b * cosine + a * sine], axis=-1)


def unrotate(v, cosine, sine):
    half = v.shape[-1] // 2
    a, b = v[..., :half], v[..., half:]
    return jnp.concatenate([a * cosine + b * sine, b * cosine - a * sine], axis=-1)


SIDE = 2
CORES = 2
MESH = pl.DeviceIdType.MESH


def place_of():
    me = lax.axis_index("grp")
    return me // (SIDE * CORES), (me // CORES) % SIDE, me % CORES


def index_of(z, x, c):
    return (z * SIDE + x) * CORES + c


def send(src, dst, sent, got, to):
    return pltpu.make_async_remote_copy(
        src_ref=src,
        dst_ref=dst,
        send_sem=sent,
        recv_sem=got,
        device_id=to if isinstance(to, dict) else {"grp": to},
        device_id_type=MESH,
    )


def meet(members, partner=None):
    barrier = pltpu.get_barrier_semaphore()
    me = lax.axis_index("grp")

    @pl.loop(1, members)
    def _(d):
        pl.semaphore_signal(barrier, 1, device_id={"grp": lax.rem(me + d, members)}, device_id_type=MESH)

    if partner is not None:
        pl.semaphore_signal(barrier, 1, device_id=partner, device_id_type=MESH)
    pl.semaphore_wait(barrier, members - 1 + (partner is not None))


def pick_from(table, z, s):
    v = 0
    for i, row in enumerate(table):
        for j, entry in enumerate(row):
            if entry:
                v = v + jnp.where((z == i) & (s == j), entry, 0)
    return v


def near_first(levels):
    return [sorted(range(levels), key=lambda v: (abs(v - k), v)) for k in range(levels)]


def far_first(levels):
    return [sorted((v for v in range(levels) if v != k), key=lambda v: (-abs(v - k), v)) + [k] for k in range(levels)]


class Gather:
    def __init__(self, src, out, sent, got, members, split=0):
        self.src, self.out, self.sent, self.got = src, out, sent, got
        self.members, self.split = members, split
        self.levels = members // (SIDE * CORES)
        self.z, self.x, self.c = z, x, c = place_of()
        self.me = lax.axis_index("grp")
        self.up, self.down = index_of(z + 1, x, c), index_of(z - 1, x, c)
        self.side, self.twin = index_of(z, 1 - x, c), index_of(z, x, 1 - c)
        if split:
            rows = src.shape[0]
            rep = lax.axis_index("rep")
            odd = rep % 2
            self.partner = {"rep": rep + 1 - 2 * odd, "grp": self.me}
            self.window = pl.ds(pl.multiple_of(odd * split, 16), rows - split)
            self.given = pl.ds(pl.multiple_of(odd * (rows - split), 16), split)
            self.lacked = pl.ds(pl.multiple_of((1 - odd) * (rows - split), 16), split)

    def copy(self, slot, kind, to, own=False, rows=None):
        rows = rows or (self.window if self.split else None)
        other = rows is not None and self.split and rows is not self.window
        src = self.src if own else self.out.at[slot]
        dst = self.out.at[slot]
        if rows is not None:
            src, dst = src.at[rows], dst.at[rows]
        return send(src, dst, self.sent.at[kind, slot], self.got.at[int(bool(other)), slot], to)

    def arrive(self, slot):
        self.copy(slot, 0, self.twin).wait_recv()

    def to_partner(self, slot):
        return self.copy(slot, 4, self.partner, rows=self.given)

    def lacked_to_twin(self, slot, own=False):
        return self.copy(slot, 5, self.twin, own, rows=self.lacked)

    def first(self):
        @pl.when(self.z < self.levels - 1)
        def _():
            self.copy(self.me, 0, self.up, True).start()

        @pl.when(self.z > 0)
        def _():
            self.copy(self.me, 1, self.down, True).start()

        self.copy(self.me, 2, self.side, True).start()
        self.copy(self.me, 3, self.twin, True).start()
        if self.split:
            self.lacked_to_twin(self.me, True).start()

    def relay(self, s):
        @pl.when(self.z >= s)
        def _():
            slot = index_of(self.z - s, self.x, self.c)
            self.arrive(slot)

            @pl.when(self.z < self.levels - 1)
            def _():
                self.copy(slot, 0, self.up).start()

            self.spread(slot)

        @pl.when(self.z + s < self.levels)
        def _():
            slot = index_of(self.z + s, self.x, self.c)
            self.arrive(slot)

            @pl.when(self.z > 0)
            def _():
                self.copy(slot, 1, self.down).start()

            self.spread(slot)

    def spread(self, slot):
        self.copy(slot, 2, self.side).start()
        self.copy(slot, 3, self.twin).start()
        if self.split:
            self.to_partner(slot).start()

    def pass_on(self, k):
        slot = index_of(k, 1 - self.x, self.c)
        self.arrive(slot)
        self.copy(slot, 3, self.twin).start()
        if self.split:
            self.to_partner(slot).start()

    def take_lacked(self, k, x):
        slot = index_of(k, x, self.c)

        @pl.when(slot != self.me)
        def _():
            self.copy(slot, 4, self.partner, rows=self.lacked).wait_recv()
            self.lacked_to_twin(slot).start()

    def take_twin(self, k):
        for x in range(SIDE):
            self.arrive(index_of(k, x, 1 - self.c))

    def take_twin_lacked(self):
        @pl.loop(0, self.members // CORES)
        def _(i):
            self.lacked_to_twin(i * CORES + 1 - self.c).wait_recv()

    def finish(self):
        @pl.loop(0, self.levels)
        def _(k):
            slot = index_of(k, self.x, self.c)
            self.copy(slot, 2, self.side).wait_send()

            @pl.when((k <= self.z) & (self.z < self.levels - 1))
            def _():
                self.copy(slot, 0, self.up).wait_send()

            @pl.when((k >= self.z) & (self.z > 0))
            def _():
                self.copy(slot, 1, self.down).wait_send()

        @pl.loop(0, self.members // CORES)
        def _(i):
            slot = i * CORES + self.c
            self.copy(slot, 3, self.twin).wait_send()
            if self.split:
                self.lacked_to_twin(slot).wait_send()

                @pl.when(slot != self.me)
                def _():
                    self.to_partner(slot).wait_send()


class SideFirst(Gather):
    def turn(self):
        slot = index_of(self.z, 1 - self.x, self.c)
        self.arrive(slot)

        @pl.when(self.z < self.levels - 1)
        def _():
            self.copy(slot, 0, self.up).start()

        @pl.when(self.z > 0)
        def _():
            self.copy(slot, 1, self.down).start()

        self.copy(slot, 3, self.twin).start()

    def relay(self, s):
        for x in (self.x, 1 - self.x):

            @pl.when(self.z >= s)
            def _():
                slot = index_of(self.z - s, x, self.c)
                self.arrive(slot)

                @pl.when(self.z < self.levels - 1)
                def _():
                    self.copy(slot, 0, self.up).start()

                self.copy(slot, 3, self.twin).start()

            @pl.when(self.z + s < self.levels)
            def _():
                slot = index_of(self.z + s, x, self.c)
                self.arrive(slot)

                @pl.when(self.z > 0)
                def _():
                    self.copy(slot, 1, self.down).start()

                self.copy(slot, 3, self.twin).start()

    def finish(self):
        self.copy(self.me, 2, self.side).wait_send()

        @pl.loop(0, self.members // CORES)
        def _(i):
            slot = i * CORES + self.c
            k = i // SIDE

            @pl.when((k <= self.z) & (self.z < self.levels - 1))
            def _():
                self.copy(slot, 0, self.up).wait_send()

            @pl.when((k >= self.z) & (self.z > 0))
            def _():
                self.copy(slot, 1, self.down).wait_send()

            self.copy(slot, 3, self.twin).wait_send()


class Exchange:
    def __init__(self, src, out, sent, got, members, halved=False):
        self.src, self.out, self.sent, self.got, self.members = src, out, sent, got, members
        self.me = lax.axis_index("grp")
        self.rows = None
        if halved:
            half = src.shape[1] // 2
            rep = lax.axis_index("rep")
            odd = rep % 2
            self.partner = {"rep": rep + 1 - 2 * odd, "grp": self.me}
            self.rows = pl.ds(pl.multiple_of(odd * half, 16), half)

    def copy(self, d):
        to = lax.rem(self.me + d, self.members)
        src, dst = self.src.at[to], self.out.at[self.me]
        if self.rows is not None:
            src, dst = src.at[self.rows], dst.at[self.rows]
        return send(src, dst, self.sent.at[d], self.got.at[d], to)

    def to_partner(self):
        ours = self.out.at[:, self.rows]
        return send(ours, ours, self.sent.at[0], self.got.at[0], self.partner)

    def start(self):
        @pl.loop(1, self.members)
        def _(d):
            self.copy(d).start()

    def wait(self):
        @pl.loop(1, self.members)
        def _(d):
            self.copy(d).wait()


class Reduce:
    def __init__(self, p, twin_in, side_in, line_in, sems, members):
        self.p, self.twin_in, self.side_in, self.line_in = p, twin_in, side_in, line_in
        self.sems = sems
        self.levels = members // (SIDE * CORES)
        self.z, self.x, self.c = place_of()

    def copy(self, kind, slot, dst, n, to):
        sent, got = self.sems[2 * kind], self.sems[2 * kind + 1]
        return send(self.p.at[slot], dst.at[n], sent.at[n], got.at[n], to)

    def to_twin(self, k, w):
        twin = index_of(self.z, self.x, 1 - self.c)
        return self.copy(0, index_of(k, w, 1 - self.c), self.twin_in, k * SIDE + w, twin)

    def to_side(self, k):
        return self.copy(1, index_of(k, 1 - self.x, self.c), self.side_in, k, index_of(self.z, 1 - self.x, self.c))

    def to_up(self, k):
        return self.copy(2, index_of(k, self.x, self.c), self.line_in, k + 1, index_of(self.z + 1, self.x, self.c))

    def to_down(self, k):
        return self.copy(3, index_of(k, self.x, self.c), self.line_in, k, index_of(self.z - 1, self.x, self.c))

    def add(self, slot, ref):
        rows = self.p.shape[1]
        chunk = next(r for r in (32, 16, 8) if rows % r == 0)

        @pl.loop(0, rows // chunk)
        def _(i):
            at = pl.ds(pl.multiple_of(i * chunk, chunk), chunk)
            self.p[slot, at, :] = (self.p[slot, at, :].astype(F32) + ref[at, :].astype(F32)).astype(self.p.dtype)

    def start(self, k):
        self.to_twin(k, self.x).start()
        self.to_twin(k, 1 - self.x).start()

    def chip(self, k):
        w = 1 - self.x
        self.to_twin(k, w).wait_recv()
        self.add(index_of(k, w, self.c), self.twin_in.at[k * SIDE + w])
        self.to_side(k).start()
        self.to_twin(k, self.x).wait_recv()
        self.add(index_of(k, self.x, self.c), self.twin_in.at[k * SIDE + self.x])

    def line(self, k):
        z, mine = self.z, index_of(k, self.x, self.c)
        self.to_side(k).wait_recv()
        self.add(mine, self.side_in.at[k])

        @pl.when((k > z) & (z > 0))
        def _():
            self.to_up(k).wait_recv()
            self.add(mine, self.line_in.at[k + 1])

        @pl.when((k < z) & (z < self.levels - 1))
        def _():
            self.to_down(k).wait_recv()
            self.add(mine, self.line_in.at[k])

        @pl.when(k > z)
        def _():
            self.to_up(k).start()

        @pl.when(k < z)
        def _():
            self.to_down(k).start()

    def last(self, out):
        z, mine = self.z, index_of(self.z, self.x, self.c)
        self.to_side(z).wait_recv()
        self.add(mine, self.side_in.at[z])

        @pl.when(z > 0)
        def _():
            self.to_up(z).wait_recv()
            self.add(mine, self.line_in.at[z + 1])

        @pl.when(z < self.levels - 1)
        def _():
            self.to_down(z).wait_recv()
            self.add(mine, self.line_in.at[z])

        out[...] = self.p[mine]

    def finish(self):
        z = self.z

        @pl.loop(0, self.levels)
        def _(k):
            self.to_twin(k, 0).wait_send()
            self.to_twin(k, 1).wait_send()
            self.to_side(k).wait_send()

            @pl.when(k > z)
            def _():
                self.to_up(k).wait_send()

            @pl.when(k < z)
            def _():
                self.to_down(k).wait_send()

    @staticmethod
    def scratch(members, r, c, kind):
        levels = members // (SIDE * CORES)
        sem = pltpu.SemaphoreType.DMA
        return [
            pltpu.VMEM((members // CORES, r, c), kind),
            pltpu.VMEM((levels, r, c), kind),
            pltpu.VMEM((levels + 1, r, c), kind),
        ] + [sem((n,)) for n in (members // CORES,) * 2 + (levels,) * 2 + (levels + 1,) * 4]


def gather(v):
    return lax.all_gather(v, "grp", axis=0, tiled=True)


def scatter_sum(v):
    return lax.psum_scatter(v, "grp", scatter_dimension=0, tiled=True)


def after(v, *others):
    return lax.optimization_barrier((v, *others))[0]


def tie(v, other):
    first = other[(0,) * other.ndim]
    return v + jnp.minimum(jnp.abs(first), 0).astype(v.dtype)


def open_kernel(
    kva_src, q_src, o_src, router_src, chosen_src, kvb_ref, sgate_ref, sup_ref,
    normed_ref, down_ref, up_ref, cos_ref, sin_ref, kvg_ref,
    all_kva, all_q, all_o, all_router, all_lat, q_out, kvb_out, chosen_out, shared_out, latent_ref, small_ref,
    *bufs, members, split
):
    stage = bufs[:5]
    kvb_src, shared_src, kva, wq, lat_st, qm = bufs[5:11]
    sems = bufs[11:]
    local, load = sems[26:]
    pairs = [sems[2 * n : 2 * n + 2] for n in range(13)]
    me = lax.axis_index("grp")
    levels = members // (SIDE * CORES)
    z = me // (SIDE * CORES)
    order = near_first(levels)
    tokens, width = normed_ref.shape
    g_kva = Gather(kva_src, all_kva, *pairs[0], members, split)
    g_q = Gather(q_src, all_q, *pairs[1], members, split)
    g_o = Gather(o_src, all_o, *pairs[2], members, o_src.shape[0] // 2 if split else 0)
    g_router = Gather(router_src, all_router, *pairs[3], members)
    g_lat = Gather(lat_st, all_lat, *pairs[4], members)
    e_kvb = Exchange(kvb_src, kvb_out, *pairs[5], members)
    e_chosen = Exchange(chosen_src, chosen_out, *pairs[6], members)
    e_shared = Exchange(shared_src, shared_out, *pairs[7], members, split > 0)
    q_sent, q_got = pairs[8]
    sources = [kva_src, q_src, o_src, router_src, chosen_src.at[me]]
    places = [all_kva, all_q, all_o, all_router, chosen_out]
    into = [pltpu.make_async_copy(a, stage[n], local.at[n]) for n, a in enumerate(sources)]
    out_of = [pltpu.make_async_copy(stage[n], b.at[me], local.at[n]) for n, b in enumerate(places)]
    cut, cut_out = shared_src.at[me], shared_out.at[me]
    if split:
        cut, cut_out = cut.at[e_shared.rows], cut_out.at[e_shared.rows]
    own_cut = [
        pltpu.make_async_copy(kvb_src.at[me], kvb_out.at[me], local.at[5]),
        pltpu.make_async_copy(cut, cut_out, local.at[6]),
    ]
    own_lat = pltpu.make_async_copy(lat_st, all_lat.at[me], local.at[7])
    own_q = pltpu.make_async_copy(qm.at[me], q_out.at[me], local.at[8])
    loads = [pltpu.make_async_copy(all_kva, kva, load.at[0]), pltpu.make_async_copy(all_q, wq, load.at[1])]

    def query_to(n):
        return send(qm.at[n], q_out.at[me], q_sent.at[n], q_got.at[me], n)

    def query_from(n):
        return send(qm.at[n], q_out.at[n], q_sent.at[n], q_got.at[n], n)

    def lacked(g, s):
        if g.split:
            k = pick_from(order, z, s)
            g.take_lacked(k, g.x)
            g.take_lacked(k, 1 - g.x)

    def events(gathers, s, before):
        for g in gathers:
            g.relay(s + 1)
        for g in gathers:
            g.pass_on(pick_from(order, z, s))

        @pl.when(before)
        def _():
            for g in gathers:
                lacked(g, s - 1)

    for copy in into:
        copy.start()
    meet(members, g_kva.partner if split else None)
    for g in (g_kva, g_q, g_router):
        g.first()
    e_chosen.start()
    cols, units = kvb_src.shape[2], shared_src.shape[2] // 2
    for g in range(members):
        kvb_src[g] = kvb_ref[:, g * cols : (g + 1) * cols]
        at = slice(g * units, (g + 1) * units)
        shared_src[g] = jnp.concatenate([sgate_ref[:, at], sup_ref[:, at]], axis=1)
    e_kvb.start()
    for copy in own_cut:
        copy.start()
    for a, b in zip(into, out_of):
        a.wait()
        b.start()

    @pl.loop(0, levels)
    def _(s):
        events((g_kva, g_q, g_router), s, s >= 1)

    lacked(g_kva, levels - 1)
    lacked(g_q, levels - 1)
    g_o.first()
    e_shared.start()
    for g in (g_kva, g_q):

        @pl.loop(0, levels)
        def _(k):
            g.take_twin(k)

        if split:
            g.take_twin_lacked()
    for copy in out_of + own_cut:
        copy.wait()
    for copy in loads:
        copy.start()
    loads[0].wait()
    latent = dot(normed_ref[...], kva[...].reshape(width, -1))
    latent_ref[...] = latent
    half = ROPE // 2

    def turn(v):
        turned = jnp.concatenate([v[:, half:], v[:, :half]], axis=1)
        return (v * cos_ref[...] - turned * sin_ref[...]).astype(BF16)

    lat_st[:, :KVR] = root_norm(latent[:, :KVR], kvg_ref[...]).astype(BF16)
    lat_st[:, KVR:] = turn(latent[:, KVR:])
    g_lat.first()
    own_lat.start()
    small_ref[...] = dot(normed_ref[...], down_ref[...]).astype(BF16)
    loads[1].wait()
    turns = members // 2

    @pl.loop(0, turns)
    def _(n):
        pair = lax.rem(me // 2 + n, turns)
        at = pl.ds(pl.multiple_of(pair * 2 * QK, 128), 2 * QK)
        both = dot(normed_ref[...], wq[:, :, at].reshape(width, 2 * QK)) + dot(small_ref[...], up_ref[:, at])
        for t in range(2):
            to = 2 * pair + t
            r = t * QK
            qm[to, :tokens, :] = both[:, r : r + NOPE].astype(BF16)
            rope = turn(both[:, r + NOPE : r + QK])
            qm[to, tokens:, :ROPE] = rope[: tokens // 2]
            qm[to, tokens:, ROPE:] = rope[tokens // 2 :]

            @pl.when(to == me)
            def _():
                own_q.start()

            @pl.when(to != me)
            def _():
                query_to(to).start()

        @pl.when(n == turns // 2)
        def _():
            events((g_lat, g_o), 0, False)

    @pl.loop(1, levels)
    def _(s):
        events((g_lat, g_o), s, s >= 1)

        @pl.when(s == 1)
        def _():
            e_shared.wait()
            if split:
                e_shared.to_partner().start()

    lacked(g_o, levels - 1)
    for g in (g_lat, g_router, g_o):

        @pl.loop(0, levels)
        def _(k):
            g.take_twin(k)

        if g.split:
            g.take_twin_lacked()
    for g in (g_kva, g_q, g_router, g_lat, g_o):
        g.finish()

    @pl.loop(1, members)
    def _(d):
        n = lax.rem(me + d, members)
        query_from(n).wait_recv()
        query_to(n).wait_send()

    for e in (e_kvb, e_chosen):
        e.wait()
    if split:
        e_shared.to_partner().wait()
    own_lat.wait()
    own_q.wait()


def opening(kva, q, o, router, chosen, kvb, sgate, sup, normed, down, up, cosine, sine, kvg, members, split, collective_id):
    tokens, width = normed.shape
    vmem = pl.BlockSpec(memory_space=pltpu.VMEM)
    anywhere = pl.BlockSpec(memory_space=pl.ANY)
    sem = pltpu.SemaphoreType.DMA
    packed = tokens + tokens // 2
    cut = (members, kvb.shape[0], kvb.shape[1] // members)
    slices = (members, sgate.shape[0], 2 * sgate.shape[1] // members)
    grown = lambda a: jax.ShapeDtypeStruct((members, *a.shape), a.dtype)
    same = lambda a: jax.ShapeDtypeStruct(a.shape, a.dtype)
    g_sems = [sem((6, members)), sem((2, members))]
    e_sems = [sem((members,)), sem((members,))]
    return pl.pallas_call(
        functools.partial(open_kernel, members=members, split=split),
        in_specs=[anywhere] * 5 + [vmem] * 9,
        out_specs=[anywhere] * 9 + [vmem] * 2,
        out_shape=[
            grown(kva), grown(q), grown(o), grown(router),
            jax.ShapeDtypeStruct((members, tokens, kva.shape[1]), BF16),
            jax.ShapeDtypeStruct((members, packed, NOPE), BF16),
            jax.ShapeDtypeStruct(cut, BF16), same(chosen), jax.ShapeDtypeStruct(slices, BF16),
            jax.ShapeDtypeStruct((tokens, kva.shape[1]), F32),
            jax.ShapeDtypeStruct((tokens, down.shape[1]), BF16),
        ],
        scratch_shapes=[pltpu.VMEM(a.shape, a.dtype) for a in (kva, q, o, router)]
        + [
            pltpu.VMEM(chosen.shape[1:], F32),
            pltpu.VMEM(cut, BF16),
            pltpu.VMEM(slices, BF16),
            pltpu.VMEM((members, *kva.shape), BF16),
            pltpu.VMEM((members, *q.shape), BF16),
            pltpu.VMEM((tokens, kva.shape[1]), BF16),
            pltpu.VMEM((members, packed, NOPE), BF16),
        ]
        + g_sems * 5
        + e_sems * 8
        + [sem((9,)), sem((2,))],
        compiler_params=pltpu.CompilerParams(
            collective_id=collective_id, has_side_effects=True, vmem_limit_bytes=48 * 1024 * 1024
        ),
        cost_estimate=pl.CostEstimate(flops=2 * tokens * width * q.shape[1], bytes_accessed=200_000_000, transcendentals=0),
        name="opening",
    )(kva, q, o, router, chosen, kvb, sgate, sup, normed, down, up, cosine, sine, kvg)


def key_blocks(start, rows, keys, length):
    end = start + rows
    end = jnp.where(start < length // 2, jnp.maximum(end, length // 2), end)
    return (start + 1) // keys, (end + keys - 1) // keys


def attend_kernel(
    prefix_ref, packed, lat_ref, kvb_ref, o_ref, lse_ref, q_ref, k_ref, v_ref, mixed, blocks, sent, got, local,
    *, members, unit
):
    me = lax.axis_index("grp")
    tokens = blocks.shape[1]
    block, keys = 2 * tokens, 4 * tokens
    turns = members // 2
    prefix = prefix_ref[0]

    def block_to(n):
        return send(blocks.at[n], mixed.at[me], sent.at[n], got.at[me], n)

    def from_device(n):
        return send(blocks.at[n], mixed.at[n], sent.at[n], got.at[n], n)

    own = pltpu.make_async_copy(blocks.at[me], mixed.at[me], local)
    half = tokens // 2

    @pl.loop(0, members)
    def _(b):
        at = pl.multiple_of(b * tokens, tokens)
        here = pl.ds(at, tokens)
        q_ref[here, :NOPE] = packed[b, :tokens, :]
        q_ref[pl.ds(at, half), NOPE:] = packed[b, tokens:, :ROPE]
        q_ref[pl.ds(at + half, half), NOPE:] = packed[b, tokens:, ROPE:]
        made = dot(lat_ref[b, :, :KVR], kvb_ref[...]).astype(BF16)
        k_ref[here, :NOPE] = made[:, :NOPE]
        k_ref[here, NOPE:] = lat_ref[b, :, KVR:]
        v_ref[here, :] = made[:, NOPE:]

    meet(members)

    @pl.loop(0, turns)
    def _(n):
        i = lax.rem(me // 2 + n, turns)
        start = pl.multiple_of(i * block, block)
        here = pl.ds(start, block)
        q = q_ref[here, :]
        rows = start + lax.broadcasted_iota(jnp.int32, (block, 1), 0)
        limit = jnp.where(rows < prefix, prefix - 1, rows)
        limit = jnp.maximum(limit, rows)

        def step(j, carry, masked):
            top, total, acc = carry
            at = pl.multiple_of(j * keys, keys)
            k = k_ref[pl.ds(at, keys), :]
            v = v_ref[pl.ds(at, keys), :]
            s = dot_t(q, k)
            if masked:
                cols = at + lax.broadcasted_iota(jnp.int32, (1, keys), 1)
                s = jnp.where(cols <= limit, s, -1e30)
            fresh = jnp.maximum(top, jnp.max(s, axis=1, keepdims=True))
            p = jnp.exp2((s - fresh) * unit)
            scale = jnp.exp2((top - fresh) * unit)
            total = total * scale + jnp.sum(p, axis=1, keepdims=True)
            acc = acc * scale + dot(p.astype(BF16), v)
            return fresh, total, acc

        carry = (
            jnp.full((block, 1), -1e30, F32),
            jnp.zeros((block, 1), F32),
            jnp.zeros((block, VD), F32),
        )
        full, stop = key_blocks(start, block, keys, q_ref.shape[0])
        carry = lax.fori_loop(0, full, functools.partial(step, masked=False), carry)
        top, total, acc = lax.fori_loop(full, stop, functools.partial(step, masked=True), carry)
        o = acc / total
        o_ref[here, :] = o
        lse_ref[here, :] = top * unit + jnp.log2(total)
        blocks[pl.ds(2 * i, 2)] = o.astype(BF16).reshape(2, tokens, VD)
        for t in range(2):
            to = 2 * i + t

            @pl.when(to == me)
            def _():
                own.start()

            @pl.when(to != me)
            def _():
                block_to(to).start()

    own.wait()

    @pl.loop(1, members)
    def _(d):
        n = lax.rem(me + d, members)
        from_device(n).wait_recv()
        block_to(n).wait_send()


def attend(prefix, packed, latents, kvb, members, collective_id):
    tokens = latents.shape[1]
    length = tokens * members
    vmem = pl.BlockSpec(memory_space=pltpu.VMEM)
    sem = pltpu.SemaphoreType.DMA
    return pl.pallas_call(
        functools.partial(attend_kernel, members=members, unit=QK**-0.5 * math.log2(math.e)),
        in_specs=[pl.BlockSpec(memory_space=pltpu.SMEM), vmem, vmem, vmem],
        out_specs=[vmem] * 5 + [pl.BlockSpec(memory_space=pl.ANY)],
        out_shape=[
            jax.ShapeDtypeStruct((length, VD), F32),
            jax.ShapeDtypeStruct((length, 1), F32),
            jax.ShapeDtypeStruct((length, QK), BF16),
            jax.ShapeDtypeStruct((length, QK), BF16),
            jax.ShapeDtypeStruct((length, VD), BF16),
            jax.ShapeDtypeStruct((members, tokens, VD), BF16),
        ],
        scratch_shapes=[pltpu.VMEM((members, tokens, VD), BF16), sem((members,)), sem((members,)), sem],
        compiler_params=pltpu.CompilerParams(
            collective_id=collective_id, has_side_effects=True, vmem_limit_bytes=40 * 1024 * 1024
        ),
        cost_estimate=pl.CostEstimate(
            flops=length * length * (QK + VD), bytes_accessed=length * 1000, transcendentals=length * length // 2
        ),
        name="attend",
    )(prefix, packed, latents, kvb)


def attend_back_kernel(
    prefix_ref, q_ref, k_ref, v_ref, o_ref, lse_ref, d_ref, small_ref, down_ref, wo_hbm, kvb_ref, part_ref, dq_out,
    d_src, wo, ds_in, blocks, dk, dv, sent, got, q_sent, q_got, local, local2,
    *, members, factor, unit
):
    me = lax.axis_index("grp")
    tokens = blocks.shape[1] * 2 // 3
    block, keys = 2 * tokens, 4 * tokens
    turns = members // 2
    prefix = prefix_ref[0]
    exchange = Exchange(d_src, ds_in, sent, got, members)
    load = pltpu.make_async_copy(wo_hbm, wo, local)
    own = pltpu.make_async_copy(blocks.at[me], dq_out.at[me], local2)

    def block_to(n):
        return send(blocks.at[n], dq_out.at[me], q_sent.at[n], q_got.at[me], n)

    def from_device(n):
        return send(blocks.at[n], dq_out.at[n], q_sent.at[n], q_got.at[n], n)

    load.start()
    dk[...] = jnp.zeros_like(dk)
    dv[...] = jnp.zeros_like(dv)
    meet(members)
    load.wait()

    @pl.loop(0, turns)
    def _(n):
        pair = lax.rem(me // 2 - n + turns, turns)
        at = pl.ds(pl.multiple_of(pair * 2 * VD, 2 * VD), 2 * VD)
        both = (dot_t(d_ref[...], wo[at, :]) + dot_t(small_ref[...], down_ref[at, :])).astype(BF16)
        for t in range(2):
            to = 2 * pair + t
            d_src[to] = both[:, t * VD : (t + 1) * VD]

            @pl.when(to == me)
            def _():
                ds_in[me] = both[:, t * VD : (t + 1) * VD]

            @pl.when(to != me)
            def _():
                exchange.copy(lax.rem(to - me + members, members)).start()


    @pl.loop(0, turns)
    def _(n):
        i = lax.rem(me // 2 + n, turns)
        start = pl.multiple_of(i * block, block)
        here = pl.ds(start, block)
        for t in range(2):
            source = 2 * i + t

            @pl.when(source != me)
            def _():
                send(ds_in.at[source], ds_in.at[source], sent.at[0], got.at[lax.rem(me - source + members, members)], source).wait_recv()

        d = ds_in[pl.ds(2 * i, 2)].reshape(block, VD)
        q = q_ref[here, :]
        lse = lse_ref[pl.ds(i, 1), 0, :]
        along = d.astype(F32) * o_ref[here, :]
        high = along.astype(BF16)
        low = (along - high.astype(F32)).astype(BF16)
        ones = jnp.ones((8, VD), BF16)
        delta = (dot_t(ones, high) + dot_t(ones, low))[0:1, :]
        rows = start + lax.broadcasted_iota(jnp.int32, (1, block), 1)
        limit = jnp.maximum(jnp.where(rows < prefix, prefix - 1, rows), rows)

        def step(j, dq, masked):
            at = pl.multiple_of(j * keys, keys)
            k = k_ref[pl.ds(at, keys), :]
            v = v_ref[pl.ds(at, keys), :]
            p = jnp.exp2(dot_t(k, q) * unit - lse)
            if masked:
                cols = at + lax.broadcasted_iota(jnp.int32, (keys, 1), 0)
                p = jnp.where(cols <= limit, p, 0.0)
            dp = dot_t(v, d)
            ds = (p * (dp - delta)).astype(BF16)
            dv[pl.ds(at, keys), :] += dot(p.astype(BF16), d)
            dk[pl.ds(at, keys), :] += dot(ds, q)
            return dq + t_dot(ds, k)

        full, stop = key_blocks(start, block, keys, q_ref.shape[0])
        dq = lax.fori_loop(0, full, functools.partial(step, masked=False), jnp.zeros((block, QK), F32))
        dq = lax.fori_loop(full, stop, functools.partial(step, masked=True), dq)
        dq = (dq * factor).astype(BF16)
        half = tokens // 2
        for t in range(2):
            to = 2 * i + t
            r = t * tokens
            blocks[to, :tokens, :] = dq[r : r + tokens, :NOPE]
            blocks[to, tokens:, :ROPE] = dq[r : r + half, NOPE:]
            blocks[to, tokens:, ROPE:] = dq[r + half : r + tokens, NOPE:]

            @pl.when(to == me)
            def _():
                own.start()

            @pl.when(to != me)
            def _():
                block_to(to).start()

    @pl.loop(0, members)
    def _(b):
        at = pl.ds(pl.multiple_of(b * tokens, tokens), tokens)
        d = jnp.concatenate([dk[at, :NOPE] * factor, dv[at, :]], axis=1).astype(BF16)
        part_ref[b, :, :KVR] = dot_t(d, kvb_ref[...]).astype(BF16)
        part_ref[b, :, KVR:] = (dk[at, NOPE:] * factor).astype(BF16)

    own.wait()

    @pl.loop(1, members)
    def _(d):
        n = lax.rem(me + d, members)
        from_device(n).wait_recv()
        block_to(n).wait_send()
        exchange.copy(d).wait_send()


def attend_back(prefix, q, k, v, o, lse, d, small, down, wo, kvb, members, collective_id):
    length = q.shape[0]
    tokens = length // members
    vmem = pl.BlockSpec(memory_space=pltpu.VMEM)
    anywhere = pl.BlockSpec(memory_space=pl.ANY)
    sem = pltpu.SemaphoreType.DMA
    factor = QK**-0.5
    packed = tokens + tokens // 2
    return pl.pallas_call(
        functools.partial(attend_back_kernel, members=members, factor=factor, unit=factor * math.log2(math.e)),
        in_specs=[pl.BlockSpec(memory_space=pltpu.SMEM)] + [vmem] * 8 + [anywhere, vmem],
        out_specs=[vmem, anywhere],
        out_shape=[
            jax.ShapeDtypeStruct((members, tokens, KVR + ROPE), BF16),
            jax.ShapeDtypeStruct((members, packed, NOPE), BF16),
        ],
        scratch_shapes=[
            pltpu.VMEM((members, tokens, VD), BF16),
            pltpu.VMEM(wo.shape, BF16),
            pltpu.VMEM((members, tokens, VD), BF16),
            pltpu.VMEM((members, packed, NOPE), BF16),
            pltpu.VMEM((length, QK), F32),
            pltpu.VMEM((length, VD), F32),
            sem((members,)), sem((members,)), sem((members,)), sem((members,)), sem, sem,
        ],
        compiler_params=pltpu.CompilerParams(
            collective_id=collective_id, has_side_effects=True, vmem_limit_bytes=50 * 1024 * 1024
        ),
        cost_estimate=pl.CostEstimate(
            flops=length * length * (3 * QK + 2 * VD), bytes_accessed=length * 2000, transcendentals=length * length // 2
        ),
        name="attend_back",
    )(prefix, q, k, v, o, lse, d, small, down, wo, kvb)


def silu_parts(v):
    logistic = 0.5 * jnp.tanh(0.5 * v) + 0.5
    return v * logistic, logistic * (1.0 + v * (1.0 - logistic))


def picks(rank, slots):
    at = lax.broadcasted_iota(jnp.int32, (slots, rank.shape[1]), 0).astype(F32)
    return at == rank


def picks_back(rank, slots):
    at = lax.broadcasted_iota(jnp.int32, (rank.shape[0], slots), 1).astype(F32)
    return at == rank


def tiles(width, size):
    return pl.ds(pl.multiple_of(width * size, size), size)


def experts_kernel(
    x_hbm, prob_hbm, c_hbm, c2_hbm, rank_ref, back_ref, gate_hbm, up_hbm, down_hbm, own_hbm, sdown_hbm,
    part_hbm, eg_hbm, eu_hbm, eo_hbm, sh_hbm, c_out, c2_out, prob_out,
    xs, probs, gate, up, down, own, sdown, tail, rows, acts, sacts, part_st, eg_st, eu_st, eo_st, sh_st,
    c_st, c2_st, sent, got, e_sent, e_got, c_sent, c_got, c2_sent, c2_got, load, store,
    *, members, slots, tile, wide
):
    me = lax.axis_index("grp")
    levels = members // (SIDE * CORES)
    group = SIDE * CORES
    width, hidden = gate.shape
    half, whole = hidden % tile, hidden // tile
    units = own.shape[1] // 2
    z = me // group
    order = near_first(levels)
    loads = [
        pltpu.make_async_copy(a, b, load.at[n])
        for n, (a, b) in enumerate(
            [
                (x_hbm, xs.at[me]),
                (prob_hbm.at[me], probs.at[me]),
                (own_hbm, own),
                (gate_hbm, gate),
                (up_hbm, up),
                (down_hbm, down),
                (sdown_hbm, sdown),
                (c_hbm, c_st),
                (c2_hbm, c2_st),
            ]
        )
    ]
    gather = Gather(x_hbm, xs, sent, got, members)
    behind = Gather(c_hbm, c_out, c_sent, c_got, members)
    behind2 = SideFirst(c2_hbm, c2_out, c2_sent, c2_got, members)
    own_c = [
        pltpu.make_async_copy(c_st, c_out.at[me], load.at[7]),
        pltpu.make_async_copy(c2_st, c2_out.at[me], load.at[8]),
    ]
    exchange = Exchange(prob_hbm, probs, e_sent, e_got, members)
    for copy in loads:
        copy.start()
    meet(members)
    gather.first()
    exchange.start()
    for copy in loads:
        copy.wait()
    for copy in own_c:
        copy.start()
    tail[:, :half] = gate[:, hidden - half :]
    tail[:, half:] = up[:, hidden - half :]
    gather.pass_on(z)
    gather.relay(1)
    exchange.wait()
    prob_out[...] = probs[...]

    def stores(s, k):
        n = s % 2
        return [
            pltpu.make_async_copy(a, b.at[k], store.at[n, m])
            for m, (a, b) in enumerate(
                [
                    (part_st.at[n], part_hbm),
                    (eg_st.at[n], eg_hbm),
                    (eu_st.at[n], eu_hbm),
                    (eo_st.at[n], eo_hbm),
                    (sh_st.at[n], sh_hbm),
                ]
            )
        ]

    @pl.loop(0, levels)
    def _(s):
        k = pick_from(order, z, s)
        n = s % 2
        gather.take_twin(k)

        @pl.when(s >= 2)
        def _():
            for copy in stores(s, pick_from(order, z, s - 2)):
                copy.wait()

        @pl.loop(0, group)
        def _(b):
            pick = picks(rank_ref[k * group + b, 0:1, :], slots).astype(BF16)
            rows[tiles(b, slots), :] = dot(pick, xs[k * group + b]).astype(BF16)

        def keep(at, g, u):
            eg_st[n, :, at] = g.astype(BF16)
            eu_st[n, :, at] = u.astype(BF16)
            acts[:, at] = (silu_parts(g)[0] * u).astype(BF16)

        @pl.loop(0, whole)
        def _(j):
            at = tiles(j, tile)
            x = rows[...]
            keep(at, dot(x, gate[:, at]), dot(x, up[:, at]))

        last = dot(rows[...], tail[...])
        keep(pl.ds(whole * tile, half), last[:, :half], last[:, half:])

        gather.relay(s + 2)

        @pl.when(s + 1 < levels)
        def _():
            gather.pass_on(pick_from(order, z, s + 1))

        @pl.when(s == levels - 3)
        def _():
            behind.first()
            behind2.first()

        @pl.when(s >= levels - 2)
        def _():
            @pl.when(s == levels - 2)
            def _():
                behind2.turn()

            behind.relay(s - levels + 3)
            behind2.relay(s - levels + 3)
            behind.pass_on(pick_from(order, z, s - levels + 2))

        @pl.loop(0, width // wide)
        def _(j):
            at = tiles(j, wide)
            eo_st[n, :, at] = dot(acts[...], down[:, at]).astype(BF16)

        @pl.loop(0, group // 2)
        def _(h):
            x = xs[pl.ds(k * group + 2 * h, 2)].reshape(-1, width)
            pre = dot(x, own[...])
            sh_st[n, pl.ds(2 * h, 2)] = pre.astype(BF16).reshape(2, -1, 2 * units)
            act = (silu_parts(pre[:, :units])[0] * pre[:, units:]).astype(BF16)
            sacts[pl.ds(2 * h, 2)] = act.reshape(2, -1, units)

        @pl.loop(0, group)
        def _(b):
            i = k * group + b
            pick = picks(rank_ref[i, 0:1, :], slots)
            back = picks_back(back_ref[i], slots).astype(BF16)
            g = jnp.sum(jnp.where(pick, probs[i, 0:1, :], 0.0), axis=1, keepdims=True)
            act = sacts[b]
            for j in range(width // wide):
                at = slice(j * wide, (j + 1) * wide)
                weighted = (g * eo_st[n, tiles(b, slots), at].astype(F32)).astype(BF16)
                part_st[n, b, :, at] = (dot(back, weighted) + dot(act, sdown[:, at])).astype(BF16)

        for copy in stores(s, k):
            copy.start()

    @pl.loop(2, levels)
    def _(s):
        behind.relay(s + 1)
        behind2.relay(s + 1)
        behind.pass_on(pick_from(order, z, s))

    @pl.loop(levels - 2, levels)
    def _(s):
        for copy in stores(s, pick_from(order, z, s)):
            copy.wait()

    @pl.loop(0, levels)
    def _(k):
        behind.take_twin(k)
        behind2.take_twin(k)

    for copy in own_c:
        copy.wait()
    gather.finish()
    behind.finish()
    behind2.finish()


def experts_forward(x, prob, c, c2, rank, back, gate, up, down, own, sdown, slots, members, collective_id):
    tokens, width = x.shape
    hidden = gate.shape[1]
    group = SIDE * CORES
    levels = members // group
    packed = group * slots
    anywhere = pl.BlockSpec(memory_space=pl.ANY)
    vmem = pl.BlockSpec(memory_space=pltpu.VMEM)
    sem = pltpu.SemaphoreType.DMA
    tile = 256
    shapes = [
        (levels, group, tokens, width),
        (levels, packed, hidden),
        (levels, packed, hidden),
        (levels, packed, width),
        (levels, group, tokens, own.shape[1]),
    ]
    return pl.pallas_call(
        functools.partial(experts_kernel, members=members, slots=slots, tile=tile, wide=512),
        in_specs=[anywhere] * 4 + [vmem, vmem] + [anywhere] * 5,
        out_specs=[anywhere] * 7 + [vmem],
        out_shape=[jax.ShapeDtypeStruct(s, BF16) for s in shapes]
        + [jax.ShapeDtypeStruct((members, *a.shape), BF16) for a in (c, c2)]
        + [jax.ShapeDtypeStruct(prob.shape, F32)],
        scratch_shapes=[
            pltpu.VMEM((members, tokens, width), BF16),
            pltpu.VMEM(prob.shape, F32),
            pltpu.VMEM(gate.shape, BF16),
            pltpu.VMEM(up.shape, BF16),
            pltpu.VMEM(down.shape, BF16),
            pltpu.VMEM(own.shape, BF16),
            pltpu.VMEM(sdown.shape, BF16),
            pltpu.VMEM((width, tile), BF16),
            pltpu.VMEM((packed, width), BF16),
            pltpu.VMEM((packed, hidden), BF16),
            pltpu.VMEM((group, tokens, own.shape[1] // 2), BF16),
        ]
        + [pltpu.VMEM((2, *s[1:]), BF16) for s in shapes]
        + [pltpu.VMEM(c.shape, BF16), pltpu.VMEM(c2.shape, BF16)]
        + [sem((6, members)), sem((2, members)), sem((members,)), sem((members,))]
        + [sem((6, members)), sem((2, members))] * 2
        + [sem((9,)), sem((2, 5))],
        compiler_params=pltpu.CompilerParams(
            collective_id=collective_id, has_side_effects=True, vmem_limit_bytes=63 * 1024 * 1024
        ),
        cost_estimate=pl.CostEstimate(
            flops=12 * members * slots * width * hidden, bytes_accessed=60_000_000, transcendentals=0
        ),
        name="experts_forward",
    )(x, prob, c, c2, rank, back, gate, up, down, own, sdown)


def experts_back_kernel(
    c_hbm, c2_hbm, c3_hbm, rank_ref, back_ref, prob_ref, eg_hbm, eu_hbm, eo_hbm, sh_hbm, gate_hbm, up_hbm, down_hbm, own_hbm, sdown_hbm,
    out, dg_out,
    part, cs, eg, eu, eo, sh, gate, up, down, own, sdown, rows, d_gate, d_up, dg_st, dg_in,
    *sems, members, slots, tile, wide
):
    twin_in, side_in, line_in = sems[:3]
    e_sent, e_got, load, fetch = sems[11:15]
    me = lax.axis_index("grp")
    levels = members // (SIDE * CORES)
    group = SIDE * CORES
    width, hidden = gate.shape
    half, whole = hidden % tile, hidden // tile
    units = own.shape[1] // 2
    z = me // group
    order = far_first(levels)
    reduce = Reduce(part, twin_in, side_in, line_in, sems[3:11], members)
    exchange = Exchange(dg_st, dg_in, e_sent, e_got, members)

    def cotangents(s):
        k = pick_from(order, z, s)
        return [
            pltpu.make_async_copy(
                a.at[k], cs.at[s % 2, :, :, pl.ds(at, a.shape[3])], fetch.at[4 + s % 2 * 3 + h]
            )
            for h, (a, at) in enumerate([(c_hbm, 0), (c2_hbm, width // 2), (c3_hbm, width // 2 + c2_hbm.shape[3])])
        ]

    def kept(s):
        k = pick_from(order, z, s)
        return [
            pltpu.make_async_copy(a.at[k], b, fetch.at[m])
            for m, (a, b) in enumerate([(eo_hbm, eo), (eg_hbm, eg), (eu_hbm, eu), (sh_hbm, sh)])
        ]

    loads = [
        pltpu.make_async_copy(a, b, load.at[n])
        for n, (a, b) in enumerate(
            [(down_hbm, down), (gate_hbm, gate), (up_hbm, up), (own_hbm, own), (sdown_hbm, sdown)]
        )
    ]
    for copy in cotangents(0) + kept(0):
        copy.start()
    for copy in loads:
        copy.start()
    meet(members)

    def early(s):
        return (z == 0) | (z == levels - 1)

    @pl.loop(0, levels)
    def _(s):
        k = pick_from(order, z, s)
        n = s % 2
        for copy in cotangents(s):
            copy.wait()
        load_eo, load_eg, load_eu, load_sh = kept(s)

        @pl.when(s + 1 < levels)
        def _():
            for copy in cotangents(s + 1):
                copy.start()

        load_eo.wait()
        @pl.loop(0, group)
        def _(b):
            i = k * group + b
            at = tiles(b, slots)
            pick = picks(rank_ref[i, 0:1, :], slots)
            c = dot(pick.astype(BF16), cs[n, b])
            g = jnp.sum(jnp.where(pick, prob_ref[i, 0:1, :], 0.0), axis=1, keepdims=True)
            along = jnp.sum(c * eo[at, :].astype(F32), axis=1, keepdims=True)
            dg_st[i] = jnp.broadcast_to(
                jnp.sum(jnp.where(pick, along, 0.0), axis=0, keepdims=True), dg_st.shape[1:]
            )
            rows[at, :] = (g * c).astype(BF16)

        @pl.when(s == 0)
        def _():
            for copy in loads:
                copy.wait()

        load_eg.wait()
        load_eu.wait()

        def slopes(at):
            d = dot_t(rows[...], down[at, :])
            act, slope = silu_parts(eg[:, at].astype(F32))
            d_gate[:, at] = (d * eu[:, at].astype(F32) * slope).astype(BF16)
            d_up[:, at] = (d * act).astype(BF16)

        @pl.loop(0, whole)
        def _(j):
            slopes(tiles(j, tile))

        slopes(pl.ds(whole * tile, half))

        @pl.when(s >= 1)
        def _():
            reduce.chip(pick_from(order, z, s - 1))

        @pl.when((s >= 2) & ~early(s))
        def _():
            reduce.line(pick_from(order, z, s - 2))

        @pl.loop(0, width // tile)
        def _(j):
            at = tiles(j, tile)
            eo[:, at] = (dot_t(d_gate[...], gate[at, :]) + dot_t(d_up[...], up[at, :])).astype(BF16)

        load_sh.wait()
        @pl.loop(0, group)
        def _(b):
            i = k * group + b
            back = picks_back(back_ref[i], slots).astype(BF16)
            d = dot_t(cs[n, b], sdown[...])
            pre = sh[b].astype(F32)
            act, slope = silu_parts(pre[:, :units])
            both = jnp.concatenate([d * pre[:, units:] * slope, d * act], axis=1).astype(BF16)
            for j in range(width // wide):
                at = slice(j * wide, (j + 1) * wide)
                part[i, :, at] = (
                    dot(back, eo[tiles(b, slots), at]) + dot_t(both, own[at, :])
                ).astype(BF16)

        reduce.start(k)

        @pl.when(s + 1 < levels)
        def _():
            for copy in kept(s + 1):
                copy.start()

        @pl.when((s >= 1) & early(s))
        def _():
            reduce.line(pick_from(order, z, s - 1))

    exchange.start()
    dg_in[me] = dg_st[me]
    reduce.chip(z)

    @pl.when(~early(0))
    def _():
        reduce.line(pick_from(order, z, levels - 2))

    reduce.last(out)
    reduce.finish()
    exchange.wait()
    dg_out[...] = dg_in[...]


def experts_backward(cs, rank, back, prob, kept, gate, up, down, own, sdown, slots, members, collective_id):
    tokens, width = cs[0].shape[1], sum(c.shape[2] for c in cs)
    hidden = gate.shape[1]
    group = SIDE * CORES
    levels = members // group
    packed = group * slots
    anywhere = pl.BlockSpec(memory_space=pl.ANY)
    vmem = pl.BlockSpec(memory_space=pltpu.VMEM)
    sem = pltpu.SemaphoreType.DMA
    eg, eu, eo, sh = kept
    return pl.pallas_call(
        functools.partial(experts_back_kernel, members=members, slots=slots, tile=256, wide=512),
        in_specs=[anywhere] * 3 + [vmem] * 3 + [anywhere] * 9,
        out_specs=[vmem, vmem],
        out_shape=[
            jax.ShapeDtypeStruct((tokens, width), BF16),
            jax.ShapeDtypeStruct((members, 8, tokens), F32),
        ],
        scratch_shapes=[
            pltpu.VMEM((members, tokens, width), BF16),
            pltpu.VMEM((2, group, tokens, width), BF16),
            pltpu.VMEM(eg.shape[1:], BF16),
            pltpu.VMEM(eu.shape[1:], BF16),
            pltpu.VMEM(eo.shape[1:], BF16),
            pltpu.VMEM(sh.shape[1:], BF16),
            pltpu.VMEM(gate.shape, BF16),
            pltpu.VMEM(up.shape, BF16),
            pltpu.VMEM(down.shape, BF16),
            pltpu.VMEM(own.shape, BF16),
            pltpu.VMEM(sdown.shape, BF16),
            pltpu.VMEM((packed, width), BF16),
            pltpu.VMEM((packed, hidden), BF16),
            pltpu.VMEM((packed, hidden), BF16),
            pltpu.VMEM((members, 8, tokens), F32),
            pltpu.VMEM((members, 8, tokens), F32),
        ]
        + Reduce.scratch(members, tokens, width, BF16)
        + [sem((members,)), sem((members,)), sem((5,)), sem((10,))],
        compiler_params=pltpu.CompilerParams(
            collective_id=collective_id, has_side_effects=True, vmem_limit_bytes=67_043_328
        ),
        cost_estimate=pl.CostEstimate(
            flops=12 * members * slots * width * hidden, bytes_accessed=60_000_000, transcendentals=0
        ),
        name="experts_backward",
    )(*(c.reshape(levels, group, tokens, -1) for c in cs), rank, back, prob, *kept, gate, up, down, own, sdown)


class Spread:
    def __init__(self, src, out, common, commons, sems, members, sequences):
        self.src, self.out, self.common, self.commons = src, out, common, commons
        self.sent, self.got, self.sent2, self.got2 = sems
        self.members, self.sequences = members, sequences
        self.me, self.mine = lax.axis_index("grp"), lax.axis_index("rep")

    def other(self, n):
        r = lax.rem(self.mine + n // self.members, self.sequences)
        return {"rep": r, "grp": lax.rem(self.me + n % self.members, self.members)}

    def meet(self):
        barrier = pltpu.get_barrier_semaphore()
        count = self.members * self.sequences

        @pl.loop(1, count)
        def _(n):
            pl.semaphore_signal(barrier, 1, device_id=self.other(n), device_id_type=MESH)

        pl.semaphore_wait(barrier, count - 1)

    def block(self, n):
        to = self.other(n)
        return send(self.src.at[to["grp"]], self.out.at[self.mine, self.me], self.sent.at[n], self.got.at[n], to)

    def whole(self, n):
        return send(self.common, self.commons.at[self.mine], self.sent2.at[n], self.got2.at[n], self.other(n * self.members))

    def start_blocks(self):
        @pl.loop(1, self.members * self.sequences)
        def _(n):
            self.block(n).start()

    def start_common(self):
        @pl.loop(1, self.sequences)
        def _(n):
            self.whole(n).start()

    def wait(self):
        @pl.loop(1, self.members * self.sequences)
        def _(n):
            self.block(n).wait()

        @pl.loop(1, self.sequences)
        def _(n):
            self.whole(n).wait()


def finish_kernel(
    part, o_src, dq_ref, cos_ref, sin_ref, q_hbm, kva_ref, up_ref, down_ref, small_ref, normed_ref, latent_ref, kvg_ref,
    x_ref, xg_ref, dmid_ref, name_ref,
    out, gqd, gqu, god, gou,
    *bufs, members, sequences
):
    twin_in, side_in, line_in = bufs[:3]
    o_in, o_common, q_parts, d_query, wq, dn, d_lat, d_latent, ds_ref, q_out, o_out = bufs[11:22]
    o_sent, o_got, b_sent, b_got, w_sent, w_got, local = bufs[22:]
    reduce = Reduce(part, twin_in, side_in, line_in, bufs[3:11], members)
    exchange = Exchange(o_src, o_in, o_sent, o_got, members)
    spread = Spread(q_parts, q_out, o_common, o_out, (b_sent, b_got, w_sent, w_got), members, sequences)
    me, mine = spread.me, spread.mine
    order = far_first(reduce.levels)
    z, levels = reduce.z, reduce.levels
    tokens, width = x_ref.shape
    tile = 256
    load = pltpu.make_async_copy(q_hbm, wq, local.at[0])
    load.start()
    spread.meet()

    @pl.loop(0, levels)
    def _(s):
        reduce.start(pick_from(order, z, s))

    exchange.start()
    o_in[me] = o_src[me]
    cosine, sine = cos_ref[...], sin_ref[...]
    half = ROPE // 2
    for pair in range(dq_ref.shape[0] // 2):
        pieces = []
        for h in (2 * pair, 2 * pair + 1):
            rope = jnp.concatenate([dq_ref[h, tokens:, :ROPE], dq_ref[h, tokens:, ROPE:]], axis=0).astype(F32)
            turned = jnp.concatenate([rope[:, half:], rope[:, :half]], axis=1)
            pieces += [dq_ref[h, :tokens, :], (rope * cosine + turned * sine).astype(BF16)]
        d_query[:, pair * 2 * QK : (pair + 1) * 2 * QK] = jnp.concatenate(pieces, axis=1)

    @pl.loop(0, levels)
    def _(s):
        reduce.chip(pick_from(order, z, s))

    grad_up = t_dot(small_ref[...], d_query[...])
    ds_ref[...] = dot_t(d_query[...], up_ref[...]).astype(BF16)
    grad_down = t_dot(ds_ref[...], normed_ref[...])
    rows = width // members
    for g in range(members):
        first = g // 2 * 2 * QK
        q_parts[g] = jnp.concatenate(
            [grad_down[:, g * rows : (g + 1) * rows], grad_up[:, first : first + 2 * QK]], axis=1
        ).astype(BF16)
    spread.start_blocks()
    q_out[mine, me] = q_parts[me]
    exchange.wait()
    total = jnp.zeros(o_in.shape[1:], F32)
    for g in range(members):
        total = total + o_in[g].astype(F32)
    o_common[...] = jnp.concatenate([total, name_ref[...]], axis=1)
    spread.start_common()
    o_out[mine] = o_common[...]
    load.wait()
    every = width // tile // (levels - 1)

    @pl.loop(0, width // tile)
    def _(j):
        dn[:, tiles(j, tile)] = dot_t(d_query[...], wq[pl.ds(j * (tile // rows), tile // rows)].reshape(tile, -1))

        @pl.when((j % every == every - 1) & (j // every < levels - 1))
        def _():
            reduce.line(pick_from(order, z, j // every))

    reduce.last(d_lat)
    gradient = d_lat[...].astype(F32)
    latent = latent_ref[...]
    d_latent[:, :KVR] = norm_back(latent[:, :KVR], kvg_ref[...], gradient[:, :KVR]).astype(BF16)
    rope = gradient[:, KVR:]
    turned = jnp.concatenate([rope[:, half:], rope[:, :half]], axis=1)
    d_latent[:, KVR:] = (rope * cosine + turned * sine).astype(BF16)

    @pl.loop(0, width // tile)
    def _(j):
        at = tiles(j, tile)
        dn[:, at] += dot_t(d_latent[...], kva_ref[at, :]) + dot_t(ds_ref[...], down_ref[at, :])

    out[...] = (dmid_ref[...] + norm_back(x_ref[...].astype(F32), xg_ref[...], dn[...])).astype(BF16)
    reduce.finish()
    spread.wait()
    o_cols = gou.shape[2]
    shares = []
    for r in range(sequences):
        q_share = lax.fori_loop(
            0, members, lambda g, total: total + q_out[r, g].astype(F32), jnp.zeros(q_out.shape[2:], F32)
        )
        up_share = jnp.where(me % 2 == 0, q_share[:, rows : rows + QK], q_share[:, rows + QK :])
        o_share = o_out[r]
        number = o_share[:, 2 * o_cols : 2 * o_cols + 1]
        shares.append((number, q_share[:, :rows], up_share, o_share[:, :o_cols], o_share[:, o_cols : 2 * o_cols]))
    for a in range(gqd.shape[0]):
        sums = [jnp.zeros(part.shape, F32) for part in shares[0][1:]]
        for number, *parts in shares:
            chosen = number == a
            sums = [total + jnp.where(chosen, part, 0.0) for total, part in zip(sums, parts)]
        for ref, total in zip((gqd, gqu, god, gou), sums):
            ref[a] = total


def finish(part, o_parts, dq, cosine, sine, all_q, kva, up, down, small, normed, latent, kvg, x, xg, dmid, name, adapters, sequences, collective_id):
    members, tokens, c = part.shape
    width = x.shape[1]
    rank = o_parts.shape[1]
    vmem = pl.BlockSpec(memory_space=pltpu.VMEM)
    anywhere = pl.BlockSpec(memory_space=pl.ANY)
    sem = pltpu.SemaphoreType.DMA
    share = width // members + 2 * QK
    common = (rank, o_parts.shape[2] + name.shape[1])
    return pl.pallas_call(
        functools.partial(finish_kernel, members=members, sequences=sequences),
        in_specs=[vmem] * 5 + [anywhere] + [vmem] * 11,
        out_specs=[vmem] * 5,
        out_shape=[jax.ShapeDtypeStruct((tokens, width), BF16)]
        + [
            jax.ShapeDtypeStruct((adapters, rank, n), F32)
            for n in (width // members, QK, o_parts.shape[2] // 2, o_parts.shape[2] // 2)
        ],
        scratch_shapes=Reduce.scratch(members, tokens, c, BF16)
        + [
            pltpu.VMEM(o_parts.shape, BF16),
            pltpu.VMEM(common, F32),
            pltpu.VMEM((members, rank, share), BF16),
            pltpu.VMEM((tokens, H * QK), BF16),
            pltpu.VMEM(all_q.shape, BF16),
            pltpu.VMEM((tokens, width), F32),
            pltpu.VMEM((tokens, c), BF16),
            pltpu.VMEM((tokens, c), BF16),
            pltpu.VMEM((tokens, rank), BF16),
            pltpu.VMEM((sequences, members, rank, share), BF16),
            pltpu.VMEM((sequences, *common), F32),
        ]
        + [sem((n,)) for n in (members,) * 2 + (members * sequences,) * 2 + (sequences,) * 2 + (3,)],
        compiler_params=pltpu.CompilerParams(
            collective_id=collective_id, has_side_effects=True, vmem_limit_bytes=56 * 1024 * 1024
        ),
        cost_estimate=pl.CostEstimate(flops=4 * tokens * width * H * QK, bytes_accessed=40_000_000, transcendentals=0),
        name="finish",
    )(part, o_parts, dq, cosine, sine, all_q, kva, up, down, small, normed, latent, kvg, x, xg, dmid, name)


def by_owner(gradient, members):
    return gradient.astype(BF16).reshape(gradient.shape[0], members, -1).transpose(1, 0, 2)


def per_device(
    hidden,
    grad_out,
    expert_ids,
    prefix_len,
    adapter_id,
    attn_gain,
    kv_gain,
    ffn_gain,
    w_q,
    w_kva,
    w_kvb,
    w_o,
    w_router,
    shared_gate,
    shared_up,
    shared_down,
    expert_gate,
    expert_up_weight,
    expert_down,
    q_down,
    q_up,
    o_down,
    o_up,
):
    tokens = hidden.shape[1]
    width = hidden.shape[2]
    members = lax.axis_size("grp")
    length = tokens * members
    experts = expert_gate.shape[0] * members
    capacity = tokens * TOP * 5 // (4 * experts)
    slots = -(-capacity // 16) * 16
    me = lax.axis_index("grp")

    inputs = hidden[0].astype(F32)
    cotangent = grad_out[0]
    c32 = cotangent.astype(F32)
    routes = expert_ids[0]
    adapter = adapter_id[0]
    pick = lambda table: lax.dynamic_index_in_dim(table, adapter, 0, keepdims=False)
    qa_down, qa_up, oa_down, oa_up = pick(q_down), pick(q_up), pick(o_down), pick(o_up)

    chosen_by = jnp.sum(
        (routes[:, :, None] == jnp.arange(experts, dtype=jnp.int32)[None, None, :]).astype(F32), axis=1
    )
    sequences = lax.axis_size("rep")
    split = w_q.shape[0] * 3 // 128 * 16 if sequences % 2 == 0 else 0
    positions = me * tokens + jnp.arange(tokens, dtype=jnp.int32)
    cosine, sine = angles(positions, ROPE)
    normed = root_norm(inputs, attn_gain).astype(BF16)
    cosine2 = jnp.concatenate([cosine, cosine], axis=1)
    sine2 = jnp.concatenate([sine, -sine], axis=1)
    (
        all_kva, all_q, all_o, all_router, all_latent, q_packed, kvb_parts, chosen_all, own_shared, latent, q_small
    ) = opening(
        w_kva,
        w_q,
        w_o,
        w_router,
        jnp.broadcast_to(chosen_by.T[:, None, :], (experts, 8, tokens)),
        w_kvb,
        shared_gate,
        shared_up,
        normed,
        qa_down,
        qa_up,
        cosine2,
        sine2,
        kv_gain[None],
        members,
        split,
        1,
    )
    full_kva, full_o, full_router = (v.reshape(-1, v.shape[2]) for v in (all_kva, all_o, all_router))
    own_kvb = kvb_parts.reshape(KVR, -1)
    own_shared = own_shared.reshape(width, -1)
    q_packed, c_first = lax.optimization_barrier((q_packed, cotangent[:, : width // 2]))
    mixture, lse, q_head, k_head, v_head, mixed_parts = attend(prefix_len, q_packed, all_latent, own_kvb, members, 3)
    mixed = mixed_parts.transpose(1, 0, 2).reshape(tokens, H * VD)
    o_small = dot(mixed, oa_down).astype(BF16)
    middle = inputs + dot(mixed, full_o) + dot(o_small, oa_up)
    ffn_in = root_norm(middle, ffn_gain).astype(BF16)
    route_probs = jax.nn.softmax(dot(ffn_in, full_router), axis=-1)

    half = width // 2
    first_c = gather(c_first).reshape(members, tokens, half)
    chosen = chosen_all[:, 0] > 0.5
    order = jnp.arange(tokens, dtype=jnp.int32)
    before = (order[:, None] < order[None, :]).astype(BF16)
    rank = jnp.where(chosen, dot(chosen.astype(BF16), before), -1.0)
    back = rank[:, :, None]
    rank = jnp.broadcast_to(rank[:, None, :], (members, 8, tokens))
    weights = (expert_gate[0], expert_up_weight[0], expert_down[0], own_shared, shared_down)
    prob_blocks = jnp.broadcast_to(route_probs.T[:, None, :], (experts, 8, tokens))
    partial, kept_gate, kept_up, kept_out, kept_shared, second_c, third_c, prob_parts = experts_forward(
        ffn_in, prob_blocks, cotangent[:, half : half + half // 2], cotangent[:, half + half // 2 :], rank, back, *weights, slots, members, 4
    )
    kept = (kept_gate, kept_up, kept_out, kept_shared)
    ffn_out = scatter_sum(partial.reshape(length, width))
    d_own, d_route = experts_backward(
        (first_c, second_c, third_c), rank, back, prob_parts, kept, *weights, slots, members, 5
    )
    d_route = d_route[:, 0].T
    d_logits = (
        route_probs * (d_route - jnp.sum(route_probs * d_route, axis=-1, keepdims=True))
    ).astype(BF16)
    d_ffn = d_own.astype(F32) + dot_t(d_logits, full_router)
    d_middle = c32 + norm_back(middle, ffn_gain, d_ffn)
    d_attn = d_middle.astype(BF16)
    grad_oup = t_dot(o_small, d_attn)
    d_osmall = dot_t(d_attn, oa_up).astype(BF16)
    grad_odown = t_dot(d_osmall, mixed)
    d_latents, d_query = attend_back(
        prefix_len,
        q_head,
        k_head,
        v_head,
        mixture,
        lse.reshape(members // 2, 1, 2 * tokens),
        d_attn,
        d_osmall,
        oa_down,
        full_o,
        own_kvb,
        members,
        6,
    )
    o_parts = jnp.concatenate([by_owner(g, members) for g in (grad_odown, grad_oup)], axis=-1)
    name = jnp.broadcast_to(adapter.astype(F32), (qa_up.shape[0], 128))
    grad_inputs, *outs = finish(
        d_latents,
        o_parts,
        d_query,
        cosine2,
        sine2,
        all_q,
        full_kva,
        qa_up,
        qa_down,
        q_small,
        normed,
        latent,
        kv_gain[None],
        hidden[0],
        attn_gain[None],
        d_middle,
        name,
        q_down.shape[0],
        sequences,
        7,
    )
    ffn_out, _ = lax.optimization_barrier((ffn_out, d_query))
    output = (middle + ffn_out.astype(F32)).astype(BF16)
    return (
        output[None],
        grad_inputs[None],
        outs[0].transpose(0, 2, 1),
        outs[1],
        outs[2].transpose(0, 2, 1),
        outs[3],
    )


def solution(mesh):
    seq = P("rep", "grp", None)
    rows = P("grp", None)
    in_specs = (
        (seq, seq, seq, P("rep"), P("rep"), P(), P(), P())
        + (rows,) * 8
        + (P("grp", None, None),) * 3
        + (P(),) * 4
    )
    out_specs = (
        seq,
        seq,
        P(None, "grp", None),
        P(None, None, "grp"),
        P(None, "grp", None),
        P(None, None, "grp"),
    )
    return jax.shard_map(
        per_device, mesh=mesh, in_specs=in_specs, out_specs=out_specs, check_vma=False
    )
```
